32 devices in a mesh: seq: 8 (over z, x), head: 4 (over y, core).
Axes of the slice: x: 2, y: 2, z: 4, core: 2. Of those that a mesh axis runs over, the one named last changes fastest.
Arguments:
- queries: bfloat16 [8192, 4096], P(('seq', 'head')), may hold values from -6 to 6
- keys: bfloat16 [8192, 4096], P(('seq', 'head')), may hold values from -6 to 6
- values: bfloat16 [8192, 4096], P(('seq', 'head')), may hold values from -6 to 6
- spikes: int32 [8192, 4096], P(('seq', 'head')), may hold values from 0 to 26
- gain: float32 [4096], P('head'), may hold values from 0.1 to 1.9
Outputs:
- attended: bfloat16 [8192, 4096], P('seq', 'head')
- cache: float32 [8, 32, 128, 128], P('seq', 'head')
The draws below stay inside these ranges and needn't reach their ends.
Inputs may be any that keep to these rules, and one draw needn't show every extreme that they name: spikes codes count_query + 3 count_key + 9 count_value with each count 0, 1 or 2.
All inputs are finite; a program needn't handle non-finite values.
Results may differ from the reference program's by a relative error of at most 0.0027.
Values may be sent and summed in bfloat16 or wider, within the bound.
No kernel may reach another device: no remote copies, remote signals or barrier semaphores. Data moves between devices by JAX's collectives and lax.ppermute only.
A program may use at most 128 MiB of HBM per device.

```python
import jax
import jax.numpy as jnp
from jax import lax

HEADS = 32
HD = 128
D = 4096
BLOCK = 1024
BLOCKS = 8
TOKENS = 8192


def set_ends(entries, rng, smallest, high):
    spot = [jax.random.randint(jax.random.fold_in(rng, axis), (), 0, length) for axis, length in enumerate(entries.shape)]
    main_axis = entries.shape.index(max(entries.shape))
    neighbour = spot[:main_axis] + [(spot[main_axis] + 1) % entries.shape[main_axis]] + spot[main_axis + 1:]
    return entries.at[tuple(spot)].set(smallest).at[tuple(neighbour)].set(high)


def level_of(rng, shape, shards, low, largest):
    level = 1.0
    for position, shards_of in shards:
        draws = jax.random.uniform(jax.random.fold_in(jax.random.fold_in(rng, 6), position), (shards_of,), jnp.float32, low / len(shards), largest / len(shards))
        level = level * jnp.repeat(jnp.exp(draws), shape[position] // shards_of).reshape((-1,) + (1,) * (len(shape) - 1 - position))
    return level


def gaussian(stream_key, dims, width, reach, cuts=(), kind=jnp.bfloat16):
    factor_of = level_of(stream_key, dims, cuts, -0.22, 0.18) if cuts else 1.0
    array = jax.random.normal(stream_key, dims, jnp.float32) * width * factor_of
    return jnp.minimum(jnp.maximum(array, -reach), reach).astype(kind)


def setup_inputs(seed: int = 0) -> dict:
    seeds = jax.random.split(jax.random.key(seed), 6)
    return {
        "queries": gaussian(seeds[0], (TOKENS, D), 1.0, 6.0, ((0, 32),)),
        "keys": gaussian(seeds[1], (TOKENS, D), 1.0, 6.0, ((0, 32),)),
        "values": gaussian(seeds[2], (TOKENS, D), 1.0, 6.0, ((0, 32),)),
        "spikes": set_ends(jax.random.randint(seeds[3], (TOKENS, D), 0, 27), jax.random.fold_in(seeds[3], 1), 0, 26).astype(jnp.int32),
        "gain": jnp.clip(1.0 + 0.18 * jax.random.normal(seeds[4], (D,), jnp.float32), 0.1, 1.9),
    }


def decode_counts(spikes):
    return (spikes % 3, spikes // 3 % 3, spikes // 9)

def reference(queries, keys, values, spikes, gain):
    count_query, count_key, count_value = decode_counts(spikes)
    spiked_query = queries * count_query.astype(queries.dtype)
    spiked_key = keys * count_key.astype(keys.dtype)
    spiked_value = values * count_value.astype(values.dtype)
    score_scale = HD ** (-0.5)
    causal = lax.broadcasted_iota(jnp.int32, (BLOCK, BLOCK), 0) >= lax.broadcasted_iota(jnp.int32, (BLOCK, BLOCK), 1)

    def one_head(head):
        start = (head * HD).astype(jnp.int32)
        query_blocks = lax.dynamic_slice_in_dim(spiked_query, start, HD, 1).reshape(BLOCKS, BLOCK, HD)
        key_blocks = lax.dynamic_slice_in_dim(spiked_key, start, HD, 1).reshape(BLOCKS, BLOCK, HD)
        value_blocks = lax.dynamic_slice_in_dim(spiked_value, start, HD, 1).reshape(BLOCKS, BLOCK, HD)
        states = jnp.einsum('nsd,nse->nde', key_blocks.astype(jnp.float32), value_blocks.astype(jnp.float32), precision=lax.Precision.HIGHEST)
        inclusive = jnp.cumsum(states, axis=0)
        earlier = jnp.concatenate([jnp.zeros((1, HD, HD), jnp.float32), inclusive[:-1]], axis=0)

        def one_block(pieces):
            query_rows, key_rows, value_rows, carried_state = pieces
            scores = jnp.dot(query_rows, key_rows.T, preferred_element_type=jnp.float32) * score_scale
            weights = jnp.where(causal, scores, 0.0).astype(jnp.bfloat16)
            local_part = jnp.dot(weights, value_rows, preferred_element_type=jnp.float32)
            carried = jnp.dot(query_rows.astype(jnp.float32), carried_state, precision=lax.Precision.HIGHEST) * score_scale
            return local_part + carried
        raw = lax.map(one_block, (query_blocks, key_blocks, value_blocks, earlier)).reshape(TOKENS, HD)
        head_gain = lax.dynamic_slice_in_dim(gain, start, HD, 0)
        normed = raw * lax.rsqrt(lax.optimization_barrier(jnp.mean(raw * raw, axis=-1, keepdims=True)) + 1e-06) * head_gain
        seen_tokens = ((jnp.arange(BLOCKS, dtype=jnp.int32) + 1) * BLOCK).astype(jnp.float32)
        scaled = inclusive * lax.rsqrt(seen_tokens)[:, None, None]
        return (normed.astype(jnp.bfloat16), scaled)
    outputs, caches = lax.map(one_head, jnp.arange(HEADS, dtype=jnp.int32))
    attended = outputs.transpose(1, 0, 2).reshape(TOKENS, HEADS * HD)
    return (attended, caches.transpose(1, 0, 2, 3))
```

```python
import functools

import jax
import jax.numpy as jnp
from jax import lax
from jax.experimental import pallas as pl
from jax.experimental.pallas import tpu as pltpu
from jax.sharding import Mesh
from jax.sharding import PartitionSpec as P

HD = 128
SCORE_SCALE = HD ** (-0.5)
CORES = 2
VMEM_BYTES = 48 * 1024 * 1024


def params(n_axes):
    return pltpu.CompilerParams(
        dimension_semantics=("arbitrary",) * n_axes, vmem_limit_bytes=VMEM_BYTES
    )


def nine(spikes):
    return (spikes >= 9).astype(jnp.int32) + (spikes >= 18).astype(jnp.int32)


def three(code):
    return (code >= 3).astype(jnp.int32) + (code >= 6).astype(jnp.int32)


def count_of(spikes, name):
    value_count = nine(spikes)
    if name == "value":
        return value_count
    rest = spikes - 9 * value_count
    key_count = three(rest)
    if name == "key":
        return key_count
    return rest - 3 * key_count


def decode_kernel(names, width, core_ref, spikes_ref, *refs):
    sources = refs[: len(names)]
    outs = refs[len(names) :]
    core = core_ref[0]
    for side in range(CORES):
        of = core if side == 0 else 1 - core
        columns = pl.ds(pl.multiple_of(of * width, width), width)
        spikes = spikes_ref[:, columns]
        for index, name in enumerate(names):
            count = count_of(spikes, name).astype(jnp.float32).astype(jnp.bfloat16)
            outs[2 * index + side][...] = sources[index][:, columns] * count


def decode(core, spikes, operands, width):
    names = tuple(operands)
    rows, model = spikes.shape
    groups = model // (CORES * width)
    step = min(rows, 64)
    in_block = pl.BlockSpec((step, CORES * width), lambda r, g, core: (r, g))
    out_block = pl.BlockSpec((step, width), lambda r, g, core: (r, g))
    n_out = 2 * len(names)
    return pl.pallas_call(
        functools.partial(decode_kernel, names, width),
        out_shape=[jax.ShapeDtypeStruct((rows, groups * width), jnp.bfloat16)] * n_out,
        grid_spec=pltpu.PrefetchScalarGridSpec(
            num_scalar_prefetch=1,
            grid=(rows // step, groups),
            in_specs=[in_block] * (1 + len(names)),
            out_specs=[out_block] * n_out,
        ),
        compiler_params=params(2),
        cost_estimate=pl.CostEstimate(
            flops=rows * model * 8 * len(names),
            bytes_accessed=rows * model * 4 * (1 + len(names)),
            transcendentals=0,
        ),
        name="decode_" + "_".join(names),
    )(core, spikes, *operands.values())


def contract_rows(left, right):
    return lax.dot_general(
        left, right, (((0,), (0,)), ((), ())), preferred_element_type=jnp.float32
    )


def contract_columns(left, right):
    return lax.dot_general(
        left, right, (((1,), (1,)), ((), ())), preferred_element_type=jnp.float32
    )


def states_kernel(heads, key_ref, key_sib_ref, value_ref, value_sib_ref, out_ref):
    for h in range(heads):
        at = slice(h * HD, (h + 1) * HD)
        out_ref[h] = contract_rows(key_ref[:, at], value_ref[:, at]) + contract_rows(
            key_sib_ref[:, at], value_sib_ref[:, at]
        )


def chunk_states(key, key_sib, value, value_sib):
    rows, width = key.shape
    heads = width // HD
    step = min(heads, 4)
    block = pl.BlockSpec((rows, step * HD), lambda h: (0, h))
    return pl.pallas_call(
        functools.partial(states_kernel, step),
        out_shape=jax.ShapeDtypeStruct((heads, HD, HD), jnp.float32),
        grid=(heads // step,),
        in_specs=[block] * 4,
        out_specs=pl.BlockSpec((step, HD, HD), lambda h: (h, 0, 0)),
        compiler_params=params(1),
        cost_estimate=pl.CostEstimate(
            flops=4 * rows * HD * HD * heads,
            bytes_accessed=8 * rows * width + 4 * heads * HD * HD,
            transcendentals=0,
        ),
        name="chunk_states",
    )(key, key_sib, value, value_sib)


def prefix_kernel(block_tokens, states_ref, carry_ref, cache_ref):
    n_y, n_seq = states_ref.shape[:2]
    total = jnp.zeros(states_ref.shape[2:], jnp.float32)
    for s in range(n_seq):
        for y in range(n_y):
            carry_ref[y, s] = total
            total = total + states_ref[y, s]
        cache_ref[s] = total * ((s + 1) * block_tokens) ** (-0.5)


def prefix(states, block_tokens):
    n_y, n_seq, rows, _ = states.shape
    return pl.pallas_call(
        functools.partial(prefix_kernel, block_tokens),
        out_shape=[
            jax.ShapeDtypeStruct(states.shape, jnp.float32),
            jax.ShapeDtypeStruct((n_seq, rows, HD), jnp.float32),
        ],
        compiler_params=params(0),
        name="prefix",
    )(states)


def attend_kernel(
    heads, core_ref, q_ref, q_sib_ref, k_ref, k_sib_ref, v_ref, v_sib_ref, carry_ref, gain_ref, out_ref
):
    rows = q_ref.shape[0]
    is_first = jnp.broadcast_to(core_ref[0], (rows, HD)) == 0
    causal = lax.broadcasted_iota(jnp.int32, (rows, rows), 0) >= lax.broadcasted_iota(
        jnp.int32, (rows, rows), 1
    )

    def ordered(mine_ref, sib_ref, at):
        mine, sib = mine_ref[:, at], sib_ref[:, at]
        return jnp.where(is_first, mine, sib), jnp.where(is_first, sib, mine)

    def weigh(queries, keys, masked):
        scores = contract_columns(queries, keys) * SCORE_SCALE
        if masked:
            scores = jnp.where(causal, scores, 0.0)
        return scores.astype(jnp.bfloat16)

    def dot(left, right):
        return jnp.dot(left, right, preferred_element_type=jnp.float32)

    for h in range(heads):
        at = slice(h * HD, (h + 1) * HD)
        q_first, q_second = ordered(q_ref, q_sib_ref, at)
        k_first, k_second = ordered(k_ref, k_sib_ref, at)
        v_first, v_second = ordered(v_ref, v_sib_ref, at)
        carry = carry_ref[h] * SCORE_SCALE
        high = carry.astype(jnp.bfloat16)
        low = (carry - high.astype(jnp.float32)).astype(jnp.bfloat16)
        both = jnp.concatenate([high, low], axis=1)
        gain = gain_ref[:, at]

        def finish(raw, queries):
            carried = dot(queries, both)
            raw = raw + (carried[:, :HD] + carried[:, HD:])
            mean = jnp.mean(raw * raw, axis=-1, keepdims=True)
            return (raw * lax.rsqrt(mean + 1e-06) * gain).astype(jnp.bfloat16)

        raw_first = dot(weigh(q_first, k_first, True), v_first)
        out_ref[0, :rows, at] = finish(raw_first, q_first)
        raw_second = dot(weigh(q_second, k_first, False), v_first) + dot(
            weigh(q_second, k_second, True), v_second
        )
        out_ref[0, rows:, at] = finish(raw_second, q_second)


def attend(core, query, key, value, carry, gain, n_y):
    rows, width = key[0].shape
    heads = width // HD
    group = heads // n_y
    step = min(group, 2)
    steps = group // step
    block = pl.BlockSpec((rows, step * HD), lambda y, h, core: (0, y * steps + h))
    return pl.pallas_call(
        functools.partial(attend_kernel, step),
        out_shape=jax.ShapeDtypeStruct((n_y, 2 * rows, group * HD), jnp.bfloat16),
        grid_spec=pltpu.PrefetchScalarGridSpec(
            num_scalar_prefetch=1,
            grid=(n_y, steps),
            in_specs=[block] * 6
            + [
                pl.BlockSpec((step, HD, HD), lambda y, h, core: (y * steps + h, 0, 0)),
                pl.BlockSpec((1, step * HD), lambda y, h, core: (0, y * steps + h)),
            ],
            out_specs=pl.BlockSpec((1, 2 * rows, step * HD), lambda y, h, core: (y, 0, h)),
        ),
        compiler_params=params(2),
        cost_estimate=pl.CostEstimate(
            flops=heads * (12 * rows * rows * HD + 8 * rows * HD * HD),
            bytes_accessed=16 * rows * width + 4 * heads * HD * HD,
            transcendentals=0,
        ),
        name="attend",
    )(core, *query, *key, *value, carry, gain)


def per_device(n_seq, n_y, queries, keys, values, spikes, gain):
    rows, model = spikes.shape
    width = model // (n_y * CORES)
    chips = n_seq * n_y
    core = lax.axis_index("core").astype(jnp.int32).reshape(1)
    swap = [(0, 1), (1, 0)]

    key, key_out, value, value_out = decode(core, spikes, {"key": keys, "value": values}, width)
    key_sib = lax.ppermute(key_out, "core", swap)
    value_sib = lax.ppermute(value_out, "core", swap)
    query, query_out = decode(core, spikes, {"query": queries}, width)
    query_sib = lax.ppermute(query_out, "core", swap)

    states = chunk_states(key, key_sib, value, value_sib)
    heads = states.shape[0]
    pieces = states.reshape(chips, heads * HD // chips, HD)
    owned = lax.all_to_all(pieces, ("y", "seq"), split_axis=0, concat_axis=0, tiled=True)
    carry, cache = prefix(owned.reshape(n_y, n_seq, -1, HD), rows * CORES * n_y)
    carry = lax.all_to_all(
        carry.reshape(pieces.shape), ("y", "seq"), split_axis=0, concat_axis=0, tiled=True
    )
    gains = lax.all_gather(gain, "y", axis=0, tiled=True).reshape(1, n_y * width)
    attended = attend(
        core,
        (query, query_sib),
        (key, key_sib),
        (value, value_sib),
        carry.reshape(heads, HD, HD),
        gains,
        n_y,
    )
    attended = lax.all_to_all(attended, "y", split_axis=0, concat_axis=0, tiled=True)
    cache = lax.all_to_all(cache, "seq", split_axis=0, concat_axis=0, tiled=True)
    return attended.reshape(-1, width), cache.reshape(1, heads // n_y, HD, HD)


def solution(mesh):
    n_seq, n_head = mesh.shape["seq"], mesh.shape["head"]
    n_y = n_head // CORES
    split = Mesh(mesh.devices.reshape(n_seq, n_y, CORES), ("seq", "y", "core"))
    tokens = P(("seq", "y", "core"), None)
    return jax.shard_map(
        functools.partial(per_device, n_seq, n_y),
        mesh=split,
        in_specs=(tokens, tokens, tokens, tokens, P(("y", "core"))),
        out_specs=(P("seq", ("y", "core")), P("seq", ("y", "core"), None, None)),
        check_vma=False,
    )
```

```python
import functools

import jax
import jax.numpy as jnp
from jax import lax
from jax.experimental import pallas as pl
from jax.experimental.pallas import tpu as pltpu
from jax.sharding import Mesh
from jax.sharding import PartitionSpec as P

HD = 128
SCORE_SCALE = HD ** (-0.5)
CORES = 2
VMEM_BYTES = 24 * 1024 * 1024
PAD = 16
TOP = 32767.0

VMEM = pl.BlockSpec(memory_space=pltpu.VMEM)
SMEM = pl.BlockSpec(memory_space=pltpu.SMEM)


def params(n_axes=0):
    return pltpu.CompilerParams(
        dimension_semantics=("arbitrary",) * n_axes or None, vmem_limit_bytes=VMEM_BYTES
    )


def cost(flops, bytes_accessed):
    return pl.CostEstimate(flops=flops, bytes_accessed=bytes_accessed, transcendentals=0)


class Plan:
    def __init__(self, mesh, rows, model):
        n_seq, n_head = mesh.shape["seq"], mesh.shape["head"]
        self.n_y = n_head // CORES
        self.width = model // n_head
        group = self.width // HD
        self.n_inner = 2 if n_seq % 2 == 0 and group % 2 == 0 else 1
        self.n_outer = n_seq // self.n_inner
        self.halves = 2 if group // self.n_inner % 2 == 0 else 1
        self.each = group // (self.n_inner * self.halves)
        self.plane = self.n_inner * self.n_y
        self.rows = rows
        self.block = rows * n_head
        self.half_width = self.width // self.halves


def decode_kernel(names, *refs):
    n = len(names)
    for side in range(CORES):
        spikes = refs[side][...].astype(jnp.float32).astype(jnp.bfloat16)
        one, two = jnp.ones_like(spikes), jnp.full_like(spikes, 2)
        zero = jnp.zeros_like(spikes)

        def ternary(code, unit):
            return jnp.where(code >= 2 * unit, two, jnp.where(code >= unit, one, zero))

        counts = {"value": ternary(spikes, 9)}
        if "value" not in names or n > 1:
            rest = spikes - 9 * counts["value"]
            counts["key"] = ternary(rest, 3)
            if "query" in names:
                counts["query"] = rest - 3 * counts["key"]
        for index, name in enumerate(names):
            at = 2 * index + side
            refs[2 + 2 * n + at][...] = refs[2 + at][...] * counts[name]


def decode(plan, place, spikes, operands, half):
    names = tuple(operands)
    rows, model = spikes.shape
    step = min(rows, 128)
    width = plan.half_width

    def block(sibling):
        def index(r, y, place):
            core = 1 - place[0] if sibling else place[0]
            return r, (y * CORES + core) * plan.halves + half

        return pl.BlockSpec((step, width), index)

    def kernel(place_ref, *refs):
        decode_kernel(names, *refs)

    n_out = 2 * len(names)
    arrays = [a for a in (spikes, *operands.values()) for _ in range(2)]
    return pl.pallas_call(
        kernel,
        out_shape=[jax.ShapeDtypeStruct((rows, plan.n_y * width), jnp.bfloat16)] * n_out,
        grid_spec=pltpu.PrefetchScalarGridSpec(
            num_scalar_prefetch=1,
            grid=(rows // step, plan.n_y),
            in_specs=[block(False), block(True)] * (1 + len(names)),
            out_specs=[pl.BlockSpec((step, width), lambda r, y, place: (r, y))] * n_out,
        ),
        compiler_params=params(2),
        cost_estimate=cost(rows * model * 4, rows * model * (2 + 2 * len(names))),
        name="decode_" + "_".join(names) + f"_{half}",
    )(place, *arrays)


def contract_rows(left, right):
    return lax.dot_general(
        left, right, (((0,), (0,)), ((), ())), preferred_element_type=jnp.float32
    )


def contract_columns(left, right):
    return lax.dot_general(
        left, right, (((1,), (1,)), ((), ())), preferred_element_type=jnp.float32
    )


def code(states, ref):
    line = lax.broadcasted_iota(jnp.int32, (PAD, HD), 0)
    exponents = jnp.zeros((PAD, HD), jnp.float32)
    for i, state in enumerate(states):
        top = jnp.max(jnp.abs(state), axis=0, keepdims=True)
        exponent = jnp.floor(jnp.log2(jnp.maximum(top, 1e-30))) + 1
        scaled = jnp.round(state * jnp.exp2(15 - exponent))
        scaled = jnp.clip(scaled, -TOP, TOP)
        ref[i * HD : (i + 1) * HD] = scaled.astype(jnp.int32).astype(jnp.int16)
        exponents = jnp.where(line == i, exponent, exponents)
    ref[len(states) * HD :] = exponents.astype(jnp.int32).astype(jnp.int16)


def decoded(ref, each):
    exponents = ref[each * HD :].astype(jnp.int32).astype(jnp.float32)
    return [
        ref[i * HD : (i + 1) * HD].astype(jnp.int32).astype(jnp.float32)
        * jnp.exp2(exponents[i : i + 1] - 15)
        for i in range(each)
    ]


def coded_shape(plan):
    return jax.ShapeDtypeStruct((plan.each * HD + PAD, HD), jnp.int16)


def states_shape(plan, *lead):
    return jax.ShapeDtypeStruct((*lead, plan.each, HD, HD), jnp.float32)


def owned_columns(plan, place_ref, offset, i):
    x = place_ref[1] ^ (offset // plan.n_y)
    y = place_ref[2] ^ (offset % plan.n_y)
    start = ((y * plan.n_inner + x) * plan.each + i) * HD
    return pl.ds(pl.multiple_of(start, HD), HD)


def chunk_states(plan, place, key, value):
    def kernel(place_ref, k_ref, k_sib_ref, v_ref, v_sib_ref, own_ref, first_ref, *send_refs):
        is_first = jnp.full((HD, HD), place_ref[0], jnp.int32) == 0
        for offset in range(plan.plane):
            states = []
            for i in range(plan.each):
                at = owned_columns(plan, place_ref, offset, i)
                mine = contract_rows(v_ref[:, at], k_ref[:, at])
                sib = contract_rows(v_sib_ref[:, at], k_sib_ref[:, at])
                first_ref[offset, i] = jnp.where(is_first, mine, sib)
                states.append(mine + sib)
            if offset:
                code(states, send_refs[offset - 1])
            else:
                for i, state in enumerate(states):
                    own_ref[i] = state

    heads = plan.plane * plan.each
    return pl.pallas_call(
        kernel,
        out_shape=[states_shape(plan), states_shape(plan, plan.plane)]
        + [coded_shape(plan)] * (plan.plane - 1),
        in_specs=[SMEM] + [VMEM] * 4,
        out_specs=[VMEM] * (1 + plan.plane),
        compiler_params=params(),
        cost_estimate=cost(
            4 * plan.rows * HD * HD * heads, 8 * plan.rows * HD * heads + 6 * heads * HD * HD
        ),
        name="chunk_states",
    )(place, *key, *value)


def level_states(plan, own, others):
    def kernel(own_ref, *refs):
        total = [own_ref[i] for i in range(plan.each)]
        for ref in refs[:-1]:
            total = [a + b for a, b in zip(total, decoded(ref, plan.each))]
        code(total, refs[-1])

    return pl.pallas_call(
        kernel,
        out_shape=coded_shape(plan),
        in_specs=[VMEM] * plan.plane,
        out_specs=VMEM,
        compiler_params=params(),
        cost_estimate=cost(0, plan.plane * plan.each * HD * HD * 2),
        name="level_states",
    )(own, *others)


def carries(plan, place, own, others, levels):
    n_others, n_levels = len(others), len(levels)

    def kernel(place_ref, own_ref, *refs):
        other_refs = refs[:n_others]
        level_refs = refs[n_others : n_others + n_levels]
        carry_refs = refs[n_others + n_levels : n_others + n_levels + plan.plane]
        cache_refs = refs[n_others + n_levels + plan.plane :]
        x, y, level = place_ref[1], place_ref[2], place_ref[3]
        here = x * plan.n_y + y
        earlier = [jnp.zeros((HD, HD), jnp.float32)] * plan.each
        for ref in level_refs:
            earlier = [a + b for a, b in zip(earlier, decoded(ref, plan.each))]
        states = [[own_ref[i] for i in range(plan.each)]]
        states += [decoded(ref, plan.each) for ref in other_refs]

        def add(totals, keep_of):
            for offset, terms in enumerate(states):
                keep = jnp.full((HD, HD), keep_of(here ^ offset), jnp.int32) == 1
                totals = [t + jnp.where(keep, s, 0.0) for t, s in zip(totals, terms)]
            return totals

        for offset, ref in enumerate(carry_refs):
            to = here ^ offset
            code(add(earlier, lambda chip: (chip < to).astype(jnp.int32)), ref)
        for offset, ref in enumerate(cache_refs):
            to = x ^ offset
            block = level * plan.n_inner + to
            seen = jnp.full((1, HD), (block + 1) * plan.block, jnp.int32).astype(jnp.float32)
            totals = add(earlier, lambda chip: (chip // plan.n_y <= to).astype(jnp.int32))
            for i, total in enumerate(totals):
                ref[i] = total.T * lax.rsqrt(seen)

    return pl.pallas_call(
        kernel,
        out_shape=[coded_shape(plan)] * plan.plane + [states_shape(plan)] * plan.n_inner,
        in_specs=[SMEM] + [VMEM] * (1 + n_others + n_levels),
        out_specs=[VMEM] * (plan.plane + plan.n_inner),
        compiler_params=params(),
        cost_estimate=cost(0, (plan.plane * 4 + n_levels) * plan.each * HD * HD * 2),
        name="carries",
    )(place, own, *others, *levels)


def attend(plan, place, query, key, value, carry, first, gain, half, offset_y):
    rows = plan.rows

    def kernel(
        place_ref, q_ref, q_sib_ref, k_ref, k_sib_ref, v_ref, v_sib_ref, first_ref, gain_ref, *refs
    ):
        core = place_ref[0]
        out_ref = refs[-1]
        causal = lax.broadcasted_iota(jnp.int32, (rows, rows), 0) >= lax.broadcasted_iota(
            jnp.int32, (rows, rows), 1
        )
        is_second = jnp.full((HD, HD), core, jnp.int32) == 1

        def attended(q_ref, k_ref, v_ref, at, carried, gain):
            queries = q_ref[:, at]
            scores = contract_columns(queries, k_ref[:, at]) * SCORE_SCALE
            weights = jnp.where(causal, scores, 0.0).astype(jnp.bfloat16)
            raw = jnp.dot(weights, v_ref[:, at], preferred_element_type=jnp.float32)
            carried = carried * SCORE_SCALE
            high = carried.astype(jnp.bfloat16)
            low = (carried - high.astype(jnp.float32)).astype(jnp.bfloat16)
            both = contract_columns(queries, jnp.concatenate([high, low], axis=0))
            raw = raw + (both[:, :HD] + both[:, HD:])
            mean = jnp.mean(raw * raw, axis=-1, keepdims=True)
            return (raw * lax.rsqrt(mean + 1e-06) * gain).astype(jnp.bfloat16)

        for offset_x in range(plan.n_inner):
            offset = offset_x * plan.n_y + offset_y
            x = place_ref[1] ^ offset_x
            carry_states = decoded(refs[offset_x], plan.each)
            for i in range(plan.each):
                at = owned_columns(plan, place_ref, offset, i)
                start = (x * plan.each + i) * HD
                in_group = pl.ds(pl.multiple_of(half * plan.half_width + start, HD), HD)
                out_at = pl.ds(pl.multiple_of(start, HD), HD)
                gain = gain_ref[:, in_group]
                first = first_ref[offset, i]
                mine = carry_states[i] + jnp.where(is_second, first, 0.0)
                sib = carry_states[i] + jnp.where(is_second, 0.0, first)
                out_ref[pl.ds(pl.multiple_of(core * rows, rows), rows), out_at] = attended(
                    q_ref, k_ref, v_ref, at, mine, gain
                )
                out_ref[pl.ds(pl.multiple_of((1 - core) * rows, rows), rows), out_at] = attended(
                    q_sib_ref, k_sib_ref, v_sib_ref, at, sib, gain
                )

    heads = plan.n_inner * plan.each
    return pl.pallas_call(
        kernel,
        out_shape=jax.ShapeDtypeStruct((CORES * rows, plan.half_width), jnp.bfloat16),
        in_specs=[SMEM] + [VMEM] * (8 + plan.n_inner),
        out_specs=VMEM,
        compiler_params=params(),
        cost_estimate=cost(
            heads * (8 * rows * rows * HD + 8 * rows * HD * HD), 16 * rows * heads * HD
        ),
        name=f"attend_{half}_{offset_y}",
    )(place, *query, *key, *value, first, gain, *carry)


def assemble(plan, place, parts):
    rows = CORES * plan.rows

    def kernel(place_ref, *refs):
        out_ref = refs[-1]
        for offset_y in range(plan.n_y):
            y = place_ref[2] ^ offset_y
            for half in range(plan.halves):
                at = slice(half * plan.half_width, (half + 1) * plan.half_width)
                part = refs[offset_y * plan.halves + half]
                out_ref[pl.ds(pl.multiple_of(y * rows, rows), rows), at] = part[...]

    return pl.pallas_call(
        kernel,
        out_shape=jax.ShapeDtypeStruct((plan.n_y * rows, plan.width), jnp.bfloat16),
        in_specs=[SMEM] + [VMEM] * (plan.n_y * plan.halves),
        out_specs=VMEM,
        compiler_params=params(),
        name="assemble",
    )(place, *[part for halves in parts for part in halves])


def assemble_cache(plan, place, parts):
    heads = plan.halves * plan.n_inner * plan.each

    def kernel(place_ref, *refs):
        out_ref = refs[-1]
        for half in range(plan.halves):
            for offset_x in range(plan.n_inner):
                x = place_ref[1] ^ offset_x
                start = (half * plan.n_inner + x) * plan.each
                out_ref[0, pl.ds(start, plan.each)] = refs[half * plan.n_inner + offset_x][...]

    return pl.pallas_call(
        kernel,
        out_shape=jax.ShapeDtypeStruct((1, heads, HD, HD), jnp.float32),
        in_specs=[SMEM] + [VMEM] * (plan.halves * plan.n_inner),
        out_specs=VMEM,
        compiler_params=params(),
        name="assemble_cache",
    )(place, *[part for offsets in parts for part in offsets])


def per_device(plan, queries, keys, values, spikes, gain):
    place = jnp.stack([lax.axis_index(a) for a in ("core", "inner", "y", "outer")]).astype(jnp.int32)
    halves = range(plan.halves)

    def swap(array, axes, offset, size):
        return lax.ppermute(array, axes, [(i, i ^ offset) for i in range(size)])

    def in_level(array, offset):
        return swap(array, ("inner", "y"), offset, plan.plane)

    def to_later(array, distance):
        pairs = [(i, i + distance) for i in range(plan.n_outer - distance)]
        return lax.ppermute(array, "outer", pairs)

    def spiked(operands, half):
        arrays = decode(plan, place, spikes, operands, half)
        return [
            (arrays[2 * i], swap(arrays[2 * i + 1], "core", 1, CORES)) for i in range(len(operands))
        ]

    gain = gain.reshape(1, plan.width)
    gains = [gain] + [swap(gain, "y", o, plan.n_y) for o in range(1, plan.n_y)]
    pairs = [spiked({"key": keys, "value": values}, half) for half in halves]
    states = []
    for half in halves:
        own, first, *sends = chunk_states(plan, place, *pairs[half])
        others = [in_level(a, o) for o, a in enumerate(sends, 1)]
        states.append((own, first, others))
    query = [spiked({"query": queries}, half)[0] for half in halves]
    levels = []
    for half in halves:
        own, _, others = states[half]
        level = level_states(plan, own, others)
        levels.append([to_later(level, d) for d in range(1, plan.n_outer)])
    carry, caches = [], []
    for half in halves:
        own, _, others = states[half]
        outs = carries(plan, place, own, others, levels[half])
        mine, *sends = outs[: plan.plane]
        carry.append([mine] + [in_level(a, o) for o, a in enumerate(sends, 1)])
        cache, *sends = outs[plan.plane :]
        caches.append([cache] + [swap(a, "inner", o, plan.n_inner) for o, a in enumerate(sends, 1)])
    parts = [[None] * plan.halves for _ in range(plan.n_y)]
    for offset_y in (*range(1, plan.n_y), 0):
        for half in halves:
            part = attend(
                plan,
                place,
                query[half],
                *pairs[half],
                carry[half][offset_y :: plan.n_y],
                states[half][1],
                gains[offset_y],
                half,
                offset_y,
            )
            parts[offset_y][half] = swap(part, "y", offset_y, plan.n_y) if offset_y else part
    return assemble(plan, place, parts), assemble_cache(plan, place, caches)


def solution(mesh):
    tokens = P(("outer", "inner", "y", "core"), None)
    seq, head = ("outer", "inner"), ("y", "core")

    def whole(queries, keys, values, spikes, gain):
        plan = Plan(mesh, spikes.shape[0] // mesh.size, spikes.shape[1])
        sizes = (plan.n_outer, plan.n_inner, plan.n_y, CORES)
        split = Mesh(mesh.devices.reshape(sizes), ("outer", "inner", "y", "core"))
        return jax.shard_map(
            functools.partial(per_device, plan),
            mesh=split,
            in_specs=(tokens, tokens, tokens, tokens, P(head)),
            out_specs=(P(seq, head), P(seq, head, None, None)),
            check_vma=False,
        )(queries, keys, values, spikes, gain)

    return whole
```

```python
import functools

import jax
import jax.numpy as jnp
from jax import lax
from jax.experimental import pallas as pl
from jax.experimental.pallas import tpu as pltpu
from jax.sharding import Mesh
from jax.sharding import PartitionSpec as P

HD = 128
SCORE_SCALE = HD ** (-0.5)
CORES = 2
VMEM_BYTES = 24 * 1024 * 1024
DECODE_VMEM_BYTES = 52 * 1024 * 1024
PAD = 16
TOP = 32767.0

VMEM = pl.BlockSpec(memory_space=pltpu.VMEM)
SMEM = pl.BlockSpec(memory_space=pltpu.SMEM)
HBM = pl.BlockSpec(memory_space=pltpu.HBM)
ANY = pl.BlockSpec(memory_space=pl.ANY)


def params(n_axes=0, vmem=VMEM_BYTES):
    return pltpu.CompilerParams(
        dimension_semantics=("arbitrary",) * n_axes or None, vmem_limit_bytes=vmem
    )


def cost(flops, bytes_accessed):
    return pl.CostEstimate(flops=flops, bytes_accessed=bytes_accessed, transcendentals=0)


class Plan:
    def __init__(self, mesh, rows, model):
        n_seq, n_head = mesh.shape["seq"], mesh.shape["head"]
        self.n_y = n_head // CORES
        self.width = model // n_head
        group = self.width // HD
        self.n_inner = 2 if n_seq % 2 == 0 and group % 2 == 0 else 1
        self.n_outer = n_seq // self.n_inner
        self.halves = 2 if group // self.n_inner % 2 == 0 else 1
        self.each = group // (self.n_inner * self.halves)
        self.plane = self.n_inner * self.n_y
        self.rows = rows
        self.block = rows * n_head
        self.owned = self.halves * self.each
        self.piece = self.each * HD


def counts_of(spikes, names):
    one, two = jnp.ones_like(spikes), jnp.full_like(spikes, 2)
    zero = jnp.zeros_like(spikes)

    def ternary(rest, unit):
        return jnp.where(rest >= 2 * unit, two, jnp.where(rest >= unit, one, zero))

    counts = {"value": ternary(spikes, 9)}
    if names != ("value",):
        rest = spikes - 9 * counts["value"]
        counts["key"] = ternary(rest, 3)
        if "query" in names:
            counts["query"] = rest - 3 * counts["key"]
    return counts


def decode(plan, place, spikes, operands, after=()):
    names = tuple(operands)
    rows, model = spikes.shape
    step = min(rows, 64)
    width = plan.width
    n = len(names)

    def kernel(place_ref, spikes_ref, *refs):
        outs = refs[n + len(after) :]
        for side in range(CORES):
            of = place_ref[0] if side == 0 else 1 - place_ref[0]
            at = pl.ds(pl.multiple_of(of * width, width), width)
            spikes = spikes_ref[:, at].astype(jnp.float32).astype(jnp.bfloat16)
            counts = counts_of(spikes, names)
            for index, name in enumerate(names):
                outs[2 * index + side][...] = refs[index][:, at] * counts[name]

    return pl.pallas_call(
        kernel,
        out_shape=[jax.ShapeDtypeStruct((rows, plan.n_y * width), jnp.bfloat16)] * (2 * n),
        grid_spec=pltpu.PrefetchScalarGridSpec(
            num_scalar_prefetch=1,
            grid=(rows // step, plan.n_y),
            in_specs=[pl.BlockSpec((step, CORES * width), lambda r, y, place: (r, y))] * (1 + n)
            + [ANY] * len(after),
            out_specs=[pl.BlockSpec((step, width), lambda r, y, place: (r, y))] * (2 * n),
        ),
        compiler_params=params(2, DECODE_VMEM_BYTES),
        cost_estimate=cost(rows * model * 4, rows * model * (4 + 4 * n)),
        name="decode_" + "_".join(names),
    )(place, spikes, *operands.values(), *after)


def contract_rows(left, right):
    return lax.dot_general(
        left, right, (((0,), (0,)), ((), ())), preferred_element_type=jnp.float32
    )


def contract_columns(left, right):
    return lax.dot_general(
        left, right, (((1,), (1,)), ((), ())), preferred_element_type=jnp.float32
    )


def code(states, ref):
    line = lax.broadcasted_iota(jnp.int32, (PAD, HD), 0)
    exponents = jnp.zeros((PAD, HD), jnp.float32)
    for i, state in enumerate(states):
        top = jnp.max(jnp.abs(state), axis=0, keepdims=True)
        exponent = jnp.floor(jnp.log2(jnp.maximum(top, 1e-30))) + 1
        scaled = jnp.round(state * jnp.exp2(15 - exponent))
        scaled = jnp.clip(scaled, -TOP, TOP)
        ref[i * HD : (i + 1) * HD] = scaled.astype(jnp.int32).astype(jnp.int16)
        exponents = jnp.where(line == i, exponent, exponents)
    ref[len(states) * HD :] = exponents.astype(jnp.int32).astype(jnp.int16)


def decoded(ref, which=None):
    count = ref.shape[0] // HD
    exponents = ref[count * HD :].astype(jnp.int32).astype(jnp.float32)
    return [
        ref[i * HD : (i + 1) * HD].astype(jnp.int32).astype(jnp.float32)
        * jnp.exp2(exponents[i : i + 1] - 15)
        for i in (range(count) if which is None else which)
    ]


def plus(left, right):
    return [a + b for a, b in zip(left, right)]


def coded_shape(heads):
    return jax.ShapeDtypeStruct((heads * HD + PAD, HD), jnp.int16)


def states_shape(*lead):
    return jax.ShapeDtypeStruct((*lead, HD, HD), jnp.float32)


def owned_columns(plan, place_ref, offset, half, i):
    x = place_ref[1] ^ (offset // plan.n_y)
    y = place_ref[2] ^ (offset % plan.n_y)
    start = (((y * plan.halves + half) * plan.n_inner + x) * plan.each + i) * HD
    return pl.ds(pl.multiple_of(start, HD), HD)


def chunk_states(plan, place, key, value, after):
    def kernel(place_ref, k_ref, k_sib_ref, v_ref, v_sib_ref, *refs):
        own_ref, first_ref, *send_refs = refs[len(after) :]
        is_first = jnp.full((HD, HD), place_ref[0], jnp.int32) == 0
        for offset in (*range(1, plan.plane), 0):
            states = []
            for half in range(plan.halves):
                for i in range(plan.each):
                    at = owned_columns(plan, place_ref, offset, half, i)
                    mine = contract_rows(v_ref[:, at], k_ref[:, at])
                    sib = contract_rows(v_sib_ref[:, at], k_sib_ref[:, at])
                    first_ref[offset, half * plan.each + i] = jnp.where(is_first, mine, sib)
                    states.append(mine + sib)
            if offset:
                code(states, send_refs[offset - 1])
            else:
                for i, state in enumerate(states):
                    own_ref[i] = state

    heads = plan.plane * plan.owned
    return pl.pallas_call(
        kernel,
        out_shape=[states_shape(plan.owned), states_shape(plan.plane, plan.owned)]
        + [coded_shape(plan.owned)] * (plan.plane - 1),
        in_specs=[SMEM] + [VMEM] * 4 + [ANY] * len(after),
        out_specs=[VMEM] * (1 + plan.plane),
        compiler_params=params(),
        cost_estimate=cost(
            4 * plan.rows * HD * HD * heads, 8 * plan.rows * HD * heads + 6 * heads * HD * HD
        ),
        name="chunk_states",
    )(place, *key, *value, *after)


def of_half(plan, half):
    return range(half * plan.each, (half + 1) * plan.each)


def level_states(plan, own, others, half):
    def kernel(own_ref, *refs):
        *other_refs, total_ref, coded_ref = refs
        total = [own_ref[i] for i in of_half(plan, half)]
        for ref in other_refs:
            total = plus(total, decoded(ref, of_half(plan, half)))
        for i, state in enumerate(total):
            total_ref[i] = state
        code(total, coded_ref)

    return pl.pallas_call(
        kernel,
        out_shape=[states_shape(plan.each), coded_shape(plan.each)],
        in_specs=[VMEM] * plan.plane,
        out_specs=[VMEM] * 2,
        compiler_params=params(),
        cost_estimate=cost(0, plan.plane * plan.each * HD * HD * 2),
        name=f"level_states_{half}",
    )(own, *others)


def levels_so_far(plan, total, arrived, half):
    def kernel(total_ref, *refs):
        total = [total_ref[i] for i in range(plan.each)]
        for ref in refs[:-1]:
            total = plus(total, decoded(ref))
        code(total, refs[-1])

    return pl.pallas_call(
        kernel,
        out_shape=coded_shape(plan.each),
        in_specs=[VMEM] * (1 + len(arrived)),
        out_specs=VMEM,
        compiler_params=params(),
        cost_estimate=cost(0, 2 * plan.each * HD * HD * 2),
        name=f"levels_so_far_{half}_{len(arrived)}",
    )(total, *arrived)


def carries(plan, place, own, others, levels, half, after=()):
    n_others, n_levels = len(others), len(levels)
    heads = of_half(plan, half)

    def kernel(place_ref, own_ref, *refs):
        other_refs = refs[:n_others]
        level_refs = refs[n_others : n_others + n_levels]
        outs = refs[n_others + n_levels + len(after) :]
        x, y, level = place_ref[1], place_ref[2], place_ref[3]
        here = x * plan.n_y + y
        earlier = [jnp.zeros((HD, HD), jnp.float32)] * plan.each
        for ref in level_refs:
            earlier = plus(earlier, decoded(ref))
        states = [[own_ref[i] for i in heads]]
        states += [decoded(ref, heads) for ref in other_refs]

        def add(totals, keep_of):
            for offset, terms in enumerate(states):
                keep = jnp.full((HD, HD), keep_of(here ^ offset), jnp.int32) == 1
                totals = plus(totals, [jnp.where(keep, s, 0.0) for s in terms])
            return totals

        for offset, ref in enumerate(outs[: plan.plane]):
            to = here ^ offset
            code(add(earlier, lambda chip: (chip < to).astype(jnp.int32)), ref)
        for offset, ref in enumerate(outs[plan.plane :]):
            to = x ^ offset
            block = level * plan.n_inner + to
            seen = jnp.full((1, HD), (block + 1) * plan.block, jnp.int32).astype(jnp.float32)
            totals = add(earlier, lambda chip: (chip // plan.n_y <= to).astype(jnp.int32))
            for i, total in enumerate(totals):
                ref[i] = total.T * lax.rsqrt(seen)

    return pl.pallas_call(
        kernel,
        out_shape=[coded_shape(plan.each)] * plan.plane + [states_shape(plan.each)] * plan.n_inner,
        in_specs=[SMEM] + [VMEM] * (1 + n_others + n_levels) + [ANY] * len(after),
        out_specs=[VMEM] * (plan.plane + plan.n_inner),
        compiler_params=params(),
        cost_estimate=cost(0, (plan.plane * 4 + n_levels) * plan.each * HD * HD * 2),
        name=f"carries_{half}",
    )(place, own, *others, *levels, *after)


def attend(plan, place, query, key, value, carry, first, gain, half, offsets):
    rows = plan.rows

    def kernel(
        place_ref, q_ref, q_sib_ref, k_ref, k_sib_ref, v_ref, v_sib_ref, first_ref, gain_ref, *refs
    ):
        core = place_ref[0]
        out_ref = refs[-1]
        causal = lax.broadcasted_iota(jnp.int32, (rows, rows), 0) >= lax.broadcasted_iota(
            jnp.int32, (rows, rows), 1
        )
        is_second = jnp.full((HD, HD), core, jnp.int32) == 1

        def attended(q_ref, k_ref, v_ref, at, carried, gain):
            queries = q_ref[:, at]
            scores = contract_columns(queries, k_ref[:, at]) * SCORE_SCALE
            weights = jnp.where(causal, scores, 0.0).astype(jnp.bfloat16)
            raw = jnp.dot(weights, v_ref[:, at], preferred_element_type=jnp.float32)
            carried = carried * SCORE_SCALE
            high = carried.astype(jnp.bfloat16)
            low = (carried - high.astype(jnp.float32)).astype(jnp.bfloat16)
            both = contract_columns(queries, jnp.concatenate([high, low], axis=0))
            raw = raw + (both[:, :HD] + both[:, HD:])
            mean = jnp.mean(raw * raw, axis=-1, keepdims=True)
            return (raw * lax.rsqrt(mean + 1e-06) * gain).astype(jnp.bfloat16)

        for piece, offset in enumerate(offsets):
            x = place_ref[1] ^ (offset // plan.n_y)
            carry_states = decoded(refs[piece])
            for i in range(plan.each):
                at = owned_columns(plan, place_ref, offset, half, i)
                start = ((half * plan.n_inner + x) * plan.each + i) * HD
                gain = gain_ref[:, pl.ds(pl.multiple_of(start, HD), HD)]
                out_at = slice(piece * plan.piece + i * HD, piece * plan.piece + (i + 1) * HD)
                first = first_ref[offset, half * plan.each + i]
                mine = carry_states[i] + jnp.where(is_second, first, 0.0)
                sib = carry_states[i] + jnp.where(is_second, 0.0, first)
                out_ref[pl.ds(pl.multiple_of(core * rows, rows), rows), out_at] = attended(
                    q_ref, k_ref, v_ref, at, mine, gain
                )
                out_ref[pl.ds(pl.multiple_of((1 - core) * rows, rows), rows), out_at] = attended(
                    q_sib_ref, k_sib_ref, v_sib_ref, at, sib, gain
                )

    heads = len(offsets) * plan.each
    return pl.pallas_call(
        kernel,
        out_shape=jax.ShapeDtypeStruct((CORES * rows, heads * HD), jnp.bfloat16),
        in_specs=[SMEM] + [VMEM] * (8 + len(offsets)),
        out_specs=VMEM,
        compiler_params=params(),
        cost_estimate=cost(
            heads * (8 * rows * rows * HD + 8 * rows * HD * HD), 16 * rows * heads * HD
        ),
        name=f"attend_{half}_" + "_".join(map(str, offsets)),
    )(place, *query, *key, *value, first, gain, *carry)


def assemble(plan, place, parts, into=None):
    rows = CORES * plan.rows
    copies = [(n, piece, half, o) for n, (_, half, os) in enumerate(parts) for piece, o in enumerate(os)]

    def kernel(place_ref, *refs):
        out_ref, sems = refs[-2:]
        started = []
        for at, (n, piece, half, offset) in enumerate(copies):
            x = place_ref[1] ^ (offset // plan.n_y)
            y = place_ref[2] ^ (offset % plan.n_y)
            column = (half * plan.n_inner + x) * plan.piece
            to_rows = pl.ds(pl.multiple_of(y * rows, rows), rows)
            to_columns = pl.ds(pl.multiple_of(column, plan.piece), plan.piece)
            started.append(
                pltpu.make_async_copy(
                    refs[n].at[:, pl.ds(piece * plan.piece, plan.piece)],
                    out_ref.at[to_rows, to_columns],
                    sems.at[at],
                )
            )
            started[-1].start()
        for copy in started:
            copy.wait()

    arrays = [array for array, _, _ in parts]
    aliased = [] if into is None else [into]
    return pl.pallas_call(
        kernel,
        out_shape=jax.ShapeDtypeStruct((plan.n_y * rows, plan.width), jnp.bfloat16),
        in_specs=[SMEM] + [VMEM] * len(arrays) + [HBM] * len(aliased),
        out_specs=HBM,
        scratch_shapes=[pltpu.SemaphoreType.DMA((len(copies),))],
        input_output_aliases={1 + len(arrays): 0} if aliased else {},
        compiler_params=params(),
        name="assemble" if into is None else "finish",
    )(place, *arrays, *aliased)


def assemble_cache(plan, place, parts):
    heads = plan.halves * plan.n_inner * plan.each

    def kernel(place_ref, *refs):
        out_ref = refs[-1]
        for half in range(plan.halves):
            for offset_x in range(plan.n_inner):
                x = place_ref[1] ^ offset_x
                start = (half * plan.n_inner + x) * plan.each
                out_ref[0, pl.ds(start, plan.each)] = refs[half * plan.n_inner + offset_x][...]

    return pl.pallas_call(
        kernel,
        out_shape=jax.ShapeDtypeStruct((1, heads, HD, HD), jnp.float32),
        in_specs=[SMEM] + [VMEM] * (plan.halves * plan.n_inner),
        out_specs=VMEM,
        compiler_params=params(),
        name="assemble_cache",
    )(place, *[part for offsets in parts for part in offsets])


def per_device(plan, queries, keys, values, spikes, gain):
    place = jnp.stack([lax.axis_index(a) for a in ("core", "inner", "y", "outer")]).astype(jnp.int32)
    halves = range(plan.halves)

    def swap(array, axes, offset, size):
        return lax.ppermute(array, axes, [(i, i ^ offset) for i in range(size)])

    def in_level(array, offset):
        return swap(array, ("inner", "y"), offset, plan.plane)

    def to_later(array, distance):
        pairs = [(i, i + distance) for i in range(plan.n_outer - distance)]
        return lax.ppermute(array, "outer", pairs)

    def spiked(operands, after=()):
        arrays = decode(plan, place, spikes, operands, after)
        return [
            (arrays[2 * i], swap(arrays[2 * i + 1], "core", 1, CORES)) for i in range(len(operands))
        ]

    gain = gain.reshape(1, plan.width)
    gains = [gain] + [swap(gain, "y", o, plan.n_y) for o in range(1, plan.n_y)]
    key, value = spiked({"key": keys, "value": values})
    own, first, *sends = chunk_states(plan, place, key, value, gains[1:])
    others = [in_level(a, o) for o, a in enumerate(sends, 1)]
    (query,) = spiked({"query": queries}, (own,))

    totals = [level_states(plan, own, others, half) for half in halves]
    sums = [coded for _, coded in totals]
    arrived = [[] for _ in halves]
    distance = 1
    while distance < plan.n_outer:
        for half in halves:
            arrived[half].append(to_later(sums[half], distance))
        distance *= 2
        if distance < plan.n_outer:
            sums = [levels_so_far(plan, totals[half][0], arrived[half], half) for half in halves]

    parts, caches = [], []
    carry = [None] * plan.halves
    of_group = [list(range(y, plan.plane, plan.n_y)) for y in range(plan.n_y)]

    def part_of(half, offsets):
        return attend(
            plan,
            place,
            query,
            key,
            value,
            [carry[half][o] for o in offsets],
            first,
            gains[offsets[0] % plan.n_y],
            half,
            offsets,
        )

    for half in halves:
        outs = carries(plan, place, own, others, arrived[half], half)
        mine, *sends = outs[: plan.plane]
        carry[half] = [mine] + [in_level(a, o) for o, a in enumerate(sends, 1)]
        cache, *sends = outs[plan.plane :]
        caches.append([cache] + [swap(a, "inner", o, plan.n_inner) for o, a in enumerate(sends, 1)])
    for half in halves:
        for y in range(1, plan.n_y):
            for offsets in [[o] for o in of_group[y]] if half == 0 else [of_group[y]]:
                part = part_of(half, offsets)
                parts.append((swap(part, "y", y, plan.n_y), half, offsets))
    early = [(part_of(half, of_group[0]), half, of_group[0]) for half in halves]
    out = assemble(plan, place, early + parts[:-1])
    out = assemble(plan, place, parts[-1:], out)
    return out, assemble_cache(plan, place, caches)


def solution(mesh):
    tokens = P(("outer", "inner", "y", "core"), None)
    seq, head = ("outer", "inner"), ("y", "core")

    def whole(queries, keys, values, spikes, gain):
        plan = Plan(mesh, spikes.shape[0] // mesh.size, spikes.shape[1])
        sizes = (plan.n_outer, plan.n_inner, plan.n_y, CORES)
        split = Mesh(mesh.devices.reshape(sizes), ("outer", "inner", "y", "core"))
        return jax.shard_map(
            functools.partial(per_device, plan),
            mesh=split,
            in_specs=(tokens, tokens, tokens, tokens, P(head)),
            out_specs=(P(seq, head), P(seq, head, None, None)),
            check_vma=False,
        )(queries, keys, values, spikes, gain)

    return whole
```

```python
import functools

import jax
import jax.numpy as jnp
from jax import lax
from jax.experimental import pallas as pl
from jax.experimental.pallas import tpu as pltpu
from jax.sharding import Mesh
from jax.sharding import PartitionSpec as P

HD = 128
SCORE_SCALE = HD ** (-0.5)
CORES = 2
VMEM_BYTES = 24 * 1024 * 1024
DECODE_VMEM_BYTES = 52 * 1024 * 1024
PAD = 16
TOP = 32767.0

VMEM = pl.BlockSpec(memory_space=pltpu.VMEM)
SMEM = pl.BlockSpec(memory_space=pltpu.SMEM)
HBM = pl.BlockSpec(memory_space=pltpu.HBM)
ANY = pl.BlockSpec(memory_space=pl.ANY)


def params(vmem=VMEM_BYTES):
    return pltpu.CompilerParams(vmem_limit_bytes=vmem)


def cost(flops, bytes_accessed):
    return pl.CostEstimate(flops=flops, bytes_accessed=bytes_accessed, transcendentals=0)


class Plan:
    def __init__(self, mesh, rows, model):
        n_seq, n_head = mesh.shape["seq"], mesh.shape["head"]
        self.n_y = n_head // CORES
        self.width = model // n_head
        group = self.width // HD
        self.n_inner = 2 if n_seq % 2 == 0 and group % 2 == 0 else 1
        self.n_outer = n_seq // self.n_inner
        self.halves = 2 if group // self.n_inner % 2 == 0 else 1
        self.each = group // (self.n_inner * self.halves)
        self.plane = self.n_inner * self.n_y
        self.rows = rows
        self.block = rows * n_head
        self.piece = self.each * HD


def counts_of(spikes, names):
    one, two = jnp.ones_like(spikes), jnp.full_like(spikes, 2)
    zero = jnp.zeros_like(spikes)

    def ternary(rest, unit):
        return jnp.where(rest >= 2 * unit, two, jnp.where(rest >= unit, one, zero))

    counts = {"value": ternary(spikes, 9)}
    if names != ("value",):
        rest = spikes - 9 * counts["value"]
        counts["key"] = ternary(rest, 3)
        if "query" in names:
            counts["query"] = rest - 3 * counts["key"]
    return counts


def decode(plan, place, spikes, operands):
    names = tuple(operands)
    rows, model = spikes.shape
    step = min(rows, 32)
    chunks = rows // step
    width = plan.width
    n = len(names)

    def kernel(place_ref, *refs):
        sources, outs = refs[: 1 + n], refs[1 + n : 1 + 3 * n]
        buffers, sems = refs[1 + 3 * n : -1], refs[-1]

        def fetch(chunk, index):
            at = pl.ds(chunk * step, step)
            return pltpu.make_async_copy(
                sources[index].at[at], buffers[index].at[at], sems.at[chunk, index]
            )

        for chunk in range(chunks):
            for index in range(1 + n):
                fetch(chunk, index).start()

        @pl.loop(0, chunks)
        def _(chunk):
            for index in range(1 + n):
                fetch(chunk, index).wait()
            at = pl.ds(pl.multiple_of(chunk * step, step), step)
            for y in range(plan.n_y):
                for side in range(CORES):
                    of = place_ref[0] if side == 0 else 1 - place_ref[0]
                    columns = pl.ds(pl.multiple_of((y * CORES + of) * width, width), width)
                    codes = buffers[0][at, columns].astype(jnp.float32).astype(jnp.bfloat16)
                    counts = counts_of(codes, names)
                    for index, name in enumerate(names):
                        outs[2 * index + side][at, y * width : (y + 1) * width] = (
                            buffers[1 + index][at, columns] * counts[name]
                        )

    return pl.pallas_call(
        kernel,
        out_shape=[jax.ShapeDtypeStruct((rows, plan.n_y * width), jnp.bfloat16)] * (2 * n),
        in_specs=[SMEM] + [HBM] * (1 + n),
        out_specs=[VMEM] * (2 * n),
        scratch_shapes=[pltpu.VMEM((rows, model), jnp.int32)]
        + [pltpu.VMEM((rows, model), jnp.bfloat16)] * n
        + [pltpu.SemaphoreType.DMA((chunks, 1 + n))],
        compiler_params=params(DECODE_VMEM_BYTES),
        cost_estimate=cost(rows * model * 4, rows * model * (4 + 4 * n)),
        name="decode",
    )(place, spikes, *operands.values())


def contract_rows(left, right):
    return lax.dot_general(
        left, right, (((0,), (0,)), ((), ())), preferred_element_type=jnp.float32
    )


def contract_columns(left, right):
    return lax.dot_general(
        left, right, (((1,), (1,)), ((), ())), preferred_element_type=jnp.float32
    )


def code(states, ref):
    line = lax.broadcasted_iota(jnp.int32, (PAD, HD), 0)
    exponents = jnp.zeros((PAD, HD), jnp.float32)
    for i, state in enumerate(states):
        top = jnp.max(jnp.abs(state), axis=0, keepdims=True)
        exponent = jnp.floor(jnp.log2(jnp.maximum(top, 1e-30))) + 1
        scaled = jnp.round(state * jnp.exp2(15 - exponent))
        scaled = jnp.clip(scaled, -TOP, TOP)
        ref[i * HD : (i + 1) * HD] = scaled.astype(jnp.int32).astype(jnp.int16)
        exponents = jnp.where(line == i, exponent, exponents)
    ref[len(states) * HD :] = exponents.astype(jnp.int32).astype(jnp.int16)


def decoded(ref):
    count = ref.shape[0] // HD
    exponents = ref[count * HD :].astype(jnp.int32).astype(jnp.float32)
    return [
        ref[i * HD : (i + 1) * HD].astype(jnp.int32).astype(jnp.float32)
        * jnp.exp2(exponents[i : i + 1] - 15)
        for i in range(count)
    ]


def plus(left, right):
    return [a + b for a, b in zip(left, right)]


def coded_shape(heads):
    return jax.ShapeDtypeStruct((heads * HD + PAD, HD), jnp.int16)


def states_shape(*lead):
    return jax.ShapeDtypeStruct((*lead, HD, HD), jnp.float32)


def owned_columns(plan, place_ref, offset, half, i):
    x = place_ref[1] ^ (offset // plan.n_y)
    y = place_ref[2] ^ (offset % plan.n_y)
    start = (((y * plan.halves + half) * plan.n_inner + x) * plan.each + i) * HD
    return pl.ds(pl.multiple_of(start, HD), HD)


def chunk_states(plan, place, key, value, half, after):
    def kernel(place_ref, k_ref, k_sib_ref, v_ref, v_sib_ref, *refs):
        own_ref, first_ref, *send_refs = refs[len(after) :]
        is_first = jnp.full((HD, HD), place_ref[0], jnp.int32) == 0
        for offset in (*range(1, plan.plane), 0):
            states = []
            for i in range(plan.each):
                at = owned_columns(plan, place_ref, offset, half, i)
                mine = contract_rows(v_ref[:, at], k_ref[:, at])
                sib = contract_rows(v_sib_ref[:, at], k_sib_ref[:, at])
                first_ref[offset, i] = jnp.where(is_first, mine, sib)
                states.append(mine + sib)
            if offset:
                code(states, send_refs[offset - 1])
            else:
                for i, state in enumerate(states):
                    own_ref[i] = state

    heads = plan.plane * plan.each
    return pl.pallas_call(
        kernel,
        out_shape=[states_shape(plan.each), states_shape(plan.plane, plan.each)]
        + [coded_shape(plan.each)] * (plan.plane - 1),
        in_specs=[SMEM] + [VMEM] * 4 + [ANY] * len(after),
        out_specs=[VMEM] * (1 + plan.plane),
        compiler_params=params(),
        cost_estimate=cost(
            4 * plan.rows * HD * HD * heads, 8 * plan.rows * HD * heads + 6 * heads * HD * HD
        ),
        name=f"chunk_states_{half}",
    )(place, *key, *value, *after)


def level_states(plan, own, others, half, after):
    def kernel(own_ref, *refs):
        total = [own_ref[i] for i in range(plan.each)]
        for ref in refs[: len(others)]:
            total = plus(total, decoded(ref))
        code(total, refs[-1])

    return pl.pallas_call(
        kernel,
        out_shape=coded_shape(plan.each),
        in_specs=[VMEM] * plan.plane + [ANY] * len(after),
        out_specs=VMEM,
        compiler_params=params(),
        cost_estimate=cost(0, plan.plane * plan.each * HD * HD * 2),
        name=f"level_states_{half}",
    )(own, *others, *after)


def carried(plan, place_ref, own, others, levels, offsets):
    x, y = place_ref[1], place_ref[2]
    here = x * plan.n_y + y
    earlier = [jnp.zeros((HD, HD), jnp.float32)] * plan.each
    for ref in levels:
        earlier = plus(earlier, decoded(ref))
    states = [[own[i] for i in range(plan.each)]] + [decoded(ref) for ref in others]

    def add(totals, keep_of):
        for offset, terms in enumerate(states):
            keep = jnp.full((HD, HD), keep_of(here ^ offset), jnp.int32) == 1
            totals = plus(totals, [jnp.where(keep, s, 0.0) for s in terms])
        return totals

    before = [add(earlier, lambda chip: (chip < here ^ o).astype(jnp.int32)) for o in offsets]
    blocks = [
        add(earlier, lambda chip: (chip // plan.n_y <= x ^ o).astype(jnp.int32))
        for o in range(plan.n_inner)
    ]
    return before, blocks


def carries(plan, place, own, others, levels, half, offsets, after):
    n_others, n_levels = len(others), len(levels)

    def kernel(place_ref, own_ref, *refs):
        before, _ = carried(
            plan, place_ref, own_ref, refs[:n_others], refs[n_others : n_others + n_levels], offsets
        )
        for states, ref in zip(before, refs[n_others + n_levels + len(after) :]):
            code(states, ref)

    return pl.pallas_call(
        kernel,
        out_shape=[coded_shape(plan.each)] * len(offsets),
        in_specs=[SMEM] + [VMEM] * (1 + n_others + n_levels) + [ANY] * len(after),
        out_specs=[VMEM] * len(offsets),
        compiler_params=params(),
        cost_estimate=cost(0, (plan.plane * 4 + n_levels) * plan.each * HD * HD * 2),
        name=f"carries_{half}",
    )(place, own, *others, *levels, *after)


def own_carries(plan, place, own, others, levels, offsets, after):
    n_others, n_levels = len(others[0]), len(levels[0])
    each_half = 1 + n_others + n_levels

    def kernel(place_ref, *refs):
        outs = refs[plan.halves * each_half + len(after) :]
        befores = [[] for _ in offsets]
        for half in range(plan.halves):
            own_ref, *of_half = refs[half * each_half : (half + 1) * each_half]
            before, blocks = carried(
                plan, place_ref, own_ref, of_half[:n_others], of_half[n_others:], offsets
            )
            for all_states, states in zip(befores, before):
                all_states.extend(states)
            for offset, (totals, ref) in enumerate(zip(blocks, outs[len(offsets) :])):
                block = place_ref[3] * plan.n_inner + (place_ref[1] ^ offset)
                seen = jnp.full((1, HD), (block + 1) * plan.block, jnp.int32).astype(jnp.float32)
                for i, total in enumerate(totals):
                    ref[half, i] = total.T * lax.rsqrt(seen)
        for states, ref in zip(befores, outs):
            code(states, ref)

    operands = [a for h in range(plan.halves) for a in (own[h], *others[h], *levels[h])]
    return pl.pallas_call(
        kernel,
        out_shape=[coded_shape(plan.halves * plan.each)] * len(offsets)
        + [states_shape(plan.halves, plan.each)] * plan.n_inner,
        in_specs=[SMEM] + [VMEM] * len(operands) + [ANY] * len(after),
        out_specs=[VMEM] * (len(offsets) + plan.n_inner),
        compiler_params=params(),
        cost_estimate=cost(0, (plan.plane * 4 + n_levels) * plan.each * HD * HD * 4),
        name="own_carries",
    )(place, *operands, *after)


def attend(plan, place, query, key, value, carry, first, gain, half, offsets, after=()):
    rows = plan.rows

    def kernel(
        place_ref, q_ref, q_sib_ref, k_ref, k_sib_ref, v_ref, v_sib_ref, first_ref, gain_ref, *refs
    ):
        core = place_ref[0]
        out_ref = refs[-1]
        causal = lax.broadcasted_iota(jnp.int32, (rows, rows), 0) >= lax.broadcasted_iota(
            jnp.int32, (rows, rows), 1
        )
        is_second = jnp.full((HD, HD), core, jnp.int32) == 1

        def attended(q_ref, k_ref, v_ref, at, carried, gain):
            queries = q_ref[:, at]
            scores = contract_columns(queries, k_ref[:, at]) * SCORE_SCALE
            weights = jnp.where(causal, scores, 0.0).astype(jnp.bfloat16)
            raw = jnp.dot(weights, v_ref[:, at], preferred_element_type=jnp.float32)
            carried = carried * SCORE_SCALE
            high = carried.astype(jnp.bfloat16)
            low = (carried - high.astype(jnp.float32)).astype(jnp.bfloat16)
            both = contract_columns(queries, jnp.concatenate([high, low], axis=0))
            raw = raw + (both[:, :HD] + both[:, HD:])
            mean = jnp.mean(raw * raw, axis=-1, keepdims=True)
            return (raw * lax.rsqrt(mean + 1e-06) * gain).astype(jnp.bfloat16)

        for piece, offset in enumerate(offsets):
            x = place_ref[1] ^ (offset // plan.n_y)
            carry_states = decoded(refs[piece])
            skip = half * plan.each if len(carry_states) > plan.each else 0
            for i in range(plan.each):
                at = owned_columns(plan, place_ref, offset, half, i)
                start = ((half * plan.n_inner + x) * plan.each + i) * HD
                gain = gain_ref[:, pl.ds(pl.multiple_of(start, HD), HD)]
                out_at = slice(piece * plan.piece + i * HD, piece * plan.piece + (i + 1) * HD)
                first = first_ref[offset, i]
                mine = carry_states[skip + i] + jnp.where(is_second, first, 0.0)
                sib = carry_states[skip + i] + jnp.where(is_second, 0.0, first)
                out_ref[pl.ds(pl.multiple_of(core * rows, rows), rows), out_at] = attended(
                    q_ref, k_ref, v_ref, at, mine, gain
                )
                out_ref[pl.ds(pl.multiple_of((1 - core) * rows, rows), rows), out_at] = attended(
                    q_sib_ref, k_sib_ref, v_sib_ref, at, sib, gain
                )

    heads = len(offsets) * plan.each
    return pl.pallas_call(
        kernel,
        out_shape=jax.ShapeDtypeStruct((CORES * rows, heads * HD), jnp.bfloat16),
        in_specs=[SMEM] + [VMEM] * (8 + len(offsets)) + [ANY] * len(after),
        out_specs=VMEM,
        compiler_params=params(),
        cost_estimate=cost(
            heads * (8 * rows * rows * HD + 8 * rows * HD * HD), 16 * rows * heads * HD
        ),
        name=f"attend_{half}_" + "_".join(map(str, offsets)),
    )(place, *query, *key, *value, first, gain, *carry, *after)


def assemble(plan, place, parts, into=None):
    rows = CORES * plan.rows
    copies = [(n, piece, half, o) for n, (_, half, os) in enumerate(parts) for piece, o in enumerate(os)]

    def kernel(place_ref, *refs):
        out_ref, sems = refs[-2:]
        started = []
        for at, (n, piece, half, offset) in enumerate(copies):
            x = place_ref[1] ^ (offset // plan.n_y)
            y = place_ref[2] ^ (offset % plan.n_y)
            column = (half * plan.n_inner + x) * plan.piece
            to_rows = pl.ds(pl.multiple_of(y * rows, rows), rows)
            to_columns = pl.ds(pl.multiple_of(column, plan.piece), plan.piece)
            started.append(
                pltpu.make_async_copy(
                    refs[n].at[:, pl.ds(piece * plan.piece, plan.piece)],
                    out_ref.at[to_rows, to_columns],
                    sems.at[at],
                )
            )
            started[-1].start()
        for copy in started:
            copy.wait()

    arrays = [array for array, _, _ in parts]
    aliased = [] if into is None else [into]
    return pl.pallas_call(
        kernel,
        out_shape=jax.ShapeDtypeStruct((plan.n_y * rows, plan.width), jnp.bfloat16),
        in_specs=[SMEM] + [VMEM] * len(arrays) + [HBM] * len(aliased),
        out_specs=HBM,
        scratch_shapes=[pltpu.SemaphoreType.DMA((len(copies),))],
        input_output_aliases={1 + len(arrays): 0} if aliased else {},
        compiler_params=params(),
        name="assemble" if into is None else "finish",
    )(place, *arrays, *aliased)


def assemble_cache(plan, place, parts):
    group = plan.n_inner * plan.each

    def kernel(place_ref, *refs):
        for half in range(plan.halves):
            for offset, ref in enumerate(refs[:-1]):
                start = half * group + (place_ref[1] ^ offset) * plan.each
                refs[-1][0, pl.ds(start, plan.each)] = ref[half]

    return pl.pallas_call(
        kernel,
        out_shape=states_shape(1, plan.halves * group),
        in_specs=[SMEM] + [VMEM] * len(parts),
        out_specs=VMEM,
        compiler_params=params(),
        name="assemble_cache",
    )(place, *parts)


def per_device(plan, queries, keys, values, spikes, gain):
    place = jnp.stack([lax.axis_index(a) for a in ("core", "inner", "y", "outer")]).astype(jnp.int32)
    halves = range(plan.halves)

    def swap(array, axes, offset, size):
        return lax.ppermute(array, axes, [(i, i ^ offset) for i in range(size)])

    def in_level(array, offset):
        return swap(array, ("inner", "y"), offset, plan.plane)

    def to_later(array, distance):
        pairs = [(i, i + distance) for i in range(plan.n_outer - distance)]
        return lax.ppermute(array, "outer", pairs)

    gain = gain.reshape(1, plan.width)
    gains = [gain] + [swap(gain, "y", o, plan.n_y) for o in range(1, plan.n_y)]
    arrays = decode(plan, place, spikes, {"key": keys, "value": values, "query": queries})
    key, value, query = (
        (mine, swap(sibling, "core", 1, CORES)) for mine, sibling in zip(arrays[::2], arrays[1::2])
    )

    after = [*gains[1:], query[1]]
    own, first, others = [], [], []
    for half in halves:
        mine, parts, *sends = chunk_states(plan, place, key, value, half, after)
        own.append(mine)
        first.append(parts)
        others.append([in_level(a, o) for o, a in enumerate(sends, 1)])
        after = [mine]
    levels = []
    for half in halves:
        level = level_states(plan, own[half], others[half], half, after)
        levels.append([to_later(level, d) for d in range(plan.n_outer - 1, 0, -1)])
        after = [level]

    of_group = [list(range(y, plan.plane, plan.n_y)) for y in range(plan.n_y)]
    abroad = [o for offsets in of_group[1:] for o in offsets]

    def part_of(half, offsets, carry, after):
        return attend(
            plan,
            place,
            query,
            key,
            value,
            [carry[o] for o in offsets],
            first[half],
            gains[offsets[0] % plan.n_y],
            half,
            offsets,
            after,
        )

    carry = []
    for half in halves:
        sends = carries(plan, place, own[half], others[half], levels[half], half, abroad, after)
        carry.append({o: in_level(a, o) for o, a in zip(abroad, sends)})
        after = [sends[0]]
    parts = []
    for half in halves:
        for y in range(1, plan.n_y):
            part = part_of(half, of_group[y], carry[half], after)
            parts.append((swap(part, "y", y, plan.n_y), half, of_group[y]))
            after = [part]
    sends = own_carries(plan, place, own, others, levels, of_group[0], after)
    own_carry = {o: in_level(a, o) if o else a for o, a in zip(of_group[0], sends)}
    caches = [
        swap(a, "inner", o, plan.n_inner) if o else a
        for o, a in enumerate(sends[len(of_group[0]) :])
    ]
    early = []
    for half in halves:
        part = part_of(half, of_group[0], own_carry, after)
        early.append((part, half, of_group[0]))
        after = [part]
    out = assemble(plan, place, early + parts[:-1])
    out = assemble(plan, place, parts[-1:], out)
    return out, assemble_cache(plan, place, caches)


def solution(mesh):
    tokens = P(("outer", "inner", "y", "core"), None)
    seq, head = ("outer", "inner"), ("y", "core")

    def whole(queries, keys, values, spikes, gain):
        plan = Plan(mesh, spikes.shape[0] // mesh.size, spikes.shape[1])
        sizes = (plan.n_outer, plan.n_inner, plan.n_y, CORES)
        split = Mesh(mesh.devices.reshape(sizes), ("outer", "inner", "y", "core"))
        return jax.shard_map(
            functools.partial(per_device, plan),
            mesh=split,
            in_specs=(tokens, tokens, tokens, tokens, P(head)),
            out_specs=(P(seq, head), P(seq, head, None, None)),
            check_vma=False,
        )(queries, keys, values, spikes, gain)

    return whole
```

```python
import functools

import jax
import jax.numpy as jnp
from jax import lax
from jax.experimental import pallas as pl
from jax.experimental.pallas import tpu as pltpu
from jax.sharding import Mesh
from jax.sharding import PartitionSpec as P

HD = 128
SCORE_SCALE = HD ** (-0.5)
CORES = 2
VMEM_BYTES = 24 * 1024 * 1024
DECODE_VMEM_BYTES = 46 * 1024 * 1024
PAD = 16
TOP = 32767.0

VMEM = pl.BlockSpec(memory_space=pltpu.VMEM)
SMEM = pl.BlockSpec(memory_space=pltpu.SMEM)
HBM = pl.BlockSpec(memory_space=pltpu.HBM)
ANY = pl.BlockSpec(memory_space=pl.ANY)


def params(vmem=VMEM_BYTES):
    return pltpu.CompilerParams(vmem_limit_bytes=vmem)


def cost(flops, bytes_accessed):
    return pl.CostEstimate(flops=flops, bytes_accessed=bytes_accessed, transcendentals=0)


class Plan:
    def __init__(self, mesh, rows, model):
        n_seq, n_head = mesh.shape["seq"], mesh.shape["head"]
        self.n_y = n_head // CORES
        self.width = model // n_head
        group = self.width // HD
        self.n_inner = 2 if n_seq % 2 == 0 and group % 2 == 0 else 1
        self.n_outer = n_seq // self.n_inner
        self.halves = 2 if group // self.n_inner % 2 == 0 else 1
        self.each = group // (self.n_inner * self.halves)
        self.plane = self.n_inner * self.n_y
        self.rows = rows
        self.block = rows * n_head
        self.piece = self.each * HD


def counts_of(spikes):
    one, two = jnp.ones_like(spikes), jnp.full_like(spikes, 2)
    zero = jnp.zeros_like(spikes)

    def ternary(rest, unit):
        return jnp.where(rest >= 2 * unit, two, jnp.where(rest >= unit, one, zero))

    value = ternary(spikes, 9)
    rest = spikes - 9 * value
    key = ternary(rest, 3)
    return value, key, rest - 3 * key


def sides(plan, place_ref):
    for y in range(plan.n_y):
        for side in range(CORES):
            of = place_ref[0] if side == 0 else 1 - place_ref[0]
            start = pl.multiple_of((y * CORES + of) * plan.width, plan.width)
            yield side, slice(y * plan.width, (y + 1) * plan.width), pl.ds(start, plan.width)


def decode(plan, place, spikes, keys, values):
    rows, model = spikes.shape
    step = min(rows, 32)
    chunks = rows // step

    def kernel(place_ref, *refs):
        sources, outs, buffers, sems = refs[:3], refs[3:9], refs[9:12], refs[12]

        def fetch(chunk, index):
            at = pl.ds(chunk * step, step)
            return pltpu.make_async_copy(
                sources[index].at[at], buffers[index].at[at], sems.at[chunk, index]
            )

        for chunk in range(chunks):
            for index in range(3):
                fetch(chunk, index).start()

        @pl.loop(0, chunks)
        def _(chunk):
            for index in range(3):
                fetch(chunk, index).wait()
            at = pl.ds(pl.multiple_of(chunk * step, step), step)
            for side, mine, columns in sides(plan, place_ref):
                spikes = buffers[0][at, columns].astype(jnp.float32).astype(jnp.bfloat16)
                value, key, query = counts_of(spikes)
                outs[side][at, mine] = buffers[1][at, columns] * key
                outs[2 + side][at, mine] = buffers[2][at, columns] * value
                outs[4 + side][at, mine] = query

    return pl.pallas_call(
        kernel,
        out_shape=[jax.ShapeDtypeStruct((rows, plan.n_y * plan.width), jnp.bfloat16)] * 6,
        in_specs=[SMEM] + [HBM] * 3,
        out_specs=[VMEM] * 6,
        scratch_shapes=[
            pltpu.VMEM((rows, model), jnp.int32),
            pltpu.VMEM((rows, model), jnp.bfloat16),
            pltpu.VMEM((rows, model), jnp.bfloat16),
            pltpu.SemaphoreType.DMA((chunks, 3)),
        ],
        compiler_params=params(DECODE_VMEM_BYTES),
        cost_estimate=cost(rows * model * 4, rows * model * 14),
        name="decode",
    )(place, spikes, keys, values)


def spike_queries(plan, place, queries, counts):
    def kernel(place_ref, queries_ref, *refs):
        for side, mine, columns in sides(plan, place_ref):
            refs[2 + side][:, mine] = queries_ref[:, columns] * refs[side][:, mine]

    return pl.pallas_call(
        kernel,
        out_shape=[jax.ShapeDtypeStruct(a.shape, jnp.bfloat16) for a in counts],
        in_specs=[SMEM] + [VMEM] * 3,
        out_specs=[VMEM] * 2,
        compiler_params=params(),
        cost_estimate=cost(queries.size, queries.size * 6),
        name="spike_queries",
    )(place, queries, *counts)


def contract_rows(left, right):
    return lax.dot_general(
        left, right, (((0,), (0,)), ((), ())), preferred_element_type=jnp.float32
    )


def contract_columns(left, right):
    return lax.dot_general(
        left, right, (((1,), (1,)), ((), ())), preferred_element_type=jnp.float32
    )


def code(states, ref):
    line = lax.broadcasted_iota(jnp.int32, (PAD, HD), 0)
    exponents = jnp.zeros((PAD, HD), jnp.float32)
    for i, state in enumerate(states):
        top = jnp.max(jnp.abs(state), axis=0, keepdims=True)
        exponent = jnp.floor(jnp.log2(jnp.maximum(top, 1e-30))) + 1
        scaled = jnp.round(state * jnp.exp2(15 - exponent))
        scaled = jnp.clip(scaled, -TOP, TOP)
        ref[i * HD : (i + 1) * HD] = scaled.astype(jnp.int32).astype(jnp.int16)
        exponents = jnp.where(line == i, exponent, exponents)
    ref[len(states) * HD :] = exponents.astype(jnp.int32).astype(jnp.int16)


def decoded(ref):
    count = ref.shape[0] // HD
    exponents = ref[count * HD :].astype(jnp.int32).astype(jnp.float32)
    return [
        ref[i * HD : (i + 1) * HD].astype(jnp.int32).astype(jnp.float32)
        * jnp.exp2(exponents[i : i + 1] - 15)
        for i in range(count)
    ]


def plus(left, right):
    return [a + b for a, b in zip(left, right)]


def coded_shape(heads):
    return jax.ShapeDtypeStruct((heads * HD + PAD, HD), jnp.int16)


def states_shape(*lead):
    return jax.ShapeDtypeStruct((*lead, HD, HD), jnp.float32)


def owned_columns(plan, place_ref, offset, half, i):
    x = place_ref[1] ^ (offset // plan.n_y)
    y = place_ref[2] ^ (offset % plan.n_y)
    start = (((y * plan.halves + half) * plan.n_inner + x) * plan.each + i) * HD
    return pl.ds(pl.multiple_of(start, HD), HD)


def chunk_states(plan, place, key, value, half, after):
    def kernel(place_ref, k_ref, k_sib_ref, v_ref, v_sib_ref, *refs):
        own_ref, first_ref, *send_refs = refs[len(after) :]
        is_first = jnp.full((HD, HD), place_ref[0], jnp.int32) == 0
        for offset in (*range(1, plan.plane), 0):
            states = []
            for i in range(plan.each):
                at = owned_columns(plan, place_ref, offset, half, i)
                mine = contract_rows(v_ref[:, at], k_ref[:, at])
                sib = contract_rows(v_sib_ref[:, at], k_sib_ref[:, at])
                first_ref[offset, i] = jnp.where(is_first, mine, sib)
                states.append(mine + sib)
            if offset:
                code(states, send_refs[offset - 1])
            else:
                for i, state in enumerate(states):
                    own_ref[i] = state

    heads = plan.plane * plan.each
    return pl.pallas_call(
        kernel,
        out_shape=[states_shape(plan.each), states_shape(plan.plane, plan.each)]
        + [coded_shape(plan.each)] * (plan.plane - 1),
        in_specs=[SMEM] + [VMEM] * 4 + [ANY] * len(after),
        out_specs=[VMEM] * (1 + plan.plane),
        compiler_params=params(),
        cost_estimate=cost(
            4 * plan.rows * HD * HD * heads, 8 * plan.rows * HD * heads + 6 * heads * HD * HD
        ),
        name=f"chunk_states_{half}",
    )(place, *key, *value, *after)


def level_states(plan, own, others, half, after):
    def kernel(own_ref, *refs):
        total = [own_ref[i] for i in range(plan.each)]
        for ref in refs[: len(others)]:
            total = plus(total, decoded(ref))
        code(total, refs[-1])

    return pl.pallas_call(
        kernel,
        out_shape=coded_shape(plan.each),
        in_specs=[VMEM] * plan.plane + [ANY] * len(after),
        out_specs=VMEM,
        compiler_params=params(),
        cost_estimate=cost(0, plan.plane * plan.each * HD * HD * 2),
        name=f"level_states_{half}",
    )(own, *others, *after)


def carried(plan, place_ref, own, others, levels, offsets):
    x, y = place_ref[1], place_ref[2]
    here = x * plan.n_y + y
    earlier = [jnp.zeros((HD, HD), jnp.float32)] * plan.each
    for ref in levels:
        earlier = plus(earlier, decoded(ref))
    states = [[own[i] for i in range(plan.each)]] + [decoded(ref) for ref in others]

    def add(totals, keep_of):
        for offset, terms in enumerate(states):
            keep = jnp.full((HD, HD), keep_of(here ^ offset), jnp.int32) == 1
            totals = plus(totals, [jnp.where(keep, s, 0.0) for s in terms])
        return totals

    before = [add(earlier, lambda chip: (chip < here ^ o).astype(jnp.int32)) for o in offsets]
    blocks = [
        add(earlier, lambda chip: (chip // plan.n_y <= x ^ o).astype(jnp.int32))
        for o in range(plan.n_inner)
    ]
    return before, blocks


def carries(plan, place, own, others, levels, half, offsets, after):
    n_others, n_levels = len(others), len(levels)

    def kernel(place_ref, own_ref, *refs):
        before, _ = carried(
            plan, place_ref, own_ref, refs[:n_others], refs[n_others : n_others + n_levels], offsets
        )
        for states, ref in zip(before, refs[n_others + n_levels + len(after) :]):
            code(states, ref)

    return pl.pallas_call(
        kernel,
        out_shape=[coded_shape(plan.each)] * len(offsets),
        in_specs=[SMEM] + [VMEM] * (1 + n_others + n_levels) + [ANY] * len(after),
        out_specs=[VMEM] * len(offsets),
        compiler_params=params(),
        cost_estimate=cost(0, (plan.plane * 4 + n_levels) * plan.each * HD * HD * 2),
        name=f"carries_{half}",
    )(place, own, *others, *levels, *after)


def own_carries(plan, place, own, others, levels, offsets, after):
    n_others, n_levels = len(others[0]), len(levels[0])
    each_half = 1 + n_others + n_levels

    def kernel(place_ref, *refs):
        outs = refs[plan.halves * each_half + len(after) :]
        befores = [[] for _ in offsets]
        for half in range(plan.halves):
            own_ref, *of_half = refs[half * each_half : (half + 1) * each_half]
            before, blocks = carried(
                plan, place_ref, own_ref, of_half[:n_others], of_half[n_others:], offsets
            )
            for all_states, states in zip(befores, before):
                all_states.extend(states)
            for offset, (totals, ref) in enumerate(zip(blocks, outs[len(offsets) :])):
                block = place_ref[3] * plan.n_inner + (place_ref[1] ^ offset)
                seen = jnp.full((1, HD), (block + 1) * plan.block, jnp.int32).astype(jnp.float32)
                for i, total in enumerate(totals):
                    ref[half, i] = total.T * lax.rsqrt(seen)
        for states, ref in zip(befores, outs):
            code(states, ref)

    operands = [a for h in range(plan.halves) for a in (own[h], *others[h], *levels[h])]
    return pl.pallas_call(
        kernel,
        out_shape=[coded_shape(plan.halves * plan.each)] * len(offsets)
        + [states_shape(plan.halves, plan.each)] * plan.n_inner,
        in_specs=[SMEM] + [VMEM] * len(operands) + [ANY] * len(after),
        out_specs=[VMEM] * (len(offsets) + plan.n_inner),
        compiler_params=params(),
        cost_estimate=cost(0, (plan.plane * 4 + n_levels) * plan.each * HD * HD * 4),
        name="own_carries",
    )(place, *operands, *after)


def attend(plan, place, query, key, value, carry, first, gain, half, offsets, after=()):
    rows = plan.rows

    def kernel(
        place_ref, q_ref, q_sib_ref, k_ref, k_sib_ref, v_ref, v_sib_ref, first_ref, gain_ref, *refs
    ):
        core = place_ref[0]
        out_ref = refs[-1]
        causal = lax.broadcasted_iota(jnp.int32, (rows, rows), 0) >= lax.broadcasted_iota(
            jnp.int32, (rows, rows), 1
        )
        is_second = jnp.full((HD, HD), core, jnp.int32) == 1

        def attended(q_ref, k_ref, v_ref, at, carried, gain):
            queries = q_ref[:, at]
            scores = contract_columns(queries, k_ref[:, at]) * SCORE_SCALE
            weights = jnp.where(causal, scores, 0.0).astype(jnp.bfloat16)
            raw = jnp.dot(weights, v_ref[:, at], preferred_element_type=jnp.float32)
            carried = carried * SCORE_SCALE
            high = carried.astype(jnp.bfloat16)
            low = (carried - high.astype(jnp.float32)).astype(jnp.bfloat16)
            both = contract_columns(queries, jnp.concatenate([high, low], axis=0))
            raw = raw + (both[:, :HD] + both[:, HD:])
            mean = jnp.mean(raw * raw, axis=-1, keepdims=True)
            return (raw * lax.rsqrt(mean + 1e-06) * gain).astype(jnp.bfloat16)

        for piece, offset in enumerate(offsets):
            x = place_ref[1] ^ (offset // plan.n_y)
            carry_states = decoded(refs[piece])
            skip = half * plan.each if len(carry_states) > plan.each else 0
            for i in range(plan.each):
                at = owned_columns(plan, place_ref, offset, half, i)
                start = ((half * plan.n_inner + x) * plan.each + i) * HD
                gain = gain_ref[:, pl.ds(pl.multiple_of(start, HD), HD)]
                out_at = slice(piece * plan.piece + i * HD, piece * plan.piece + (i + 1) * HD)
                first = first_ref[offset, i]
                mine = carry_states[skip + i] + jnp.where(is_second, first, 0.0)
                sib = carry_states[skip + i] + jnp.where(is_second, 0.0, first)
                out_ref[pl.ds(pl.multiple_of(core * rows, rows), rows), out_at] = attended(
                    q_ref, k_ref, v_ref, at, mine, gain
                )
                out_ref[pl.ds(pl.multiple_of((1 - core) * rows, rows), rows), out_at] = attended(
                    q_sib_ref, k_sib_ref, v_sib_ref, at, sib, gain
                )

    heads = len(offsets) * plan.each
    return pl.pallas_call(
        kernel,
        out_shape=jax.ShapeDtypeStruct((CORES * rows, heads * HD), jnp.bfloat16),
        in_specs=[SMEM] + [VMEM] * (8 + len(offsets)) + [ANY] * len(after),
        out_specs=VMEM,
        compiler_params=params(),
        cost_estimate=cost(
            heads * (8 * rows * rows * HD + 8 * rows * HD * HD), 16 * rows * heads * HD
        ),
        name=f"attend_{half}_" + "_".join(map(str, offsets)),
    )(place, *query, *key, *value, first, gain, *carry, *after)


def assemble(plan, place, parts, into=None):
    rows = CORES * plan.rows
    copies = [(n, piece, half, o) for n, (_, half, os) in enumerate(parts) for piece, o in enumerate(os)]

    def kernel(place_ref, *refs):
        out_ref, sems = refs[-2:]
        started = []
        for at, (n, piece, half, offset) in enumerate(copies):
            x = place_ref[1] ^ (offset // plan.n_y)
            y = place_ref[2] ^ (offset % plan.n_y)
            column = (half * plan.n_inner + x) * plan.piece
            to_rows = pl.ds(pl.multiple_of(y * rows, rows), rows)
            to_columns = pl.ds(pl.multiple_of(column, plan.piece), plan.piece)
            started.append(
                pltpu.make_async_copy(
                    refs[n].at[:, pl.ds(piece * plan.piece, plan.piece)],
                    out_ref.at[to_rows, to_columns],
                    sems.at[at],
                )
            )
            started[-1].start()
        for copy in started:
            copy.wait()

    arrays = [array for array, _, _ in parts]
    aliased = [] if into is None else [into]
    return pl.pallas_call(
        kernel,
        out_shape=jax.ShapeDtypeStruct((plan.n_y * rows, plan.width), jnp.bfloat16),
        in_specs=[SMEM] + [VMEM] * len(arrays) + [HBM] * len(aliased),
        out_specs=HBM,
        scratch_shapes=[pltpu.SemaphoreType.DMA((len(copies),))],
        input_output_aliases={1 + len(arrays): 0} if aliased else {},
        compiler_params=params(),
        name="assemble" if into is None else "finish",
    )(place, *arrays, *aliased)


def assemble_cache(plan, place, parts):
    group = plan.n_inner * plan.each

    def kernel(place_ref, *refs):
        for half in range(plan.halves):
            for offset, ref in enumerate(refs[:-1]):
                start = half * group + (place_ref[1] ^ offset) * plan.each
                refs[-1][0, pl.ds(start, plan.each)] = ref[half]

    return pl.pallas_call(
        kernel,
        out_shape=states_shape(1, plan.halves * group),
        in_specs=[SMEM] + [VMEM] * len(parts),
        out_specs=VMEM,
        compiler_params=params(),
        name="assemble_cache",
    )(place, *parts)


def per_device(plan, queries, keys, values, spikes, gain):
    place = jnp.stack([lax.axis_index(a) for a in ("core", "inner", "y", "outer")]).astype(jnp.int32)
    halves = range(plan.halves)

    def swap(array, axes, offset, size):
        return lax.ppermute(array, axes, [(i, i ^ offset) for i in range(size)])

    def in_level(array, offset):
        return swap(array, ("inner", "y"), offset, plan.plane)

    def to_later(array, distance):
        pairs = [(i, i + distance) for i in range(plan.n_outer - distance)]
        return lax.ppermute(array, "outer", pairs)

    gain = gain.reshape(1, plan.width)
    gains = [gain] + [swap(gain, "y", o, plan.n_y) for o in range(1, plan.n_y)]
    key, key_out, value, value_out, *counts = decode(plan, place, spikes, keys, values)
    key, value = ((a, swap(b, "core", 1, CORES)) for a, b in ((key, key_out), (value, value_out)))
    query, query_out = spike_queries(plan, place, queries, counts)
    query = (query, swap(query_out, "core", 1, CORES))

    own, first, others, levels, coded = [], [], [], [], []

    def owner_stage(half, after):
        mine, parts, *sends = chunk_states(plan, place, key, value, half, after)
        own.append(mine)
        first.append(parts)
        others.append([in_level(a, o) for o, a in enumerate(sends, 1)])

    def level_stage(half, after):
        level = level_states(plan, own[half], others[half], half, after)
        coded.append(level)
        levels.append([to_later(level, d) for d in range(plan.n_outer - 1, 0, -1)])

    of_group = [list(range(y, plan.plane, plan.n_y)) for y in range(plan.n_y)]
    abroad = [o for offsets in of_group[1:] for o in offsets]

    def part_of(half, offsets, carry, after):
        return attend(
            plan,
            place,
            query,
            key,
            value,
            [carry[o] for o in offsets],
            first[half],
            gains[offsets[0] % plan.n_y],
            half,
            offsets,
            after,
        )

    def carry_stage(half, after):
        sends = carries(plan, place, own[half], others[half], levels[half], half, abroad, after)
        return sends[0], {o: in_level(a, o) for o, a in zip(abroad, sends)}

    parts = []

    def send_stage(half, carry, after):
        for y in range(1, plan.n_y):
            group = of_group[y]
            pieces = [group[:-1], group[-1:]] if half and len(group) > 1 else [group]
            for offsets in pieces:
                arrived = [a for a, h, os in parts if h == 0 and offsets == group[-1:] and os == group]
                part = part_of(half, offsets, carry, after + arrived)
                parts.append((swap(part, "y", y, plan.n_y), half, offsets))
                after = [part]
        return after

    owner_stage(0, [query[0]])
    level_stage(0, gains[1:])
    if plan.halves > 1:
        owner_stage(1, [coded[0], query[1]])
    done, carry = carry_stage(0, [own[-1]])
    if plan.halves > 1:
        level_stage(1, [done])
    after = send_stage(0, carry, [coded[-1]])
    if plan.halves > 1:
        _, carry = carry_stage(1, after)
        after = send_stage(1, carry, [])
    sends = own_carries(plan, place, own, others, levels, of_group[0], after)
    own_carry = {o: in_level(a, o) if o else a for o, a in zip(of_group[0], sends)}
    caches = [
        swap(a, "inner", o, plan.n_inner) if o else a
        for o, a in enumerate(sends[len(of_group[0]) :])
    ]
    early = []
    for half in halves:
        part = part_of(half, of_group[0], own_carry, after)
        early.append((part, half, of_group[0]))
        after = [part]
    out = assemble(plan, place, early + parts[:-1])
    out = assemble(plan, place, parts[-1:], out)
    return out, assemble_cache(plan, place, caches)


def solution(mesh):
    tokens = P(("outer", "inner", "y", "core"), None)
    seq, head = ("outer", "inner"), ("y", "core")

    def whole(queries, keys, values, spikes, gain):
        plan = Plan(mesh, spikes.shape[0] // mesh.size, spikes.shape[1])
        sizes = (plan.n_outer, plan.n_inner, plan.n_y, CORES)
        split = Mesh(mesh.devices.reshape(sizes), ("outer", "inner", "y", "core"))
        return jax.shard_map(
            functools.partial(per_device, plan),
            mesh=split,
            in_specs=(tokens, tokens, tokens, tokens, P(head)),
            out_specs=(P(seq, head), P(seq, head, None, None)),
            check_vma=False,
        )(queries, keys, values, spikes, gain)

    return whole
```

```python
import functools

import jax
import jax.numpy as jnp
from jax import lax
from jax.experimental import pallas as pl
from jax.experimental.pallas import tpu as pltpu
from jax.sharding import Mesh
from jax.sharding import PartitionSpec as P

HD = 128
SCORE_SCALE = HD ** (-0.5)
CORES = 2
VMEM_BYTES = 24 * 1024 * 1024
DECODE_VMEM_BYTES = 46 * 1024 * 1024
PAD = 16
TOP = 32767.0

VMEM = pl.BlockSpec(memory_space=pltpu.VMEM)
SMEM = pl.BlockSpec(memory_space=pltpu.SMEM)
HBM = pl.BlockSpec(memory_space=pltpu.HBM)
ANY = pl.BlockSpec(memory_space=pl.ANY)


def params(vmem=VMEM_BYTES):
    return pltpu.CompilerParams(vmem_limit_bytes=vmem)


def cost(flops, bytes_accessed):
    return pl.CostEstimate(flops=flops, bytes_accessed=bytes_accessed, transcendentals=0)


class Plan:
    def __init__(self, mesh, rows, model):
        n_seq, n_head = mesh.shape["seq"], mesh.shape["head"]
        self.n_y = n_head // CORES
        self.width = model // n_head
        group = self.width // HD
        self.n_inner = 2 if n_seq % 2 == 0 and group % 2 == 0 else 1
        self.n_outer = n_seq // self.n_inner
        self.halves = 2 if group // self.n_inner % 2 == 0 else 1
        self.each = group // (self.n_inner * self.halves)
        self.plane = self.n_inner * self.n_y
        self.rows = rows
        self.block = rows * n_head
        self.piece = self.each * HD


def counts_of(spikes):
    one, two = jnp.ones_like(spikes), jnp.full_like(spikes, 2)
    zero = jnp.zeros_like(spikes)

    def ternary(rest, unit):
        return jnp.where(rest >= 2 * unit, two, jnp.where(rest >= unit, one, zero))

    value = ternary(spikes, 9)
    rest = spikes - 9 * value
    key = ternary(rest, 3)
    return value, key, rest - 3 * key


def sides(plan, place_ref):
    for y in range(plan.n_y):
        for side in range(CORES):
            of = place_ref[0] if side == 0 else 1 - place_ref[0]
            start = pl.multiple_of((y * CORES + of) * plan.width, plan.width)
            yield side, slice(y * plan.width, (y + 1) * plan.width), pl.ds(start, plan.width)


def decode(plan, place, spikes, keys, values):
    rows, model = spikes.shape
    step = min(rows, 32)
    chunks = rows // step

    def kernel(place_ref, *refs):
        sources, outs, buffers, sems = refs[:3], refs[3:9], refs[9:12], refs[12]

        def fetch(chunk, index):
            at = pl.ds(chunk * step, step)
            return pltpu.make_async_copy(
                sources[index].at[at], buffers[index].at[at], sems.at[chunk, index]
            )

        for chunk in range(chunks):
            for index in range(3):
                fetch(chunk, index).start()

        @pl.loop(0, chunks)
        def _(chunk):
            for index in range(3):
                fetch(chunk, index).wait()
            at = pl.ds(pl.multiple_of(chunk * step, step), step)
            for side, mine, columns in sides(plan, place_ref):
                spikes = buffers[0][at, columns].astype(jnp.float32).astype(jnp.bfloat16)
                value, key, query = counts_of(spikes)
                outs[side][at, mine] = buffers[1][at, columns] * key
                outs[2 + side][at, mine] = buffers[2][at, columns] * value
                outs[4 + side][at, mine] = query

    return pl.pallas_call(
        kernel,
        out_shape=[jax.ShapeDtypeStruct((rows, plan.n_y * plan.width), jnp.bfloat16)] * 6,
        in_specs=[SMEM] + [HBM] * 3,
        out_specs=[VMEM] * 6,
        scratch_shapes=[
            pltpu.VMEM((rows, model), jnp.int32),
            pltpu.VMEM((rows, model), jnp.bfloat16),
            pltpu.VMEM((rows, model), jnp.bfloat16),
            pltpu.SemaphoreType.DMA((chunks, 3)),
        ],
        compiler_params=params(DECODE_VMEM_BYTES),
        cost_estimate=cost(rows * model * 4, rows * model * 14),
        name="decode",
    )(place, spikes, keys, values)


def spike_queries(plan, place, queries, counts):
    def kernel(place_ref, queries_ref, *refs):
        for side, mine, columns in sides(plan, place_ref):
            refs[2 + side][:, mine] = queries_ref[:, columns] * refs[side][:, mine]

    return pl.pallas_call(
        kernel,
        out_shape=[jax.ShapeDtypeStruct(a.shape, jnp.bfloat16) for a in counts],
        in_specs=[SMEM] + [VMEM] * 3,
        out_specs=[VMEM] * 2,
        compiler_params=params(),
        cost_estimate=cost(queries.size, queries.size * 6),
        name="spike_queries",
    )(place, queries, *counts)


def contract_rows(left, right):
    return lax.dot_general(
        left, right, (((0,), (0,)), ((), ())), preferred_element_type=jnp.float32
    )


def contract_columns(left, right):
    return lax.dot_general(
        left, right, (((1,), (1,)), ((), ())), preferred_element_type=jnp.float32
    )


def code(states, ref):
    line = lax.broadcasted_iota(jnp.int32, (PAD, HD), 0)
    exponents = jnp.zeros((PAD, HD), jnp.float32)
    for i, state in enumerate(states):
        top = jnp.max(jnp.abs(state), axis=0, keepdims=True)
        exponent = jnp.floor(jnp.log2(jnp.maximum(top, 1e-30))) + 1
        scaled = jnp.round(state * jnp.exp2(15 - exponent))
        scaled = jnp.clip(scaled, -TOP, TOP)
        ref[i * HD : (i + 1) * HD] = scaled.astype(jnp.int32).astype(jnp.int16)
        exponents = jnp.where(line == i, exponent, exponents)
    ref[len(states) * HD :] = exponents.astype(jnp.int32).astype(jnp.int16)


def decoded(ref, which=None):
    count = ref.shape[0] // HD
    exponents = ref[count * HD :].astype(jnp.int32).astype(jnp.float32)
    return [
        ref[i * HD : (i + 1) * HD].astype(jnp.int32).astype(jnp.float32)
        * jnp.exp2(exponents[i : i + 1] - 15)
        for i in which or range(count)
    ]


def plus(left, right):
    return [a + b for a, b in zip(left, right)]


def states_in(ref, which):
    return decoded(ref, which) if ref.dtype == jnp.int16 else [ref[i] for i in which]


def total_of(refs, which):
    total = [jnp.zeros((HD, HD), jnp.float32)] * len(which)
    for ref in refs:
        total = plus(total, states_in(ref, which))
    return total


def coded_shape(heads):
    return jax.ShapeDtypeStruct((heads * HD + PAD, HD), jnp.int16)


def states_shape(*lead):
    return jax.ShapeDtypeStruct((*lead, HD, HD), jnp.float32)


def owned_columns(plan, place_ref, offset, half, i):
    x = place_ref[1] ^ (offset // plan.n_y)
    y = place_ref[2] ^ (offset % plan.n_y)
    start = (((y * plan.halves + half) * plan.n_inner + x) * plan.each + i) * HD
    return pl.ds(pl.multiple_of(start, HD), HD)


def chunk_states(plan, place, key, value, after):
    owned = plan.halves * plan.each

    def kernel(place_ref, k_ref, k_sib_ref, v_ref, v_sib_ref, *refs):
        own_ref, first_ref, *send_refs = refs[len(after) :]
        is_first = jnp.full((HD, HD), place_ref[0], jnp.int32) == 0
        for offset in (*range(plan.plane - 1, 0, -1), 0):
            states = []
            for n in range(owned):
                at = owned_columns(plan, place_ref, offset, *divmod(n, plan.each))
                mine = contract_rows(v_ref[:, at], k_ref[:, at])
                sib = contract_rows(v_sib_ref[:, at], k_sib_ref[:, at])
                first_ref[offset, n] = jnp.where(is_first, mine, sib)
                states.append(mine + sib)
            if offset:
                code(states, send_refs[offset - 1])
            else:
                for n, state in enumerate(states):
                    own_ref[n] = state

    heads = plan.plane * owned
    return pl.pallas_call(
        kernel,
        out_shape=[states_shape(owned), states_shape(plan.plane, owned)]
        + [coded_shape(owned)] * (plan.plane - 1),
        in_specs=[SMEM] + [VMEM] * 4 + [ANY] * len(after),
        out_specs=[VMEM] * (1 + plan.plane),
        compiler_params=params(),
        cost_estimate=cost(
            4 * plan.rows * HD * HD * heads, 8 * plan.rows * HD * heads + 6 * heads * HD * HD
        ),
        name="chunk_states",
    )(place, *key, *value, *after)


def of_half(plan, half):
    return range(half * plan.each, (half + 1) * plan.each)


def level_states(plan, own, others, half, after):
    def kernel(own_ref, *refs):
        code(total_of((own_ref, *refs[: len(others)]), of_half(plan, half)), refs[-1])

    return pl.pallas_call(
        kernel,
        out_shape=coded_shape(plan.each),
        in_specs=[VMEM] * plan.plane + [ANY] * len(after),
        out_specs=VMEM,
        compiler_params=params(),
        cost_estimate=cost(0, plan.plane * plan.each * HD * HD * 2),
        name=f"level_states_{half}",
    )(own, *others, *after)


def earlier_levels(plan, levels, after):
    def kernel(*refs):
        for i, state in enumerate(total_of(refs[: len(levels)], range(plan.each))):
            refs[-1][i] = state

    return pl.pallas_call(
        kernel,
        out_shape=states_shape(plan.each),
        in_specs=[VMEM] * len(levels) + [ANY] * len(after),
        out_specs=VMEM,
        compiler_params=params(),
        cost_estimate=cost(0, len(levels) * plan.each * HD * HD * 2),
        name="earlier_levels",
    )(*levels, *after)


def carried(plan, place_ref, own, others, levels, half, offsets):
    x, y = place_ref[1], place_ref[2]
    here = x * plan.n_y + y
    earlier = total_of(levels, range(plan.each))
    states = [states_in(ref, of_half(plan, half)) for ref in (own, *others)]

    def add(totals, keep_of):
        for offset, terms in enumerate(states):
            keep = jnp.full((HD, HD), keep_of(here ^ offset), jnp.int32) == 1
            totals = plus(totals, [jnp.where(keep, s, 0.0) for s in terms])
        return totals

    before = [add(earlier, lambda chip: (chip < here ^ o).astype(jnp.int32)) for o in offsets]
    blocks = [
        add(earlier, lambda chip: (chip // plan.n_y <= x ^ o).astype(jnp.int32))
        for o in range(plan.n_inner)
    ]
    return before, blocks


def carries(plan, place, own, others, levels, half, offsets, after):
    n_others, n_levels = len(others), len(levels)

    def kernel(place_ref, own_ref, *refs):
        others_refs, level_refs = refs[:n_others], refs[n_others : n_others + n_levels]
        before, _ = carried(plan, place_ref, own_ref, others_refs, level_refs, half, offsets)
        for states, ref in zip(before, refs[n_others + n_levels + len(after) :]):
            code(states, ref)

    return pl.pallas_call(
        kernel,
        out_shape=[coded_shape(plan.each)] * len(offsets),
        in_specs=[SMEM] + [VMEM] * (1 + n_others + n_levels) + [ANY] * len(after),
        out_specs=[VMEM] * len(offsets),
        compiler_params=params(),
        cost_estimate=cost(0, (plan.plane * 4 + n_levels) * plan.each * HD * HD * 2),
        name=f"carries_{half}",
    )(place, own, *others, *levels, *after)


def own_carries(plan, place, own, others, levels, offsets, after):
    n_others = len(others)
    starts = [1 + n_others + sum(map(len, levels[:h])) for h in range(plan.halves + 1)]

    def kernel(place_ref, own_ref, *refs):
        refs = (own_ref, *refs)
        outs = refs[starts[-1] + len(after) :]
        befores = [[] for _ in offsets]
        for half in range(plan.halves):
            level_refs = refs[starts[half] : starts[half + 1]]
            before, blocks = carried(
                plan, place_ref, own_ref, refs[1 : starts[0]], level_refs, half, offsets
            )
            for all_states, states in zip(befores, before):
                all_states.extend(states)
            for offset, (totals, ref) in enumerate(zip(blocks, outs[len(offsets) :])):
                block = place_ref[3] * plan.n_inner + (place_ref[1] ^ offset)
                seen = jnp.full((1, HD), (block + 1) * plan.block, jnp.int32).astype(jnp.float32)
                for i, total in enumerate(totals):
                    ref[half, i] = total.T * lax.rsqrt(seen)
        for states, ref in zip(befores, outs):
            code(states, ref)

    return pl.pallas_call(
        kernel,
        out_shape=[coded_shape(plan.halves * plan.each)] * len(offsets)
        + [states_shape(plan.halves, plan.each)] * plan.n_inner,
        in_specs=[SMEM] + [VMEM] * starts[-1] + [ANY] * len(after),
        out_specs=[VMEM] * (len(offsets) + plan.n_inner),
        compiler_params=params(),
        cost_estimate=cost(0, plan.plane * plan.each * HD * HD * 20),
        name="own_carries",
    )(place, own, *others, *[a for arrays in levels for a in arrays], *after)


def attend(plan, place, query, key, value, carry, first, gain, half, offsets, after=()):
    rows = plan.rows

    def kernel(
        place_ref, q_ref, q_sib_ref, k_ref, k_sib_ref, v_ref, v_sib_ref, first_ref, gain_ref, *refs
    ):
        core = place_ref[0]
        out_ref = refs[-1]
        causal = lax.broadcasted_iota(jnp.int32, (rows, rows), 0) >= lax.broadcasted_iota(
            jnp.int32, (rows, rows), 1
        )
        is_second = jnp.full((HD, HD), core, jnp.int32) == 1

        def attended(q_ref, k_ref, v_ref, at, carried, gain):
            queries = q_ref[:, at]
            scores = contract_columns(queries, k_ref[:, at]) * SCORE_SCALE
            weights = jnp.where(causal, scores, 0.0).astype(jnp.bfloat16)
            raw = jnp.dot(weights, v_ref[:, at], preferred_element_type=jnp.float32)
            carried = carried * SCORE_SCALE
            high = carried.astype(jnp.bfloat16)
            low = (carried - high.astype(jnp.float32)).astype(jnp.bfloat16)
            both = contract_columns(queries, jnp.concatenate([high, low], axis=0))
            raw = raw + (both[:, :HD] + both[:, HD:])
            mean = jnp.mean(raw * raw, axis=-1, keepdims=True)
            return (raw * lax.rsqrt(mean + 1e-06) * gain).astype(jnp.bfloat16)

        for piece, offset in enumerate(offsets):
            x = place_ref[1] ^ (offset // plan.n_y)
            carry_states = decoded(refs[piece])
            skip = half * plan.each if len(carry_states) > plan.each else 0
            for i in range(plan.each):
                at = owned_columns(plan, place_ref, offset, half, i)
                start = ((half * plan.n_inner + x) * plan.each + i) * HD
                gain = gain_ref[:, pl.ds(pl.multiple_of(start, HD), HD)]
                out_at = slice(piece * plan.piece + i * HD, piece * plan.piece + (i + 1) * HD)
                first = first_ref[offset, half * plan.each + i]
                mine = carry_states[skip + i] + jnp.where(is_second, first, 0.0)
                sib = carry_states[skip + i] + jnp.where(is_second, 0.0, first)
                out_ref[pl.ds(pl.multiple_of(core * rows, rows), rows), out_at] = attended(
                    q_ref, k_ref, v_ref, at, mine, gain
                )
                out_ref[pl.ds(pl.multiple_of((1 - core) * rows, rows), rows), out_at] = attended(
                    q_sib_ref, k_sib_ref, v_sib_ref, at, sib, gain
                )

    heads = len(offsets) * plan.each
    return pl.pallas_call(
        kernel,
        out_shape=jax.ShapeDtypeStruct((CORES * rows, heads * HD), jnp.bfloat16),
        in_specs=[SMEM] + [VMEM] * (8 + len(offsets)) + [ANY] * len(after),
        out_specs=VMEM,
        compiler_params=params(),
        cost_estimate=cost(
            heads * (8 * rows * rows * HD + 8 * rows * HD * HD), 16 * rows * heads * HD
        ),
        name=f"attend_{half}_" + "_".join(map(str, offsets)),
    )(place, *query, *key, *value, first, gain, *carry, *after)


def assemble(plan, place, parts, into=None):
    rows = CORES * plan.rows
    copies = [(n, piece, half, o) for n, (_, half, os) in enumerate(parts) for piece, o in enumerate(os)]

    def kernel(place_ref, *refs):
        out_ref, sems = refs[-2:]
        started = []
        for at, (n, piece, half, offset) in enumerate(copies):
            x = place_ref[1] ^ (offset // plan.n_y)
            y = place_ref[2] ^ (offset % plan.n_y)
            column = (half * plan.n_inner + x) * plan.piece
            to_rows = pl.ds(pl.multiple_of(y * rows, rows), rows)
            to_columns = pl.ds(pl.multiple_of(column, plan.piece), plan.piece)
            started.append(
                pltpu.make_async_copy(
                    refs[n].at[:, pl.ds(piece * plan.piece, plan.piece)],
                    out_ref.at[to_rows, to_columns],
                    sems.at[at],
                )
            )
            started[-1].start()
        for copy in started:
            copy.wait()

    arrays = [array for array, _, _ in parts]
    aliased = [] if into is None else [into]
    return pl.pallas_call(
        kernel,
        out_shape=jax.ShapeDtypeStruct((plan.n_y * rows, plan.width), jnp.bfloat16),
        in_specs=[SMEM] + [VMEM] * len(arrays) + [HBM] * len(aliased),
        out_specs=HBM,
        scratch_shapes=[pltpu.SemaphoreType.DMA((len(copies),))],
        input_output_aliases={1 + len(arrays): 0} if aliased else {},
        compiler_params=params(),
        name="assemble" if into is None else "finish",
    )(place, *arrays, *aliased)


def assemble_cache(plan, place, parts):
    group = plan.n_inner * plan.each

    def kernel(place_ref, *refs):
        for half in range(plan.halves):
            for offset, ref in enumerate(refs[:-1]):
                start = half * group + (place_ref[1] ^ offset) * plan.each
                refs[-1][0, pl.ds(start, plan.each)] = ref[half]

    return pl.pallas_call(
        kernel,
        out_shape=states_shape(1, plan.halves * group),
        in_specs=[SMEM] + [VMEM] * len(parts),
        out_specs=VMEM,
        compiler_params=params(),
        name="assemble_cache",
    )(place, *parts)


def per_device(plan, queries, keys, values, spikes, gain):
    place = jnp.stack([lax.axis_index(a) for a in ("core", "inner", "y", "outer")]).astype(jnp.int32)
    halves = range(plan.halves)

    def swap(array, axes, offset, size):
        return lax.ppermute(array, axes, [(i, i ^ offset) for i in range(size)])

    def in_level(array, offset):
        return swap(array, ("inner", "y"), offset, plan.plane)

    def to_later(array, distance):
        pairs = [(i, i + distance) for i in range(plan.n_outer - distance)]
        return lax.ppermute(array, "outer", pairs)

    gain = gain.reshape(1, plan.width)
    gains = [gain] + [swap(gain, "y", o, plan.n_y) for o in range(1, plan.n_y)]
    key, key_out, value, value_out, *counts = decode(plan, place, spikes, keys, values)
    key, value = ((a, swap(b, "core", 1, CORES)) for a, b in ((key, key_out), (value, value_out)))
    query, query_out = spike_queries(plan, place, queries, counts)
    query = (query, swap(query_out, "core", 1, CORES))

    own, first, *sends = chunk_states(plan, place, key, value, [query[0]])
    others = [in_level(a, o) for o, a in enumerate(sends, 1)]
    levels = []
    after = [query[1], *gains[1:]]
    for half in halves:
        level = level_states(plan, own, others, half, after)
        levels.append([to_later(level, d) for d in range(plan.n_outer - 1, 0, -1)])
        after = [level]

    of_group = [list(range(y, plan.plane, plan.n_y)) for y in range(plan.n_y)]
    abroad = [o for offsets in of_group[1:] for o in offsets]

    def part_of(half, offsets, carry, after):
        return attend(
            plan,
            place,
            query,
            key,
            value,
            [carry[o] for o in offsets],
            first,
            gains[offsets[0] % plan.n_y],
            half,
            offsets,
            after,
        )

    def carry_stage(half, after):
        sends = carries(plan, place, own, others, levels[half], half, abroad, after)
        return sends[0], {o: in_level(a, o) for o, a in zip(abroad, sends)}

    parts = []

    def send_stage(half, carry, after):
        for y in range(1, plan.n_y):
            group = of_group[y]
            pieces = [group[:-1], group[-1:]] if half and len(group) > 1 else [group]
            for offsets in pieces:
                arrived = [a for a, h, os in parts if h == 0 and offsets == group[-1:] and os == group]
                part = part_of(half, offsets, carry, after + arrived)
                parts.append((swap(part, "y", y, plan.n_y), half, offsets))
                after = [part]
        return after

    done, carry = carry_stage(0, after)
    after = []
    if plan.halves > 1 and levels[1]:
        levels[1] = [earlier_levels(plan, levels[1], [done])]
        after = levels[1]
    after = send_stage(0, carry, after)
    if plan.halves > 1:
        _, carry = carry_stage(1, after)
        after = send_stage(1, carry, [])
    sends = own_carries(plan, place, own, others, levels, of_group[0], after)
    own_carry = {o: in_level(a, o) if o else a for o, a in zip(of_group[0], sends)}
    caches = [
        swap(a, "inner", o, plan.n_inner) if o else a
        for o, a in enumerate(sends[len(of_group[0]) :])
    ]
    early = []
    for half in halves:
        part = part_of(half, of_group[0], own_carry, after)
        early.append((part, half, of_group[0]))
        after = [part]
    out = assemble(plan, place, early + parts[:-1])
    out = assemble(plan, place, parts[-1:], out)
    return out, assemble_cache(plan, place, caches)


def solution(mesh):
    tokens = P(("outer", "inner", "y", "core"), None)
    seq, head = ("outer", "inner"), ("y", "core")

    def whole(queries, keys, values, spikes, gain):
        plan = Plan(mesh, spikes.shape[0] // mesh.size, spikes.shape[1])
        sizes = (plan.n_outer, plan.n_inner, plan.n_y, CORES)
        split = Mesh(mesh.devices.reshape(sizes), ("outer", "inner", "y", "core"))
        return jax.shard_map(
            functools.partial(per_device, plan),
            mesh=split,
            in_specs=(tokens, tokens, tokens, tokens, P(head)),
            out_specs=(P(seq, head), P(seq, head, None, None)),
            check_vma=False,
        )(queries, keys, values, spikes, gain)

    return whole
```

```python
import functools

import jax
import jax.numpy as jnp
from jax import lax
from jax.experimental import pallas as pl
from jax.experimental.pallas import tpu as pltpu
from jax.sharding import Mesh
from jax.sharding import PartitionSpec as P

HD = 128
SCORE_SCALE = HD ** (-0.5)
CORES = 2
VMEM_BYTES = 24 * 1024 * 1024
DECODE_VMEM_BYTES = 46 * 1024 * 1024
PAD = 16
TOP = 32767.0

VMEM = pl.BlockSpec(memory_space=pltpu.VMEM)
SMEM = pl.BlockSpec(memory_space=pltpu.SMEM)
HBM = pl.BlockSpec(memory_space=pltpu.HBM)
ANY = pl.BlockSpec(memory_space=pl.ANY)


def params(vmem=VMEM_BYTES):
    return pltpu.CompilerParams(vmem_limit_bytes=vmem)


def cost(flops, bytes_accessed):
    return pl.CostEstimate(flops=flops, bytes_accessed=bytes_accessed, transcendentals=0)


class Plan:
    def __init__(self, mesh, rows, model):
        n_seq, n_head = mesh.shape["seq"], mesh.shape["head"]
        self.n_y = n_head // CORES
        self.width = model // n_head
        group = self.width // HD
        self.n_inner = 2 if n_seq % 2 == 0 and group % 2 == 0 else 1
        self.n_outer = n_seq // self.n_inner
        self.halves = 2 if group // self.n_inner % 2 == 0 else 1
        self.each = group // (self.n_inner * self.halves)
        self.plane = self.n_inner * self.n_y
        self.rows = rows
        self.block = rows * n_head
        self.piece = self.each * HD


def counts_of(spikes):
    one, two = jnp.ones_like(spikes), jnp.full_like(spikes, 2)
    zero = jnp.zeros_like(spikes)

    def ternary(rest, unit):
        return jnp.where(rest >= 2 * unit, two, jnp.where(rest >= unit, one, zero))

    value = ternary(spikes, 9)
    rest = spikes - 9 * value
    key = ternary(rest, 3)
    return value, key, rest - 3 * key


def sides(plan, place_ref):
    for y in range(plan.n_y):
        for side in range(CORES):
            of = place_ref[0] if side == 0 else 1 - place_ref[0]
            start = pl.multiple_of((y * CORES + of) * plan.width, plan.width)
            yield side, slice(y * plan.width, (y + 1) * plan.width), pl.ds(start, plan.width)


def decode(plan, place, spikes, keys, values):
    rows, model = spikes.shape
    step = min(rows, 32)
    chunks = rows // step

    def kernel(place_ref, *refs):
        sources, outs, buffers, sems = refs[:3], refs[3:9], refs[9:12], refs[12]

        def fetch(chunk, index):
            at = pl.ds(chunk * step, step)
            return pltpu.make_async_copy(
                sources[index].at[at], buffers[index].at[at], sems.at[chunk, index]
            )

        for chunk in range(chunks):
            for index in range(3):
                fetch(chunk, index).start()

        @pl.loop(0, chunks)
        def _(chunk):
            for index in range(3):
                fetch(chunk, index).wait()
            at = pl.ds(pl.multiple_of(chunk * step, step), step)
            for side, mine, columns in sides(plan, place_ref):
                spikes = buffers[0][at, columns].astype(jnp.float32).astype(jnp.bfloat16)
                value, key, query = counts_of(spikes)
                outs[side][at, mine] = buffers[1][at, columns] * key
                outs[2 + side][at, mine] = buffers[2][at, columns] * value
                outs[4 + side][at, mine] = query

    return pl.pallas_call(
        kernel,
        out_shape=[jax.ShapeDtypeStruct((rows, plan.n_y * plan.width), jnp.bfloat16)] * 6,
        in_specs=[SMEM] + [HBM] * 3,
        out_specs=[VMEM] * 6,
        scratch_shapes=[
            pltpu.VMEM((rows, model), jnp.int32),
            pltpu.VMEM((rows, model), jnp.bfloat16),
            pltpu.VMEM((rows, model), jnp.bfloat16),
            pltpu.SemaphoreType.DMA((chunks, 3)),
        ],
        compiler_params=params(DECODE_VMEM_BYTES),
        cost_estimate=cost(rows * model * 4, rows * model * 14),
        name="decode",
    )(place, spikes, keys, values)


def spike_queries(plan, place, queries, counts):
    def kernel(place_ref, queries_ref, *refs):
        for side, mine, columns in sides(plan, place_ref):
            refs[2 + side][:, mine] = queries_ref[:, columns] * refs[side][:, mine]

    return pl.pallas_call(
        kernel,
        out_shape=[jax.ShapeDtypeStruct(a.shape, jnp.bfloat16) for a in counts],
        in_specs=[SMEM] + [VMEM] * 3,
        out_specs=[VMEM] * 2,
        compiler_params=params(),
        cost_estimate=cost(queries.size, queries.size * 6),
        name="spike_queries",
    )(place, queries, *counts)


def contract_rows(left, right):
    return lax.dot_general(
        left, right, (((0,), (0,)), ((), ())), preferred_element_type=jnp.float32
    )


def contract_columns(left, right):
    return lax.dot_general(
        left, right, (((1,), (1,)), ((), ())), preferred_element_type=jnp.float32
    )


def code(states, ref):
    line = lax.broadcasted_iota(jnp.int32, (PAD, HD), 0)
    exponents = jnp.zeros((PAD, HD), jnp.float32)
    for i, state in enumerate(states):
        top = jnp.max(jnp.abs(state), axis=0, keepdims=True)
        exponent = jnp.floor(jnp.log2(jnp.maximum(top, 1e-30))) + 1
        scaled = jnp.round(state * jnp.exp2(15 - exponent))
        scaled = jnp.clip(scaled, -TOP, TOP)
        ref[i * HD : (i + 1) * HD] = scaled.astype(jnp.int32).astype(jnp.int16)
        exponents = jnp.where(line == i, exponent, exponents)
    ref[len(states) * HD :] = exponents.astype(jnp.int32).astype(jnp.int16)


def decoded(ref):
    count = ref.shape[0] // HD
    exponents = ref[count * HD :].astype(jnp.int32).astype(jnp.float32)
    return [
        ref[i * HD : (i + 1) * HD].astype(jnp.int32).astype(jnp.float32)
        * jnp.exp2(exponents[i : i + 1] - 15)
        for i in range(count)
    ]


def plus(left, right):
    return [a + b for a, b in zip(left, right)]


def total_of(refs, each):
    total = [jnp.zeros((HD, HD), jnp.float32)] * each
    for ref in refs:
        coded = ref.dtype == jnp.int16
        total = plus(total, decoded(ref) if coded else [ref[i] for i in range(each)])
    return total


def coded_shape(heads):
    return jax.ShapeDtypeStruct((heads * HD + PAD, HD), jnp.int16)


def states_shape(*lead):
    return jax.ShapeDtypeStruct((*lead, HD, HD), jnp.float32)


def owned_columns(plan, place_ref, offset, half, i):
    x = place_ref[1] ^ (offset // plan.n_y)
    y = place_ref[2] ^ (offset % plan.n_y)
    start = (((y * plan.halves + half) * plan.n_inner + x) * plan.each + i) * HD
    return pl.ds(pl.multiple_of(start, HD), HD)


def chunk_states(plan, place, key, value, half, after):
    def kernel(place_ref, k_ref, k_sib_ref, v_ref, v_sib_ref, *refs):
        own_ref, first_ref, *send_refs = refs[len(after) :]
        is_first = jnp.full((HD, HD), place_ref[0], jnp.int32) == 0
        for offset in (*range(1, plan.plane), 0):
            states = []
            for i in range(plan.each):
                at = owned_columns(plan, place_ref, offset, half, i)
                mine = contract_rows(v_ref[:, at], k_ref[:, at])
                sib = contract_rows(v_sib_ref[:, at], k_sib_ref[:, at])
                first_ref[offset, i] = jnp.where(is_first, mine, sib)
                states.append(mine + sib)
            if offset:
                code(states, send_refs[offset - 1])
            else:
                for i, state in enumerate(states):
                    own_ref[i] = state

    heads = plan.plane * plan.each
    return pl.pallas_call(
        kernel,
        out_shape=[states_shape(plan.each), states_shape(plan.plane, plan.each)]
        + [coded_shape(plan.each)] * (plan.plane - 1),
        in_specs=[SMEM] + [VMEM] * 4 + [ANY] * len(after),
        out_specs=[VMEM] * (1 + plan.plane),
        compiler_params=params(),
        cost_estimate=cost(
            4 * plan.rows * HD * HD * heads, 8 * plan.rows * HD * heads + 6 * heads * HD * HD
        ),
        name=f"chunk_states_{half}",
    )(place, *key, *value, *after)


def level_states(plan, own, others, half, after):
    def kernel(own_ref, *refs):
        code(total_of((own_ref, *refs[: len(others)]), plan.each), refs[-1])

    return pl.pallas_call(
        kernel,
        out_shape=coded_shape(plan.each),
        in_specs=[VMEM] * plan.plane + [ANY] * len(after),
        out_specs=VMEM,
        compiler_params=params(),
        cost_estimate=cost(0, plan.plane * plan.each * HD * HD * 2),
        name=f"level_states_{half}",
    )(own, *others, *after)


def carried(plan, place_ref, own, others, levels, offsets):
    x, y = place_ref[1], place_ref[2]
    here = x * plan.n_y + y
    earlier = total_of(levels, plan.each)
    states = [[own[i] for i in range(plan.each)]] + [decoded(ref) for ref in others]

    def add(totals, keep_of):
        for offset, terms in enumerate(states):
            keep = jnp.full((HD, HD), keep_of(here ^ offset), jnp.int32) == 1
            totals = plus(totals, [jnp.where(keep, s, 0.0) for s in terms])
        return totals

    before = [add(earlier, lambda chip: (chip < here ^ o).astype(jnp.int32)) for o in offsets]
    blocks = [
        add(earlier, lambda chip: (chip // plan.n_y <= x ^ o).astype(jnp.int32))
        for o in range(plan.n_inner)
    ]
    return before, blocks


def carries(plan, place, own, others, levels, half, offsets, after):
    n_others, n_levels = len(others), len(levels)

    def kernel(place_ref, own_ref, *refs):
        before, _ = carried(
            plan, place_ref, own_ref, refs[:n_others], refs[n_others : n_others + n_levels], offsets
        )
        for states, ref in zip(before, refs[n_others + n_levels + len(after) :]):
            code(states, ref)

    return pl.pallas_call(
        kernel,
        out_shape=[coded_shape(plan.each)] * len(offsets),
        in_specs=[SMEM] + [VMEM] * (1 + n_others + n_levels) + [ANY] * len(after),
        out_specs=[VMEM] * len(offsets),
        compiler_params=params(),
        cost_estimate=cost(0, (plan.plane * 4 + n_levels) * plan.each * HD * HD * 2),
        name=f"carries_{half}",
    )(place, own, *others, *levels, *after)


def own_carries(plan, place, own, others, levels, offsets, after):
    n_others = len(others[0])
    operands = [(own[h], *others[h], *levels[h]) for h in range(plan.halves)]
    starts = [sum(map(len, operands[:h])) for h in range(plan.halves + 1)]

    def kernel(place_ref, *refs):
        outs = refs[starts[-1] + len(after) :]
        befores = [[] for _ in offsets]
        for half in range(plan.halves):
            own_ref, *of_half = refs[starts[half] : starts[half + 1]]
            before, blocks = carried(
                plan, place_ref, own_ref, of_half[:n_others], of_half[n_others:], offsets
            )
            for all_states, states in zip(befores, before):
                all_states.extend(states)
            for offset, (totals, ref) in enumerate(zip(blocks, outs[len(offsets) :])):
                block = place_ref[3] * plan.n_inner + (place_ref[1] ^ offset)
                seen = jnp.full((1, HD), (block + 1) * plan.block, jnp.int32).astype(jnp.float32)
                for i, total in enumerate(totals):
                    ref[half, i] = total.T * lax.rsqrt(seen)
        for states, ref in zip(befores, outs):
            code(states, ref)

    return pl.pallas_call(
        kernel,
        out_shape=[coded_shape(plan.halves * plan.each)] * len(offsets)
        + [states_shape(plan.halves, plan.each)] * plan.n_inner,
        in_specs=[SMEM] + [VMEM] * starts[-1] + [ANY] * len(after),
        out_specs=[VMEM] * (len(offsets) + plan.n_inner),
        compiler_params=params(),
        cost_estimate=cost(0, plan.plane * plan.each * HD * HD * 20),
        name="own_carries",
    )(place, *[a for arrays in operands for a in arrays], *after)


def attend(plan, place, query, key, value, carry, first, gain, half, offsets, after=()):
    rows = plan.rows

    def kernel(
        place_ref, q_ref, q_sib_ref, k_ref, k_sib_ref, v_ref, v_sib_ref, first_ref, gain_ref, *refs
    ):
        core = place_ref[0]
        out_ref = refs[-1]
        causal = lax.broadcasted_iota(jnp.int32, (rows, rows), 0) >= lax.broadcasted_iota(
            jnp.int32, (rows, rows), 1
        )
        is_second = jnp.full((HD, HD), core, jnp.int32) == 1

        def attended(q_ref, k_ref, v_ref, at, carried, gain):
            queries = q_ref[:, at]
            scores = contract_columns(queries, k_ref[:, at]) * SCORE_SCALE
            weights = jnp.where(causal, scores, 0.0).astype(jnp.bfloat16)
            raw = jnp.dot(weights, v_ref[:, at], preferred_element_type=jnp.float32)
            carried = carried * SCORE_SCALE
            high = carried.astype(jnp.bfloat16)
            low = (carried - high.astype(jnp.float32)).astype(jnp.bfloat16)
            both = contract_columns(queries, jnp.concatenate([high, low], axis=0))
            raw = raw + (both[:, :HD] + both[:, HD:])
            mean = jnp.mean(raw * raw, axis=-1, keepdims=True)
            return (raw * lax.rsqrt(mean + 1e-06) * gain).astype(jnp.bfloat16)

        for piece, offset in enumerate(offsets):
            x = place_ref[1] ^ (offset // plan.n_y)
            carry_states = decoded(refs[piece])
            skip = half * plan.each if len(carry_states) > plan.each else 0
            for i in range(plan.each):
                at = owned_columns(plan, place_ref, offset, half, i)
                start = ((half * plan.n_inner + x) * plan.each + i) * HD
                gain = gain_ref[:, pl.ds(pl.multiple_of(start, HD), HD)]
                out_at = slice(piece * plan.piece + i * HD, piece * plan.piece + (i + 1) * HD)
                first = first_ref[offset, i]
                mine = carry_states[skip + i] + jnp.where(is_second, first, 0.0)
                sib = carry_states[skip + i] + jnp.where(is_second, 0.0, first)
                out_ref[pl.ds(pl.multiple_of(core * rows, rows), rows), out_at] = attended(
                    q_ref, k_ref, v_ref, at, mine, gain
                )
                out_ref[pl.ds(pl.multiple_of((1 - core) * rows, rows), rows), out_at] = attended(
                    q_sib_ref, k_sib_ref, v_sib_ref, at, sib, gain
                )

    heads = len(offsets) * plan.each
    return pl.pallas_call(
        kernel,
        out_shape=jax.ShapeDtypeStruct((CORES * rows, heads * HD), jnp.bfloat16),
        in_specs=[SMEM] + [VMEM] * (8 + len(offsets)) + [ANY] * len(after),
        out_specs=VMEM,
        compiler_params=params(),
        cost_estimate=cost(
            heads * (8 * rows * rows * HD + 8 * rows * HD * HD), 16 * rows * heads * HD
        ),
        name=f"attend_{half}_" + "_".join(map(str, offsets)),
    )(place, *query, *key, *value, first, gain, *carry, *after)


def assemble(plan, place, parts, into=None):
    rows = CORES * plan.rows
    copies = [(n, piece, half, o) for n, (_, half, os) in enumerate(parts) for piece, o in enumerate(os)]

    def kernel(place_ref, *refs):
        out_ref, sems = refs[-2:]
        started = []
        for at, (n, piece, half, offset) in enumerate(copies):
            x = place_ref[1] ^ (offset // plan.n_y)
            y = place_ref[2] ^ (offset % plan.n_y)
            column = (half * plan.n_inner + x) * plan.piece
            to_rows = pl.ds(pl.multiple_of(y * rows, rows), rows)
            to_columns = pl.ds(pl.multiple_of(column, plan.piece), plan.piece)
            started.append(
                pltpu.make_async_copy(
                    refs[n].at[:, pl.ds(piece * plan.piece, plan.piece)],
                    out_ref.at[to_rows, to_columns],
                    sems.at[at],
                )
            )
            started[-1].start()
        for copy in started:
            copy.wait()

    arrays = [array for array, _, _ in parts]
    aliased = [] if into is None else [into]
    return pl.pallas_call(
        kernel,
        out_shape=jax.ShapeDtypeStruct((plan.n_y * rows, plan.width), jnp.bfloat16),
        in_specs=[SMEM] + [VMEM] * len(arrays) + [HBM] * len(aliased),
        out_specs=HBM,
        scratch_shapes=[pltpu.SemaphoreType.DMA((len(copies),))],
        input_output_aliases={1 + len(arrays): 0} if aliased else {},
        compiler_params=params(),
        name="assemble" if into is None else "finish",
    )(place, *arrays, *aliased)


def assemble_cache(plan, place, parts):
    group = plan.n_inner * plan.each

    def kernel(place_ref, *refs):
        for half in range(plan.halves):
            for offset, ref in enumerate(refs[:-1]):
                start = half * group + (place_ref[1] ^ offset) * plan.each
                refs[-1][0, pl.ds(start, plan.each)] = ref[half]

    return pl.pallas_call(
        kernel,
        out_shape=states_shape(1, plan.halves * group),
        in_specs=[SMEM] + [VMEM] * len(parts),
        out_specs=VMEM,
        compiler_params=params(),
        name="assemble_cache",
    )(place, *parts)


def per_device(plan, queries, keys, values, spikes, gain):
    place = jnp.stack([lax.axis_index(a) for a in ("core", "inner", "y", "outer")]).astype(jnp.int32)
    halves = range(plan.halves)

    def swap(array, axes, offset, size):
        return lax.ppermute(array, axes, [(i, i ^ offset) for i in range(size)])

    def in_level(array, offset):
        return swap(array, ("inner", "y"), offset, plan.plane)

    def to_later(array, distance):
        pairs = [(i, i + distance) for i in range(plan.n_outer - distance)]
        return lax.ppermute(array, "outer", pairs)

    gain = gain.reshape(1, plan.width)
    gains = [gain] + [swap(gain, "y", o, plan.n_y) for o in range(1, plan.n_y)]
    key, key_out, value, value_out, *counts = decode(plan, place, spikes, keys, values)
    key, value = ((a, swap(b, "core", 1, CORES)) for a, b in ((key, key_out), (value, value_out)))
    query, query_out = spike_queries(plan, place, queries, counts)
    query = (query, swap(query_out, "core", 1, CORES))

    own, first, others, levels, coded = [], [], [], [], []

    def owner_stage(half, after):
        mine, parts, *sends = chunk_states(plan, place, key, value, half, after)
        own.append(mine)
        first.append(parts)
        others.append([in_level(a, o) for o, a in enumerate(sends, 1)])

    def level_stage(half, after):
        level = level_states(plan, own[half], others[half], half, after)
        coded.append(level)
        levels.append([to_later(level, d) for d in range(plan.n_outer - 1, 0, -1)])

    of_group = [list(range(y, plan.plane, plan.n_y)) for y in range(plan.n_y)]
    abroad = [o for offsets in of_group[1:] for o in offsets]

    def part_of(half, offsets, carry, after):
        return attend(
            plan,
            place,
            query,
            key,
            value,
            [carry[o] for o in offsets],
            first[half],
            gains[offsets[0] % plan.n_y],
            half,
            offsets,
            after,
        )

    def carry_stage(half, after):
        sends = carries(plan, place, own[half], others[half], levels[half], half, abroad, after)
        return sends[0], {o: in_level(a, o) for o, a in zip(abroad, sends)}

    parts = []

    def send_stage(half, carry, after):
        for y in range(1, plan.n_y):
            part = part_of(half, of_group[y], carry, after)
            parts.append((swap(part, "y", y, plan.n_y), half, of_group[y]))
            after = [part]
        return after

    after = [query[0]]
    for half in halves:
        owner_stage(half, after)
        after = [own[-1], query[1]]
    for half in halves:
        level_stage(half, after)
        after = [coded[-1]]
    carry = []
    after = [*after, *gains[1:]]
    for half in halves:
        done, of_half = carry_stage(half, after)
        carry.append(of_half)
        after = [done]
    for half in halves:
        after = send_stage(half, carry[half], after)
    sends = own_carries(plan, place, own, others, levels, of_group[0], after)
    own_carry = {o: in_level(a, o) if o else a for o, a in zip(of_group[0], sends)}
    caches = [
        swap(a, "inner", o, plan.n_inner) if o else a
        for o, a in enumerate(sends[len(of_group[0]) :])
    ]
    early = []
    for half in halves:
        part = part_of(half, of_group[0], own_carry, after)
        early.append((part, half, of_group[0]))
        after = [part]
    out = assemble(plan, place, early + parts[:-1])
    out = assemble(plan, place, parts[-1:], out)
    return out, assemble_cache(plan, place, caches)


def solution(mesh):
    tokens = P(("outer", "inner", "y", "core"), None)
    seq, head = ("outer", "inner"), ("y", "core")

    def whole(queries, keys, values, spikes, gain):
        plan = Plan(mesh, spikes.shape[0] // mesh.size, spikes.shape[1])
        sizes = (plan.n_outer, plan.n_inner, plan.n_y, CORES)
        split = Mesh(mesh.devices.reshape(sizes), ("outer", "inner", "y", "core"))
        return jax.shard_map(
            functools.partial(per_device, plan),
            mesh=split,
            in_specs=(tokens, tokens, tokens, tokens, P(head)),
            out_specs=(P(seq, head), P(seq, head, None, None)),
            check_vma=False,
        )(queries, keys, values, spikes, gain)

    return whole
```

```python
import functools

import jax
import jax.numpy as jnp
from jax import lax
from jax.experimental import pallas as pl
from jax.experimental.pallas import tpu as pltpu
from jax.sharding import Mesh
from jax.sharding import PartitionSpec as P

HD = 128
SCORE_SCALE = HD ** (-0.5)
CORES = 2
VMEM_BYTES = 24 * 1024 * 1024
DECODE_VMEM_BYTES = 46 * 1024 * 1024
PAD = 16
TOP = 32767.0

VMEM = pl.BlockSpec(memory_space=pltpu.VMEM)
SMEM = pl.BlockSpec(memory_space=pltpu.SMEM)
HBM = pl.BlockSpec(memory_space=pltpu.HBM)
ANY = pl.BlockSpec(memory_space=pl.ANY)


def params(vmem=VMEM_BYTES):
    return pltpu.CompilerParams(vmem_limit_bytes=vmem)


def cost(flops, bytes_accessed):
    return pl.CostEstimate(flops=flops, bytes_accessed=bytes_accessed, transcendentals=0)


class Plan:
    def __init__(self, mesh, rows, model):
        n_seq, n_head = mesh.shape["seq"], mesh.shape["head"]
        self.n_y = n_head // CORES
        self.width = model // n_head
        group = self.width // HD
        self.n_inner = 2 if n_seq % 2 == 0 and group % 2 == 0 else 1
        self.n_outer = n_seq // self.n_inner
        self.halves = 2 if group // self.n_inner % 2 == 0 else 1
        self.each = group // (self.n_inner * self.halves)
        self.plane = self.n_inner * self.n_y
        self.rows = rows
        self.block = rows * n_head
        self.piece = self.each * HD


def counts_of(spikes):
    one, two = jnp.ones_like(spikes), jnp.full_like(spikes, 2)
    zero = jnp.zeros_like(spikes)

    def ternary(rest, unit):
        return jnp.where(rest >= 2 * unit, two, jnp.where(rest >= unit, one, zero))

    value = ternary(spikes, 9)
    rest = spikes - 9 * value
    key = ternary(rest, 3)
    return value, key, rest - 3 * key


def sides(plan, place_ref):
    for y in range(plan.n_y):
        for side in range(CORES):
            of = place_ref[0] if side == 0 else 1 - place_ref[0]
            start = pl.multiple_of((y * CORES + of) * plan.width, plan.width)
            yield side, slice(y * plan.width, (y + 1) * plan.width), pl.ds(start, plan.width)


def decode(plan, place, spikes, keys, values):
    rows, model = spikes.shape
    step = min(rows, 32)
    chunks = rows // step

    def kernel(place_ref, *refs):
        sources, outs, buffers, sems = refs[:3], refs[3:9], refs[9:12], refs[12]

        def fetch(chunk, index):
            at = pl.ds(chunk * step, step)
            return pltpu.make_async_copy(
                sources[index].at[at], buffers[index].at[at], sems.at[chunk, index]
            )

        for chunk in range(chunks):
            for index in range(3):
                fetch(chunk, index).start()

        @pl.loop(0, chunks)
        def _(chunk):
            for index in range(3):
                fetch(chunk, index).wait()
            at = pl.ds(pl.multiple_of(chunk * step, step), step)
            for side, mine, columns in sides(plan, place_ref):
                spikes = buffers[0][at, columns].astype(jnp.float32).astype(jnp.bfloat16)
                value, key, query = counts_of(spikes)
                outs[side][at, mine] = buffers[1][at, columns] * key
                outs[2 + side][at, mine] = buffers[2][at, columns] * value
                outs[4 + side][at, mine] = query

    return pl.pallas_call(
        kernel,
        out_shape=[jax.ShapeDtypeStruct((rows, plan.n_y * plan.width), jnp.bfloat16)] * 6,
        in_specs=[SMEM] + [HBM] * 3,
        out_specs=[VMEM] * 6,
        scratch_shapes=[
            pltpu.VMEM((rows, model), jnp.int32),
            pltpu.VMEM((rows, model), jnp.bfloat16),
            pltpu.VMEM((rows, model), jnp.bfloat16),
            pltpu.SemaphoreType.DMA((chunks, 3)),
        ],
        compiler_params=params(DECODE_VMEM_BYTES),
        cost_estimate=cost(rows * model * 4, rows * model * 14),
        name="decode",
    )(place, spikes, keys, values)


def spike_queries(plan, place, queries, counts):
    def kernel(place_ref, queries_ref, *refs):
        for side, mine, columns in sides(plan, place_ref):
            refs[2 + side][:, mine] = queries_ref[:, columns] * refs[side][:, mine]

    return pl.pallas_call(
        kernel,
        out_shape=[jax.ShapeDtypeStruct(a.shape, jnp.bfloat16) for a in counts],
        in_specs=[SMEM] + [VMEM] * 3,
        out_specs=[VMEM] * 2,
        compiler_params=params(),
        cost_estimate=cost(queries.size, queries.size * 6),
        name="spike_queries",
    )(place, queries, *counts)


def contract_rows(left, right):
    return lax.dot_general(
        left, right, (((0,), (0,)), ((), ())), preferred_element_type=jnp.float32
    )


def contract_columns(left, right):
    return lax.dot_general(
        left, right, (((1,), (1,)), ((), ())), preferred_element_type=jnp.float32
    )


def code(states, ref):
    line = lax.broadcasted_iota(jnp.int32, (PAD, HD), 0)
    exponents = jnp.zeros((PAD, HD), jnp.float32)
    for i, state in enumerate(states):
        top = jnp.max(jnp.abs(state), axis=0, keepdims=True)
        exponent = jnp.floor(jnp.log2(jnp.maximum(top, 1e-30))) + 1
        scaled = jnp.round(state * jnp.exp2(15 - exponent))
        scaled = jnp.clip(scaled, -TOP, TOP)
        ref[i * HD : (i + 1) * HD] = scaled.astype(jnp.int32).astype(jnp.int16)
        exponents = jnp.where(line == i, exponent, exponents)
    ref[len(states) * HD :] = exponents.astype(jnp.int32).astype(jnp.int16)


def decoded(ref):
    count = ref.shape[0] // HD
    exponents = ref[count * HD :].astype(jnp.int32).astype(jnp.float32)
    return [
        ref[i * HD : (i + 1) * HD].astype(jnp.int32).astype(jnp.float32)
        * jnp.exp2(exponents[i : i + 1] - 15)
        for i in range(count)
    ]


def plus(left, right):
    return [a + b for a, b in zip(left, right)]


def total_of(refs, each):
    total = [jnp.zeros((HD, HD), jnp.float32)] * each
    for ref in refs:
        coded = ref.dtype == jnp.int16
        total = plus(total, decoded(ref) if coded else [ref[i] for i in range(each)])
    return total


def coded_shape(heads):
    return jax.ShapeDtypeStruct((heads * HD + PAD, HD), jnp.int16)


def states_shape(*lead):
    return jax.ShapeDtypeStruct((*lead, HD, HD), jnp.float32)


def owned_columns(plan, place_ref, offset, half, i):
    x = place_ref[1] ^ (offset // plan.n_y)
    y = place_ref[2] ^ (offset % plan.n_y)
    start = (((y * plan.halves + half) * plan.n_inner + x) * plan.each + i) * HD
    return pl.ds(pl.multiple_of(start, HD), HD)


def chunk_states(plan, place, key, value, half, after):
    def kernel(place_ref, k_ref, k_sib_ref, v_ref, v_sib_ref, *refs):
        own_ref, first_ref, *send_refs = refs[len(after) :]
        is_first = jnp.full((HD, HD), place_ref[0], jnp.int32) == 0
        for offset in (*range(1, plan.plane), 0):
            states = []
            for i in range(plan.each):
                at = owned_columns(plan, place_ref, offset, half, i)
                mine = contract_rows(v_ref[:, at], k_ref[:, at])
                sib = contract_rows(v_sib_ref[:, at], k_sib_ref[:, at])
                first_ref[offset, i] = jnp.where(is_first, mine, sib)
                states.append(mine + sib)
            if offset:
                code(states, send_refs[offset - 1])
            else:
                for i, state in enumerate(states):
                    own_ref[i] = state

    heads = plan.plane * plan.each
    return pl.pallas_call(
        kernel,
        out_shape=[states_shape(plan.each), states_shape(plan.plane, plan.each)]
        + [coded_shape(plan.each)] * (plan.plane - 1),
        in_specs=[SMEM] + [VMEM] * 4 + [ANY] * len(after),
        out_specs=[VMEM] * (1 + plan.plane),
        compiler_params=params(),
        cost_estimate=cost(
            4 * plan.rows * HD * HD * heads, 8 * plan.rows * HD * heads + 6 * heads * HD * HD
        ),
        name=f"chunk_states_{half}",
    )(place, *key, *value, *after)


def level_states(plan, own, others, half, after):
    def kernel(own_ref, *refs):
        total = total_of((own_ref, *refs[: len(others)]), plan.each)
        for i, state in enumerate(total):
            refs[-2][i] = state
        code(total, refs[-1])

    return pl.pallas_call(
        kernel,
        out_shape=[states_shape(plan.each), coded_shape(plan.each)],
        in_specs=[VMEM] * plan.plane + [ANY] * len(after),
        out_specs=[VMEM] * 2,
        compiler_params=params(),
        cost_estimate=cost(0, plan.plane * plan.each * HD * HD * 2),
        name=f"level_states_{half}",
    )(own, *others, *after)


def levels_so_far(plan, total, arrived, half, after):
    def kernel(total_ref, *refs):
        code(total_of((total_ref, *refs[: len(arrived)]), plan.each), refs[-1])

    return pl.pallas_call(
        kernel,
        out_shape=coded_shape(plan.each),
        in_specs=[VMEM] * (1 + len(arrived)) + [ANY] * len(after),
        out_specs=VMEM,
        compiler_params=params(),
        cost_estimate=cost(0, 2 * plan.each * HD * HD * 2),
        name=f"levels_so_far_{half}_{len(arrived)}",
    )(total, *arrived, *after)


def carried(plan, place_ref, own, others, levels, offsets):
    x, y = place_ref[1], place_ref[2]
    here = x * plan.n_y + y
    earlier = total_of(levels, plan.each)
    states = [[own[i] for i in range(plan.each)]] + [decoded(ref) for ref in others]

    def add(totals, keep_of):
        for offset, terms in enumerate(states):
            keep = jnp.full((HD, HD), keep_of(here ^ offset), jnp.int32) == 1
            totals = plus(totals, [jnp.where(keep, s, 0.0) for s in terms])
        return totals

    before = [add(earlier, lambda chip: (chip < here ^ o).astype(jnp.int32)) for o in offsets]
    blocks = [
        add(earlier, lambda chip: (chip // plan.n_y <= x ^ o).astype(jnp.int32))
        for o in range(plan.n_inner)
    ]
    return before, blocks


def carries(plan, place, own, others, levels, half, offsets, after):
    n_others, n_levels = len(others), len(levels)

    def kernel(place_ref, own_ref, *refs):
        before, _ = carried(
            plan, place_ref, own_ref, refs[:n_others], refs[n_others : n_others + n_levels], offsets
        )
        for states, ref in zip(before, refs[n_others + n_levels + len(after) :]):
            code(states, ref)

    return pl.pallas_call(
        kernel,
        out_shape=[coded_shape(plan.each)] * len(offsets),
        in_specs=[SMEM] + [VMEM] * (1 + n_others + n_levels) + [ANY] * len(after),
        out_specs=[VMEM] * len(offsets),
        compiler_params=params(),
        cost_estimate=cost(0, (plan.plane * 4 + n_levels) * plan.each * HD * HD * 2),
        name=f"carries_{half}",
    )(place, own, *others, *levels, *after)


def own_carries(plan, place, own, others, levels, offsets, after):
    n_others = len(others[0])
    operands = [(own[h], *others[h], *levels[h]) for h in range(plan.halves)]
    starts = [sum(map(len, operands[:h])) for h in range(plan.halves + 1)]

    def kernel(place_ref, *refs):
        outs = refs[starts[-1] + len(after) :]
        befores = [[] for _ in offsets]
        for half in range(plan.halves):
            own_ref, *of_half = refs[starts[half] : starts[half + 1]]
            before, blocks = carried(
                plan, place_ref, own_ref, of_half[:n_others], of_half[n_others:], offsets
            )
            for all_states, states in zip(befores, before):
                all_states.extend(states)
            for offset, (totals, ref) in enumerate(zip(blocks, outs[len(offsets) :])):
                block = place_ref[3] * plan.n_inner + (place_ref[1] ^ offset)
                seen = jnp.full((1, HD), (block + 1) * plan.block, jnp.int32).astype(jnp.float32)
                for i, total in enumerate(totals):
                    ref[half, i] = total.T * lax.rsqrt(seen)
        for states, ref in zip(befores, outs):
            code(states, ref)

    return pl.pallas_call(
        kernel,
        out_shape=[coded_shape(plan.halves * plan.each)] * len(offsets)
        + [states_shape(plan.halves, plan.each)] * plan.n_inner,
        in_specs=[SMEM] + [VMEM] * starts[-1] + [ANY] * len(after),
        out_specs=[VMEM] * (len(offsets) + plan.n_inner),
        compiler_params=params(),
        cost_estimate=cost(0, plan.plane * plan.each * HD * HD * 20),
        name="own_carries",
    )(place, *[a for arrays in operands for a in arrays], *after)


def attend_local(plan, place, query, key, value, half, offsets, after):
    rows = plan.rows

    def kernel(place_ref, q_ref, q_sib_ref, k_ref, k_sib_ref, v_ref, v_sib_ref, *refs):
        for piece, offset in enumerate(offsets):
            for i in range(plan.each):
                at = owned_columns(plan, place_ref, offset, half, i)
                out_at = slice(piece * plan.piece + i * HD, piece * plan.piece + (i + 1) * HD)
                refs[-1][0, :, out_at] = local_part(q_ref, k_ref, v_ref, at)
                refs[-1][1, :, out_at] = local_part(q_sib_ref, k_sib_ref, v_sib_ref, at)

    heads = len(offsets) * plan.each
    return pl.pallas_call(
        kernel,
        out_shape=jax.ShapeDtypeStruct((CORES, rows, heads * HD), jnp.float32),
        in_specs=[SMEM] + [VMEM] * 6 + [ANY] * len(after),
        out_specs=VMEM,
        compiler_params=params(),
        cost_estimate=cost(heads * 8 * rows * rows * HD, 16 * rows * heads * HD),
        name=f"attend_local_{half}_" + "_".join(map(str, offsets)),
    )(place, *query, *key, *value, *after)


def local_part(q_ref, k_ref, v_ref, at):
    rows = q_ref.shape[0]
    causal = lax.broadcasted_iota(jnp.int32, (rows, rows), 0) >= lax.broadcasted_iota(
        jnp.int32, (rows, rows), 1
    )
    scores = contract_columns(q_ref[:, at], k_ref[:, at]) * SCORE_SCALE
    weights = jnp.where(causal, scores, 0.0).astype(jnp.bfloat16)
    return jnp.dot(weights, v_ref[:, at], preferred_element_type=jnp.float32)


def finished(queries, local, carried, gain):
    carried = carried * SCORE_SCALE
    high = carried.astype(jnp.bfloat16)
    low = (carried - high.astype(jnp.float32)).astype(jnp.bfloat16)
    both = contract_columns(queries, jnp.concatenate([high, low], axis=0))
    raw = local + (both[:, :HD] + both[:, HD:])
    mean = jnp.mean(raw * raw, axis=-1, keepdims=True)
    return (raw * lax.rsqrt(mean + 1e-06) * gain).astype(jnp.bfloat16)


def attend(
    plan, place, query, key, value, carry, first, gain, half, offsets, after=(), local=None
):
    rows = plan.rows
    operands = [*query, local] if local is not None else [*query, *key, *value]
    n = len(operands)

    def kernel(place_ref, *refs):
        core = place_ref[0]
        first_ref, gain_ref, *carry_refs = refs[n : n + 2 + len(offsets)]
        out_ref = refs[-1]
        is_second = jnp.full((HD, HD), core, jnp.int32) == 1
        for piece, offset in enumerate(offsets):
            x = place_ref[1] ^ (offset // plan.n_y)
            carry_states = decoded(carry_refs[piece])
            skip = half * plan.each if len(carry_states) > plan.each else 0
            for i in range(plan.each):
                at = owned_columns(plan, place_ref, offset, half, i)
                start = ((half * plan.n_inner + x) * plan.each + i) * HD
                gain = gain_ref[:, pl.ds(pl.multiple_of(start, HD), HD)]
                out_at = slice(piece * plan.piece + i * HD, piece * plan.piece + (i + 1) * HD)
                carried = carry_states[skip + i]
                first = first_ref[offset, i]
                for side in range(CORES):
                    if local is None:
                        raw = local_part(refs[side], refs[2 + side], refs[4 + side], at)
                    else:
                        raw = refs[2][side, :, out_at]
                    behind = is_second if side == 0 else ~is_second
                    state = carried + jnp.where(behind, first, 0.0)
                    of = core if side == 0 else 1 - core
                    out_rows = pl.ds(pl.multiple_of(of * rows, rows), rows)
                    out_ref[out_rows, out_at] = finished(refs[side][:, at], raw, state, gain)

    heads = len(offsets) * plan.each
    return pl.pallas_call(
        kernel,
        out_shape=jax.ShapeDtypeStruct((CORES * rows, heads * HD), jnp.bfloat16),
        in_specs=[SMEM] + [VMEM] * (n + 2 + len(offsets)) + [ANY] * len(after),
        out_specs=VMEM,
        compiler_params=params(),
        cost_estimate=cost(
            heads * (8 * rows * rows * HD + 8 * rows * HD * HD), 16 * rows * heads * HD
        ),
        name=f"attend_{half}_" + "_".join(map(str, offsets)),
    )(place, *operands, first, gain, *carry, *after)


def assemble(plan, place, parts, into=None):
    rows = CORES * plan.rows
    copies = [(n, piece, half, o) for n, (_, half, os) in enumerate(parts) for piece, o in enumerate(os)]

    def kernel(place_ref, *refs):
        out_ref, sems = refs[-2:]
        started = []
        for at, (n, piece, half, offset) in enumerate(copies):
            x = place_ref[1] ^ (offset // plan.n_y)
            y = place_ref[2] ^ (offset % plan.n_y)
            column = (half * plan.n_inner + x) * plan.piece
            to_rows = pl.ds(pl.multiple_of(y * rows, rows), rows)
            to_columns = pl.ds(pl.multiple_of(column, plan.piece), plan.piece)
            started.append(
                pltpu.make_async_copy(
                    refs[n].at[:, pl.ds(piece * plan.piece, plan.piece)],
                    out_ref.at[to_rows, to_columns],
                    sems.at[at],
                )
            )
            started[-1].start()
        for copy in started:
            copy.wait()

    arrays = [array for array, _, _ in parts]
    aliased = [] if into is None else [into]
    return pl.pallas_call(
        kernel,
        out_shape=jax.ShapeDtypeStruct((plan.n_y * rows, plan.width), jnp.bfloat16),
        in_specs=[SMEM] + [VMEM] * len(arrays) + [HBM] * len(aliased),
        out_specs=HBM,
        scratch_shapes=[pltpu.SemaphoreType.DMA((len(copies),))],
        input_output_aliases={1 + len(arrays): 0} if aliased else {},
        compiler_params=params(),
        name="assemble" if into is None else "finish",
    )(place, *arrays, *aliased)


def assemble_cache(plan, place, parts):
    group = plan.n_inner * plan.each

    def kernel(place_ref, *refs):
        for half in range(plan.halves):
            for offset, ref in enumerate(refs[:-1]):
                start = half * group + (place_ref[1] ^ offset) * plan.each
                refs[-1][0, pl.ds(start, plan.each)] = ref[half]

    return pl.pallas_call(
        kernel,
        out_shape=states_shape(1, plan.halves * group),
        in_specs=[SMEM] + [VMEM] * len(parts),
        out_specs=VMEM,
        compiler_params=params(),
        name="assemble_cache",
    )(place, *parts)


def per_device(plan, queries, keys, values, spikes, gain):
    place = jnp.stack([lax.axis_index(a) for a in ("core", "inner", "y", "outer")]).astype(jnp.int32)
    halves = range(plan.halves)

    def swap(array, axes, offset, size):
        return lax.ppermute(array, axes, [(i, i ^ offset) for i in range(size)])

    def in_level(array, offset):
        return swap(array, ("inner", "y"), offset, plan.plane)

    def to_later(array, distance):
        pairs = [(i, i + distance) for i in range(plan.n_outer - distance)]
        return lax.ppermute(array, "outer", pairs)

    gain = gain.reshape(1, plan.width)
    gains = [gain] + [swap(gain, "y", o, plan.n_y) for o in range(1, plan.n_y)]
    key, key_out, value, value_out, *counts = decode(plan, place, spikes, keys, values)
    key, value = ((a, swap(b, "core", 1, CORES)) for a, b in ((key, key_out), (value, value_out)))
    query, query_out = spike_queries(plan, place, queries, counts)
    query = (query, swap(query_out, "core", 1, CORES))

    own, first, others = [], [], []

    def owner_stage(half, after):
        mine, parts, *sends = chunk_states(plan, place, key, value, half, after)
        own.append(mine)
        first.append(parts)
        others.append([in_level(a, o) for o, a in enumerate(sends, 1)])

    of_group = [list(range(y, plan.plane, plan.n_y)) for y in range(plan.n_y)]
    abroad = [o for offsets in of_group[1:] for o in offsets]

    def part_of(half, offsets, carry, after, local=None):
        return attend(
            plan,
            place,
            query,
            key,
            value,
            [carry[o] for o in offsets],
            first[half],
            gains[offsets[0] % plan.n_y],
            half,
            offsets,
            after,
            local,
        )

    def carry_stage(half, after):
        sends = carries(plan, place, own[half], others[half], levels[half], half, abroad, after)
        return sends[0], {o: in_level(a, o) for o, a in zip(abroad, sends)}

    parts = []

    def send_stage(half, carry, after, local):
        for y in range(1, plan.n_y):
            part = part_of(half, of_group[y], carry, after, local.get(y))
            parts.append((swap(part, "y", y, plan.n_y), half, of_group[y]))
            after = [part]
        return after

    after = [query[0]]
    for half in halves:
        owner_stage(half, after)
        after = [own[-1], query[1]]
    totals, sums = [], []
    for half in halves:
        total, coded = level_states(plan, own[half], others[half], half, after)
        totals.append(total)
        sums.append(coded)
        after = [coded]
    levels = [[] for _ in halves]
    distance = 1
    after = [*after, *gains[1:]]
    while distance < plan.n_outer:
        for half in halves:
            if distance > 1:
                sums[half] = levels_so_far(plan, totals[half], levels[half], half, after)
                after = [sums[half]]
            levels[half].append(to_later(sums[half], distance))
        distance *= 2
    local = {}
    for y in range(1, plan.n_y):
        local[y] = attend_local(plan, place, query, key, value, 0, of_group[y], after)
        after = [local[y]]
    carry = []
    for half in halves:
        done, of_half = carry_stage(half, after)
        carry.append(of_half)
        after = [done]
    for half in halves:
        after = send_stage(half, carry[half], after, {} if half else local)
    sends = own_carries(plan, place, own, others, levels, of_group[0], after)
    own_carry = {o: in_level(a, o) if o else a for o, a in zip(of_group[0], sends)}
    caches = [
        swap(a, "inner", o, plan.n_inner) if o else a
        for o, a in enumerate(sends[len(of_group[0]) :])
    ]
    early = []
    for half in halves:
        part = part_of(half, of_group[0], own_carry, after)
        early.append((part, half, of_group[0]))
        after = [part]
    out = assemble(plan, place, early + parts[:-1])
    out = assemble(plan, place, parts[-1:], out)
    return out, assemble_cache(plan, place, caches)


def solution(mesh):
    tokens = P(("outer", "inner", "y", "core"), None)
    seq, head = ("outer", "inner"), ("y", "core")

    def whole(queries, keys, values, spikes, gain):
        plan = Plan(mesh, spikes.shape[0] // mesh.size, spikes.shape[1])
        sizes = (plan.n_outer, plan.n_inner, plan.n_y, CORES)
        split = Mesh(mesh.devices.reshape(sizes), ("outer", "inner", "y", "core"))
        return jax.shard_map(
            functools.partial(per_device, plan),
            mesh=split,
            in_specs=(tokens, tokens, tokens, tokens, P(head)),
            out_specs=(P(seq, head), P(seq, head, None, None)),
            check_vma=False,
        )(queries, keys, values, spikes, gain)

    return whole
```

```python
import functools

import jax
import jax.numpy as jnp
from jax import lax
from jax.experimental import pallas as pl
from jax.experimental.pallas import tpu as pltpu
from jax.sharding import Mesh
from jax.sharding import PartitionSpec as P

HD = 128
SCORE_SCALE = HD ** (-0.5)
CORES = 2
VMEM_BYTES = 24 * 1024 * 1024
DECODE_VMEM_BYTES = 46 * 1024 * 1024
PAD = 16
TOP = 32767.0

VMEM = pl.BlockSpec(memory_space=pltpu.VMEM)
SMEM = pl.BlockSpec(memory_space=pltpu.SMEM)
HBM = pl.BlockSpec(memory_space=pltpu.HBM)
ANY = pl.BlockSpec(memory_space=pl.ANY)


def params(vmem=VMEM_BYTES):
    return pltpu.CompilerParams(vmem_limit_bytes=vmem)


def cost(flops, bytes_accessed):
    return pl.CostEstimate(flops=flops, bytes_accessed=bytes_accessed, transcendentals=0)


class Plan:
    def __init__(self, mesh, rows, model):
        n_seq, n_head = mesh.shape["seq"], mesh.shape["head"]
        self.n_y = n_head // CORES
        self.width = model // n_head
        group = self.width // HD
        self.n_inner = 2 if n_seq % 2 == 0 and group % 2 == 0 else 1
        self.n_outer = n_seq // self.n_inner
        self.halves = 2 if group // self.n_inner % 2 == 0 else 1
        self.each = group // (self.n_inner * self.halves)
        self.plane = self.n_inner * self.n_y
        self.rows = rows
        self.block = rows * n_head
        self.piece = self.each * HD


def counts_of(spikes):
    one, two = jnp.ones_like(spikes), jnp.full_like(spikes, 2)
    zero = jnp.zeros_like(spikes)

    def ternary(rest, unit):
        return jnp.where(rest >= 2 * unit, two, jnp.where(rest >= unit, one, zero))

    value = ternary(spikes, 9)
    rest = spikes - 9 * value
    key = ternary(rest, 3)
    return value, key, rest - 3 * key


def sides(plan, place_ref):
    for y in range(plan.n_y):
        for side in range(CORES):
            of = place_ref[0] if side == 0 else 1 - place_ref[0]
            start = pl.multiple_of((y * CORES + of) * plan.width, plan.width)
            yield side, slice(y * plan.width, (y + 1) * plan.width), pl.ds(start, plan.width)


def decode(plan, place, spikes, keys, values):
    rows, model = spikes.shape
    step = min(rows, 32)
    chunks = rows // step

    def kernel(place_ref, *refs):
        sources, outs, buffers, sems = refs[:3], refs[3:9], refs[9:12], refs[12]

        def fetch(chunk, index):
            at = pl.ds(chunk * step, step)
            return pltpu.make_async_copy(
                sources[index].at[at], buffers[index].at[at], sems.at[chunk, index]
            )

        for chunk in range(chunks):
            for index in range(3):
                fetch(chunk, index).start()

        @pl.loop(0, chunks)
        def _(chunk):
            for index in range(3):
                fetch(chunk, index).wait()
            at = pl.ds(pl.multiple_of(chunk * step, step), step)
            for side, mine, columns in sides(plan, place_ref):
                spikes = buffers[0][at, columns].astype(jnp.float32).astype(jnp.bfloat16)
                value, key, query = counts_of(spikes)
                outs[side][at, mine] = buffers[1][at, columns] * key
                outs[2 + side][at, mine] = buffers[2][at, columns] * value
                outs[4 + side][at, mine] = query

    return pl.pallas_call(
        kernel,
        out_shape=[jax.ShapeDtypeStruct((rows, plan.n_y * plan.width), jnp.bfloat16)] * 6,
        in_specs=[SMEM] + [HBM] * 3,
        out_specs=[VMEM] * 6,
        scratch_shapes=[
            pltpu.VMEM((rows, model), jnp.int32),
            pltpu.VMEM((rows, model), jnp.bfloat16),
            pltpu.VMEM((rows, model), jnp.bfloat16),
            pltpu.SemaphoreType.DMA((chunks, 3)),
        ],
        compiler_params=params(DECODE_VMEM_BYTES),
        cost_estimate=cost(rows * model * 4, rows * model * 14),
        name="decode",
    )(place, spikes, keys, values)


def spike_queries(plan, place, queries, counts):
    def kernel(place_ref, queries_ref, *refs):
        for side, mine, columns in sides(plan, place_ref):
            refs[2 + side][:, mine] = queries_ref[:, columns] * refs[side][:, mine]

    return pl.pallas_call(
        kernel,
        out_shape=[jax.ShapeDtypeStruct(a.shape, jnp.bfloat16) for a in counts],
        in_specs=[SMEM] + [VMEM] * 3,
        out_specs=[VMEM] * 2,
        compiler_params=params(),
        cost_estimate=cost(queries.size, queries.size * 6),
        name="spike_queries",
    )(place, queries, *counts)


def contract_rows(left, right):
    return lax.dot_general(
        left, right, (((0,), (0,)), ((), ())), preferred_element_type=jnp.float32
    )


def contract_columns(left, right):
    return lax.dot_general(
        left, right, (((1,), (1,)), ((), ())), preferred_element_type=jnp.float32
    )


def code(states, ref):
    line = lax.broadcasted_iota(jnp.int32, (PAD, HD), 0)
    exponents = jnp.zeros((PAD, HD), jnp.float32)
    for i, state in enumerate(states):
        top = jnp.max(jnp.abs(state), axis=0, keepdims=True)
        exponent = jnp.floor(jnp.log2(jnp.maximum(top, 1e-30))) + 1
        scaled = jnp.round(state * jnp.exp2(15 - exponent))
        scaled = jnp.clip(scaled, -TOP, TOP)
        ref[i * HD : (i + 1) * HD] = scaled.astype(jnp.int32).astype(jnp.int16)
        exponents = jnp.where(line == i, exponent, exponents)
    ref[len(states) * HD : len(states) * HD + PAD] = exponents.astype(jnp.int32).astype(jnp.int16)


def decoded(ref):
    count = ref.shape[0] // HD
    exponents = ref[count * HD : count * HD + PAD].astype(jnp.int32).astype(jnp.float32)
    return [
        ref[i * HD : (i + 1) * HD].astype(jnp.int32).astype(jnp.float32)
        * jnp.exp2(exponents[i : i + 1] - 15)
        for i in range(count)
    ]


def code_gain(gain_ref, ref):
    line = lax.broadcasted_iota(jnp.int32, (PAD // 2, HD), 0)
    gain = jnp.zeros((PAD // 2, HD), jnp.float32)
    for i in range(gain_ref.shape[1] // HD):
        gain = jnp.where(line == i, gain_ref[:, i * HD : (i + 1) * HD], gain)
    coarse = jnp.round(gain * 2.0**12)
    fine = jnp.round((gain - coarse * 2.0**-12) * 2.0**27)
    planes = jnp.concatenate([coarse, fine], axis=0)
    ref[ref.shape[0] - PAD :] = planes.astype(jnp.int32).astype(jnp.int16)


def decoded_gain(ref):
    planes = ref[ref.shape[0] - PAD :].astype(jnp.int32).astype(jnp.float32)
    return planes[: PAD // 2] * 2.0**-12 + planes[PAD // 2 :] * 2.0**-27


def plus(left, right):
    return [a + b for a, b in zip(left, right)]


def total_of(refs, each):
    total = [jnp.zeros((HD, HD), jnp.float32)] * each
    for ref in refs:
        coded = ref.dtype == jnp.int16
        total = plus(total, decoded(ref) if coded else [ref[i] for i in range(each)])
    return total


def coded_shape(heads, more=0):
    return jax.ShapeDtypeStruct((heads * HD + PAD + more, HD), jnp.int16)


def states_shape(*lead):
    return jax.ShapeDtypeStruct((*lead, HD, HD), jnp.float32)


def owned_columns(plan, place_ref, offset, half, i):
    x = place_ref[1] ^ (offset // plan.n_y)
    y = place_ref[2] ^ (offset % plan.n_y)
    start = (((y * plan.halves + half) * plan.n_inner + x) * plan.each + i) * HD
    return pl.ds(pl.multiple_of(start, HD), HD)


def chunk_states(plan, place, key, value, half, after, gain=None):
    gains = [] if gain is None else [gain]

    def kernel(place_ref, k_ref, k_sib_ref, v_ref, v_sib_ref, *refs):
        own_ref, first_ref, *send_refs = refs[len(gains) + len(after) :]
        is_first = jnp.full((HD, HD), place_ref[0], jnp.int32) == 0
        for offset in (*range(1, plan.plane), 0):
            states = []
            for i in range(plan.each):
                at = owned_columns(plan, place_ref, offset, half, i)
                mine = contract_rows(v_ref[:, at], k_ref[:, at])
                sib = contract_rows(v_sib_ref[:, at], k_sib_ref[:, at])
                first_ref[offset, i] = jnp.where(is_first, mine, sib)
                states.append(mine + sib)
            if offset:
                code(states, send_refs[offset - 1])
                if gains and offset < plan.n_y:
                    code_gain(refs[0], send_refs[offset - 1])
            else:
                for i, state in enumerate(states):
                    own_ref[i] = state

    heads = plan.plane * plan.each
    return pl.pallas_call(
        kernel,
        out_shape=[states_shape(plan.each), states_shape(plan.plane, plan.each)]
        + [
            coded_shape(plan.each, PAD if gains and o < plan.n_y else 0)
            for o in range(1, plan.plane)
        ],
        in_specs=[SMEM] + [VMEM] * (4 + len(gains)) + [ANY] * len(after),
        out_specs=[VMEM] * (1 + plan.plane),
        compiler_params=params(),
        cost_estimate=cost(
            4 * plan.rows * HD * HD * heads, 8 * plan.rows * HD * heads + 6 * heads * HD * HD
        ),
        name=f"chunk_states_{half}",
    )(place, *key, *value, *gains, *after)


def level_states(plan, own, others, half, after):
    def kernel(own_ref, *refs):
        total = total_of((own_ref, *refs[: len(others)]), plan.each)
        for i, state in enumerate(total):
            refs[-2][i] = state
        code(total, refs[-1])

    return pl.pallas_call(
        kernel,
        out_shape=[states_shape(plan.each), coded_shape(plan.each)],
        in_specs=[VMEM] * plan.plane + [ANY] * len(after),
        out_specs=[VMEM] * 2,
        compiler_params=params(),
        cost_estimate=cost(0, plan.plane * plan.each * HD * HD * 2),
        name=f"level_states_{half}",
    )(own, *others, *after)


def levels_so_far(plan, total, arrived, half, after):
    def kernel(total_ref, *refs):
        code(total_of((total_ref, *refs[: len(arrived)]), plan.each), refs[-1])

    return pl.pallas_call(
        kernel,
        out_shape=coded_shape(plan.each),
        in_specs=[VMEM] * (1 + len(arrived)) + [ANY] * len(after),
        out_specs=VMEM,
        compiler_params=params(),
        cost_estimate=cost(0, 2 * plan.each * HD * HD * 2),
        name=f"levels_so_far_{half}_{len(arrived)}",
    )(total, *arrived, *after)


def carried(plan, place_ref, own, others, levels, offsets):
    x, y = place_ref[1], place_ref[2]
    here = x * plan.n_y + y
    earlier = total_of(levels, plan.each)
    states = [[own[i] for i in range(plan.each)]] + [decoded(ref) for ref in others]

    def add(totals, keep_of):
        for offset, terms in enumerate(states):
            keep = jnp.full((HD, HD), keep_of(here ^ offset), jnp.int32) == 1
            totals = plus(totals, [jnp.where(keep, s, 0.0) for s in terms])
        return totals

    before = [add(earlier, lambda chip: (chip < here ^ o).astype(jnp.int32)) for o in offsets]
    blocks = [
        add(earlier, lambda chip: (chip // plan.n_y <= x ^ o).astype(jnp.int32))
        for o in range(plan.n_inner)
    ]
    return before, blocks


def carries(plan, place, own, others, levels, half, offsets, after):
    n_others, n_levels = len(others), len(levels)

    def kernel(place_ref, own_ref, *refs):
        before, _ = carried(
            plan, place_ref, own_ref, refs[:n_others], refs[n_others : n_others + n_levels], offsets
        )
        for states, ref in zip(before, refs[n_others + n_levels + len(after) :]):
            code(states, ref)

    return pl.pallas_call(
        kernel,
        out_shape=[coded_shape(plan.each)] * len(offsets),
        in_specs=[SMEM] + [VMEM] * (1 + n_others + n_levels) + [ANY] * len(after),
        out_specs=[VMEM] * len(offsets),
        compiler_params=params(),
        cost_estimate=cost(0, (plan.plane * 4 + n_levels) * plan.each * HD * HD * 2),
        name=f"carries_{half}",
    )(place, own, *others, *levels, *after)


def own_carries(plan, place, own, others, levels, offsets, after):
    n_others = len(others[0])
    operands = [(own[h], *others[h], *levels[h]) for h in range(plan.halves)]
    starts = [sum(map(len, operands[:h])) for h in range(plan.halves + 1)]

    def kernel(place_ref, *refs):
        outs = refs[starts[-1] + len(after) :]
        befores = [[] for _ in offsets]
        for half in range(plan.halves):
            own_ref, *of_half = refs[starts[half] : starts[half + 1]]
            before, blocks = carried(
                plan, place_ref, own_ref, of_half[:n_others], of_half[n_others:], offsets
            )
            for all_states, states in zip(befores, before):
                all_states.extend(states)
            for offset, (totals, ref) in enumerate(zip(blocks, outs[len(offsets) :])):
                block = place_ref[3] * plan.n_inner + (place_ref[1] ^ offset)
                seen = jnp.full((1, HD), (block + 1) * plan.block, jnp.int32).astype(jnp.float32)
                for i, total in enumerate(totals):
                    ref[half, i] = total.T * lax.rsqrt(seen)
        for states, ref in zip(befores, outs):
            code(states, ref)

    return pl.pallas_call(
        kernel,
        out_shape=[coded_shape(plan.halves * plan.each)] * len(offsets)
        + [states_shape(plan.halves, plan.each)] * plan.n_inner,
        in_specs=[SMEM] + [VMEM] * starts[-1] + [ANY] * len(after),
        out_specs=[VMEM] * (len(offsets) + plan.n_inner),
        compiler_params=params(),
        cost_estimate=cost(0, plan.plane * plan.each * HD * HD * 20),
        name="own_carries",
    )(place, *[a for arrays in operands for a in arrays], *after)


def attend_local(plan, place, query, key, value, half, offsets, after):
    rows = plan.rows

    def kernel(place_ref, q_ref, q_sib_ref, k_ref, k_sib_ref, v_ref, v_sib_ref, *refs):
        for piece, offset in enumerate(offsets):
            for i in range(plan.each):
                at = owned_columns(plan, place_ref, offset, half, i)
                out_at = slice(piece * plan.piece + i * HD, piece * plan.piece + (i + 1) * HD)
                refs[-1][0, :, out_at] = local_part(q_ref, k_ref, v_ref, at)
                refs[-1][1, :, out_at] = local_part(q_sib_ref, k_sib_ref, v_sib_ref, at)

    heads = len(offsets) * plan.each
    return pl.pallas_call(
        kernel,
        out_shape=jax.ShapeDtypeStruct((CORES, rows, heads * HD), jnp.float32),
        in_specs=[SMEM] + [VMEM] * 6 + [ANY] * len(after),
        out_specs=VMEM,
        compiler_params=params(),
        cost_estimate=cost(heads * 8 * rows * rows * HD, 16 * rows * heads * HD),
        name=f"attend_local_{half}_" + "_".join(map(str, offsets)),
    )(place, *query, *key, *value, *after)


def local_part(q_ref, k_ref, v_ref, at):
    rows = q_ref.shape[0]
    causal = lax.broadcasted_iota(jnp.int32, (rows, rows), 0) >= lax.broadcasted_iota(
        jnp.int32, (rows, rows), 1
    )
    scores = contract_columns(q_ref[:, at], k_ref[:, at]) * SCORE_SCALE
    weights = jnp.where(causal, scores, 0.0).astype(jnp.bfloat16)
    return jnp.dot(weights, v_ref[:, at], preferred_element_type=jnp.float32)


def finished(queries, local, carried, gain):
    carried = carried * SCORE_SCALE
    high = carried.astype(jnp.bfloat16)
    low = (carried - high.astype(jnp.float32)).astype(jnp.bfloat16)
    both = contract_columns(queries, jnp.concatenate([high, low], axis=0))
    raw = local + (both[:, :HD] + both[:, HD:])
    mean = jnp.mean(raw * raw, axis=-1, keepdims=True)
    return (raw * lax.rsqrt(mean + 1e-06) * gain).astype(jnp.bfloat16)


def attend(
    plan, place, query, key, value, carry, first, gain, half, offsets, after=(), local=None
):
    rows = plan.rows
    operands = [*query, local] if local is not None else [*query, *key, *value]
    n = len(operands)

    def kernel(place_ref, *refs):
        core = place_ref[0]
        first_ref, gain_ref, *carry_refs = refs[n : n + 2 + len(offsets)]
        out_ref = refs[-1]
        is_second = jnp.full((HD, HD), core, jnp.int32) == 1
        coded_gain = gain_ref.dtype == jnp.int16
        line = lax.broadcasted_iota(jnp.int32, (PAD // 2, HD), 0)
        for piece, offset in enumerate(offsets):
            x = place_ref[1] ^ (offset // plan.n_y)
            carry_states = decoded(carry_refs[piece])
            skip = half * plan.each if len(carry_states) > plan.each else 0
            for i in range(plan.each):
                at = owned_columns(plan, place_ref, offset, half, i)
                head = (half * plan.n_inner + x) * plan.each + i
                if coded_gain:
                    gain = jnp.where(line == head, decoded_gain(gain_ref), 0.0)
                    gain = jnp.sum(gain, axis=0, keepdims=True)
                else:
                    gain = gain_ref[:, pl.ds(pl.multiple_of(head * HD, HD), HD)]
                out_at = slice(piece * plan.piece + i * HD, piece * plan.piece + (i + 1) * HD)
                carried = carry_states[skip + i]
                first = first_ref[offset, i]
                for side in range(CORES):
                    if local is None:
                        raw = local_part(refs[side], refs[2 + side], refs[4 + side], at)
                    else:
                        raw = refs[2][side, :, out_at]
                    behind = is_second if side == 0 else ~is_second
                    state = carried + jnp.where(behind, first, 0.0)
                    of = core if side == 0 else 1 - core
                    out_rows = pl.ds(pl.multiple_of(of * rows, rows), rows)
                    out_ref[out_rows, out_at] = finished(refs[side][:, at], raw, state, gain)

    heads = len(offsets) * plan.each
    return pl.pallas_call(
        kernel,
        out_shape=jax.ShapeDtypeStruct((CORES * rows, heads * HD), jnp.bfloat16),
        in_specs=[SMEM] + [VMEM] * (n + 2 + len(offsets)) + [ANY] * len(after),
        out_specs=VMEM,
        compiler_params=params(),
        cost_estimate=cost(
            heads * (8 * rows * rows * HD + 8 * rows * HD * HD), 16 * rows * heads * HD
        ),
        name=f"attend_{half}_" + "_".join(map(str, offsets)),
    )(place, *operands, first, gain, *carry, *after)


def assemble(plan, place, parts, into=None):
    rows = CORES * plan.rows
    copies = [(n, piece, half, o) for n, (_, half, os) in enumerate(parts) for piece, o in enumerate(os)]

    def kernel(place_ref, *refs):
        out_ref, sems = refs[-2:]
        started = []
        for at, (n, piece, half, offset) in enumerate(copies):
            x = place_ref[1] ^ (offset // plan.n_y)
            y = place_ref[2] ^ (offset % plan.n_y)
            column = (half * plan.n_inner + x) * plan.piece
            to_rows = pl.ds(pl.multiple_of(y * rows, rows), rows)
            to_columns = pl.ds(pl.multiple_of(column, plan.piece), plan.piece)
            started.append(
                pltpu.make_async_copy(
                    refs[n].at[:, pl.ds(piece * plan.piece, plan.piece)],
                    out_ref.at[to_rows, to_columns],
                    sems.at[at],
                )
            )
            started[-1].start()
        for copy in started:
            copy.wait()

    arrays = [array for array, _, _ in parts]
    aliased = [] if into is None else [into]
    return pl.pallas_call(
        kernel,
        out_shape=jax.ShapeDtypeStruct((plan.n_y * rows, plan.width), jnp.bfloat16),
        in_specs=[SMEM] + [VMEM] * len(arrays) + [HBM] * len(aliased),
        out_specs=HBM,
        scratch_shapes=[pltpu.SemaphoreType.DMA((len(copies),))],
        input_output_aliases={1 + len(arrays): 0} if aliased else {},
        compiler_params=params(),
        name="assemble" if into is None else "finish",
    )(place, *arrays, *aliased)


def assemble_cache(plan, place, parts):
    group = plan.n_inner * plan.each

    def kernel(place_ref, *refs):
        for half in range(plan.halves):
            for offset, ref in enumerate(refs[:-1]):
                start = half * group + (place_ref[1] ^ offset) * plan.each
                refs[-1][0, pl.ds(start, plan.each)] = ref[half]

    return pl.pallas_call(
        kernel,
        out_shape=states_shape(1, plan.halves * group),
        in_specs=[SMEM] + [VMEM] * len(parts),
        out_specs=VMEM,
        compiler_params=params(),
        name="assemble_cache",
    )(place, *parts)


def per_device(plan, queries, keys, values, spikes, gain):
    place = jnp.stack([lax.axis_index(a) for a in ("core", "inner", "y", "outer")]).astype(jnp.int32)
    halves = range(plan.halves)

    def swap(array, axes, offset, size):
        return lax.ppermute(array, axes, [(i, i ^ offset) for i in range(size)])

    def in_level(array, offset):
        return swap(array, ("inner", "y"), offset, plan.plane)

    def to_later(array, distance):
        pairs = [(i, i + distance) for i in range(plan.n_outer - distance)]
        return lax.ppermute(array, "outer", pairs)

    gain = gain.reshape(1, plan.width)
    key, key_out, value, value_out, *counts = decode(plan, place, spikes, keys, values)
    key, value = ((a, swap(b, "core", 1, CORES)) for a, b in ((key, key_out), (value, value_out)))
    query, query_out = spike_queries(plan, place, queries, counts)
    query = (query, swap(query_out, "core", 1, CORES))

    own, first, others = [], [], []

    def owner_stage(half, after):
        with_gain = gain if half == 0 else None
        mine, parts, *sends = chunk_states(plan, place, key, value, half, after, with_gain)
        own.append(mine)
        first.append(parts)
        others.append([in_level(a, o) for o, a in enumerate(sends, 1)])

    of_group = [list(range(y, plan.plane, plan.n_y)) for y in range(plan.n_y)]
    abroad = [o for offsets in of_group[1:] for o in offsets]

    def part_of(half, offsets, carry, after, local=None):
        return attend(
            plan,
            place,
            query,
            key,
            value,
            [carry[o] for o in offsets],
            first[half],
            others[0][offsets[0] % plan.n_y - 1] if offsets[0] % plan.n_y else gain,
            half,
            offsets,
            after,
            local,
        )

    def carry_stage(half, after):
        sends = carries(plan, place, own[half], others[half], levels[half], half, abroad, after)
        return sends[0], {o: in_level(a, o) for o, a in zip(abroad, sends)}

    parts = []

    def send_stage(half, carry, after, local):
        for y in range(1, plan.n_y):
            part = part_of(half, of_group[y], carry, after, local.get(y))
            parts.append((swap(part, "y", y, plan.n_y), half, of_group[y]))
            after = [part]
        return after

    after = [query[0]]
    for half in halves:
        owner_stage(half, after)
        after = [own[-1], query[1]]
    totals, sums = [], []
    for half in halves:
        total, coded = level_states(plan, own[half], others[half], half, after)
        totals.append(total)
        sums.append(coded)
        after = [coded]
    levels = [[] for _ in halves]
    distance = 1
    while distance < plan.n_outer:
        for half in halves:
            if distance > 1:
                sums[half] = levels_so_far(plan, totals[half], levels[half], half, after)
                after = [sums[half]]
            levels[half].append(to_later(sums[half], distance))
        distance *= 2
    local = {}
    for y in range(1, plan.n_y):
        local[y] = attend_local(plan, place, query, key, value, 0, of_group[y], after)
        after = [local[y]]
    carry = []
    for half in halves:
        done, of_half = carry_stage(half, after)
        carry.append(of_half)
        after = [done]
    for half in halves:
        after = send_stage(half, carry[half], after, {} if half else local)
    sends = own_carries(plan, place, own, others, levels, of_group[0], after)
    own_carry = {o: in_level(a, o) if o else a for o, a in zip(of_group[0], sends)}
    caches = [
        swap(a, "inner", o, plan.n_inner) if o else a
        for o, a in enumerate(sends[len(of_group[0]) :])
    ]
    early = []
    for half in halves:
        part = part_of(half, of_group[0], own_carry, after)
        early.append((part, half, of_group[0]))
        after = [part]
    out = assemble(plan, place, early + parts[:-1])
    out = assemble(plan, place, parts[-1:], out)
    return out, assemble_cache(plan, place, caches)


def solution(mesh):
    tokens = P(("outer", "inner", "y", "core"), None)
    seq, head = ("outer", "inner"), ("y", "core")

    def whole(queries, keys, values, spikes, gain):
        plan = Plan(mesh, spikes.shape[0] // mesh.size, spikes.shape[1])
        sizes = (plan.n_outer, plan.n_inner, plan.n_y, CORES)
        split = Mesh(mesh.devices.reshape(sizes), ("outer", "inner", "y", "core"))
        return jax.shard_map(
            functools.partial(per_device, plan),
            mesh=split,
            in_specs=(tokens, tokens, tokens, tokens, P(head)),
            out_specs=(P(seq, head), P(seq, head, None, None)),
            check_vma=False,
        )(queries, keys, values, spikes, gain)

    return whole
```

```python
import functools

import jax
import jax.numpy as jnp
from jax import lax
from jax.experimental import pallas as pl
from jax.experimental.pallas import tpu as pltpu
from jax.sharding import Mesh
from jax.sharding import PartitionSpec as P

HD = 128
SCORE_SCALE = HD ** (-0.5)
CORES = 2
VMEM_BYTES = 24 * 1024 * 1024
DECODE_VMEM_BYTES = 46 * 1024 * 1024
PAD = 16
TOP = 32767.0

VMEM = pl.BlockSpec(memory_space=pltpu.VMEM)
SMEM = pl.BlockSpec(memory_space=pltpu.SMEM)
HBM = pl.BlockSpec(memory_space=pltpu.HBM)
ANY = pl.BlockSpec(memory_space=pl.ANY)


def params(vmem=VMEM_BYTES):
    return pltpu.CompilerParams(vmem_limit_bytes=vmem)


def cost(flops, bytes_accessed):
    return pl.CostEstimate(flops=flops, bytes_accessed=bytes_accessed, transcendentals=0)


class Plan:
    def __init__(self, mesh, rows, model):
        n_seq, n_head = mesh.shape["seq"], mesh.shape["head"]
        self.n_y = n_head // CORES
        self.width = model // n_head
        group = self.width // HD
        self.n_inner = 2 if n_seq % 2 == 0 and group % 2 == 0 else 1
        self.n_outer = n_seq // self.n_inner
        self.halves = 2 if group // self.n_inner % 2 == 0 else 1
        self.each = group // (self.n_inner * self.halves)
        self.plane = self.n_inner * self.n_y
        self.rows = rows
        self.block = rows * n_head
        self.piece = self.each * HD


def counts_of(spikes):
    one, two = jnp.ones_like(spikes), jnp.full_like(spikes, 2)
    zero = jnp.zeros_like(spikes)

    def ternary(rest, unit):
        return jnp.where(rest >= 2 * unit, two, jnp.where(rest >= unit, one, zero))

    value = ternary(spikes, 9)
    rest = spikes - 9 * value
    key = ternary(rest, 3)
    return value, key, rest - 3 * key


def sides(plan, place_ref):
    for y in range(plan.n_y):
        for side in range(CORES):
            of = place_ref[0] if side == 0 else 1 - place_ref[0]
            start = pl.multiple_of((y * CORES + of) * plan.width, plan.width)
            yield side, slice(y * plan.width, (y + 1) * plan.width), pl.ds(start, plan.width)


def decode(plan, place, spikes, keys, values):
    rows, model = spikes.shape
    step = min(rows, 32)
    chunks = rows // step

    def kernel(place_ref, *refs):
        sources, outs, buffers, sems = refs[:3], refs[3:9], refs[9:12], refs[12]

        def fetch(chunk, index):
            at = pl.ds(chunk * step, step)
            return pltpu.make_async_copy(
                sources[index].at[at], buffers[index].at[at], sems.at[chunk, index]
            )

        for chunk in range(chunks):
            for index in range(3):
                fetch(chunk, index).start()

        @pl.loop(0, chunks)
        def _(chunk):
            for index in range(3):
                fetch(chunk, index).wait()
            at = pl.ds(pl.multiple_of(chunk * step, step), step)
            for side, mine, columns in sides(plan, place_ref):
                spikes = buffers[0][at, columns].astype(jnp.float32).astype(jnp.bfloat16)
                value, key, query = counts_of(spikes)
                outs[side][at, mine] = buffers[1][at, columns] * key
                outs[2 + side][at, mine] = buffers[2][at, columns] * value
                outs[4 + side][at, mine] = query

    return pl.pallas_call(
        kernel,
        out_shape=[jax.ShapeDtypeStruct((rows, plan.n_y * plan.width), jnp.bfloat16)] * 6,
        in_specs=[SMEM] + [HBM] * 3,
        out_specs=[VMEM] * 6,
        scratch_shapes=[
            pltpu.VMEM((rows, model), jnp.int32),
            pltpu.VMEM((rows, model), jnp.bfloat16),
            pltpu.VMEM((rows, model), jnp.bfloat16),
            pltpu.SemaphoreType.DMA((chunks, 3)),
        ],
        compiler_params=params(DECODE_VMEM_BYTES),
        cost_estimate=cost(rows * model * 4, rows * model * 14),
        name="decode",
    )(place, spikes, keys, values)


def spike_queries(plan, place, queries, counts):
    def kernel(place_ref, queries_ref, *refs):
        for side, mine, columns in sides(plan, place_ref):
            refs[2 + side][:, mine] = queries_ref[:, columns] * refs[side][:, mine]

    return pl.pallas_call(
        kernel,
        out_shape=[jax.ShapeDtypeStruct(a.shape, jnp.bfloat16) for a in counts],
        in_specs=[SMEM] + [VMEM] * 3,
        out_specs=[VMEM] * 2,
        compiler_params=params(),
        cost_estimate=cost(queries.size, queries.size * 6),
        name="spike_queries",
    )(place, queries, *counts)


def contract_rows(left, right):
    return lax.dot_general(
        left, right, (((0,), (0,)), ((), ())), preferred_element_type=jnp.float32
    )


def contract_columns(left, right):
    return lax.dot_general(
        left, right, (((1,), (1,)), ((), ())), preferred_element_type=jnp.float32
    )


def code(states, ref):
    line = lax.broadcasted_iota(jnp.int32, (PAD, HD), 0)
    exponents = jnp.zeros((PAD, HD), jnp.float32)
    for i, state in enumerate(states):
        top = jnp.max(jnp.abs(state), axis=0, keepdims=True)
        exponent = jnp.floor(jnp.log2(jnp.maximum(top, 1e-30))) + 1
        scaled = jnp.round(state * jnp.exp2(15 - exponent))
        scaled = jnp.clip(scaled, -TOP, TOP)
        ref[i * HD : (i + 1) * HD] = scaled.astype(jnp.int32).astype(jnp.int16)
        exponents = jnp.where(line == i, exponent, exponents)
    ref[len(states) * HD : len(states) * HD + PAD] = exponents.astype(jnp.int32).astype(jnp.int16)


def decoded(ref):
    count = ref.shape[0] // HD
    exponents = ref[count * HD : count * HD + PAD].astype(jnp.int32).astype(jnp.float32)
    return [
        ref[i * HD : (i + 1) * HD].astype(jnp.int32).astype(jnp.float32)
        * jnp.exp2(exponents[i : i + 1] - 15)
        for i in range(count)
    ]


def code_gain(gain_ref, ref):
    line = lax.broadcasted_iota(jnp.int32, (PAD // 2, HD), 0)
    gain = jnp.zeros((PAD // 2, HD), jnp.float32)
    for i in range(gain_ref.shape[1] // HD):
        gain = jnp.where(line == i, gain_ref[:, i * HD : (i + 1) * HD], gain)
    coarse = jnp.round(gain * 2.0**12)
    fine = jnp.round((gain - coarse * 2.0**-12) * 2.0**27)
    planes = jnp.concatenate([coarse, fine], axis=0)
    ref[ref.shape[0] - PAD :] = planes.astype(jnp.int32).astype(jnp.int16)


def decoded_gain(ref):
    planes = ref[ref.shape[0] - PAD :].astype(jnp.int32).astype(jnp.float32)
    return planes[: PAD // 2] * 2.0**-12 + planes[PAD // 2 :] * 2.0**-27


def plus(left, right):
    return [a + b for a, b in zip(left, right)]


def total_of(refs, each):
    total = [jnp.zeros((HD, HD), jnp.float32)] * each
    for ref in refs:
        coded = ref.dtype == jnp.int16
        total = plus(total, decoded(ref) if coded else [ref[i] for i in range(each)])
    return total


def coded_shape(heads, more=0):
    return jax.ShapeDtypeStruct((heads * HD + PAD + more, HD), jnp.int16)


def states_shape(*lead):
    return jax.ShapeDtypeStruct((*lead, HD, HD), jnp.float32)


def owned_columns(plan, place_ref, offset, half, i):
    x = place_ref[1] ^ (offset // plan.n_y)
    y = place_ref[2] ^ (offset % plan.n_y)
    start = (((y * plan.halves + half) * plan.n_inner + x) * plan.each + i) * HD
    return pl.ds(pl.multiple_of(start, HD), HD)


def core_states(plan, place, key, value, after):
    def kernel(place_ref, k_ref, v_ref, *refs):
        for half in range(plan.halves):
            for offset in range(plan.plane):
                for i in range(plan.each):
                    at = owned_columns(plan, place_ref, offset, half, i)
                    refs[-1][half, offset, i] = contract_rows(v_ref[:, at], k_ref[:, at])

    heads = plan.halves * plan.plane * plan.each
    return pl.pallas_call(
        kernel,
        out_shape=states_shape(plan.halves, plan.plane, plan.each),
        in_specs=[SMEM] + [VMEM] * 2 + [ANY] * len(after),
        out_specs=VMEM,
        compiler_params=params(),
        cost_estimate=cost(2 * plan.rows * HD * HD * heads, 4 * heads * HD * (plan.rows + HD)),
        name="core_states",
    )(place, key, value, *after)


def chunk_states(plan, place, mine, key_sib, value_sib, half, after, gain=None):
    gains = [] if gain is None else [gain]

    def kernel(place_ref, mine_ref, k_sib_ref, v_sib_ref, *refs):
        own_ref, first_ref, *send_refs = refs[len(gains) + len(after) :]
        is_first = jnp.full((HD, HD), place_ref[0], jnp.int32) == 0
        for offset in (*range(1, plan.plane), 0):
            states = []
            for i in range(plan.each):
                at = owned_columns(plan, place_ref, offset, half, i)
                mine = mine_ref[half, offset, i]
                sib = contract_rows(v_sib_ref[:, at], k_sib_ref[:, at])
                first_ref[offset, i] = jnp.where(is_first, mine, sib)
                states.append(mine + sib)
            if offset:
                code(states, send_refs[offset - 1])
                if gains and offset < plan.n_y:
                    code_gain(refs[0], send_refs[offset - 1])
            else:
                for i, state in enumerate(states):
                    own_ref[i] = state

    heads = plan.plane * plan.each
    return pl.pallas_call(
        kernel,
        out_shape=[states_shape(plan.each), states_shape(plan.plane, plan.each)]
        + [
            coded_shape(plan.each, PAD if gains and o < plan.n_y else 0)
            for o in range(1, plan.plane)
        ],
        in_specs=[SMEM] + [VMEM] * (3 + len(gains)) + [ANY] * len(after),
        out_specs=[VMEM] * (1 + plan.plane),
        compiler_params=params(),
        cost_estimate=cost(
            2 * plan.rows * HD * HD * heads, 4 * plan.rows * HD * heads + 10 * heads * HD * HD
        ),
        name=f"chunk_states_{half}",
    )(place, mine, key_sib, value_sib, *gains, *after)


def level_states(plan, own, others, half, after):
    def kernel(own_ref, *refs):
        code(total_of((own_ref, *refs[: len(others)]), plan.each), refs[-1])

    return pl.pallas_call(
        kernel,
        out_shape=coded_shape(plan.each),
        in_specs=[VMEM] * plan.plane + [ANY] * len(after),
        out_specs=VMEM,
        compiler_params=params(),
        cost_estimate=cost(0, plan.plane * plan.each * HD * HD * 2),
        name=f"level_states_{half}",
    )(own, *others, *after)


def carried(plan, place_ref, own, others, levels, offsets):
    x, y = place_ref[1], place_ref[2]
    here = x * plan.n_y + y
    earlier = total_of(levels, plan.each)
    states = [[own[i] for i in range(plan.each)]] + [decoded(ref) for ref in others]

    def add(totals, keep_of):
        for offset, terms in enumerate(states):
            keep = jnp.full((HD, HD), keep_of(here ^ offset), jnp.int32) == 1
            totals = plus(totals, [jnp.where(keep, s, 0.0) for s in terms])
        return totals

    before = [add(earlier, lambda chip: (chip < here ^ o).astype(jnp.int32)) for o in offsets]
    blocks = [
        add(earlier, lambda chip: (chip // plan.n_y <= x ^ o).astype(jnp.int32))
        for o in range(plan.n_inner)
    ]
    return before, blocks


def carries(plan, place, own, others, levels, half, offsets, after):
    n_others, n_levels = len(others), len(levels)

    def kernel(place_ref, own_ref, *refs):
        before, _ = carried(
            plan, place_ref, own_ref, refs[:n_others], refs[n_others : n_others + n_levels], offsets
        )
        for states, ref in zip(before, refs[n_others + n_levels + len(after) :]):
            code(states, ref)

    return pl.pallas_call(
        kernel,
        out_shape=[coded_shape(plan.each)] * len(offsets),
        in_specs=[SMEM] + [VMEM] * (1 + n_others + n_levels) + [ANY] * len(after),
        out_specs=[VMEM] * len(offsets),
        compiler_params=params(),
        cost_estimate=cost(0, (plan.plane * 4 + n_levels) * plan.each * HD * HD * 2),
        name=f"carries_{half}",
    )(place, own, *others, *levels, *after)


def own_carries(plan, place, own, others, levels, offsets, after):
    n_others = len(others[0])
    operands = [(own[h], *others[h], *levels[h]) for h in range(plan.halves)]
    starts = [sum(map(len, operands[:h])) for h in range(plan.halves + 1)]

    def kernel(place_ref, *refs):
        outs = refs[starts[-1] + len(after) :]
        befores = [[] for _ in offsets]
        for half in range(plan.halves):
            own_ref, *of_half = refs[starts[half] : starts[half + 1]]
            before, blocks = carried(
                plan, place_ref, own_ref, of_half[:n_others], of_half[n_others:], offsets
            )
            for all_states, states in zip(befores, before):
                all_states.extend(states)
            for offset, (totals, ref) in enumerate(zip(blocks, outs[len(offsets) :])):
                block = place_ref[3] * plan.n_inner + (place_ref[1] ^ offset)
                seen = jnp.full((1, HD), (block + 1) * plan.block, jnp.int32).astype(jnp.float32)
                for i, total in enumerate(totals):
                    ref[half, i] = total.T * lax.rsqrt(seen)
        for states, ref in zip(befores, outs):
            code(states, ref)

    return pl.pallas_call(
        kernel,
        out_shape=[coded_shape(plan.halves * plan.each)] * len(offsets)
        + [states_shape(plan.halves, plan.each)] * plan.n_inner,
        in_specs=[SMEM] + [VMEM] * starts[-1] + [ANY] * len(after),
        out_specs=[VMEM] * (len(offsets) + plan.n_inner),
        compiler_params=params(),
        cost_estimate=cost(0, plan.plane * plan.each * HD * HD * 20),
        name="own_carries",
    )(place, *[a for arrays in operands for a in arrays], *after)


def attend_local(plan, place, query, key, value, half, offsets, after):
    rows = plan.rows

    def kernel(place_ref, q_ref, q_sib_ref, k_ref, k_sib_ref, v_ref, v_sib_ref, *refs):
        for piece, offset in enumerate(offsets):
            for i in range(plan.each):
                at = owned_columns(plan, place_ref, offset, half, i)
                out_at = slice(piece * plan.piece + i * HD, piece * plan.piece + (i + 1) * HD)
                refs[-1][0, :, out_at] = local_part(q_ref, k_ref, v_ref, at)
                refs[-1][1, :, out_at] = local_part(q_sib_ref, k_sib_ref, v_sib_ref, at)

    heads = len(offsets) * plan.each
    return pl.pallas_call(
        kernel,
        out_shape=jax.ShapeDtypeStruct((CORES, rows, heads * HD), jnp.float32),
        in_specs=[SMEM] + [VMEM] * 6 + [ANY] * len(after),
        out_specs=VMEM,
        compiler_params=params(),
        cost_estimate=cost(heads * 8 * rows * rows * HD, 16 * rows * heads * HD),
        name=f"attend_local_{half}_" + "_".join(map(str, offsets)),
    )(place, *query, *key, *value, *after)


def local_part(q_ref, k_ref, v_ref, at):
    rows = q_ref.shape[0]
    causal = lax.broadcasted_iota(jnp.int32, (rows, rows), 0) >= lax.broadcasted_iota(
        jnp.int32, (rows, rows), 1
    )
    scores = contract_columns(q_ref[:, at], k_ref[:, at]) * SCORE_SCALE
    weights = jnp.where(causal, scores, 0.0).astype(jnp.bfloat16)
    return jnp.dot(weights, v_ref[:, at], preferred_element_type=jnp.float32)


def finished(queries, local, carried, gain):
    carried = carried * SCORE_SCALE
    high = carried.astype(jnp.bfloat16)
    low = (carried - high.astype(jnp.float32)).astype(jnp.bfloat16)
    both = contract_columns(queries, jnp.concatenate([high, low], axis=0))
    raw = local + (both[:, :HD] + both[:, HD:])
    mean = jnp.mean(raw * raw, axis=-1, keepdims=True)
    return (raw * lax.rsqrt(mean + 1e-06) * gain).astype(jnp.bfloat16)


def attend(
    plan, place, query, key, value, carry, first, gain, half, offsets, after=(), local=None
):
    rows = plan.rows
    operands = [*query, local] if local is not None else [*query, *key, *value]
    n = len(operands)

    def kernel(place_ref, *refs):
        core = place_ref[0]
        first_ref, gain_ref, *carry_refs = refs[n : n + 2 + len(offsets)]
        out_ref = refs[-1]
        is_second = jnp.full((HD, HD), core, jnp.int32) == 1
        coded_gain = gain_ref.dtype == jnp.int16
        line = lax.broadcasted_iota(jnp.int32, (PAD // 2, HD), 0)
        for piece, offset in enumerate(offsets):
            x = place_ref[1] ^ (offset // plan.n_y)
            carry_states = decoded(carry_refs[piece])
            skip = half * plan.each if len(carry_states) > plan.each else 0
            for i in range(plan.each):
                at = owned_columns(plan, place_ref, offset, half, i)
                head = (half * plan.n_inner + x) * plan.each + i
                if coded_gain:
                    gain = jnp.where(line == head, decoded_gain(gain_ref), 0.0)
                    gain = jnp.sum(gain, axis=0, keepdims=True)
                else:
                    gain = gain_ref[:, pl.ds(pl.multiple_of(head * HD, HD), HD)]
                out_at = slice(piece * plan.piece + i * HD, piece * plan.piece + (i + 1) * HD)
                carried = carry_states[skip + i]
                first = first_ref[offset, i]
                for side in range(CORES):
                    if local is None:
                        raw = local_part(refs[side], refs[2 + side], refs[4 + side], at)
                    else:
                        raw = refs[2][side, :, out_at]
                    behind = is_second if side == 0 else ~is_second
                    state = carried + jnp.where(behind, first, 0.0)
                    of = core if side == 0 else 1 - core
                    out_rows = pl.ds(pl.multiple_of(of * rows, rows), rows)
                    out_ref[out_rows, out_at] = finished(refs[side][:, at], raw, state, gain)

    heads = len(offsets) * plan.each
    return pl.pallas_call(
        kernel,
        out_shape=jax.ShapeDtypeStruct((CORES * rows, heads * HD), jnp.bfloat16),
        in_specs=[SMEM] + [VMEM] * (n + 2 + len(offsets)) + [ANY] * len(after),
        out_specs=VMEM,
        compiler_params=params(),
        cost_estimate=cost(
            heads * (8 * rows * rows * HD + 8 * rows * HD * HD), 16 * rows * heads * HD
        ),
        name=f"attend_{half}_" + "_".join(map(str, offsets)),
    )(place, *operands, first, gain, *carry, *after)


def assemble(plan, place, parts, into=None):
    rows = CORES * plan.rows
    copies = [(n, piece, half, o) for n, (_, half, os) in enumerate(parts) for piece, o in enumerate(os)]

    def kernel(place_ref, *refs):
        out_ref, sems = refs[-2:]
        started = []
        for at, (n, piece, half, offset) in enumerate(copies):
            x = place_ref[1] ^ (offset // plan.n_y)
            y = place_ref[2] ^ (offset % plan.n_y)
            column = (half * plan.n_inner + x) * plan.piece
            to_rows = pl.ds(pl.multiple_of(y * rows, rows), rows)
            to_columns = pl.ds(pl.multiple_of(column, plan.piece), plan.piece)
            started.append(
                pltpu.make_async_copy(
                    refs[n].at[:, pl.ds(piece * plan.piece, plan.piece)],
                    out_ref.at[to_rows, to_columns],
                    sems.at[at],
                )
            )
            started[-1].start()
        for copy in started:
            copy.wait()

    arrays = [array for array, _, _ in parts]
    aliased = [] if into is None else [into]
    return pl.pallas_call(
        kernel,
        out_shape=jax.ShapeDtypeStruct((plan.n_y * rows, plan.width), jnp.bfloat16),
        in_specs=[SMEM] + [VMEM] * len(arrays) + [HBM] * len(aliased),
        out_specs=HBM,
        scratch_shapes=[pltpu.SemaphoreType.DMA((len(copies),))],
        input_output_aliases={1 + len(arrays): 0} if aliased else {},
        compiler_params=params(),
        name="assemble" if into is None else "finish",
    )(place, *arrays, *aliased)


def assemble_cache(plan, place, parts):
    group = plan.n_inner * plan.each

    def kernel(place_ref, *refs):
        for half in range(plan.halves):
            for offset, ref in enumerate(refs[:-1]):
                start = half * group + (place_ref[1] ^ offset) * plan.each
                refs[-1][0, pl.ds(start, plan.each)] = ref[half]

    return pl.pallas_call(
        kernel,
        out_shape=states_shape(1, plan.halves * group),
        in_specs=[SMEM] + [VMEM] * len(parts),
        out_specs=VMEM,
        compiler_params=params(),
        name="assemble_cache",
    )(place, *parts)


def per_device(plan, queries, keys, values, spikes, gain):
    place = jnp.stack([lax.axis_index(a) for a in ("core", "inner", "y", "outer")]).astype(jnp.int32)
    halves = range(plan.halves)

    def swap(array, axes, offset, size):
        return lax.ppermute(array, axes, [(i, i ^ offset) for i in range(size)])

    def in_level(array, offset):
        return swap(array, ("inner", "y"), offset, plan.plane)

    def to_later(array, distance):
        pairs = [(i, i + distance) for i in range(plan.n_outer - distance)]
        return lax.ppermute(array, "outer", pairs)

    gain = gain.reshape(1, plan.width)
    key, key_out, value, value_out, *counts = decode(plan, place, spikes, keys, values)
    key, value = ((a, swap(b, "core", 1, CORES)) for a, b in ((key, key_out), (value, value_out)))
    query, query_out = spike_queries(plan, place, queries, counts)
    query = (query, swap(query_out, "core", 1, CORES))

    of_core = core_states(plan, place, key[0], value[0], [query[0]])
    own, first, others = [], [], []

    def owner_stage(half, after):
        with_gain = gain if half == 0 else None
        mine, parts, *sends = chunk_states(plan, place, of_core, key[1], value[1], half, after, with_gain)
        own.append(mine)
        first.append(parts)
        others.append([in_level(a, o) for o, a in enumerate(sends, 1)])

    of_group = [list(range(y, plan.plane, plan.n_y)) for y in range(plan.n_y)]
    abroad = [o for offsets in of_group[1:] for o in offsets]

    def part_of(half, offsets, carry, after, local=None):
        return attend(
            plan,
            place,
            query,
            key,
            value,
            [carry[o] for o in offsets],
            first[half],
            others[0][offsets[0] % plan.n_y - 1] if offsets[0] % plan.n_y else gain,
            half,
            offsets,
            after,
            local,
        )

    def carry_stage(half, after):
        sends = carries(plan, place, own[half], others[half], levels[half], half, abroad, after)
        return sends[0], {o: in_level(a, o) for o, a in zip(abroad, sends)}

    parts = []

    def send_stage(half, carry, after, local):
        for y in range(1, plan.n_y):
            part = part_of(half, of_group[y], carry, after, local.get(y))
            parts.append((swap(part, "y", y, plan.n_y), half, of_group[y]))
            after = [part]
        return after

    after = []
    for half in halves:
        owner_stage(half, after)
        after = [own[-1], query[1]]
    levels = []
    for half in halves:
        level = level_states(plan, own[half], others[half], half, after)
        levels.append([to_later(level, d) for d in range(plan.n_outer - 1, 0, -1)])
        after = [level]
    local = {}
    for y in range(1, plan.n_y):
        local[y] = attend_local(plan, place, query, key, value, 0, of_group[y], after)
        after = [local[y]]
    carry = []
    for half in halves:
        done, of_half = carry_stage(half, after)
        carry.append(of_half)
        after = [done]
    for half in halves:
        after = send_stage(half, carry[half], after, {} if half else local)
    sends = own_carries(plan, place, own, others, levels, of_group[0], after)
    own_carry = {o: in_level(a, o) if o else a for o, a in zip(of_group[0], sends)}
    caches = [
        swap(a, "inner", o, plan.n_inner) if o else a
        for o, a in enumerate(sends[len(of_group[0]) :])
    ]
    early = []
    for half in halves:
        part = part_of(half, of_group[0], own_carry, after)
        early.append((part, half, of_group[0]))
        after = [part]
    out = assemble(plan, place, early + parts[:-1])
    out = assemble(plan, place, parts[-1:], out)
    return out, assemble_cache(plan, place, caches)


def solution(mesh):
    tokens = P(("outer", "inner", "y", "core"), None)
    seq, head = ("outer", "inner"), ("y", "core")

    def whole(queries, keys, values, spikes, gain):
        plan = Plan(mesh, spikes.shape[0] // mesh.size, spikes.shape[1])
        sizes = (plan.n_outer, plan.n_inner, plan.n_y, CORES)
        split = Mesh(mesh.devices.reshape(sizes), ("outer", "inner", "y", "core"))
        return jax.shard_map(
            functools.partial(per_device, plan),
            mesh=split,
            in_specs=(tokens, tokens, tokens, tokens, P(head)),
            out_specs=(P(seq, head), P(seq, head, None, None)),
            check_vma=False,
        )(queries, keys, values, spikes, gain)

    return whole
```

```python
import functools

import jax
import jax.numpy as jnp
from jax import lax
from jax.experimental import pallas as pl
from jax.experimental.pallas import tpu as pltpu
from jax.sharding import Mesh
from jax.sharding import PartitionSpec as P

HD = 128
SCORE_SCALE = HD ** (-0.5)
CORES = 2
VMEM_BYTES = 24 * 1024 * 1024
DECODE_VMEM_BYTES = 46 * 1024 * 1024
PAD = 16
TOP = 32767.0

VMEM = pl.BlockSpec(memory_space=pltpu.VMEM)
SMEM = pl.BlockSpec(memory_space=pltpu.SMEM)
HBM = pl.BlockSpec(memory_space=pltpu.HBM)
ANY = pl.BlockSpec(memory_space=pl.ANY)


def params(vmem=VMEM_BYTES):
    return pltpu.CompilerParams(vmem_limit_bytes=vmem)


def cost(flops, bytes_accessed):
    return pl.CostEstimate(flops=flops, bytes_accessed=bytes_accessed, transcendentals=0)


class Plan:
    def __init__(self, mesh, rows, model):
        n_seq, n_head = mesh.shape["seq"], mesh.shape["head"]
        self.n_y = n_head // CORES
        self.width = model // n_head
        group = self.width // HD
        self.n_inner = 2 if n_seq % 2 == 0 and group % 2 == 0 else 1
        self.n_outer = n_seq // self.n_inner
        self.halves = 2 if group // self.n_inner % 2 == 0 else 1
        self.each = group // (self.n_inner * self.halves)
        self.plane = self.n_inner * self.n_y
        self.rows = rows
        self.block = rows * n_head
        self.piece = self.each * HD


def counts_of(spikes):
    one, two = jnp.ones_like(spikes), jnp.full_like(spikes, 2)
    zero = jnp.zeros_like(spikes)

    def ternary(rest, unit):
        return jnp.where(rest >= 2 * unit, two, jnp.where(rest >= unit, one, zero))

    value = ternary(spikes, 9)
    rest = spikes - 9 * value
    key = ternary(rest, 3)
    return value, key, rest - 3 * key


def sides(plan, place_ref):
    for y in range(plan.n_y):
        for side in range(CORES):
            of = place_ref[0] if side == 0 else 1 - place_ref[0]
            start = pl.multiple_of((y * CORES + of) * plan.width, plan.width)
            yield side, slice(y * plan.width, (y + 1) * plan.width), pl.ds(start, plan.width)


def decode(plan, place, spikes, keys, values):
    rows, model = spikes.shape
    step = min(rows, 32)
    chunks = rows // step

    def kernel(place_ref, *refs):
        sources, outs, buffers, sems = refs[:3], refs[3:9], refs[9:12], refs[12]

        def fetch(chunk, index):
            at = pl.ds(chunk * step, step)
            return pltpu.make_async_copy(
                sources[index].at[at], buffers[index].at[at], sems.at[chunk, index]
            )

        for chunk in range(chunks):
            for index in range(3):
                fetch(chunk, index).start()

        @pl.loop(0, chunks)
        def _(chunk):
            for index in range(3):
                fetch(chunk, index).wait()
            at = pl.ds(pl.multiple_of(chunk * step, step), step)
            for side, mine, columns in sides(plan, place_ref):
                spikes = buffers[0][at, columns].astype(jnp.float32).astype(jnp.bfloat16)
                value, key, query = counts_of(spikes)
                outs[side][at, mine] = buffers[1][at, columns] * key
                outs[2 + side][at, mine] = buffers[2][at, columns] * value
                outs[4 + side][at, mine] = query

    return pl.pallas_call(
        kernel,
        out_shape=[jax.ShapeDtypeStruct((rows, plan.n_y * plan.width), jnp.bfloat16)] * 6,
        in_specs=[SMEM] + [HBM] * 3,
        out_specs=[VMEM] * 6,
        scratch_shapes=[
            pltpu.VMEM((rows, model), jnp.int32),
            pltpu.VMEM((rows, model), jnp.bfloat16),
            pltpu.VMEM((rows, model), jnp.bfloat16),
            pltpu.SemaphoreType.DMA((chunks, 3)),
        ],
        compiler_params=params(DECODE_VMEM_BYTES),
        cost_estimate=cost(rows * model * 4, rows * model * 14),
        name="decode",
    )(place, spikes, keys, values)


def spike_queries(plan, place, queries, counts):
    def kernel(place_ref, queries_ref, *refs):
        for side, mine, columns in sides(plan, place_ref):
            refs[2 + side][:, mine] = queries_ref[:, columns] * refs[side][:, mine]

    return pl.pallas_call(
        kernel,
        out_shape=[jax.ShapeDtypeStruct(a.shape, jnp.bfloat16) for a in counts],
        in_specs=[SMEM] + [VMEM] * 3,
        out_specs=[VMEM] * 2,
        compiler_params=params(),
        cost_estimate=cost(queries.size, queries.size * 6),
        name="spike_queries",
    )(place, queries, *counts)


def contract_rows(left, right):
    return lax.dot_general(
        left, right, (((0,), (0,)), ((), ())), preferred_element_type=jnp.float32
    )


def contract_columns(left, right):
    return lax.dot_general(
        left, right, (((1,), (1,)), ((), ())), preferred_element_type=jnp.float32
    )


def code(states, ref):
    line = lax.broadcasted_iota(jnp.int32, (PAD, HD), 0)
    exponents = jnp.zeros((PAD, HD), jnp.float32)
    for i, state in enumerate(states):
        top = jnp.max(jnp.abs(state), axis=0, keepdims=True)
        exponent = jnp.floor(jnp.log2(jnp.maximum(top, 1e-30))) + 1
        scaled = jnp.round(state * jnp.exp2(15 - exponent))
        scaled = jnp.clip(scaled, -TOP, TOP)
        ref[i * HD : (i + 1) * HD] = scaled.astype(jnp.int32).astype(jnp.int16)
        exponents = jnp.where(line == i, exponent, exponents)
    ref[len(states) * HD : len(states) * HD + PAD] = exponents.astype(jnp.int32).astype(jnp.int16)


def decoded(ref):
    count = ref.shape[0] // HD
    exponents = ref[count * HD : count * HD + PAD].astype(jnp.int32).astype(jnp.float32)
    return [
        ref[i * HD : (i + 1) * HD].astype(jnp.int32).astype(jnp.float32)
        * jnp.exp2(exponents[i : i + 1] - 15)
        for i in range(count)
    ]


def code_gain(gain_ref, ref):
    line = lax.broadcasted_iota(jnp.int32, (PAD // 2, HD), 0)
    gain = jnp.zeros((PAD // 2, HD), jnp.float32)
    for i in range(gain_ref.shape[1] // HD):
        gain = jnp.where(line == i, gain_ref[:, i * HD : (i + 1) * HD], gain)
    coarse = jnp.round(gain * 2.0**12)
    fine = jnp.round((gain - coarse * 2.0**-12) * 2.0**27)
    planes = jnp.concatenate([coarse, fine], axis=0)
    ref[ref.shape[0] - PAD :] = planes.astype(jnp.int32).astype(jnp.int16)


def decoded_gain(ref):
    planes = ref[ref.shape[0] - PAD :].astype(jnp.int32).astype(jnp.float32)
    return planes[: PAD // 2] * 2.0**-12 + planes[PAD // 2 :] * 2.0**-27


def plus(left, right):
    return [a + b for a, b in zip(left, right)]


def total_of(refs, each):
    total = [jnp.zeros((HD, HD), jnp.float32)] * each
    for ref in refs:
        coded = ref.dtype == jnp.int16
        total = plus(total, decoded(ref) if coded else [ref[i] for i in range(each)])
    return total


def coded_shape(heads, more=0):
    return jax.ShapeDtypeStruct((heads * HD + PAD + more, HD), jnp.int16)


def states_shape(*lead):
    return jax.ShapeDtypeStruct((*lead, HD, HD), jnp.float32)


def owned_columns(plan, place_ref, offset, half, i):
    x = place_ref[1] ^ (offset // plan.n_y)
    y = place_ref[2] ^ (offset % plan.n_y)
    start = (((y * plan.halves + half) * plan.n_inner + x) * plan.each + i) * HD
    return pl.ds(pl.multiple_of(start, HD), HD)


def core_states(plan, place, key, value, after):
    def kernel(place_ref, k_ref, v_ref, *refs):
        for half in range(plan.halves):
            for offset in range(plan.plane):
                for i in range(plan.each):
                    at = owned_columns(plan, place_ref, offset, half, i)
                    refs[-1][half, offset, i] = contract_rows(v_ref[:, at], k_ref[:, at])

    heads = plan.halves * plan.plane * plan.each
    return pl.pallas_call(
        kernel,
        out_shape=states_shape(plan.halves, plan.plane, plan.each),
        in_specs=[SMEM] + [VMEM] * 2 + [ANY] * len(after),
        out_specs=VMEM,
        compiler_params=params(),
        cost_estimate=cost(2 * plan.rows * HD * HD * heads, 4 * heads * HD * (plan.rows + HD)),
        name="core_states",
    )(place, key, value, *after)


def chunk_states(plan, place, mine, key_sib, value_sib, half, after, gain=None):
    gains = [] if gain is None else [gain]

    def kernel(place_ref, mine_ref, k_sib_ref, v_sib_ref, *refs):
        own_ref, first_ref, *send_refs = refs[len(gains) + len(after) :]
        is_first = jnp.full((HD, HD), place_ref[0], jnp.int32) == 0
        for offset in (*range(1, plan.plane), 0):
            states = []
            for i in range(plan.each):
                at = owned_columns(plan, place_ref, offset, half, i)
                mine = mine_ref[half, offset, i]
                sib = contract_rows(v_sib_ref[:, at], k_sib_ref[:, at])
                first_ref[offset, i] = jnp.where(is_first, mine, sib)
                states.append(mine + sib)
            if offset:
                code(states, send_refs[offset - 1])
                if gains and offset < plan.n_y:
                    code_gain(refs[0], send_refs[offset - 1])
            else:
                for i, state in enumerate(states):
                    own_ref[i] = state

    heads = plan.plane * plan.each
    return pl.pallas_call(
        kernel,
        out_shape=[states_shape(plan.each), states_shape(plan.plane, plan.each)]
        + [
            coded_shape(plan.each, PAD if gains and o < plan.n_y else 0)
            for o in range(1, plan.plane)
        ],
        in_specs=[SMEM] + [VMEM] * (3 + len(gains)) + [ANY] * len(after),
        out_specs=[VMEM] * (1 + plan.plane),
        compiler_params=params(),
        cost_estimate=cost(
            2 * plan.rows * HD * HD * heads, 4 * plan.rows * HD * heads + 10 * heads * HD * HD
        ),
        name=f"chunk_states_{half}",
    )(place, mine, key_sib, value_sib, *gains, *after)


def level_states(plan, own, others, half, after):
    def kernel(own_ref, *refs):
        code(total_of((own_ref, *refs[: len(others)]), plan.each), refs[-1])

    return pl.pallas_call(
        kernel,
        out_shape=coded_shape(plan.each),
        in_specs=[VMEM] * plan.plane + [ANY] * len(after),
        out_specs=VMEM,
        compiler_params=params(),
        cost_estimate=cost(0, plan.plane * plan.each * HD * HD * 2),
        name=f"level_states_{half}",
    )(own, *others, *after)


def carried(plan, place_ref, own, others, levels, offsets):
    x, y = place_ref[1], place_ref[2]
    here = x * plan.n_y + y
    earlier = total_of(levels, plan.each)
    states = [[own[i] for i in range(plan.each)]] + [decoded(ref) for ref in others]

    def add(totals, keep_of):
        for offset, terms in enumerate(states):
            keep = jnp.full((HD, HD), keep_of(here ^ offset), jnp.int32) == 1
            totals = plus(totals, [jnp.where(keep, s, 0.0) for s in terms])
        return totals

    before = [add(earlier, lambda chip: (chip < here ^ o).astype(jnp.int32)) for o in offsets]
    blocks = [
        add(earlier, lambda chip: (chip // plan.n_y <= x ^ o).astype(jnp.int32))
        for o in range(plan.n_inner)
    ]
    return before, blocks


def carries(plan, place, own, others, levels, half, offsets, after):
    n_others, n_levels = len(others), len(levels)

    def kernel(place_ref, own_ref, *refs):
        before, _ = carried(
            plan, place_ref, own_ref, refs[:n_others], refs[n_others : n_others + n_levels], offsets
        )
        for states, ref in zip(before, refs[n_others + n_levels + len(after) :]):
            code(states, ref)

    return pl.pallas_call(
        kernel,
        out_shape=[coded_shape(plan.each)] * len(offsets),
        in_specs=[SMEM] + [VMEM] * (1 + n_others + n_levels) + [ANY] * len(after),
        out_specs=[VMEM] * len(offsets),
        compiler_params=params(),
        cost_estimate=cost(0, (plan.plane * 4 + n_levels) * plan.each * HD * HD * 2),
        name=f"carries_{half}",
    )(place, own, *others, *levels, *after)


def own_carries(plan, place, own, others, levels, offsets, after):
    n_others = len(others[0])
    operands = [(own[h], *others[h], *levels[h]) for h in range(plan.halves)]
    starts = [sum(map(len, operands[:h])) for h in range(plan.halves + 1)]

    def kernel(place_ref, *refs):
        outs = refs[starts[-1] + len(after) :]
        befores = [[] for _ in offsets]
        for half in range(plan.halves):
            own_ref, *of_half = refs[starts[half] : starts[half + 1]]
            before, blocks = carried(
                plan, place_ref, own_ref, of_half[:n_others], of_half[n_others:], offsets
            )
            for all_states, states in zip(befores, before):
                all_states.extend(states)
            for offset, (totals, ref) in enumerate(zip(blocks, outs[len(offsets) :])):
                block = place_ref[3] * plan.n_inner + (place_ref[1] ^ offset)
                seen = jnp.full((1, HD), (block + 1) * plan.block, jnp.int32).astype(jnp.float32)
                for i, total in enumerate(totals):
                    ref[half, i] = total.T * lax.rsqrt(seen)
        for states, ref in zip(befores, outs):
            code(states, ref)

    return pl.pallas_call(
        kernel,
        out_shape=[coded_shape(plan.halves * plan.each)] * len(offsets)
        + [states_shape(plan.halves, plan.each)] * plan.n_inner,
        in_specs=[SMEM] + [VMEM] * starts[-1] + [ANY] * len(after),
        out_specs=[VMEM] * (len(offsets) + plan.n_inner),
        compiler_params=params(),
        cost_estimate=cost(0, plan.plane * plan.each * HD * HD * 20),
        name="own_carries",
    )(place, *[a for arrays in operands for a in arrays], *after)


def attend_local(plan, place, query, key, value, half, offsets, after):
    rows = plan.rows

    def kernel(place_ref, q_ref, q_sib_ref, k_ref, k_sib_ref, v_ref, v_sib_ref, *refs):
        for piece, offset in enumerate(offsets):
            for i in range(plan.each):
                at = owned_columns(plan, place_ref, offset, half, i)
                out_at = slice(piece * plan.piece + i * HD, piece * plan.piece + (i + 1) * HD)
                refs[-1][0, :, out_at] = local_part(q_ref, k_ref, v_ref, at)
                refs[-1][1, :, out_at] = local_part(q_sib_ref, k_sib_ref, v_sib_ref, at)

    heads = len(offsets) * plan.each
    return pl.pallas_call(
        kernel,
        out_shape=jax.ShapeDtypeStruct((CORES, rows, heads * HD), jnp.float32),
        in_specs=[SMEM] + [VMEM] * 6 + [ANY] * len(after),
        out_specs=VMEM,
        compiler_params=params(),
        cost_estimate=cost(heads * 8 * rows * rows * HD, 16 * rows * heads * HD),
        name=f"attend_local_{half}_" + "_".join(map(str, offsets)),
    )(place, *query, *key, *value, *after)


def local_part(q_ref, k_ref, v_ref, at):
    rows = q_ref.shape[0]
    causal = lax.broadcasted_iota(jnp.int32, (rows, rows), 0) >= lax.broadcasted_iota(
        jnp.int32, (rows, rows), 1
    )
    scores = contract_columns(q_ref[:, at], k_ref[:, at]) * SCORE_SCALE
    weights = jnp.where(causal, scores, 0.0).astype(jnp.bfloat16)
    return jnp.dot(weights, v_ref[:, at], preferred_element_type=jnp.float32)


def finished(queries, local, carried, gain):
    carried = carried * SCORE_SCALE
    high = carried.astype(jnp.bfloat16)
    low = (carried - high.astype(jnp.float32)).astype(jnp.bfloat16)
    both = contract_columns(queries, jnp.concatenate([high, low], axis=0))
    raw = local + (both[:, :HD] + both[:, HD:])
    mean = jnp.mean(raw * raw, axis=-1, keepdims=True)
    return (raw * lax.rsqrt(mean + 1e-06) * gain).astype(jnp.bfloat16)


def attend(
    plan, place, query, key, value, carry, first, gain, half, offsets, after=(), local=None
):
    rows = plan.rows
    operands = [*query, local] if local is not None else [*query, *key, *value]
    n = len(operands)

    def kernel(place_ref, *refs):
        core = place_ref[0]
        first_ref, gain_ref, *carry_refs = refs[n : n + 2 + len(offsets)]
        out_ref = refs[-1]
        is_second = jnp.full((HD, HD), core, jnp.int32) == 1
        coded_gain = gain_ref.dtype == jnp.int16
        line = lax.broadcasted_iota(jnp.int32, (PAD // 2, HD), 0)
        for piece, offset in enumerate(offsets):
            x = place_ref[1] ^ (offset // plan.n_y)
            carry_states = decoded(carry_refs[piece])
            skip = half * plan.each if len(carry_states) > plan.each else 0
            for i in range(plan.each):
                at = owned_columns(plan, place_ref, offset, half, i)
                head = (half * plan.n_inner + x) * plan.each + i
                if coded_gain:
                    gain = jnp.where(line == head, decoded_gain(gain_ref), 0.0)
                    gain = jnp.sum(gain, axis=0, keepdims=True)
                else:
                    gain = gain_ref[:, pl.ds(pl.multiple_of(head * HD, HD), HD)]
                out_at = slice(piece * plan.piece + i * HD, piece * plan.piece + (i + 1) * HD)
                carried = carry_states[skip + i]
                first = first_ref[offset, i]
                for side in range(CORES):
                    if local is None:
                        raw = local_part(refs[side], refs[2 + side], refs[4 + side], at)
                    else:
                        raw = refs[2][side, :, out_at]
                    behind = is_second if side == 0 else ~is_second
                    state = carried + jnp.where(behind, first, 0.0)
                    of = core if side == 0 else 1 - core
                    out_rows = pl.ds(pl.multiple_of(of * rows, rows), rows)
                    out_ref[out_rows, out_at] = finished(refs[side][:, at], raw, state, gain)

    heads = len(offsets) * plan.each
    return pl.pallas_call(
        kernel,
        out_shape=jax.ShapeDtypeStruct((CORES * rows, heads * HD), jnp.bfloat16),
        in_specs=[SMEM] + [VMEM] * (n + 2 + len(offsets)) + [ANY] * len(after),
        out_specs=VMEM,
        compiler_params=params(),
        cost_estimate=cost(
            heads * (8 * rows * rows * HD + 8 * rows * HD * HD), 16 * rows * heads * HD
        ),
        name=f"attend_{half}_" + "_".join(map(str, offsets)),
    )(place, *operands, first, gain, *carry, *after)


def assemble(plan, place, parts, into=None):
    rows = CORES * plan.rows
    copies = [(n, piece, half, o) for n, (_, half, os) in enumerate(parts) for piece, o in enumerate(os)]

    def kernel(place_ref, *refs):
        out_ref, sems = refs[-2:]
        started = []
        for at, (n, piece, half, offset) in enumerate(copies):
            x = place_ref[1] ^ (offset // plan.n_y)
            y = place_ref[2] ^ (offset % plan.n_y)
            column = (half * plan.n_inner + x) * plan.piece
            to_rows = pl.ds(pl.multiple_of(y * rows, rows), rows)
            to_columns = pl.ds(pl.multiple_of(column, plan.piece), plan.piece)
            started.append(
                pltpu.make_async_copy(
                    refs[n].at[:, pl.ds(piece * plan.piece, plan.piece)],
                    out_ref.at[to_rows, to_columns],
                    sems.at[at],
                )
            )
            started[-1].start()
        for copy in started:
            copy.wait()

    arrays = [array for array, _, _ in parts]
    aliased = [] if into is None else [into]
    return pl.pallas_call(
        kernel,
        out_shape=jax.ShapeDtypeStruct((plan.n_y * rows, plan.width), jnp.bfloat16),
        in_specs=[SMEM] + [VMEM] * len(arrays) + [HBM] * len(aliased),
        out_specs=HBM,
        scratch_shapes=[pltpu.SemaphoreType.DMA((len(copies),))],
        input_output_aliases={1 + len(arrays): 0} if aliased else {},
        compiler_params=params(),
        name="assemble" if into is None else "finish",
    )(place, *arrays, *aliased)


def assemble_cache(plan, place, parts):
    group = plan.n_inner * plan.each

    def kernel(place_ref, *refs):
        for half in range(plan.halves):
            for offset, ref in enumerate(refs[:-1]):
                start = half * group + (place_ref[1] ^ offset) * plan.each
                refs[-1][0, pl.ds(start, plan.each)] = ref[half]

    return pl.pallas_call(
        kernel,
        out_shape=states_shape(1, plan.halves * group),
        in_specs=[SMEM] + [VMEM] * len(parts),
        out_specs=VMEM,
        compiler_params=params(),
        name="assemble_cache",
    )(place, *parts)


def per_device(plan, queries, keys, values, spikes, gain):
    place = jnp.stack([lax.axis_index(a) for a in ("core", "inner", "y", "outer")]).astype(jnp.int32)
    halves = range(plan.halves)

    def swap(array, axes, offset, size):
        return lax.ppermute(array, axes, [(i, i ^ offset) for i in range(size)])

    def in_level(array, offset):
        return swap(array, ("inner", "y"), offset, plan.plane)

    def to_later(array, distance):
        pairs = [(i, i + distance) for i in range(plan.n_outer - distance)]
        return lax.ppermute(array, "outer", pairs)

    gain = gain.reshape(1, plan.width)
    key, key_out, value, value_out, *counts = decode(plan, place, spikes, keys, values)
    key, value = ((a, swap(b, "core", 1, CORES)) for a, b in ((key, key_out), (value, value_out)))
    query, query_out = spike_queries(plan, place, queries, counts)
    query = (query, swap(query_out, "core", 1, CORES))

    of_core = core_states(plan, place, key[0], value[0], [query[0]])
    own, first, others = [], [], []

    def owner_stage(half, after):
        with_gain = gain if half == 0 else None
        mine, parts, *sends = chunk_states(plan, place, of_core, key[1], value[1], half, after, with_gain)
        own.append(mine)
        first.append(parts)
        others.append([in_level(a, o) for o, a in enumerate(sends, 1)])

    of_group = [list(range(y, plan.plane, plan.n_y)) for y in range(plan.n_y)]
    abroad = [o for offsets in of_group[1:] for o in offsets]

    def part_of(half, offsets, carry, after, local=None):
        return attend(
            plan,
            place,
            query,
            key,
            value,
            [carry[o] for o in offsets],
            first[half],
            others[0][offsets[0] % plan.n_y - 1] if offsets[0] % plan.n_y else gain,
            half,
            offsets,
            after,
            local,
        )

    def carry_stage(half, after):
        sends = carries(plan, place, own[half], others[half], levels[half], half, abroad, after)
        return sends[0], {o: in_level(a, o) for o, a in zip(abroad, sends)}

    parts = []

    def send_stage(half, carry, after, local):
        for y in range(1, plan.n_y):
            part = part_of(half, of_group[y], carry, after, local.get(y))
            parts.append((swap(part, "y", y, plan.n_y), half, of_group[y]))
            after = [part]
        return after

    after = []
    for half in halves:
        owner_stage(half, after)
        after = [own[-1], query[1]]
    levels = []
    for half in halves:
        level = level_states(plan, own[half], others[half][::-1], half, after)
        levels.append([to_later(level, d) for d in range(1, plan.n_outer)])
        after = [level]
    local = {}
    for y in range(1, plan.n_y):
        local[y] = attend_local(plan, place, query, key, value, 0, of_group[y], after)
        after = [local[y]]
    carry = []
    for half in halves:
        done, of_half = carry_stage(half, after)
        carry.append(of_half)
        after = [done]
    for half in halves:
        after = send_stage(half, carry[half], after, {} if half else local)
    sends = own_carries(plan, place, own, others, levels, of_group[0], after)
    own_carry = {o: in_level(a, o) if o else a for o, a in zip(of_group[0], sends)}
    caches = [
        swap(a, "inner", o, plan.n_inner) if o else a
        for o, a in enumerate(sends[len(of_group[0]) :])
    ]
    early = []
    for half in halves:
        part = part_of(half, of_group[0], own_carry, after)
        early.append((part, half, of_group[0]))
        after = [part]
    out = assemble(plan, place, early + parts[:-1])
    out = assemble(plan, place, parts[-1:], out)
    return out, assemble_cache(plan, place, caches)


def solution(mesh):
    tokens = P(("outer", "inner", "y", "core"), None)
    seq, head = ("outer", "inner"), ("y", "core")

    def whole(queries, keys, values, spikes, gain):
        plan = Plan(mesh, spikes.shape[0] // mesh.size, spikes.shape[1])
        sizes = (plan.n_outer, plan.n_inner, plan.n_y, CORES)
        split = Mesh(mesh.devices.reshape(sizes), ("outer", "inner", "y", "core"))
        return jax.shard_map(
            functools.partial(per_device, plan),
            mesh=split,
            in_specs=(tokens, tokens, tokens, tokens, P(head)),
            out_specs=(P(seq, head), P(seq, head, None, None)),
            check_vma=False,
        )(queries, keys, values, spikes, gain)

    return whole
```

```python
import functools

import jax
import jax.numpy as jnp
from jax import lax
from jax.experimental import pallas as pl
from jax.experimental.pallas import tpu as pltpu
from jax.sharding import Mesh
from jax.sharding import PartitionSpec as P

HD = 128
SCORE_SCALE = HD ** (-0.5)
CORES = 2
VMEM_BYTES = 24 * 1024 * 1024
DECODE_VMEM_BYTES = 46 * 1024 * 1024
PAD = 16
TOP = 32767.0

VMEM = pl.BlockSpec(memory_space=pltpu.VMEM)
SMEM = pl.BlockSpec(memory_space=pltpu.SMEM)
HBM = pl.BlockSpec(memory_space=pltpu.HBM)
ANY = pl.BlockSpec(memory_space=pl.ANY)


def params(vmem=VMEM_BYTES):
    return pltpu.CompilerParams(vmem_limit_bytes=vmem)


def cost(flops, bytes_accessed):
    return pl.CostEstimate(flops=flops, bytes_accessed=bytes_accessed, transcendentals=0)


class Plan:
    def __init__(self, mesh, rows, model):
        n_seq, n_head = mesh.shape["seq"], mesh.shape["head"]
        self.n_y = n_head // CORES
        self.width = model // n_head
        group = self.width // HD
        self.n_inner = 2 if n_seq % 2 == 0 and group % 2 == 0 else 1
        self.n_outer = n_seq // self.n_inner
        self.halves = 2 if group // self.n_inner % 2 == 0 else 1
        self.each = group // (self.n_inner * self.halves)
        self.plane = self.n_inner * self.n_y
        self.rows = rows
        self.block = rows * n_head
        self.piece = self.each * HD


def counts_of(spikes):
    one, two = jnp.ones_like(spikes), jnp.full_like(spikes, 2)
    zero = jnp.zeros_like(spikes)

    def ternary(rest, unit):
        return jnp.where(rest >= 2 * unit, two, jnp.where(rest >= unit, one, zero))

    value = ternary(spikes, 9)
    rest = spikes - 9 * value
    key = ternary(rest, 3)
    return value, key, rest - 3 * key


def sides(plan, place_ref):
    for y in range(plan.n_y):
        for side in range(CORES):
            of = place_ref[0] if side == 0 else 1 - place_ref[0]
            start = pl.multiple_of((y * CORES + of) * plan.width, plan.width)
            yield side, slice(y * plan.width, (y + 1) * plan.width), pl.ds(start, plan.width)


def decode(plan, place, spikes, keys, values):
    rows, model = spikes.shape
    step = min(rows, 32)
    chunks = rows // step

    def kernel(place_ref, *refs):
        sources, outs, buffers, sems = refs[:3], refs[3:9], refs[9:12], refs[12]

        def fetch(chunk, index):
            at = pl.ds(chunk * step, step)
            return pltpu.make_async_copy(
                sources[index].at[at], buffers[index].at[at], sems.at[chunk, index]
            )

        for chunk in range(chunks):
            for index in range(3):
                fetch(chunk, index).start()

        @pl.loop(0, chunks)
        def _(chunk):
            for index in range(3):
                fetch(chunk, index).wait()
            at = pl.ds(pl.multiple_of(chunk * step, step), step)
            for side, mine, columns in sides(plan, place_ref):
                spikes = buffers[0][at, columns].astype(jnp.float32).astype(jnp.bfloat16)
                value, key, query = counts_of(spikes)
                outs[side][at, mine] = buffers[1][at, columns] * key
                outs[2 + side][at, mine] = buffers[2][at, columns] * value
                outs[4 + side][at, mine] = query

    return pl.pallas_call(
        kernel,
        out_shape=[jax.ShapeDtypeStruct((rows, plan.n_y * plan.width), jnp.bfloat16)] * 6,
        in_specs=[SMEM] + [HBM] * 3,
        out_specs=[VMEM] * 6,
        scratch_shapes=[
            pltpu.VMEM((rows, model), jnp.int32),
            pltpu.VMEM((rows, model), jnp.bfloat16),
            pltpu.VMEM((rows, model), jnp.bfloat16),
            pltpu.SemaphoreType.DMA((chunks, 3)),
        ],
        compiler_params=params(DECODE_VMEM_BYTES),
        cost_estimate=cost(rows * model * 4, rows * model * 14),
        name="decode",
    )(place, spikes, keys, values)


def spike_queries(plan, place, queries, counts):
    def kernel(place_ref, queries_ref, *refs):
        for side, mine, columns in sides(plan, place_ref):
            refs[2 + side][:, mine] = queries_ref[:, columns] * refs[side][:, mine]

    return pl.pallas_call(
        kernel,
        out_shape=[jax.ShapeDtypeStruct(a.shape, jnp.bfloat16) for a in counts],
        in_specs=[SMEM] + [VMEM] * 3,
        out_specs=[VMEM] * 2,
        compiler_params=params(),
        cost_estimate=cost(queries.size, queries.size * 6),
        name="spike_queries",
    )(place, queries, *counts)


def contract_rows(left, right):
    return lax.dot_general(
        left, right, (((0,), (0,)), ((), ())), preferred_element_type=jnp.float32
    )


def contract_columns(left, right):
    return lax.dot_general(
        left, right, (((1,), (1,)), ((), ())), preferred_element_type=jnp.float32
    )


def code(states, ref):
    line = lax.broadcasted_iota(jnp.int32, (PAD, HD), 0)
    exponents = jnp.zeros((PAD, HD), jnp.float32)
    for i, state in enumerate(states):
        top = jnp.max(jnp.abs(state), axis=0, keepdims=True)
        exponent = jnp.floor(jnp.log2(jnp.maximum(top, 1e-30))) + 1
        scaled = jnp.round(state * jnp.exp2(15 - exponent))
        scaled = jnp.clip(scaled, -TOP, TOP)
        ref[i * HD : (i + 1) * HD] = scaled.astype(jnp.int32).astype(jnp.int16)
        exponents = jnp.where(line == i, exponent, exponents)
    ref[len(states) * HD : len(states) * HD + PAD] = exponents.astype(jnp.int32).astype(jnp.int16)


def decoded(ref):
    count = ref.shape[0] // HD
    exponents = ref[count * HD : count * HD + PAD].astype(jnp.int32).astype(jnp.float32)
    return [
        ref[i * HD : (i + 1) * HD].astype(jnp.int32).astype(jnp.float32)
        * jnp.exp2(exponents[i : i + 1] - 15)
        for i in range(count)
    ]


def code_gain(gain_ref, ref):
    line = lax.broadcasted_iota(jnp.int32, (PAD // 2, HD), 0)
    gain = jnp.zeros((PAD // 2, HD), jnp.float32)
    for i in range(gain_ref.shape[1] // HD):
        gain = jnp.where(line == i, gain_ref[:, i * HD : (i + 1) * HD], gain)
    coarse = jnp.round(gain * 2.0**12)
    fine = jnp.round((gain - coarse * 2.0**-12) * 2.0**27)
    planes = jnp.concatenate([coarse, fine], axis=0)
    ref[ref.shape[0] - PAD :] = planes.astype(jnp.int32).astype(jnp.int16)


def decoded_gain(ref):
    planes = ref[ref.shape[0] - PAD :].astype(jnp.int32).astype(jnp.float32)
    return planes[: PAD // 2] * 2.0**-12 + planes[PAD // 2 :] * 2.0**-27


def plus(left, right):
    return [a + b for a, b in zip(left, right)]


def total_of(refs, each):
    total = [jnp.zeros((HD, HD), jnp.float32)] * each
    for ref in refs:
        coded = ref.dtype == jnp.int16
        total = plus(total, decoded(ref) if coded else [ref[i] for i in range(each)])
    return total


def coded_shape(heads, more=0):
    return jax.ShapeDtypeStruct((heads * HD + PAD + more, HD), jnp.int16)


def states_shape(*lead):
    return jax.ShapeDtypeStruct((*lead, HD, HD), jnp.float32)


def owned_columns(plan, place_ref, offset, half, i):
    x = place_ref[1] ^ (offset // plan.n_y)
    y = place_ref[2] ^ (offset % plan.n_y)
    start = (((y * plan.halves + half) * plan.n_inner + x) * plan.each + i) * HD
    return pl.ds(pl.multiple_of(start, HD), HD)


def core_states(plan, place, key, value, after):
    def kernel(place_ref, k_ref, v_ref, *refs):
        for half in range(plan.halves):
            for offset in range(plan.plane):
                for i in range(plan.each):
                    at = owned_columns(plan, place_ref, offset, half, i)
                    refs[-1][half, offset, i] = contract_rows(v_ref[:, at], k_ref[:, at])

    heads = plan.halves * plan.plane * plan.each
    return pl.pallas_call(
        kernel,
        out_shape=states_shape(plan.halves, plan.plane, plan.each),
        in_specs=[SMEM] + [VMEM] * 2 + [ANY] * len(after),
        out_specs=VMEM,
        compiler_params=params(),
        cost_estimate=cost(2 * plan.rows * HD * HD * heads, 4 * heads * HD * (plan.rows + HD)),
        name="core_states",
    )(place, key, value, *after)


def chunk_states(plan, place, mine, key_sib, value_sib, half, after, gain=None):
    gains = [] if gain is None else [gain]

    def kernel(place_ref, mine_ref, k_sib_ref, v_sib_ref, *refs):
        own_ref, first_ref, *send_refs = refs[len(gains) + len(after) :]
        is_first = jnp.full((HD, HD), place_ref[0], jnp.int32) == 0
        for offset in (*range(1, plan.plane), 0):
            states = []
            for i in range(plan.each):
                at = owned_columns(plan, place_ref, offset, half, i)
                mine = mine_ref[half, offset, i]
                sib = contract_rows(v_sib_ref[:, at], k_sib_ref[:, at])
                first_ref[offset, i] = jnp.where(is_first, mine, sib)
                states.append(mine + sib)
            if offset:
                code(states, send_refs[offset - 1])
                if gains and offset < plan.n_y:
                    code_gain(refs[0], send_refs[offset - 1])
            else:
                for i, state in enumerate(states):
                    own_ref[i] = state

    heads = plan.plane * plan.each
    return pl.pallas_call(
        kernel,
        out_shape=[states_shape(plan.each), states_shape(plan.plane, plan.each)]
        + [
            coded_shape(plan.each, PAD if gains and o < plan.n_y else 0)
            for o in range(1, plan.plane)
        ],
        in_specs=[SMEM] + [VMEM] * (3 + len(gains)) + [ANY] * len(after),
        out_specs=[VMEM] * (1 + plan.plane),
        compiler_params=params(),
        cost_estimate=cost(
            2 * plan.rows * HD * HD * heads, 4 * plan.rows * HD * heads + 10 * heads * HD * HD
        ),
        name=f"chunk_states_{half}",
    )(place, mine, key_sib, value_sib, *gains, *after)


def level_states(plan, own, others, half, after):
    def kernel(own_ref, *refs):
        total = total_of((own_ref, *refs[: len(others)]), plan.each)
        for i, state in enumerate(total):
            refs[-2][i] = state
        code(total, refs[-1])

    return pl.pallas_call(
        kernel,
        out_shape=[states_shape(plan.each), coded_shape(plan.each)],
        in_specs=[VMEM] * plan.plane + [ANY] * len(after),
        out_specs=[VMEM] * 2,
        compiler_params=params(),
        cost_estimate=cost(0, plan.plane * plan.each * HD * HD * 2),
        name=f"level_states_{half}",
    )(own, *others, *after)


def two_levels(plan, total, before, half, after):
    def kernel(total_ref, before_ref, *refs):
        code(total_of((total_ref, before_ref), plan.each), refs[-1])

    return pl.pallas_call(
        kernel,
        out_shape=coded_shape(plan.each),
        in_specs=[VMEM] * 2 + [ANY] * len(after),
        out_specs=VMEM,
        compiler_params=params(),
        cost_estimate=cost(0, 2 * plan.each * HD * HD * 2),
        name=f"two_levels_{half}",
    )(total, before, *after)


def carried(plan, place_ref, own, others, levels, offsets):
    x, y = place_ref[1], place_ref[2]
    here = x * plan.n_y + y
    earlier = total_of(levels, plan.each)
    states = [[own[i] for i in range(plan.each)]] + [decoded(ref) for ref in others]

    def add(totals, keep_of):
        for offset, terms in enumerate(states):
            keep = jnp.full((HD, HD), keep_of(here ^ offset), jnp.int32) == 1
            totals = plus(totals, [jnp.where(keep, s, 0.0) for s in terms])
        return totals

    before = [add(earlier, lambda chip: (chip < here ^ o).astype(jnp.int32)) for o in offsets]
    blocks = [
        add(earlier, lambda chip: (chip // plan.n_y <= x ^ o).astype(jnp.int32))
        for o in range(plan.n_inner)
    ]
    return before, blocks


def carries(plan, place, own, others, levels, half, offsets, after):
    n_others, n_levels = len(others), len(levels)

    def kernel(place_ref, own_ref, *refs):
        before, _ = carried(
            plan, place_ref, own_ref, refs[:n_others], refs[n_others : n_others + n_levels], offsets
        )
        for states, ref in zip(before, refs[n_others + n_levels + len(after) :]):
            code(states, ref)

    return pl.pallas_call(
        kernel,
        out_shape=[coded_shape(plan.each)] * len(offsets),
        in_specs=[SMEM] + [VMEM] * (1 + n_others + n_levels) + [ANY] * len(after),
        out_specs=[VMEM] * len(offsets),
        compiler_params=params(),
        cost_estimate=cost(0, (plan.plane * 4 + n_levels) * plan.each * HD * HD * 2),
        name=f"carries_{half}",
    )(place, own, *others, *levels, *after)


def own_carries(plan, place, own, others, levels, offsets, after):
    n_others = len(others[0])
    operands = [(own[h], *others[h], *levels[h]) for h in range(plan.halves)]
    starts = [sum(map(len, operands[:h])) for h in range(plan.halves + 1)]

    def kernel(place_ref, *refs):
        outs = refs[starts[-1] + len(after) :]
        befores = [[] for _ in offsets]
        for half in range(plan.halves):
            own_ref, *of_half = refs[starts[half] : starts[half + 1]]
            before, blocks = carried(
                plan, place_ref, own_ref, of_half[:n_others], of_half[n_others:], offsets
            )
            for all_states, states in zip(befores, before):
                all_states.extend(states)
            for offset, (totals, ref) in enumerate(zip(blocks, outs[len(offsets) :])):
                block = place_ref[3] * plan.n_inner + (place_ref[1] ^ offset)
                seen = jnp.full((1, HD), (block + 1) * plan.block, jnp.int32).astype(jnp.float32)
                for i, total in enumerate(totals):
                    ref[half, i] = total.T * lax.rsqrt(seen)
        for states, ref in zip(befores, outs):
            code(states, ref)

    return pl.pallas_call(
        kernel,
        out_shape=[coded_shape(plan.halves * plan.each)] * len(offsets)
        + [states_shape(plan.halves, plan.each)] * plan.n_inner,
        in_specs=[SMEM] + [VMEM] * starts[-1] + [ANY] * len(after),
        out_specs=[VMEM] * (len(offsets) + plan.n_inner),
        compiler_params=params(),
        cost_estimate=cost(0, plan.plane * plan.each * HD * HD * 20),
        name="own_carries",
    )(place, *[a for arrays in operands for a in arrays], *after)


def attend_local(plan, place, query, key, value, half, offsets, after):
    rows = plan.rows

    def kernel(place_ref, q_ref, q_sib_ref, k_ref, k_sib_ref, v_ref, v_sib_ref, *refs):
        for piece, offset in enumerate(offsets):
            for i in range(plan.each):
                at = owned_columns(plan, place_ref, offset, half, i)
                out_at = slice(piece * plan.piece + i * HD, piece * plan.piece + (i + 1) * HD)
                refs[-1][0, :, out_at] = local_part(q_ref, k_ref, v_ref, at)
                refs[-1][1, :, out_at] = local_part(q_sib_ref, k_sib_ref, v_sib_ref, at)

    heads = len(offsets) * plan.each
    return pl.pallas_call(
        kernel,
        out_shape=jax.ShapeDtypeStruct((CORES, rows, heads * HD), jnp.float32),
        in_specs=[SMEM] + [VMEM] * 6 + [ANY] * len(after),
        out_specs=VMEM,
        compiler_params=params(),
        cost_estimate=cost(heads * 8 * rows * rows * HD, 16 * rows * heads * HD),
        name=f"attend_local_{half}_" + "_".join(map(str, offsets)),
    )(place, *query, *key, *value, *after)


def local_part(q_ref, k_ref, v_ref, at):
    rows = q_ref.shape[0]
    causal = lax.broadcasted_iota(jnp.int32, (rows, rows), 0) >= lax.broadcasted_iota(
        jnp.int32, (rows, rows), 1
    )
    scores = contract_columns(q_ref[:, at], k_ref[:, at]) * SCORE_SCALE
    weights = jnp.where(causal, scores, 0.0).astype(jnp.bfloat16)
    return jnp.dot(weights, v_ref[:, at], preferred_element_type=jnp.float32)


def finished(queries, local, carried, gain):
    carried = carried * SCORE_SCALE
    high = carried.astype(jnp.bfloat16)
    low = (carried - high.astype(jnp.float32)).astype(jnp.bfloat16)
    both = contract_columns(queries, jnp.concatenate([high, low], axis=0))
    raw = local + (both[:, :HD] + both[:, HD:])
    mean = jnp.mean(raw * raw, axis=-1, keepdims=True)
    return (raw * lax.rsqrt(mean + 1e-06) * gain).astype(jnp.bfloat16)


def attend(
    plan, place, query, key, value, carry, first, gain, half, offsets, after=(), local=None
):
    rows = plan.rows
    operands = [*query, local] if local is not None else [*query, *key, *value]
    n = len(operands)

    def kernel(place_ref, *refs):
        core = place_ref[0]
        first_ref, gain_ref, *carry_refs = refs[n : n + 2 + len(offsets)]
        out_ref = refs[-1]
        is_second = jnp.full((HD, HD), core, jnp.int32) == 1
        coded_gain = gain_ref.dtype == jnp.int16
        line = lax.broadcasted_iota(jnp.int32, (PAD // 2, HD), 0)
        for piece, offset in enumerate(offsets):
            x = place_ref[1] ^ (offset // plan.n_y)
            carry_states = decoded(carry_refs[piece])
            skip = half * plan.each if len(carry_states) > plan.each else 0
            for i in range(plan.each):
                at = owned_columns(plan, place_ref, offset, half, i)
                head = (half * plan.n_inner + x) * plan.each + i
                if coded_gain:
                    gain = jnp.where(line == head, decoded_gain(gain_ref), 0.0)
                    gain = jnp.sum(gain, axis=0, keepdims=True)
                else:
                    gain = gain_ref[:, pl.ds(pl.multiple_of(head * HD, HD), HD)]
                out_at = slice(piece * plan.piece + i * HD, piece * plan.piece + (i + 1) * HD)
                carried = carry_states[skip + i]
                first = first_ref[offset, i]
                for side in range(CORES):
                    if local is None:
                        raw = local_part(refs[side], refs[2 + side], refs[4 + side], at)
                    else:
                        raw = refs[2][side, :, out_at]
                    behind = is_second if side == 0 else ~is_second
                    state = carried + jnp.where(behind, first, 0.0)
                    of = core if side == 0 else 1 - core
                    out_rows = pl.ds(pl.multiple_of(of * rows, rows), rows)
                    out_ref[out_rows, out_at] = finished(refs[side][:, at], raw, state, gain)

    heads = len(offsets) * plan.each
    return pl.pallas_call(
        kernel,
        out_shape=jax.ShapeDtypeStruct((CORES * rows, heads * HD), jnp.bfloat16),
        in_specs=[SMEM] + [VMEM] * (n + 2 + len(offsets)) + [ANY] * len(after),
        out_specs=VMEM,
        compiler_params=params(),
        cost_estimate=cost(
            heads * (8 * rows * rows * HD + 8 * rows * HD * HD), 16 * rows * heads * HD
        ),
        name=f"attend_{half}_" + "_".join(map(str, offsets)),
    )(place, *operands, first, gain, *carry, *after)


def assemble(plan, place, parts, into=None):
    rows = CORES * plan.rows
    copies = [(n, piece, half, o) for n, (_, half, os) in enumerate(parts) for piece, o in enumerate(os)]

    def kernel(place_ref, *refs):
        out_ref, sems = refs[-2:]
        started = []
        for at, (n, piece, half, offset) in enumerate(copies):
            x = place_ref[1] ^ (offset // plan.n_y)
            y = place_ref[2] ^ (offset % plan.n_y)
            column = (half * plan.n_inner + x) * plan.piece
            to_rows = pl.ds(pl.multiple_of(y * rows, rows), rows)
            to_columns = pl.ds(pl.multiple_of(column, plan.piece), plan.piece)
            started.append(
                pltpu.make_async_copy(
                    refs[n].at[:, pl.ds(piece * plan.piece, plan.piece)],
                    out_ref.at[to_rows, to_columns],
                    sems.at[at],
                )
            )
            started[-1].start()
        for copy in started:
            copy.wait()

    arrays = [array for array, _, _ in parts]
    aliased = [] if into is None else [into]
    return pl.pallas_call(
        kernel,
        out_shape=jax.ShapeDtypeStruct((plan.n_y * rows, plan.width), jnp.bfloat16),
        in_specs=[SMEM] + [VMEM] * len(arrays) + [HBM] * len(aliased),
        out_specs=HBM,
        scratch_shapes=[pltpu.SemaphoreType.DMA((len(copies),))],
        input_output_aliases={1 + len(arrays): 0} if aliased else {},
        compiler_params=params(),
        name="assemble" if into is None else "finish",
    )(place, *arrays, *aliased)


def assemble_cache(plan, place, parts):
    group = plan.n_inner * plan.each

    def kernel(place_ref, *refs):
        for half in range(plan.halves):
            for offset, ref in enumerate(refs[:-1]):
                start = half * group + (place_ref[1] ^ offset) * plan.each
                refs[-1][0, pl.ds(start, plan.each)] = ref[half]

    return pl.pallas_call(
        kernel,
        out_shape=states_shape(1, plan.halves * group),
        in_specs=[SMEM] + [VMEM] * len(parts),
        out_specs=VMEM,
        compiler_params=params(),
        name="assemble_cache",
    )(place, *parts)


def per_device(plan, queries, keys, values, spikes, gain):
    place = jnp.stack([lax.axis_index(a) for a in ("core", "inner", "y", "outer")]).astype(jnp.int32)
    halves = range(plan.halves)

    def swap(array, axes, offset, size):
        return lax.ppermute(array, axes, [(i, i ^ offset) for i in range(size)])

    def in_level(array, offset):
        return swap(array, ("inner", "y"), offset, plan.plane)

    def to_later(array, pairs):
        return lax.ppermute(array, "outer", pairs)

    def ahead(distance):
        return [(i, i + distance) for i in range(plan.n_outer - distance)]

    gain = gain.reshape(1, plan.width)
    key, key_out, value, value_out, *counts = decode(plan, place, spikes, keys, values)
    key, value = ((a, swap(b, "core", 1, CORES)) for a, b in ((key, key_out), (value, value_out)))
    query, query_out = spike_queries(plan, place, queries, counts)
    query = (query, swap(query_out, "core", 1, CORES))

    of_core = core_states(plan, place, key[0], value[0], [query[0]])
    own, first, others = [], [], []

    def owner_stage(half, after):
        with_gain = gain if half == 0 else None
        mine, parts, *sends = chunk_states(plan, place, of_core, key[1], value[1], half, after, with_gain)
        own.append(mine)
        first.append(parts)
        others.append([in_level(a, o) for o, a in enumerate(sends, 1)])

    of_group = [list(range(y, plan.plane, plan.n_y)) for y in range(plan.n_y)]
    abroad = [o for offsets in of_group[1:] for o in offsets]

    def part_of(half, offsets, carry, after, local=None):
        return attend(
            plan,
            place,
            query,
            key,
            value,
            [carry[o] for o in offsets],
            first[half],
            others[0][offsets[0] % plan.n_y - 1] if offsets[0] % plan.n_y else gain,
            half,
            offsets,
            after,
            local,
        )

    def carry_stage(half, after):
        sends = carries(plan, place, own[half], others[half], levels[half], half, abroad, after)
        return sends[0], {o: in_level(a, o) for o, a in zip(abroad, sends)}

    parts = []

    def send_stage(half, carry, after, local):
        for y in range(1, plan.n_y):
            part = part_of(half, of_group[y], carry, after, local.get(y))
            parts.append((swap(part, "y", y, plan.n_y), half, of_group[y]))
            after = [part]
        return after

    after = []
    for half in halves:
        owner_stage(half, after)
        after = [own[-1], query[1]]
    levels, totals = [], []
    for half in halves:
        total, level = level_states(plan, own[half], others[half][::-1], half, after)
        totals.append(total)
        if plan.n_outer == 4:
            levels.append([to_later(level, ahead(1)), to_later(level, [(0, 2)])])
        else:
            levels.append([to_later(level, ahead(d)) for d in range(1, plan.n_outer)])
        after = [level]
    if plan.n_outer == 4:
        for half in halves:
            level = two_levels(plan, totals[half], levels[half][0], half, after)
            levels[half].append(to_later(level, [(1, 3)]))
            after = [level]
    local = {}
    for y in range(1, plan.n_y):
        local[y] = attend_local(plan, place, query, key, value, 0, of_group[y], after)
        after = [local[y]]
    carry = []
    for half in halves:
        done, of_half = carry_stage(half, after)
        carry.append(of_half)
        after = [done]
    for half in halves:
        after = send_stage(half, carry[half], after, {} if half else local)
    sends = own_carries(plan, place, own, others, levels, of_group[0], after)
    own_carry = {o: in_level(a, o) if o else a for o, a in zip(of_group[0], sends)}
    caches = [
        swap(a, "inner", o, plan.n_inner) if o else a
        for o, a in enumerate(sends[len(of_group[0]) :])
    ]
    early = []
    for half in halves:
        part = part_of(half, of_group[0], own_carry, after)
        early.append((part, half, of_group[0]))
        after = [part]
    out = assemble(plan, place, early + parts[:-1])
    out = assemble(plan, place, parts[-1:], out)
    return out, assemble_cache(plan, place, caches)


def solution(mesh):
    tokens = P(("outer", "inner", "y", "core"), None)
    seq, head = ("outer", "inner"), ("y", "core")

    def whole(queries, keys, values, spikes, gain):
        plan = Plan(mesh, spikes.shape[0] // mesh.size, spikes.shape[1])
        sizes = (plan.n_outer, plan.n_inner, plan.n_y, CORES)
        split = Mesh(mesh.devices.reshape(sizes), ("outer", "inner", "y", "core"))
        return jax.shard_map(
            functools.partial(per_device, plan),
            mesh=split,
            in_specs=(tokens, tokens, tokens, tokens, P(head)),
            out_specs=(P(seq, head), P(seq, head, None, None)),
            check_vma=False,
        )(queries, keys, values, spikes, gain)

    return whole
```

```python
import functools

import jax
import jax.numpy as jnp
from jax import lax
from jax.experimental import pallas as pl
from jax.experimental.pallas import tpu as pltpu
from jax.sharding import Mesh
from jax.sharding import PartitionSpec as P

HD = 128
SCORE_SCALE = HD ** (-0.5)
CORES = 2
VMEM_BYTES = 24 * 1024 * 1024
DECODE_VMEM_BYTES = 46 * 1024 * 1024
PAD = 16
TOP = 32767.0

VMEM = pl.BlockSpec(memory_space=pltpu.VMEM)
SMEM = pl.BlockSpec(memory_space=pltpu.SMEM)
HBM = pl.BlockSpec(memory_space=pltpu.HBM)
ANY = pl.BlockSpec(memory_space=pl.ANY)


def params(vmem=VMEM_BYTES):
    return pltpu.CompilerParams(vmem_limit_bytes=vmem)


def cost(flops, bytes_accessed):
    return pl.CostEstimate(flops=flops, bytes_accessed=bytes_accessed, transcendentals=0)


class Plan:
    def __init__(self, mesh, rows, model):
        n_seq, n_head = mesh.shape["seq"], mesh.shape["head"]
        self.n_y = n_head // CORES
        self.width = model // n_head
        group = self.width // HD
        self.n_inner = 2 if n_seq % 2 == 0 and group % 2 == 0 else 1
        self.n_outer = n_seq // self.n_inner
        self.halves = 2 if group // self.n_inner % 2 == 0 else 1
        self.each = group // (self.n_inner * self.halves)
        self.plane = self.n_inner * self.n_y
        self.rows = rows
        self.block = rows * n_head
        self.piece = self.each * HD
        self.half_width = self.width // self.halves


def counts_of(spikes):
    one, two = jnp.ones_like(spikes), jnp.full_like(spikes, 2)
    zero = jnp.zeros_like(spikes)

    def ternary(rest, unit):
        return jnp.where(rest >= 2 * unit, two, jnp.where(rest >= unit, one, zero))

    value = ternary(spikes, 9)
    rest = spikes - 9 * value
    key = ternary(rest, 3)
    return value, key, rest - 3 * key


def sides(plan, place_ref):
    width = plan.half_width
    for y in range(plan.n_y):
        for side in range(CORES):
            of = place_ref[0] if side == 0 else 1 - place_ref[0]
            for half in range(plan.halves):
                start = ((y * CORES + of) * plan.halves + half) * width
                at = pl.ds(pl.multiple_of(start, width), width)
                yield side, half, slice(y * width, (y + 1) * width), at


def decode(plan, place, spikes, keys, values):
    rows, model = spikes.shape
    step = min(rows, 32)
    chunks = rows // step
    n_out = 3 * CORES * plan.halves

    def kernel(place_ref, *refs):
        sources, *outs, b0, b1, b2, sems = refs[:3], *refs[3:]
        buffers = (b0, b1, b2)

        def fetch(chunk, index):
            at = pl.ds(chunk * step, step)
            return pltpu.make_async_copy(
                sources[index].at[at], buffers[index].at[at], sems.at[chunk, index]
            )

        for chunk in range(chunks):
            for index in range(3):
                fetch(chunk, index).start()

        @pl.loop(0, chunks)
        def _(chunk):
            for index in range(3):
                fetch(chunk, index).wait()
            at = pl.ds(pl.multiple_of(chunk * step, step), step)
            for side, half, mine, columns in sides(plan, place_ref):
                spikes = buffers[0][at, columns].astype(jnp.float32).astype(jnp.bfloat16)
                value, key, query = counts_of(spikes)
                spiked = (buffers[1][at, columns] * key, buffers[2][at, columns] * value, query)
                for index, array in enumerate(spiked):
                    outs[(index * CORES + side) * plan.halves + half][at, mine] = array

    return pl.pallas_call(
        kernel,
        out_shape=[jax.ShapeDtypeStruct((rows, plan.n_y * plan.half_width), jnp.bfloat16)] * n_out,
        in_specs=[SMEM] + [HBM] * 3,
        out_specs=[VMEM] * n_out,
        scratch_shapes=[
            pltpu.VMEM((rows, model), jnp.int32),
            pltpu.VMEM((rows, model), jnp.bfloat16),
            pltpu.VMEM((rows, model), jnp.bfloat16),
            pltpu.SemaphoreType.DMA((chunks, 3)),
        ],
        compiler_params=params(DECODE_VMEM_BYTES),
        cost_estimate=cost(rows * model * 4, rows * model * 14),
        name="decode",
    )(place, spikes, keys, values)


def spike_queries(plan, place, queries, counts):
    n = len(counts)

    def kernel(place_ref, queries_ref, *refs):
        for side, half, mine, columns in sides(plan, place_ref):
            at = side * plan.halves + half
            refs[n + at][:, mine] = queries_ref[:, columns] * refs[at][:, mine]

    return pl.pallas_call(
        kernel,
        out_shape=[jax.ShapeDtypeStruct(a.shape, jnp.bfloat16) for a in counts],
        in_specs=[SMEM] + [VMEM] * (1 + n),
        out_specs=[VMEM] * n,
        compiler_params=params(),
        cost_estimate=cost(queries.size, queries.size * 6),
        name="spike_queries",
    )(place, queries, *counts)


def contract_rows(left, right):
    return lax.dot_general(
        left, right, (((0,), (0,)), ((), ())), preferred_element_type=jnp.float32
    )


def contract_columns(left, right):
    return lax.dot_general(
        left, right, (((1,), (1,)), ((), ())), preferred_element_type=jnp.float32
    )


def code(states, ref):
    line = lax.broadcasted_iota(jnp.int32, (PAD, HD), 0)
    exponents = jnp.zeros((PAD, HD), jnp.float32)
    for i, state in enumerate(states):
        top = jnp.max(jnp.abs(state), axis=0, keepdims=True)
        exponent = jnp.floor(jnp.log2(jnp.maximum(top, 1e-30))) + 1
        scaled = jnp.round(state * jnp.exp2(15 - exponent))
        scaled = jnp.clip(scaled, -TOP, TOP)
        ref[i * HD : (i + 1) * HD] = scaled.astype(jnp.int32).astype(jnp.int16)
        exponents = jnp.where(line == i, exponent, exponents)
    ref[len(states) * HD : len(states) * HD + PAD] = exponents.astype(jnp.int32).astype(jnp.int16)


def decoded(ref):
    count = ref.shape[0] // HD
    exponents = ref[count * HD : count * HD + PAD].astype(jnp.int32).astype(jnp.float32)
    return [
        ref[i * HD : (i + 1) * HD].astype(jnp.int32).astype(jnp.float32)
        * jnp.exp2(exponents[i : i + 1] - 15)
        for i in range(count)
    ]


def code_gain(gain_ref, ref):
    line = lax.broadcasted_iota(jnp.int32, (PAD // 2, HD), 0)
    gain = jnp.zeros((PAD // 2, HD), jnp.float32)
    for i in range(gain_ref.shape[1] // HD):
        gain = jnp.where(line == i, gain_ref[:, i * HD : (i + 1) * HD], gain)
    coarse = jnp.round(gain * 2.0**12)
    fine = jnp.round((gain - coarse * 2.0**-12) * 2.0**27)
    planes = jnp.concatenate([coarse, fine], axis=0)
    ref[ref.shape[0] - PAD :] = planes.astype(jnp.int32).astype(jnp.int16)


def decoded_gain(ref):
    planes = ref[ref.shape[0] - PAD :].astype(jnp.int32).astype(jnp.float32)
    return planes[: PAD // 2] * 2.0**-12 + planes[PAD // 2 :] * 2.0**-27


def plus(left, right):
    return [a + b for a, b in zip(left, right)]


def total_of(refs, each):
    total = [jnp.zeros((HD, HD), jnp.float32)] * each
    for ref in refs:
        coded = ref.dtype == jnp.int16
        total = plus(total, decoded(ref) if coded else [ref[i] for i in range(each)])
    return total


def coded_shape(heads, more=0):
    return jax.ShapeDtypeStruct((heads * HD + PAD + more, HD), jnp.int16)


def states_shape(*lead):
    return jax.ShapeDtypeStruct((*lead, HD, HD), jnp.float32)


def owned_columns(plan, place_ref, offset, i):
    x = place_ref[1] ^ (offset // plan.n_y)
    y = place_ref[2] ^ (offset % plan.n_y)
    start = ((y * plan.n_inner + x) * plan.each + i) * HD
    return pl.ds(pl.multiple_of(start, HD), HD)


def core_states(plan, place, key, value, half, after):
    def kernel(place_ref, k_ref, v_ref, *refs):
        for offset in range(plan.plane):
            for i in range(plan.each):
                at = owned_columns(plan, place_ref, offset, i)
                refs[-1][offset, i] = contract_rows(v_ref[:, at], k_ref[:, at])

    heads = plan.plane * plan.each
    return pl.pallas_call(
        kernel,
        out_shape=states_shape(plan.plane, plan.each),
        in_specs=[SMEM] + [VMEM] * 2 + [ANY] * len(after),
        out_specs=VMEM,
        compiler_params=params(),
        cost_estimate=cost(2 * plan.rows * HD * HD * heads, 4 * heads * HD * (plan.rows + HD)),
        name=f"core_states_{half}",
    )(place, key, value, *after)


def chunk_states(plan, place, mine, key_sib, value_sib, half, after, gain=None):
    gains = [] if gain is None else [gain]

    def kernel(place_ref, mine_ref, k_sib_ref, v_sib_ref, *refs):
        own_ref, first_ref, *send_refs = refs[len(gains) + len(after) :]
        is_first = jnp.full((HD, HD), place_ref[0], jnp.int32) == 0
        for offset in (*range(1, plan.plane), 0):
            states = []
            for i in range(plan.each):
                at = owned_columns(plan, place_ref, offset, i)
                mine = mine_ref[offset, i]
                sib = contract_rows(v_sib_ref[:, at], k_sib_ref[:, at])
                first_ref[offset, i] = jnp.where(is_first, mine, sib)
                states.append(mine + sib)
            if offset:
                code(states, send_refs[offset - 1])
                if gains and offset < plan.n_y:
                    code_gain(refs[0], send_refs[offset - 1])
            else:
                for i, state in enumerate(states):
                    own_ref[i] = state

    heads = plan.plane * plan.each
    return pl.pallas_call(
        kernel,
        out_shape=[states_shape(plan.each), states_shape(plan.plane, plan.each)]
        + [
            coded_shape(plan.each, PAD if gains and o < plan.n_y else 0)
            for o in range(1, plan.plane)
        ],
        in_specs=[SMEM] + [VMEM] * (3 + len(gains)) + [ANY] * len(after),
        out_specs=[VMEM] * (1 + plan.plane),
        compiler_params=params(),
        cost_estimate=cost(
            2 * plan.rows * HD * HD * heads, 4 * plan.rows * HD * heads + 10 * heads * HD * HD
        ),
        name=f"chunk_states_{half}",
    )(place, mine, key_sib, value_sib, *gains, *after)


def level_states(plan, own, others, half, after):
    def kernel(own_ref, *refs):
        code(total_of((own_ref, *refs[: len(others)]), plan.each), refs[-1])

    return pl.pallas_call(
        kernel,
        out_shape=coded_shape(plan.each),
        in_specs=[VMEM] * plan.plane + [ANY] * len(after),
        out_specs=VMEM,
        compiler_params=params(),
        cost_estimate=cost(0, plan.plane * plan.each * HD * HD * 2),
        name=f"level_states_{half}",
    )(own, *others, *after)


def carried(plan, place_ref, own, others, levels, offsets):
    x, y = place_ref[1], place_ref[2]
    here = x * plan.n_y + y
    earlier = total_of(levels, plan.each)
    states = [[own[i] for i in range(plan.each)]] + [decoded(ref) for ref in others]

    def add(totals, keep_of):
        for offset, terms in enumerate(states):
            keep = jnp.full((HD, HD), keep_of(here ^ offset), jnp.int32) == 1
            totals = plus(totals, [jnp.where(keep, s, 0.0) for s in terms])
        return totals

    before = [add(earlier, lambda chip: (chip < here ^ o).astype(jnp.int32)) for o in offsets]
    blocks = [
        add(earlier, lambda chip: (chip // plan.n_y <= x ^ o).astype(jnp.int32))
        for o in range(plan.n_inner)
    ]
    return before, blocks


def carries(plan, place, own, others, levels, half, offsets, after):
    n_others, n_levels = len(others), len(levels)

    def kernel(place_ref, own_ref, *refs):
        before, _ = carried(
            plan, place_ref, own_ref, refs[:n_others], refs[n_others : n_others + n_levels], offsets
        )
        for states, ref in zip(before, refs[n_others + n_levels + len(after) :]):
            code(states, ref)

    return pl.pallas_call(
        kernel,
        out_shape=[coded_shape(plan.each)] * len(offsets),
        in_specs=[SMEM] + [VMEM] * (1 + n_others + n_levels) + [ANY] * len(after),
        out_specs=[VMEM] * len(offsets),
        compiler_params=params(),
        cost_estimate=cost(0, (plan.plane * 4 + n_levels) * plan.each * HD * HD * 2),
        name=f"carries_{half}",
    )(place, own, *others, *levels, *after)


def own_carries(plan, place, own, others, levels, offsets, after):
    n_others = len(others[0])
    operands = [(own[h], *others[h], *levels[h]) for h in range(plan.halves)]
    starts = [sum(map(len, operands[:h])) for h in range(plan.halves + 1)]

    def kernel(place_ref, *refs):
        outs = refs[starts[-1] + len(after) :]
        befores = [[] for _ in offsets]
        for half in range(plan.halves):
            own_ref, *of_half = refs[starts[half] : starts[half + 1]]
            before, blocks = carried(
                plan, place_ref, own_ref, of_half[:n_others], of_half[n_others:], offsets
            )
            for all_states, states in zip(befores, before):
                all_states.extend(states)
            for offset, (totals, ref) in enumerate(zip(blocks, outs[len(offsets) :])):
                block = place_ref[3] * plan.n_inner + (place_ref[1] ^ offset)
                seen = jnp.full((1, HD), (block + 1) * plan.block, jnp.int32).astype(jnp.float32)
                for i, total in enumerate(totals):
                    ref[half, i] = total.T * lax.rsqrt(seen)
        for states, ref in zip(befores, outs):
            code(states, ref)

    return pl.pallas_call(
        kernel,
        out_shape=[coded_shape(plan.halves * plan.each)] * len(offsets)
        + [states_shape(plan.halves, plan.each)] * plan.n_inner,
        in_specs=[SMEM] + [VMEM] * starts[-1] + [ANY] * len(after),
        out_specs=[VMEM] * (len(offsets) + plan.n_inner),
        compiler_params=params(),
        cost_estimate=cost(0, plan.plane * plan.each * HD * HD * 20),
        name="own_carries",
    )(place, *[a for arrays in operands for a in arrays], *after)


def attend_local(plan, place, query, key, value, half, offsets, after):
    rows = plan.rows

    def kernel(place_ref, q_ref, q_sib_ref, k_ref, k_sib_ref, v_ref, v_sib_ref, *refs):
        for piece, offset in enumerate(offsets):
            for i in range(plan.each):
                at = owned_columns(plan, place_ref, offset, i)
                out_at = slice(piece * plan.piece + i * HD, piece * plan.piece + (i + 1) * HD)
                refs[-1][0, :, out_at] = local_part(q_ref, k_ref, v_ref, at)
                refs[-1][1, :, out_at] = local_part(q_sib_ref, k_sib_ref, v_sib_ref, at)

    heads = len(offsets) * plan.each
    return pl.pallas_call(
        kernel,
        out_shape=jax.ShapeDtypeStruct((CORES, rows, heads * HD), jnp.float32),
        in_specs=[SMEM] + [VMEM] * 6 + [ANY] * len(after),
        out_specs=VMEM,
        compiler_params=params(),
        cost_estimate=cost(heads * 8 * rows * rows * HD, 16 * rows * heads * HD),
        name=f"attend_local_{half}_" + "_".join(map(str, offsets)),
    )(place, *query, *key, *value, *after)


def local_part(q_ref, k_ref, v_ref, at):
    rows = q_ref.shape[0]
    causal = lax.broadcasted_iota(jnp.int32, (rows, rows), 0) >= lax.broadcasted_iota(
        jnp.int32, (rows, rows), 1
    )
    scores = contract_columns(q_ref[:, at], k_ref[:, at]) * SCORE_SCALE
    weights = jnp.where(causal, scores, 0.0).astype(jnp.bfloat16)
    return jnp.dot(weights, v_ref[:, at], preferred_element_type=jnp.float32)


def finished(queries, local, carried, gain):
    carried = carried * SCORE_SCALE
    high = carried.astype(jnp.bfloat16)
    low = (carried - high.astype(jnp.float32)).astype(jnp.bfloat16)
    both = contract_columns(queries, jnp.concatenate([high, low], axis=0))
    raw = local + (both[:, :HD] + both[:, HD:])
    mean = jnp.mean(raw * raw, axis=-1, keepdims=True)
    return (raw * lax.rsqrt(mean + 1e-06) * gain).astype(jnp.bfloat16)


def attend(
    plan, place, query, key, value, carry, first, gain, half, offsets, after=(), local=None
):
    rows = plan.rows
    operands = [*query, local] if local is not None else [*query, *key, *value]
    n = len(operands)

    def kernel(place_ref, *refs):
        core = place_ref[0]
        first_ref, gain_ref, *carry_refs = refs[n : n + 2 + len(offsets)]
        out_ref = refs[-1]
        is_second = jnp.full((HD, HD), core, jnp.int32) == 1
        coded_gain = gain_ref.dtype == jnp.int16
        line = lax.broadcasted_iota(jnp.int32, (PAD // 2, HD), 0)
        for piece, offset in enumerate(offsets):
            x = place_ref[1] ^ (offset // plan.n_y)
            carry_states = decoded(carry_refs[piece])
            skip = half * plan.each if len(carry_states) > plan.each else 0
            for i in range(plan.each):
                at = owned_columns(plan, place_ref, offset, i)
                head = (half * plan.n_inner + x) * plan.each + i
                if coded_gain:
                    gain = jnp.where(line == head, decoded_gain(gain_ref), 0.0)
                    gain = jnp.sum(gain, axis=0, keepdims=True)
                else:
                    gain = gain_ref[:, pl.ds(pl.multiple_of(head * HD, HD), HD)]
                out_at = slice(piece * plan.piece + i * HD, piece * plan.piece + (i + 1) * HD)
                carried = carry_states[skip + i]
                first = first_ref[offset, i]
                for side in range(CORES):
                    if local is None:
                        raw = local_part(refs[side], refs[2 + side], refs[4 + side], at)
                    else:
                        raw = refs[2][side, :, out_at]
                    behind = is_second if side == 0 else ~is_second
                    state = carried + jnp.where(behind, first, 0.0)
                    of = core if side == 0 else 1 - core
                    out_rows = pl.ds(pl.multiple_of(of * rows, rows), rows)
                    out_ref[out_rows, out_at] = finished(refs[side][:, at], raw, state, gain)

    heads = len(offsets) * plan.each
    return pl.pallas_call(
        kernel,
        out_shape=jax.ShapeDtypeStruct((CORES * rows, heads * HD), jnp.bfloat16),
        in_specs=[SMEM] + [VMEM] * (n + 2 + len(offsets)) + [ANY] * len(after),
        out_specs=VMEM,
        compiler_params=params(),
        cost_estimate=cost(
            heads * (8 * rows * rows * HD + 8 * rows * HD * HD), 16 * rows * heads * HD
        ),
        name=f"attend_{half}_" + "_".join(map(str, offsets)),
    )(place, *operands, first, gain, *carry, *after)


def assemble(plan, place, parts, into=None):
    rows = CORES * plan.rows
    copies = [(n, piece, half, o) for n, (_, half, os) in enumerate(parts) for piece, o in enumerate(os)]

    def kernel(place_ref, *refs):
        out_ref, sems = refs[-2:]
        started = []
        for at, (n, piece, half, offset) in enumerate(copies):
            x = place_ref[1] ^ (offset // plan.n_y)
            y = place_ref[2] ^ (offset % plan.n_y)
            column = (half * plan.n_inner + x) * plan.piece
            to_rows = pl.ds(pl.multiple_of(y * rows, rows), rows)
            to_columns = pl.ds(pl.multiple_of(column, plan.piece), plan.piece)
            started.append(
                pltpu.make_async_copy(
                    refs[n].at[:, pl.ds(piece * plan.piece, plan.piece)],
                    out_ref.at[to_rows, to_columns],
                    sems.at[at],
                )
            )
            started[-1].start()
        for copy in started:
            copy.wait()

    arrays = [array for array, _, _ in parts]
    aliased = [] if into is None else [into]
    return pl.pallas_call(
        kernel,
        out_shape=jax.ShapeDtypeStruct((plan.n_y * rows, plan.width), jnp.bfloat16),
        in_specs=[SMEM] + [VMEM] * len(arrays) + [HBM] * len(aliased),
        out_specs=HBM,
        scratch_shapes=[pltpu.SemaphoreType.DMA((len(copies),))],
        input_output_aliases={1 + len(arrays): 0} if aliased else {},
        compiler_params=params(),
        name="assemble" if into is None else "finish",
    )(place, *arrays, *aliased)


def assemble_cache(plan, place, parts):
    group = plan.n_inner * plan.each

    def kernel(place_ref, *refs):
        for half in range(plan.halves):
            for offset, ref in enumerate(refs[:-1]):
                start = half * group + (place_ref[1] ^ offset) * plan.each
                refs[-1][0, pl.ds(start, plan.each)] = ref[half]

    return pl.pallas_call(
        kernel,
        out_shape=states_shape(1, plan.halves * group),
        in_specs=[SMEM] + [VMEM] * len(parts),
        out_specs=VMEM,
        compiler_params=params(),
        name="assemble_cache",
    )(place, *parts)


def per_device(plan, queries, keys, values, spikes, gain):
    place = jnp.stack([lax.axis_index(a) for a in ("core", "inner", "y", "outer")]).astype(jnp.int32)
    halves = range(plan.halves)

    def swap(array, axes, offset, size):
        return lax.ppermute(array, axes, [(i, i ^ offset) for i in range(size)])

    def in_level(array, offset):
        return swap(array, ("inner", "y"), offset, plan.plane)

    def to_later(array, distance):
        pairs = [(i, i + distance) for i in range(plan.n_outer - distance)]
        return lax.ppermute(array, "outer", pairs)

    gain = gain.reshape(1, plan.width)
    arrays = decode(plan, place, spikes, keys, values)
    parts = [arrays[k : k + plan.halves] for k in range(0, len(arrays), plan.halves)]

    def with_siblings(mine, theirs):
        return [(a, swap(b, "core", 1, CORES)) for a, b in zip(mine, theirs)]

    key, value = with_siblings(*parts[0:2]), with_siblings(*parts[2:4])
    spiked = spike_queries(plan, place, queries, [*parts[4], *parts[5]])
    query = with_siblings(spiked[: plan.halves], spiked[plan.halves :])

    after = [query[0][0]]
    of_core = []
    for half in halves:
        of_core.append(core_states(plan, place, key[half][0], value[half][0], half, after))
        after = [of_core[half]]
    own, first, others = [], [], []

    def owner_stage(half, after):
        with_gain = gain if half == 0 else None
        mine, of_first, *sends = chunk_states(
            plan, place, of_core[half], key[half][1], value[half][1], half, after, with_gain
        )
        own.append(mine)
        first.append(of_first)
        others.append([in_level(a, o) for o, a in enumerate(sends, 1)])

    of_group = [list(range(y, plan.plane, plan.n_y)) for y in range(plan.n_y)]
    abroad = [o for offsets in of_group[1:] for o in offsets]

    def part_of(half, offsets, carry, after, local=None):
        return attend(
            plan,
            place,
            query[half],
            key[half],
            value[half],
            [carry[o] for o in offsets],
            first[half],
            others[0][offsets[0] % plan.n_y - 1] if offsets[0] % plan.n_y else gain,
            half,
            offsets,
            after,
            local,
        )

    def carry_stage(half, after):
        sends = carries(plan, place, own[half], others[half], levels[half], half, abroad, after)
        return sends[0], {o: in_level(a, o) for o, a in zip(abroad, sends)}

    parts = []

    def send_stage(half, carry, after, local):
        for y in range(1, plan.n_y):
            part = part_of(half, of_group[y], carry, after, local.get(y))
            parts.append((swap(part, "y", y, plan.n_y), half, of_group[y]))
            after = [part]
        return after

    after = []
    for half in halves:
        owner_stage(half, after)
        after = [own[-1], *[a for _, a in query]]
    levels = []
    for half in halves:
        level = level_states(plan, own[half], others[half][::-1], half, after)
        levels.append([to_later(level, d) for d in range(1, plan.n_outer)])
        after = [level]
    carry, local = [], {}
    for half in halves:
        done, of_half = carry_stage(half, after)
        carry.append(of_half)
        after = [done]
        for y in range(1, plan.n_y):
            if half == 0:
                local[y] = attend_local(plan, place, query[0], key[0], value[0], 0, of_group[y], after)
                after = [local[y]]
    for half in halves:
        after = send_stage(half, carry[half], after, {} if half else local)
    sends = own_carries(plan, place, own, others, levels, of_group[0], after)
    own_carry = {o: in_level(a, o) if o else a for o, a in zip(of_group[0], sends)}
    caches = [
        swap(a, "inner", o, plan.n_inner) if o else a
        for o, a in enumerate(sends[len(of_group[0]) :])
    ]
    early = []
    for half in halves:
        part = part_of(half, of_group[0], own_carry, after)
        early.append((part, half, of_group[0]))
        after = [part]
    out = assemble(plan, place, early + parts[:-1])
    out = assemble(plan, place, parts[-1:], out)
    return out, assemble_cache(plan, place, caches)


def solution(mesh):
    tokens = P(("outer", "inner", "y", "core"), None)
    seq, head = ("outer", "inner"), ("y", "core")

    def whole(queries, keys, values, spikes, gain):
        plan = Plan(mesh, spikes.shape[0] // mesh.size, spikes.shape[1])
        sizes = (plan.n_outer, plan.n_inner, plan.n_y, CORES)
        split = Mesh(mesh.devices.reshape(sizes), ("outer", "inner", "y", "core"))
        return jax.shard_map(
            functools.partial(per_device, plan),
            mesh=split,
            in_specs=(tokens, tokens, tokens, tokens, P(head)),
            out_specs=(P(seq, head), P(seq, head, None, None)),
            check_vma=False,
        )(queries, keys, values, spikes, gain)

    return whole
```

```python
import functools

import jax
import jax.numpy as jnp
from jax import lax
from jax.experimental import pallas as pl
from jax.experimental.pallas import tpu as pltpu
from jax.sharding import Mesh
from jax.sharding import PartitionSpec as P

HD = 128
SCORE_SCALE = HD ** (-0.5)
CORES = 2
VMEM_BYTES = 24 * 1024 * 1024
DECODE_VMEM_BYTES = 46 * 1024 * 1024
PAD = 16
TOP = 32767.0

VMEM = pl.BlockSpec(memory_space=pltpu.VMEM)
SMEM = pl.BlockSpec(memory_space=pltpu.SMEM)
HBM = pl.BlockSpec(memory_space=pltpu.HBM)
ANY = pl.BlockSpec(memory_space=pl.ANY)


def params(vmem=VMEM_BYTES):
    return pltpu.CompilerParams(vmem_limit_bytes=vmem)


def cost(flops, bytes_accessed):
    return pl.CostEstimate(flops=flops, bytes_accessed=bytes_accessed, transcendentals=0)


class Plan:
    def __init__(self, mesh, rows, model):
        n_seq, n_head = mesh.shape["seq"], mesh.shape["head"]
        self.n_y = n_head // CORES
        self.width = model // n_head
        group = self.width // HD
        self.n_inner = 2 if n_seq % 2 == 0 and group % 2 == 0 else 1
        self.n_outer = n_seq // self.n_inner
        self.halves = 2 if group // self.n_inner % 2 == 0 else 1
        self.each = group // (self.n_inner * self.halves)
        self.plane = self.n_inner * self.n_y
        self.rows = rows
        self.block = rows * n_head
        self.piece = self.each * HD
        self.half_width = self.width // self.halves


def counts_of(spikes):
    one, two = jnp.ones_like(spikes), jnp.full_like(spikes, 2)
    zero = jnp.zeros_like(spikes)

    def ternary(rest, unit):
        return jnp.where(rest >= 2 * unit, two, jnp.where(rest >= unit, one, zero))

    value = ternary(spikes, 9)
    rest = spikes - 9 * value
    key = ternary(rest, 3)
    return value, key, rest - 3 * key


def sides(plan, place_ref):
    width = plan.half_width
    for y in range(plan.n_y):
        for side in range(CORES):
            of = place_ref[0] if side == 0 else 1 - place_ref[0]
            for half in range(plan.halves):
                start = ((y * CORES + of) * plan.halves + half) * width
                at = pl.ds(pl.multiple_of(start, width), width)
                yield side, half, slice(y * width, (y + 1) * width), at


def decode(plan, place, spikes, keys, values):
    rows, model = spikes.shape
    step = min(rows, 32)
    chunks = rows // step
    n_out = 3 * CORES * plan.halves

    def kernel(place_ref, *refs):
        sources, *outs, b0, b1, b2, sems = refs[:3], *refs[3:]
        buffers = (b0, b1, b2)

        def fetch(chunk, index):
            at = pl.ds(chunk * step, step)
            return pltpu.make_async_copy(
                sources[index].at[at], buffers[index].at[at], sems.at[chunk, index]
            )

        for chunk in range(chunks):
            for index in range(3):
                fetch(chunk, index).start()

        @pl.loop(0, chunks)
        def _(chunk):
            for index in range(3):
                fetch(chunk, index).wait()
            at = pl.ds(pl.multiple_of(chunk * step, step), step)
            for side, half, mine, columns in sides(plan, place_ref):
                spikes = buffers[0][at, columns].astype(jnp.float32).astype(jnp.bfloat16)
                value, key, query = counts_of(spikes)
                spiked = (buffers[1][at, columns] * key, buffers[2][at, columns] * value, query)
                for index, array in enumerate(spiked):
                    outs[(index * CORES + side) * plan.halves + half][at, mine] = array

    return pl.pallas_call(
        kernel,
        out_shape=[jax.ShapeDtypeStruct((rows, plan.n_y * plan.half_width), jnp.bfloat16)] * n_out,
        in_specs=[SMEM] + [HBM] * 3,
        out_specs=[VMEM] * n_out,
        scratch_shapes=[
            pltpu.VMEM((rows, model), jnp.int32),
            pltpu.VMEM((rows, model), jnp.bfloat16),
            pltpu.VMEM((rows, model), jnp.bfloat16),
            pltpu.SemaphoreType.DMA((chunks, 3)),
        ],
        compiler_params=params(DECODE_VMEM_BYTES),
        cost_estimate=cost(rows * model * 4, rows * model * 14),
        name="decode",
    )(place, spikes, keys, values)


def spike_queries(plan, place, queries, counts):
    n = len(counts)

    def kernel(place_ref, queries_ref, *refs):
        for side, half, mine, columns in sides(plan, place_ref):
            at = side * plan.halves + half
            refs[n + at][:, mine] = queries_ref[:, columns] * refs[at][:, mine]

    return pl.pallas_call(
        kernel,
        out_shape=[jax.ShapeDtypeStruct(a.shape, jnp.bfloat16) for a in counts],
        in_specs=[SMEM] + [VMEM] * (1 + n),
        out_specs=[VMEM] * n,
        compiler_params=params(),
        cost_estimate=cost(queries.size, queries.size * 6),
        name="spike_queries",
    )(place, queries, *counts)


def contract_rows(left, right):
    return lax.dot_general(
        left, right, (((0,), (0,)), ((), ())), preferred_element_type=jnp.float32
    )


def contract_columns(left, right):
    return lax.dot_general(
        left, right, (((1,), (1,)), ((), ())), preferred_element_type=jnp.float32
    )


def code(states, ref):
    line = lax.broadcasted_iota(jnp.int32, (PAD, HD), 0)
    exponents = jnp.zeros((PAD, HD), jnp.float32)
    for i, state in enumerate(states):
        top = jnp.max(jnp.abs(state), axis=0, keepdims=True)
        exponent = jnp.floor(jnp.log2(jnp.maximum(top, 1e-30))) + 1
        scaled = jnp.round(state * jnp.exp2(15 - exponent))
        scaled = jnp.clip(scaled, -TOP, TOP)
        ref[i * HD : (i + 1) * HD] = scaled.astype(jnp.int32).astype(jnp.int16)
        exponents = jnp.where(line == i, exponent, exponents)
    ref[len(states) * HD : len(states) * HD + PAD] = exponents.astype(jnp.int32).astype(jnp.int16)


def decoded(ref):
    count = ref.shape[0] // HD
    exponents = ref[count * HD : count * HD + PAD].astype(jnp.int32).astype(jnp.float32)
    return [
        ref[i * HD : (i + 1) * HD].astype(jnp.int32).astype(jnp.float32)
        * jnp.exp2(exponents[i : i + 1] - 15)
        for i in range(count)
    ]


def code_gain(gain_ref, ref):
    line = lax.broadcasted_iota(jnp.int32, (PAD // 2, HD), 0)
    gain = jnp.zeros((PAD // 2, HD), jnp.float32)
    for i in range(gain_ref.shape[1] // HD):
        gain = jnp.where(line == i, gain_ref[:, i * HD : (i + 1) * HD], gain)
    coarse = jnp.round(gain * 2.0**12)
    fine = jnp.round((gain - coarse * 2.0**-12) * 2.0**27)
    planes = jnp.concatenate([coarse, fine], axis=0)
    ref[ref.shape[0] - PAD :] = planes.astype(jnp.int32).astype(jnp.int16)


def decoded_gain(ref):
    planes = ref[ref.shape[0] - PAD :].astype(jnp.int32).astype(jnp.float32)
    return planes[: PAD // 2] * 2.0**-12 + planes[PAD // 2 :] * 2.0**-27


def plus(left, right):
    return [a + b for a, b in zip(left, right)]


def total_of(refs, each):
    total = [jnp.zeros((HD, HD), jnp.float32)] * each
    for ref in refs:
        coded = ref.dtype == jnp.int16
        total = plus(total, decoded(ref) if coded else [ref[i] for i in range(each)])
    return total


def coded_shape(heads, more=0):
    return jax.ShapeDtypeStruct((heads * HD + PAD + more, HD), jnp.int16)


def states_shape(*lead):
    return jax.ShapeDtypeStruct((*lead, HD, HD), jnp.float32)


def owned_columns(plan, place_ref, offset, i):
    x = place_ref[1] ^ (offset // plan.n_y)
    y = place_ref[2] ^ (offset % plan.n_y)
    start = ((y * plan.n_inner + x) * plan.each + i) * HD
    return pl.ds(pl.multiple_of(start, HD), HD)


def chunk_states(plan, place, key, value, half, after, gain=None):
    gains = [] if gain is None else [gain]

    def kernel(place_ref, k_ref, k_sib_ref, v_ref, v_sib_ref, *refs):
        own_ref, first_ref, *send_refs = refs[len(gains) + len(after) :]
        is_first = jnp.full((HD, HD), place_ref[0], jnp.int32) == 0
        for offset in (*range(1, plan.plane), 0):
            states = []
            for i in range(plan.each):
                at = owned_columns(plan, place_ref, offset, i)
                mine = contract_rows(v_ref[:, at], k_ref[:, at])
                sib = contract_rows(v_sib_ref[:, at], k_sib_ref[:, at])
                first_ref[offset, i] = jnp.where(is_first, mine, sib)
                states.append(mine + sib)
            if offset:
                code(states, send_refs[offset - 1])
                if gains and offset < plan.n_y:
                    code_gain(refs[0], send_refs[offset - 1])
            else:
                for i, state in enumerate(states):
                    own_ref[i] = state

    heads = plan.plane * plan.each
    return pl.pallas_call(
        kernel,
        out_shape=[states_shape(plan.each), states_shape(plan.plane, plan.each)]
        + [
            coded_shape(plan.each, PAD if gains and o < plan.n_y else 0)
            for o in range(1, plan.plane)
        ],
        in_specs=[SMEM] + [VMEM] * (4 + len(gains)) + [ANY] * len(after),
        out_specs=[VMEM] * (1 + plan.plane),
        compiler_params=params(),
        cost_estimate=cost(
            4 * plan.rows * HD * HD * heads, 8 * plan.rows * HD * heads + 6 * heads * HD * HD
        ),
        name=f"chunk_states_{half}",
    )(place, *key, *value, *gains, *after)


def level_states(plan, own, others, half, after):
    def kernel(own_ref, *refs):
        code(total_of((own_ref, *refs[: len(others)]), plan.each), refs[-1])

    return pl.pallas_call(
        kernel,
        out_shape=coded_shape(plan.each),
        in_specs=[VMEM] * plan.plane + [ANY] * len(after),
        out_specs=VMEM,
        compiler_params=params(),
        cost_estimate=cost(0, plan.plane * plan.each * HD * HD * 2),
        name=f"level_states_{half}",
    )(own, *others, *after)


def carried(plan, place_ref, own, others, levels, offsets):
    x, y = place_ref[1], place_ref[2]
    here = x * plan.n_y + y
    earlier = total_of(levels, plan.each)
    states = [[own[i] for i in range(plan.each)]] + [decoded(ref) for ref in others]

    def add(totals, keep_of):
        for offset, terms in enumerate(states):
            keep = jnp.full((HD, HD), keep_of(here ^ offset), jnp.int32) == 1
            totals = plus(totals, [jnp.where(keep, s, 0.0) for s in terms])
        return totals

    before = [add(earlier, lambda chip: (chip < here ^ o).astype(jnp.int32)) for o in offsets]
    blocks = [
        add(earlier, lambda chip: (chip // plan.n_y <= x ^ o).astype(jnp.int32))
        for o in range(plan.n_inner)
    ]
    return before, blocks


def carries(plan, place, own, others, levels, half, offsets, after):
    n_others, n_levels = len(others), len(levels)

    def kernel(place_ref, own_ref, *refs):
        before, _ = carried(
            plan, place_ref, own_ref, refs[:n_others], refs[n_others : n_others + n_levels], offsets
        )
        for states, ref in zip(before, refs[n_others + n_levels + len(after) :]):
            code(states, ref)

    return pl.pallas_call(
        kernel,
        out_shape=[coded_shape(plan.each)] * len(offsets),
        in_specs=[SMEM] + [VMEM] * (1 + n_others + n_levels) + [ANY] * len(after),
        out_specs=[VMEM] * len(offsets),
        compiler_params=params(),
        cost_estimate=cost(0, (plan.plane * 4 + n_levels) * plan.each * HD * HD * 2),
        name=f"carries_{half}",
    )(place, own, *others, *levels, *after)


def own_carries(plan, place, own, others, levels, offsets, after):
    n_others = len(others[0])
    operands = [(own[h], *others[h], *levels[h]) for h in range(plan.halves)]
    starts = [sum(map(len, operands[:h])) for h in range(plan.halves + 1)]

    def kernel(place_ref, *refs):
        outs = refs[starts[-1] + len(after) :]
        befores = [[] for _ in offsets]
        for half in range(plan.halves):
            own_ref, *of_half = refs[starts[half] : starts[half + 1]]
            before, blocks = carried(
                plan, place_ref, own_ref, of_half[:n_others], of_half[n_others:], offsets
            )
            for all_states, states in zip(befores, before):
                all_states.extend(states)
            for offset, (totals, ref) in enumerate(zip(blocks, outs[len(offsets) :])):
                block = place_ref[3] * plan.n_inner + (place_ref[1] ^ offset)
                seen = jnp.full((1, HD), (block + 1) * plan.block, jnp.int32).astype(jnp.float32)
                for i, total in enumerate(totals):
                    ref[half, i] = total.T * lax.rsqrt(seen)
        for states, ref in zip(befores, outs):
            code(states, ref)

    return pl.pallas_call(
        kernel,
        out_shape=[coded_shape(plan.halves * plan.each)] * len(offsets)
        + [states_shape(plan.halves, plan.each)] * plan.n_inner,
        in_specs=[SMEM] + [VMEM] * starts[-1] + [ANY] * len(after),
        out_specs=[VMEM] * (len(offsets) + plan.n_inner),
        compiler_params=params(),
        cost_estimate=cost(0, plan.plane * plan.each * HD * HD * 20),
        name="own_carries",
    )(place, *[a for arrays in operands for a in arrays], *after)


def attend_local(plan, place, query, key, value, half, offsets, after):
    rows = plan.rows

    def kernel(place_ref, q_ref, q_sib_ref, k_ref, k_sib_ref, v_ref, v_sib_ref, *refs):
        for piece, offset in enumerate(offsets):
            for i in range(plan.each):
                at = owned_columns(plan, place_ref, offset, i)
                out_at = slice(piece * plan.piece + i * HD, piece * plan.piece + (i + 1) * HD)
                refs[-1][0, :, out_at] = local_part(q_ref, k_ref, v_ref, at)
                refs[-1][1, :, out_at] = local_part(q_sib_ref, k_sib_ref, v_sib_ref, at)

    heads = len(offsets) * plan.each
    return pl.pallas_call(
        kernel,
        out_shape=jax.ShapeDtypeStruct((CORES, rows, heads * HD), jnp.float32),
        in_specs=[SMEM] + [VMEM] * 6 + [ANY] * len(after),
        out_specs=VMEM,
        compiler_params=params(),
        cost_estimate=cost(heads * 8 * rows * rows * HD, 16 * rows * heads * HD),
        name=f"attend_local_{half}_" + "_".join(map(str, offsets)),
    )(place, *query, *key, *value, *after)


def local_part(q_ref, k_ref, v_ref, at):
    rows = q_ref.shape[0]
    causal = lax.broadcasted_iota(jnp.int32, (rows, rows), 0) >= lax.broadcasted_iota(
        jnp.int32, (rows, rows), 1
    )
    scores = contract_columns(q_ref[:, at], k_ref[:, at]) * SCORE_SCALE
    weights = jnp.where(causal, scores, 0.0).astype(jnp.bfloat16)
    return jnp.dot(weights, v_ref[:, at], preferred_element_type=jnp.float32)


def finished(queries, local, carried, gain):
    carried = carried * SCORE_SCALE
    high = carried.astype(jnp.bfloat16)
    low = (carried - high.astype(jnp.float32)).astype(jnp.bfloat16)
    both = contract_columns(queries, jnp.concatenate([high, low], axis=0))
    raw = local + (both[:, :HD] + both[:, HD:])
    mean = jnp.mean(raw * raw, axis=-1, keepdims=True)
    return (raw * lax.rsqrt(mean + 1e-06) * gain).astype(jnp.bfloat16)


def attend(
    plan, place, query, key, value, carry, first, gain, half, offsets, after=(), local=None
):
    rows = plan.rows
    operands = [*query, local] if local is not None else [*query, *key, *value]
    n = len(operands)

    def kernel(place_ref, *refs):
        core = place_ref[0]
        first_ref, gain_ref, *carry_refs = refs[n : n + 2 + len(offsets)]
        out_ref = refs[-1]
        is_second = jnp.full((HD, HD), core, jnp.int32) == 1
        coded_gain = gain_ref.dtype == jnp.int16
        line = lax.broadcasted_iota(jnp.int32, (PAD // 2, HD), 0)
        for piece, offset in enumerate(offsets):
            x = place_ref[1] ^ (offset // plan.n_y)
            carry_states = decoded(carry_refs[piece])
            skip = half * plan.each if len(carry_states) > plan.each else 0
            for i in range(plan.each):
                at = owned_columns(plan, place_ref, offset, i)
                head = (half * plan.n_inner + x) * plan.each + i
                if coded_gain:
                    gain = jnp.where(line == head, decoded_gain(gain_ref), 0.0)
                    gain = jnp.sum(gain, axis=0, keepdims=True)
                else:
                    gain = gain_ref[:, pl.ds(pl.multiple_of(head * HD, HD), HD)]
                out_at = slice(piece * plan.piece + i * HD, piece * plan.piece + (i + 1) * HD)
                carried = carry_states[skip + i]
                first = first_ref[offset, i]
                for side in range(CORES):
                    if local is None:
                        raw = local_part(refs[side], refs[2 + side], refs[4 + side], at)
                    else:
                        raw = refs[2][side, :, out_at]
                    behind = is_second if side == 0 else ~is_second
                    state = carried + jnp.where(behind, first, 0.0)
                    of = core if side == 0 else 1 - core
                    out_rows = pl.ds(pl.multiple_of(of * rows, rows), rows)
                    out_ref[out_rows, out_at] = finished(refs[side][:, at], raw, state, gain)

    heads = len(offsets) * plan.each
    return pl.pallas_call(
        kernel,
        out_shape=jax.ShapeDtypeStruct((CORES * rows, heads * HD), jnp.bfloat16),
        in_specs=[SMEM] + [VMEM] * (n + 2 + len(offsets)) + [ANY] * len(after),
        out_specs=VMEM,
        compiler_params=params(),
        cost_estimate=cost(
            heads * (8 * rows * rows * HD + 8 * rows * HD * HD), 16 * rows * heads * HD
        ),
        name=f"attend_{half}_" + "_".join(map(str, offsets)),
    )(place, *operands, first, gain, *carry, *after)


def assemble(plan, place, parts, into=None):
    rows = CORES * plan.rows
    copies = [(n, piece, half, o) for n, (_, half, os) in enumerate(parts) for piece, o in enumerate(os)]

    def kernel(place_ref, *refs):
        out_ref, sems = refs[-2:]
        started = []
        for at, (n, piece, half, offset) in enumerate(copies):
            x = place_ref[1] ^ (offset // plan.n_y)
            y = place_ref[2] ^ (offset % plan.n_y)
            column = (half * plan.n_inner + x) * plan.piece
            to_rows = pl.ds(pl.multiple_of(y * rows, rows), rows)
            to_columns = pl.ds(pl.multiple_of(column, plan.piece), plan.piece)
            started.append(
                pltpu.make_async_copy(
                    refs[n].at[:, pl.ds(piece * plan.piece, plan.piece)],
                    out_ref.at[to_rows, to_columns],
                    sems.at[at],
                )
            )
            started[-1].start()
        for copy in started:
            copy.wait()

    arrays = [array for array, _, _ in parts]
    aliased = [] if into is None else [into]
    return pl.pallas_call(
        kernel,
        out_shape=jax.ShapeDtypeStruct((plan.n_y * rows, plan.width), jnp.bfloat16),
        in_specs=[SMEM] + [VMEM] * len(arrays) + [HBM] * len(aliased),
        out_specs=HBM,
        scratch_shapes=[pltpu.SemaphoreType.DMA((len(copies),))],
        input_output_aliases={1 + len(arrays): 0} if aliased else {},
        compiler_params=params(),
        name="assemble" if into is None else "finish",
    )(place, *arrays, *aliased)


def assemble_cache(plan, place, parts):
    group = plan.n_inner * plan.each

    def kernel(place_ref, *refs):
        for half in range(plan.halves):
            for offset, ref in enumerate(refs[:-1]):
                start = half * group + (place_ref[1] ^ offset) * plan.each
                refs[-1][0, pl.ds(start, plan.each)] = ref[half]

    return pl.pallas_call(
        kernel,
        out_shape=states_shape(1, plan.halves * group),
        in_specs=[SMEM] + [VMEM] * len(parts),
        out_specs=VMEM,
        compiler_params=params(),
        name="assemble_cache",
    )(place, *parts)


def per_device(plan, queries, keys, values, spikes, gain):
    place = jnp.stack([lax.axis_index(a) for a in ("core", "inner", "y", "outer")]).astype(jnp.int32)
    halves = range(plan.halves)

    def swap(array, axes, offset, size):
        return lax.ppermute(array, axes, [(i, i ^ offset) for i in range(size)])

    def in_level(array, offset):
        return swap(array, ("inner", "y"), offset, plan.plane)

    def to_later(array, distance):
        pairs = [(i, i + distance) for i in range(plan.n_outer - distance)]
        return lax.ppermute(array, "outer", pairs)

    gain = gain.reshape(1, plan.width)
    arrays = decode(plan, place, spikes, keys, values)
    parts = [arrays[k : k + plan.halves] for k in range(0, len(arrays), plan.halves)]

    def with_siblings(mine, theirs):
        return [(a, swap(b, "core", 1, CORES)) for a, b in zip(mine, theirs)]

    key, value = with_siblings(*parts[0:2]), with_siblings(*parts[2:4])
    spiked = spike_queries(plan, place, queries, [*parts[4], *parts[5]])
    query = with_siblings(spiked[: plan.halves], spiked[plan.halves :])

    own, first, others = [], [], []

    def owner_stage(half, after):
        with_gain = gain if half == 0 else None
        mine, of_first, *sends = chunk_states(
            plan, place, key[half], value[half], half, after, with_gain
        )
        own.append(mine)
        first.append(of_first)
        others.append([in_level(a, o) for o, a in enumerate(sends, 1)])

    of_group = [list(range(y, plan.plane, plan.n_y)) for y in range(plan.n_y)]
    abroad = [o for offsets in of_group[1:] for o in offsets]

    def part_of(half, offsets, carry, after, local=None):
        return attend(
            plan,
            place,
            query[half],
            key[half],
            value[half],
            [carry[o] for o in offsets],
            first[half],
            others[0][offsets[0] % plan.n_y - 1] if offsets[0] % plan.n_y else gain,
            half,
            offsets,
            after,
            local,
        )

    def carry_stage(half, after):
        sends = carries(plan, place, own[half], others[half], levels[half], half, abroad, after)
        return sends[0], {o: in_level(a, o) for o, a in zip(abroad, sends)}

    parts = []

    def send_stage(half, carry, after, local):
        for y in range(1, plan.n_y):
            part = part_of(half, of_group[y], carry, after, local.get(y))
            parts.append((swap(part, "y", y, plan.n_y), half, of_group[y]))
            after = [part]
        return after

    after = [query[0][0]]
    for half in halves:
        owner_stage(half, after)
        after = [own[-1], *[a for _, a in query]]
    levels = []
    for half in halves:
        level = level_states(plan, own[half], others[half][::-1], half, after)
        levels.append([to_later(level, d) for d in range(1, plan.n_outer)])
        after = [level]
    local = {}
    for y in range(1, plan.n_y):
        local[y] = attend_local(plan, place, query[0], key[0], value[0], 0, of_group[y], after)
        after = [local[y]]
    carry = []
    for half in halves:
        done, of_half = carry_stage(half, after)
        carry.append(of_half)
        after = [done]
    for half in halves:
        after = send_stage(half, carry[half], after, {} if half else local)
    sends = own_carries(plan, place, own, others, levels, of_group[0], after)
    own_carry = {o: in_level(a, o) if o else a for o, a in zip(of_group[0], sends)}
    caches = [
        swap(a, "inner", o, plan.n_inner) if o else a
        for o, a in enumerate(sends[len(of_group[0]) :])
    ]
    early = []
    for half in halves:
        part = part_of(half, of_group[0], own_carry, after)
        early.append((part, half, of_group[0]))
        after = [part]
    out = assemble(plan, place, early + parts[:-1])
    out = assemble(plan, place, parts[-1:], out)
    return out, assemble_cache(plan, place, caches)


def solution(mesh):
    tokens = P(("outer", "inner", "y", "core"), None)
    seq, head = ("outer", "inner"), ("y", "core")

    def whole(queries, keys, values, spikes, gain):
        plan = Plan(mesh, spikes.shape[0] // mesh.size, spikes.shape[1])
        sizes = (plan.n_outer, plan.n_inner, plan.n_y, CORES)
        split = Mesh(mesh.devices.reshape(sizes), ("outer", "inner", "y", "core"))
        return jax.shard_map(
            functools.partial(per_device, plan),
            mesh=split,
            in_specs=(tokens, tokens, tokens, tokens, P(head)),
            out_specs=(P(seq, head), P(seq, head, None, None)),
            check_vma=False,
        )(queries, keys, values, spikes, gain)

    return whole
```

```python
import functools

import jax
import jax.numpy as jnp
from jax import lax
from jax.experimental import pallas as pl
from jax.experimental.pallas import tpu as pltpu
from jax.sharding import Mesh
from jax.sharding import PartitionSpec as P

HD = 128
SCORE_SCALE = HD ** (-0.5)
CORES = 2
VMEM_BYTES = 24 * 1024 * 1024
DECODE_VMEM_BYTES = 46 * 1024 * 1024
PAD = 16
TOP = 32767.0

VMEM = pl.BlockSpec(memory_space=pltpu.VMEM)
HBM = pl.BlockSpec(memory_space=pltpu.HBM)
ANY = pl.BlockSpec(memory_space=pl.ANY)


def params(vmem=VMEM_BYTES):
    return pltpu.CompilerParams(vmem_limit_bytes=vmem)


def cost(flops, bytes_accessed):
    return pl.CostEstimate(flops=flops, bytes_accessed=bytes_accessed, transcendentals=0)


def at_place(kernel):
    def placed(*refs):
        place = [lax.axis_index(a) for a in ("core", "inner", "y", "outer")]
        kernel(place, *refs)

    return placed


class Plan:
    def __init__(self, mesh, rows, model):
        n_seq, n_head = mesh.shape["seq"], mesh.shape["head"]
        self.n_y = n_head // CORES
        self.width = model // n_head
        group = self.width // HD
        self.n_inner = 2 if n_seq % 2 == 0 and group % 2 == 0 else 1
        self.n_outer = n_seq // self.n_inner
        self.halves = 2 if group // self.n_inner % 2 == 0 else 1
        self.each = group // (self.n_inner * self.halves)
        self.plane = self.n_inner * self.n_y
        self.rows = rows
        self.block = rows * n_head
        self.piece = self.each * HD
        self.half_width = self.width // self.halves


def counts_of(spikes):
    one, two = jnp.ones_like(spikes), jnp.full_like(spikes, 2)
    zero = jnp.zeros_like(spikes)

    def ternary(rest, unit):
        return jnp.where(rest >= 2 * unit, two, jnp.where(rest >= unit, one, zero))

    value = ternary(spikes, 9)
    rest = spikes - 9 * value
    key = ternary(rest, 3)
    return value, key, rest - 3 * key


def sides(plan, core):
    width = plan.half_width
    for y in range(plan.n_y):
        for side in range(CORES):
            of = core if side == 0 else 1 - core
            for half in range(plan.halves):
                start = ((y * CORES + of) * plan.halves + half) * width
                at = pl.ds(pl.multiple_of(start, width), width)
                yield side, half, slice(y * width, (y + 1) * width), at


def decode(plan, spikes, keys, values):
    rows, model = spikes.shape
    step = min(rows, 32)
    chunks = rows // step
    n_out = 3 * CORES * plan.halves

    def kernel(*refs):
        core = lax.axis_index("core")
        sources, *outs, b0, b1, b2, sems = refs[:3], *refs[3:]
        buffers = (b0, b1, b2)

        def fetch(chunk, index):
            at = pl.ds(chunk * step, step)
            return pltpu.make_async_copy(
                sources[index].at[at], buffers[index].at[at], sems.at[chunk, index]
            )

        for chunk in range(chunks):
            for index in range(3):
                fetch(chunk, index).start()

        @pl.loop(0, chunks)
        def _(chunk):
            for index in range(3):
                fetch(chunk, index).wait()
            at = pl.ds(pl.multiple_of(chunk * step, step), step)
            for side, half, mine, columns in sides(plan, core):
                spikes = buffers[0][at, columns].astype(jnp.float32).astype(jnp.bfloat16)
                value, key, query = counts_of(spikes)
                spiked = (buffers[1][at, columns] * key, buffers[2][at, columns] * value, query)
                for index, array in enumerate(spiked):
                    outs[(index * CORES + side) * plan.halves + half][at, mine] = array

    return pl.pallas_call(
        kernel,
        out_shape=[jax.ShapeDtypeStruct((rows, plan.n_y * plan.half_width), jnp.bfloat16)] * n_out,
        in_specs=[HBM] * 3,
        out_specs=[VMEM] * n_out,
        scratch_shapes=[
            pltpu.VMEM((rows, model), jnp.int32),
            pltpu.VMEM((rows, model), jnp.bfloat16),
            pltpu.VMEM((rows, model), jnp.bfloat16),
            pltpu.SemaphoreType.DMA((chunks, 3)),
        ],
        compiler_params=params(DECODE_VMEM_BYTES),
        cost_estimate=cost(rows * model * 4, rows * model * 14),
        name="decode",
    )(spikes, keys, values)


def spike_queries(plan, queries, counts):
    n = len(counts)

    def kernel(place_ref, queries_ref, *refs):
        for side, half, mine, columns in sides(plan, place_ref[0]):
            at = side * plan.halves + half
            refs[n + at][:, mine] = queries_ref[:, columns] * refs[at][:, mine]

    return pl.pallas_call(
        at_place(kernel),
        out_shape=[jax.ShapeDtypeStruct(a.shape, jnp.bfloat16) for a in counts],
        in_specs=[VMEM] * (1 + n),
        out_specs=[VMEM] * n,
        compiler_params=params(),
        cost_estimate=cost(queries.size, queries.size * 6),
        name="spike_queries",
    )(queries, *counts)


def contract_rows(left, right):
    return lax.dot_general(
        left, right, (((0,), (0,)), ((), ())), preferred_element_type=jnp.float32
    )


def contract_columns(left, right):
    return lax.dot_general(
        left, right, (((1,), (1,)), ((), ())), preferred_element_type=jnp.float32
    )


def code(states, ref):
    line = lax.broadcasted_iota(jnp.int32, (PAD, HD), 0)
    exponents = jnp.zeros((PAD, HD), jnp.float32)
    for i, state in enumerate(states):
        top = jnp.max(jnp.abs(state), axis=0, keepdims=True)
        exponent = jnp.floor(jnp.log2(jnp.maximum(top, 1e-30))) + 1
        scaled = jnp.round(state * jnp.exp2(15 - exponent))
        scaled = jnp.clip(scaled, -TOP, TOP)
        ref[i * HD : (i + 1) * HD] = scaled.astype(jnp.int32).astype(jnp.int16)
        exponents = jnp.where(line == i, exponent, exponents)
    ref[len(states) * HD : len(states) * HD + PAD] = exponents.astype(jnp.int32).astype(jnp.int16)


def decoded(ref):
    count = ref.shape[0] // HD
    exponents = ref[count * HD : count * HD + PAD].astype(jnp.int32).astype(jnp.float32)
    return [
        ref[i * HD : (i + 1) * HD].astype(jnp.int32).astype(jnp.float32)
        * jnp.exp2(exponents[i : i + 1] - 15)
        for i in range(count)
    ]


def code_gain(gain_ref, ref):
    line = lax.broadcasted_iota(jnp.int32, (PAD // 2, HD), 0)
    gain = jnp.zeros((PAD // 2, HD), jnp.float32)
    for i in range(gain_ref.shape[1] // HD):
        gain = jnp.where(line == i, gain_ref[:, i * HD : (i + 1) * HD], gain)
    coarse = jnp.round(gain * 2.0**12)
    fine = jnp.round((gain - coarse * 2.0**-12) * 2.0**27)
    planes = jnp.concatenate([coarse, fine], axis=0)
    ref[ref.shape[0] - PAD :] = planes.astype(jnp.int32).astype(jnp.int16)


def decoded_gain(ref):
    planes = ref[ref.shape[0] - PAD :].astype(jnp.int32).astype(jnp.float32)
    return planes[: PAD // 2] * 2.0**-12 + planes[PAD // 2 :] * 2.0**-27


def plus(left, right):
    return [a + b for a, b in zip(left, right)]


def total_of(refs, each):
    total = [jnp.zeros((HD, HD), jnp.float32)] * each
    for ref in refs:
        coded = ref.dtype == jnp.int16
        total = plus(total, decoded(ref) if coded else [ref[i] for i in range(each)])
    return total


def coded_shape(heads, more=0):
    return jax.ShapeDtypeStruct((heads * HD + PAD + more, HD), jnp.int16)


def states_shape(*lead):
    return jax.ShapeDtypeStruct((*lead, HD, HD), jnp.float32)


def owned_columns(plan, place_ref, offset, i):
    x = place_ref[1] ^ (offset // plan.n_y)
    y = place_ref[2] ^ (offset % plan.n_y)
    start = ((y * plan.n_inner + x) * plan.each + i) * HD
    return pl.ds(pl.multiple_of(start, HD), HD)


def chunk_states(plan, key, value, half, after, gain=None):
    gains = [] if gain is None else [gain]

    def kernel(place_ref, k_ref, k_sib_ref, v_ref, v_sib_ref, *refs):
        own_ref, first_ref, *send_refs = refs[len(gains) + len(after) :]
        is_first = jnp.full((HD, HD), place_ref[0], jnp.int32) == 0
        for offset in (*range(1, plan.plane), 0):
            states = []
            for i in range(plan.each):
                at = owned_columns(plan, place_ref, offset, i)
                mine = contract_rows(v_ref[:, at], k_ref[:, at])
                sib = contract_rows(v_sib_ref[:, at], k_sib_ref[:, at])
                first_ref[offset, i] = jnp.where(is_first, mine, sib)
                states.append(mine + sib)
            if offset:
                code(states, send_refs[offset - 1])
                if gains and offset < plan.n_y:
                    code_gain(refs[0], send_refs[offset - 1])
            else:
                for i, state in enumerate(states):
                    own_ref[i] = state

    heads = plan.plane * plan.each
    return pl.pallas_call(
        at_place(kernel),
        out_shape=[states_shape(plan.each), states_shape(plan.plane, plan.each)]
        + [
            coded_shape(plan.each, PAD if gains and o < plan.n_y else 0)
            for o in range(1, plan.plane)
        ],
        in_specs=[VMEM] * (4 + len(gains)) + [ANY] * len(after),
        out_specs=[VMEM] * (1 + plan.plane),
        compiler_params=params(),
        cost_estimate=cost(
            4 * plan.rows * HD * HD * heads, 8 * plan.rows * HD * heads + 6 * heads * HD * HD
        ),
        name=f"chunk_states_{half}",
    )(*key, *value, *gains, *after)


def level_states(plan, own, others, half, after):
    def kernel(own_ref, *refs):
        code(total_of((own_ref, *refs[: len(others)]), plan.each), refs[-1])

    return pl.pallas_call(
        kernel,
        out_shape=coded_shape(plan.each),
        in_specs=[VMEM] * plan.plane + [ANY] * len(after),
        out_specs=VMEM,
        compiler_params=params(),
        cost_estimate=cost(0, plan.plane * plan.each * HD * HD * 2),
        name=f"level_states_{half}",
    )(own, *others, *after)


def carried(plan, place_ref, own, others, levels, offsets):
    x, y = place_ref[1], place_ref[2]
    here = x * plan.n_y + y
    earlier = total_of(levels, plan.each)
    states = [[own[i] for i in range(plan.each)]] + [decoded(ref) for ref in others]

    def add(totals, keep_of):
        for offset, terms in enumerate(states):
            keep = jnp.full((HD, HD), keep_of(here ^ offset), jnp.int32) == 1
            totals = plus(totals, [jnp.where(keep, s, 0.0) for s in terms])
        return totals

    before = [add(earlier, lambda chip: (chip < here ^ o).astype(jnp.int32)) for o in offsets]
    blocks = [
        add(earlier, lambda chip: (chip // plan.n_y <= x ^ o).astype(jnp.int32))
        for o in range(plan.n_inner)
    ]
    return before, blocks


def carries(plan, own, others, levels, half, offsets, after):
    n_others, n_levels = len(others), len(levels)

    def kernel(place_ref, own_ref, *refs):
        before, _ = carried(
            plan, place_ref, own_ref, refs[:n_others], refs[n_others : n_others + n_levels], offsets
        )
        for states, ref in zip(before, refs[n_others + n_levels + len(after) :]):
            code(states, ref)

    return pl.pallas_call(
        at_place(kernel),
        out_shape=[coded_shape(plan.each)] * len(offsets),
        in_specs=[VMEM] * (1 + n_others + n_levels) + [ANY] * len(after),
        out_specs=[VMEM] * len(offsets),
        compiler_params=params(),
        cost_estimate=cost(0, (plan.plane * 4 + n_levels) * plan.each * HD * HD * 2),
        name=f"carries_{half}",
    )(own, *others, *levels, *after)


def own_carries(plan, own, others, levels, offsets, after):
    n_others = len(others[0])
    operands = [(own[h], *others[h], *levels[h]) for h in range(plan.halves)]
    starts = [sum(map(len, operands[:h])) for h in range(plan.halves + 1)]

    def kernel(place_ref, *refs):
        outs = refs[starts[-1] + len(after) :]
        befores = [[] for _ in offsets]
        for half in range(plan.halves):
            own_ref, *of_half = refs[starts[half] : starts[half + 1]]
            before, blocks = carried(
                plan, place_ref, own_ref, of_half[:n_others], of_half[n_others:], offsets
            )
            for all_states, states in zip(befores, before):
                all_states.extend(states)
            for offset, (totals, ref) in enumerate(zip(blocks, outs[len(offsets) :])):
                block = place_ref[3] * plan.n_inner + (place_ref[1] ^ offset)
                seen = jnp.full((1, HD), (block + 1) * plan.block, jnp.int32).astype(jnp.float32)
                for i, total in enumerate(totals):
                    ref[half, i] = total.T * lax.rsqrt(seen)
        for states, ref in zip(befores, outs):
            code(states, ref)

    return pl.pallas_call(
        at_place(kernel),
        out_shape=[coded_shape(plan.halves * plan.each)] * len(offsets)
        + [states_shape(plan.halves, plan.each)] * plan.n_inner,
        in_specs=[VMEM] * starts[-1] + [ANY] * len(after),
        out_specs=[VMEM] * (len(offsets) + plan.n_inner),
        compiler_params=params(),
        cost_estimate=cost(0, plan.plane * plan.each * HD * HD * 20),
        name="own_carries",
    )(*[a for arrays in operands for a in arrays], *after)


def local_part(q_ref, k_ref, v_ref, at):
    rows = q_ref.shape[0]
    causal = lax.broadcasted_iota(jnp.int32, (rows, rows), 0) >= lax.broadcasted_iota(
        jnp.int32, (rows, rows), 1
    )
    scores = contract_columns(q_ref[:, at], k_ref[:, at]) * SCORE_SCALE
    weights = jnp.where(causal, scores, 0.0).astype(jnp.bfloat16)
    return jnp.dot(weights, v_ref[:, at], preferred_element_type=jnp.float32)


def finished(queries, local, carried, gain):
    carried = carried * SCORE_SCALE
    high = carried.astype(jnp.bfloat16)
    low = (carried - high.astype(jnp.float32)).astype(jnp.bfloat16)
    both = contract_columns(queries, jnp.concatenate([high, low], axis=0))
    raw = local + (both[:, :HD] + both[:, HD:])
    mean = jnp.mean(raw * raw, axis=-1, keepdims=True)
    return (raw * lax.rsqrt(mean + 1e-06) * gain).astype(jnp.bfloat16)


def attend(plan, query, key, value, carry, first, gain, half, offsets, after):
    rows = plan.rows
    operands = [*query, *key, *value]
    n = len(operands)

    def kernel(place_ref, *refs):
        core = place_ref[0]
        first_ref, gain_ref, *carry_refs = refs[n : n + 2 + len(offsets)]
        out_ref = refs[-1]
        is_second = jnp.full((HD, HD), core, jnp.int32) == 1
        coded_gain = gain_ref.dtype == jnp.int16
        line = lax.broadcasted_iota(jnp.int32, (PAD // 2, HD), 0)
        for piece, offset in enumerate(offsets):
            x = place_ref[1] ^ (offset // plan.n_y)
            carry_states = decoded(carry_refs[piece])
            skip = half * plan.each if len(carry_states) > plan.each else 0
            for i in range(plan.each):
                at = owned_columns(plan, place_ref, offset, i)
                head = (half * plan.n_inner + x) * plan.each + i
                if coded_gain:
                    gain = jnp.where(line == head, decoded_gain(gain_ref), 0.0)
                    gain = jnp.sum(gain, axis=0, keepdims=True)
                else:
                    gain = gain_ref[:, pl.ds(pl.multiple_of(head * HD, HD), HD)]
                out_at = slice(piece * plan.piece + i * HD, piece * plan.piece + (i + 1) * HD)
                carried = carry_states[skip + i]
                first = first_ref[offset, i]
                for side in range(CORES):
                    raw = local_part(refs[side], refs[2 + side], refs[4 + side], at)
                    behind = is_second if side == 0 else ~is_second
                    state = carried + jnp.where(behind, first, 0.0)
                    of = core if side == 0 else 1 - core
                    out_rows = pl.ds(pl.multiple_of(of * rows, rows), rows)
                    out_ref[out_rows, out_at] = finished(refs[side][:, at], raw, state, gain)

    heads = len(offsets) * plan.each
    return pl.pallas_call(
        at_place(kernel),
        out_shape=jax.ShapeDtypeStruct((CORES * rows, heads * HD), jnp.bfloat16),
        in_specs=[VMEM] * (n + 2 + len(offsets)) + [ANY] * len(after),
        out_specs=VMEM,
        compiler_params=params(),
        cost_estimate=cost(
            heads * (8 * rows * rows * HD + 8 * rows * HD * HD), 16 * rows * heads * HD
        ),
        name=f"attend_{half}_" + "_".join(map(str, offsets)),
    )(*operands, first, gain, *carry, *after)


def assemble(plan, parts, into=None):
    rows = CORES * plan.rows
    copies = [(n, piece, half, o) for n, (_, half, os) in enumerate(parts) for piece, o in enumerate(os)]

    def kernel(place_ref, *refs):
        out_ref, sems = refs[-2:]
        started = []
        for at, (n, piece, half, offset) in enumerate(copies):
            x = place_ref[1] ^ (offset // plan.n_y)
            y = place_ref[2] ^ (offset % plan.n_y)
            column = (half * plan.n_inner + x) * plan.piece
            to_rows = pl.ds(pl.multiple_of(y * rows, rows), rows)
            to_columns = pl.ds(pl.multiple_of(column, plan.piece), plan.piece)
            started.append(
                pltpu.make_async_copy(
                    refs[n].at[:, pl.ds(piece * plan.piece, plan.piece)],
                    out_ref.at[to_rows, to_columns],
                    sems.at[at],
                )
            )
            started[-1].start()
        for copy in started:
            copy.wait()

    arrays = [array for array, _, _ in parts]
    aliased = [] if into is None else [into]
    return pl.pallas_call(
        at_place(kernel),
        out_shape=jax.ShapeDtypeStruct((plan.n_y * rows, plan.width), jnp.bfloat16),
        in_specs=[VMEM] * len(arrays) + [HBM] * len(aliased),
        out_specs=HBM,
        scratch_shapes=[pltpu.SemaphoreType.DMA((len(copies),))],
        input_output_aliases={len(arrays): 0} if aliased else {},
        compiler_params=params(),
        name="assemble" if into is None else "finish",
    )(*arrays, *aliased)


def assemble_cache(plan, parts):
    group = plan.n_inner * plan.each

    def kernel(place_ref, *refs):
        for half in range(plan.halves):
            for offset, ref in enumerate(refs[:-1]):
                start = half * group + (place_ref[1] ^ offset) * plan.each
                refs[-1][0, pl.ds(start, plan.each)] = ref[half]

    return pl.pallas_call(
        at_place(kernel),
        out_shape=states_shape(1, plan.halves * group),
        in_specs=[VMEM] * len(parts),
        out_specs=VMEM,
        compiler_params=params(),
        name="assemble_cache",
    )(*parts)


def per_device(plan, queries, keys, values, spikes, gain):
    halves = range(plan.halves)

    def swap(array, axes, offset, size):
        return lax.ppermute(array, axes, [(i, i ^ offset) for i in range(size)])

    def in_level(array, offset):
        return swap(array, ("inner", "y"), offset, plan.plane)

    def to_later(array, distance):
        pairs = [(i, i + distance) for i in range(plan.n_outer - distance)]
        return lax.ppermute(array, "outer", pairs)

    gain = gain.reshape(1, plan.width)
    arrays = decode(plan, spikes, keys, values)
    parts = [arrays[k : k + plan.halves] for k in range(0, len(arrays), plan.halves)]

    def with_siblings(mine, theirs):
        return [(a, swap(b, "core", 1, CORES)) for a, b in zip(mine, theirs)]

    key, value = with_siblings(*parts[0:2]), with_siblings(*parts[2:4])
    spiked = spike_queries(plan, queries, [*parts[4], *parts[5]])
    query = with_siblings(spiked[: plan.halves], spiked[plan.halves :])

    own, first, others = [], [], []

    def owner_stage(half, after):
        with_gain = gain if half == 0 else None
        mine, of_first, *sends = chunk_states(
            plan, key[half], value[half], half, after, with_gain
        )
        own.append(mine)
        first.append(of_first)
        others.append([in_level(a, o) for o, a in enumerate(sends, 1)])

    of_group = [list(range(y, plan.plane, plan.n_y)) for y in range(plan.n_y)]
    abroad = [o for offsets in of_group[1:] for o in offsets]

    def part_of(half, offsets, carry, after):
        return attend(
            plan,
            query[half],
            key[half],
            value[half],
            [carry[o] for o in offsets],
            first[half],
            others[0][offsets[0] % plan.n_y - 1] if offsets[0] % plan.n_y else gain,
            half,
            offsets,
            after,
        )

    def carry_stage(half, after):
        sends = carries(plan, own[half], others[half], levels[half], half, abroad, after)
        return sends[0], {o: in_level(a, o) for o, a in zip(abroad, sends)}

    parts = []

    def send_stage(half, carry, after):
        for y in range(1, plan.n_y):
            part = part_of(half, of_group[y], carry, after)
            parts.append((swap(part, "y", y, plan.n_y), half, of_group[y]))
            after = [part]
        return after

    after = [query[0][0]]
    for half in halves:
        owner_stage(half, after)
        after = [own[-1], *[a for _, a in query]]
    levels = []
    for half in halves:
        level = level_states(plan, own[half], others[half][::-1], half, after)
        levels.append([to_later(level, d) for d in range(1, plan.n_outer)])
        after = [level]
    carry = []
    for half in halves:
        done, of_half = carry_stage(half, after)
        carry.append(of_half)
        after = [done]
    for half in halves:
        after = send_stage(half, carry[half], after)
    sends = own_carries(plan, own, others, levels, of_group[0], after)
    own_carry = {o: in_level(a, o) if o else a for o, a in zip(of_group[0], sends)}
    caches = [
        swap(a, "inner", o, plan.n_inner) if o else a
        for o, a in enumerate(sends[len(of_group[0]) :])
    ]
    early = []
    for half in halves:
        part = part_of(half, of_group[0], own_carry, after)
        early.append((part, half, of_group[0]))
        after = [part]
    out = assemble(plan, early + parts[:-1])
    out = assemble(plan, parts[-1:], out)
    return out, assemble_cache(plan, caches)


def solution(mesh):
    tokens = P(("outer", "inner", "y", "core"), None)
    seq, head = ("outer", "inner"), ("y", "core")

    def whole(queries, keys, values, spikes, gain):
        plan = Plan(mesh, spikes.shape[0] // mesh.size, spikes.shape[1])
        sizes = (plan.n_outer, plan.n_inner, plan.n_y, CORES)
        split = Mesh(mesh.devices.reshape(sizes), ("outer", "inner", "y", "core"))
        return jax.shard_map(
            functools.partial(per_device, plan),
            mesh=split,
            in_specs=(tokens, tokens, tokens, tokens, P(head)),
            out_specs=(P(seq, head), P(seq, head, None, None)),
            check_vma=False,
        )(queries, keys, values, spikes, gain)

    return whole
```

```python
import functools

import jax
import jax.numpy as jnp
from jax import lax
from jax.experimental import pallas as pl
from jax.experimental.pallas import tpu as pltpu
from jax.sharding import Mesh
from jax.sharding import PartitionSpec as P

HD = 128
SCORE_SCALE = HD ** (-0.5)
CORES = 2
VMEM_BYTES = 24 * 1024 * 1024
DECODE_VMEM_BYTES = 46 * 1024 * 1024
PAD = 16
TOP = 32767.0

VMEM = pl.BlockSpec(memory_space=pltpu.VMEM)
HBM = pl.BlockSpec(memory_space=pltpu.HBM)
ANY = pl.BlockSpec(memory_space=pl.ANY)


def params(vmem=VMEM_BYTES):
    return pltpu.CompilerParams(vmem_limit_bytes=vmem)


def cost(flops, bytes_accessed):
    return pl.CostEstimate(flops=flops, bytes_accessed=bytes_accessed, transcendentals=0)


def at_place(kernel):
    def placed(*refs):
        place = [lax.axis_index(a) for a in ("core", "inner", "y", "outer")]
        kernel(place, *refs)

    return placed


class Plan:
    def __init__(self, mesh, rows, model):
        n_seq, n_head = mesh.shape["seq"], mesh.shape["head"]
        self.n_y = n_head // CORES
        self.width = model // n_head
        group = self.width // HD
        self.n_inner = 2 if n_seq % 2 == 0 and group % 2 == 0 else 1
        self.n_outer = n_seq // self.n_inner
        self.halves = 2 if group // self.n_inner % 2 == 0 else 1
        self.each = group // (self.n_inner * self.halves)
        self.plane = self.n_inner * self.n_y
        self.rows = rows
        self.block = rows * n_head
        self.piece = self.each * HD
        self.half_width = self.width // self.halves


def counts_of(spikes):
    one, two = jnp.ones_like(spikes), jnp.full_like(spikes, 2)
    zero = jnp.zeros_like(spikes)

    def ternary(rest, unit):
        return jnp.where(rest >= 2 * unit, two, jnp.where(rest >= unit, one, zero))

    value = ternary(spikes, 9)
    rest = spikes - 9 * value
    key = ternary(rest, 3)
    return value, key, rest - 3 * key


def sides(plan, core):
    width = plan.half_width
    for y in range(plan.n_y):
        for side in range(CORES):
            of = core if side == 0 else 1 - core
            for half in range(plan.halves):
                start = ((y * CORES + of) * plan.halves + half) * width
                at = pl.ds(pl.multiple_of(start, width), width)
                yield side, half, slice(y * width, (y + 1) * width), at


def decode(plan, spikes, keys, values):
    rows, model = spikes.shape
    step = min(rows, 32)
    chunks = rows // step
    n_out = 3 * CORES * plan.halves

    def kernel(*refs):
        core = lax.axis_index("core")
        sources, *outs, b0, b1, b2, sems = refs[:3], *refs[3:]
        buffers = (b0, b1, b2)

        def fetch(chunk, index):
            at = pl.ds(chunk * step, step)
            return pltpu.make_async_copy(
                sources[index].at[at], buffers[index].at[at], sems.at[chunk, index]
            )

        for chunk in range(chunks):
            for index in range(3):
                fetch(chunk, index).start()

        @pl.loop(0, chunks)
        def _(chunk):
            for index in range(3):
                fetch(chunk, index).wait()
            at = pl.ds(pl.multiple_of(chunk * step, step), step)
            for side, half, mine, columns in sides(plan, core):
                spikes = buffers[0][at, columns].astype(jnp.float32).astype(jnp.bfloat16)
                value, key, query = counts_of(spikes)
                spiked = (buffers[1][at, columns] * key, buffers[2][at, columns] * value, query)
                for index, array in enumerate(spiked):
                    outs[(index * CORES + side) * plan.halves + half][at, mine] = array

    return pl.pallas_call(
        kernel,
        out_shape=[jax.ShapeDtypeStruct((rows, plan.n_y * plan.half_width), jnp.bfloat16)] * n_out,
        in_specs=[HBM] * 3,
        out_specs=[VMEM] * n_out,
        scratch_shapes=[
            pltpu.VMEM((rows, model), jnp.int32),
            pltpu.VMEM((rows, model), jnp.bfloat16),
            pltpu.VMEM((rows, model), jnp.bfloat16),
            pltpu.SemaphoreType.DMA((chunks, 3)),
        ],
        compiler_params=params(DECODE_VMEM_BYTES),
        cost_estimate=cost(rows * model * 4, rows * model * 14),
        name="decode",
    )(spikes, keys, values)


def spike_queries(plan, queries, counts):
    n = len(counts)

    def kernel(place_ref, queries_ref, *refs):
        for side, half, mine, columns in sides(plan, place_ref[0]):
            at = side * plan.halves + half
            refs[n + at][:, mine] = queries_ref[:, columns] * refs[at][:, mine]

    return pl.pallas_call(
        at_place(kernel),
        out_shape=[jax.ShapeDtypeStruct(a.shape, jnp.bfloat16) for a in counts],
        in_specs=[VMEM] * (1 + n),
        out_specs=[VMEM] * n,
        compiler_params=params(),
        cost_estimate=cost(queries.size, queries.size * 6),
        name="spike_queries",
    )(queries, *counts)


def contract_rows(left, right):
    return lax.dot_general(
        left, right, (((0,), (0,)), ((), ())), preferred_element_type=jnp.float32
    )


def contract_columns(left, right):
    return lax.dot_general(
        left, right, (((1,), (1,)), ((), ())), preferred_element_type=jnp.float32
    )


def code(states, ref):
    line = lax.broadcasted_iota(jnp.int32, (PAD, HD), 0)
    exponents = jnp.zeros((PAD, HD), jnp.float32)
    for i, state in enumerate(states):
        top = jnp.max(jnp.abs(state), axis=0, keepdims=True)
        exponent = jnp.floor(jnp.log2(jnp.maximum(top, 1e-30))) + 1
        scaled = jnp.round(state * jnp.exp2(15 - exponent))
        scaled = jnp.clip(scaled, -TOP, TOP)
        ref[i * HD : (i + 1) * HD] = scaled.astype(jnp.int32).astype(jnp.int16)
        exponents = jnp.where(line == i, exponent, exponents)
    ref[len(states) * HD : len(states) * HD + PAD] = exponents.astype(jnp.int32).astype(jnp.int16)


def decoded(ref):
    count = ref.shape[0] // HD
    exponents = ref[count * HD : count * HD + PAD].astype(jnp.int32).astype(jnp.float32)
    return [
        ref[i * HD : (i + 1) * HD].astype(jnp.int32).astype(jnp.float32)
        * jnp.exp2(exponents[i : i + 1] - 15)
        for i in range(count)
    ]


def code_gain(gain_ref, ref):
    line = lax.broadcasted_iota(jnp.int32, (PAD // 2, HD), 0)
    gain = jnp.zeros((PAD // 2, HD), jnp.float32)
    for i in range(gain_ref.shape[1] // HD):
        gain = jnp.where(line == i, gain_ref[:, i * HD : (i + 1) * HD], gain)
    coarse = jnp.round(gain * 2.0**12)
    fine = jnp.round((gain - coarse * 2.0**-12) * 2.0**27)
    planes = jnp.concatenate([coarse, fine], axis=0)
    ref[ref.shape[0] - PAD :] = planes.astype(jnp.int32).astype(jnp.int16)


def decoded_gain(ref):
    planes = ref[ref.shape[0] - PAD :].astype(jnp.int32).astype(jnp.float32)
    return planes[: PAD // 2] * 2.0**-12 + planes[PAD // 2 :] * 2.0**-27


def plus(left, right):
    return [a + b for a, b in zip(left, right)]


def total_of(refs, each):
    total = [jnp.zeros((HD, HD), jnp.float32)] * each
    for ref in refs:
        coded = ref.dtype == jnp.int16
        total = plus(total, decoded(ref) if coded else [ref[i] for i in range(each)])
    return total


def coded_shape(heads, more=0):
    return jax.ShapeDtypeStruct((heads * HD + PAD + more, HD), jnp.int16)


def states_shape(*lead):
    return jax.ShapeDtypeStruct((*lead, HD, HD), jnp.float32)


def owned_columns(plan, place_ref, offset, i):
    x = place_ref[1] ^ (offset // plan.n_y)
    y = place_ref[2] ^ (offset % plan.n_y)
    start = ((y * plan.n_inner + x) * plan.each + i) * HD
    return pl.ds(pl.multiple_of(start, HD), HD)


def chunk_states(plan, key, value, half, after, gain=None):
    gains = [] if gain is None else [gain]

    def kernel(place_ref, k_ref, k_sib_ref, v_ref, v_sib_ref, *refs):
        own_ref, first_ref, *send_refs = refs[len(gains) + len(after) :]
        is_first = jnp.full((HD, HD), place_ref[0], jnp.int32) == 0
        for offset in (*range(1, plan.plane), 0):
            states = []
            for i in range(plan.each):
                at = owned_columns(plan, place_ref, offset, i)
                mine = contract_rows(v_ref[:, at], k_ref[:, at])
                sib = contract_rows(v_sib_ref[:, at], k_sib_ref[:, at])
                first_ref[offset, i] = jnp.where(is_first, mine, sib)
                states.append(mine + sib)
            if offset:
                code(states, send_refs[offset - 1])
                if gains and offset < plan.n_y:
                    code_gain(refs[0], send_refs[offset - 1])
            else:
                for i, state in enumerate(states):
                    own_ref[i] = state

    heads = plan.plane * plan.each
    return pl.pallas_call(
        at_place(kernel),
        out_shape=[states_shape(plan.each), states_shape(plan.plane, plan.each)]
        + [
            coded_shape(plan.each, PAD if gains and o < plan.n_y else 0)
            for o in range(1, plan.plane)
        ],
        in_specs=[VMEM] * (4 + len(gains)) + [ANY] * len(after),
        out_specs=[VMEM] * (1 + plan.plane),
        compiler_params=params(),
        cost_estimate=cost(
            4 * plan.rows * HD * HD * heads, 8 * plan.rows * HD * heads + 6 * heads * HD * HD
        ),
        name=f"chunk_states_{half}",
    )(*key, *value, *gains, *after)


def level_states(plan, own, others, half, after):
    def kernel(own_ref, *refs):
        code(total_of((own_ref, *refs[: len(others)]), plan.each), refs[-1])

    return pl.pallas_call(
        kernel,
        out_shape=coded_shape(plan.each),
        in_specs=[VMEM] * plan.plane + [ANY] * len(after),
        out_specs=VMEM,
        compiler_params=params(),
        cost_estimate=cost(0, plan.plane * plan.each * HD * HD * 2),
        name=f"level_states_{half}",
    )(own, *others, *after)


def carried(plan, place_ref, own, others, levels, offsets):
    x, y = place_ref[1], place_ref[2]
    here = x * plan.n_y + y
    earlier = total_of(levels, plan.each)
    states = [[own[i] for i in range(plan.each)]] + [decoded(ref) for ref in others]

    def add(totals, keep_of):
        for offset, terms in enumerate(states):
            keep = jnp.full((HD, HD), keep_of(here ^ offset), jnp.int32) == 1
            totals = plus(totals, [jnp.where(keep, s, 0.0) for s in terms])
        return totals

    before = [add(earlier, lambda chip: (chip < here ^ o).astype(jnp.int32)) for o in offsets]
    blocks = [
        add(earlier, lambda chip: (chip // plan.n_y <= x ^ o).astype(jnp.int32))
        for o in range(plan.n_inner)
    ]
    return before, blocks


def carries(plan, own, others, levels, half, offsets, after):
    n_others, n_levels = len(others), len(levels)

    def kernel(place_ref, own_ref, *refs):
        before, _ = carried(
            plan, place_ref, own_ref, refs[:n_others], refs[n_others : n_others + n_levels], offsets
        )
        for states, ref in zip(before, refs[n_others + n_levels + len(after) :]):
            code(states, ref)

    return pl.pallas_call(
        at_place(kernel),
        out_shape=[coded_shape(plan.each)] * len(offsets),
        in_specs=[VMEM] * (1 + n_others + n_levels) + [ANY] * len(after),
        out_specs=[VMEM] * len(offsets),
        compiler_params=params(),
        cost_estimate=cost(0, (plan.plane * 4 + n_levels) * plan.each * HD * HD * 2),
        name=f"carries_{half}",
    )(own, *others, *levels, *after)


def own_carries(plan, own, others, levels, offsets, after):
    n_others = len(others[0])
    operands = [(own[h], *others[h], *levels[h]) for h in range(plan.halves)]
    starts = [sum(map(len, operands[:h])) for h in range(plan.halves + 1)]

    def kernel(place_ref, *refs):
        outs = refs[starts[-1] + len(after) :]
        befores = [[] for _ in offsets]
        for half in range(plan.halves):
            own_ref, *of_half = refs[starts[half] : starts[half + 1]]
            before, blocks = carried(
                plan, place_ref, own_ref, of_half[:n_others], of_half[n_others:], offsets
            )
            for all_states, states in zip(befores, before):
                all_states.extend(states)
            for offset, (totals, ref) in enumerate(zip(blocks, outs[len(offsets) :])):
                block = place_ref[3] * plan.n_inner + (place_ref[1] ^ offset)
                seen = jnp.full((1, HD), (block + 1) * plan.block, jnp.int32).astype(jnp.float32)
                for i, total in enumerate(totals):
                    ref[half, i] = total.T * lax.rsqrt(seen)
        for states, ref in zip(befores, outs):
            code(states, ref)

    return pl.pallas_call(
        at_place(kernel),
        out_shape=[coded_shape(plan.halves * plan.each)] * len(offsets)
        + [states_shape(plan.halves, plan.each)] * plan.n_inner,
        in_specs=[VMEM] * starts[-1] + [ANY] * len(after),
        out_specs=[VMEM] * (len(offsets) + plan.n_inner),
        compiler_params=params(),
        cost_estimate=cost(0, plan.plane * plan.each * HD * HD * 20),
        name="own_carries",
    )(*[a for arrays in operands for a in arrays], *after)


def local_part(q_ref, k_ref, v_ref, at):
    rows = q_ref.shape[0]
    causal = lax.broadcasted_iota(jnp.int32, (rows, rows), 0) >= lax.broadcasted_iota(
        jnp.int32, (rows, rows), 1
    )
    scores = contract_columns(q_ref[:, at], k_ref[:, at]) * SCORE_SCALE
    weights = jnp.where(causal, scores, 0.0).astype(jnp.bfloat16)
    return jnp.dot(weights, v_ref[:, at], preferred_element_type=jnp.float32)


def finished(queries, local, carried, gain):
    carried = carried * SCORE_SCALE
    high = carried.astype(jnp.bfloat16)
    low = (carried - high.astype(jnp.float32)).astype(jnp.bfloat16)
    both = contract_columns(queries, jnp.concatenate([high, low], axis=0))
    raw = local + (both[:, :HD] + both[:, HD:])
    mean = jnp.mean(raw * raw, axis=-1, keepdims=True)
    return (raw * lax.rsqrt(mean + 1e-06) * gain).astype(jnp.bfloat16)


def attend(plan, query, key, value, carry, first, gain, half, offsets, after):
    rows = plan.rows
    operands = [*query, *key, *value]
    n = len(operands)

    def kernel(place_ref, *refs):
        core = place_ref[0]
        first_ref, gain_ref, *carry_refs = refs[n : n + 2 + len(offsets)]
        out_ref = refs[-1]
        is_second = jnp.full((HD, HD), core, jnp.int32) == 1
        coded_gain = gain_ref.dtype == jnp.int16
        line = lax.broadcasted_iota(jnp.int32, (PAD // 2, HD), 0)
        for piece, offset in enumerate(offsets):
            x = place_ref[1] ^ (offset // plan.n_y)
            carry_states = decoded(carry_refs[piece])
            skip = half * plan.each if len(carry_states) > plan.each else 0
            for i in range(plan.each):
                at = owned_columns(plan, place_ref, offset, i)
                head = (half * plan.n_inner + x) * plan.each + i
                if coded_gain:
                    gain = jnp.where(line == head, decoded_gain(gain_ref), 0.0)
                    gain = jnp.sum(gain, axis=0, keepdims=True)
                else:
                    gain = gain_ref[:, pl.ds(pl.multiple_of(head * HD, HD), HD)]
                out_at = slice(piece * plan.piece + i * HD, piece * plan.piece + (i + 1) * HD)
                carried = carry_states[skip + i]
                first = first_ref[offset, i]
                for side in range(CORES):
                    raw = local_part(refs[side], refs[2 + side], refs[4 + side], at)
                    behind = is_second if side == 0 else ~is_second
                    state = carried + jnp.where(behind, first, 0.0)
                    of = core if side == 0 else 1 - core
                    out_rows = pl.ds(pl.multiple_of(of * rows, rows), rows)
                    out_ref[out_rows, out_at] = finished(refs[side][:, at], raw, state, gain)

    heads = len(offsets) * plan.each
    return pl.pallas_call(
        at_place(kernel),
        out_shape=jax.ShapeDtypeStruct((CORES * rows, heads * HD), jnp.bfloat16),
        in_specs=[VMEM] * (n + 2 + len(offsets)) + [ANY] * len(after),
        out_specs=VMEM,
        compiler_params=params(),
        cost_estimate=cost(
            heads * (8 * rows * rows * HD + 8 * rows * HD * HD), 16 * rows * heads * HD
        ),
        name=f"attend_{half}_" + "_".join(map(str, offsets)),
    )(*operands, first, gain, *carry, *after)


def assemble(plan, parts, into=None):
    rows = CORES * plan.rows
    copies = [(n, piece, half, o) for n, (_, half, os) in enumerate(parts) for piece, o in enumerate(os)]

    def kernel(place_ref, *refs):
        out_ref, sems = refs[-2:]
        started = []
        for at, (n, piece, half, offset) in enumerate(copies):
            x = place_ref[1] ^ (offset // plan.n_y)
            y = place_ref[2] ^ (offset % plan.n_y)
            column = (half * plan.n_inner + x) * plan.piece
            to_rows = pl.ds(pl.multiple_of(y * rows, rows), rows)
            to_columns = pl.ds(pl.multiple_of(column, plan.piece), plan.piece)
            started.append(
                pltpu.make_async_copy(
                    refs[n].at[:, pl.ds(piece * plan.piece, plan.piece)],
                    out_ref.at[to_rows, to_columns],
                    sems.at[at],
                )
            )
            started[-1].start()
        for copy in started:
            copy.wait()

    arrays = [array for array, _, _ in parts]
    aliased = [] if into is None else [into]
    return pl.pallas_call(
        at_place(kernel),
        out_shape=jax.ShapeDtypeStruct((plan.n_y * rows, plan.width), jnp.bfloat16),
        in_specs=[VMEM] * len(arrays) + [HBM] * len(aliased),
        out_specs=HBM,
        scratch_shapes=[pltpu.SemaphoreType.DMA((len(copies),))],
        input_output_aliases={len(arrays): 0} if aliased else {},
        compiler_params=params(),
        name="assemble" if into is None else "finish",
    )(*arrays, *aliased)


def assemble_cache(plan, parts):
    group = plan.n_inner * plan.each

    def kernel(place_ref, *refs):
        for half in range(plan.halves):
            for offset, ref in enumerate(refs[:-1]):
                start = half * group + (place_ref[1] ^ offset) * plan.each
                refs[-1][0, pl.ds(start, plan.each)] = ref[half]

    return pl.pallas_call(
        at_place(kernel),
        out_shape=states_shape(1, plan.halves * group),
        in_specs=[VMEM] * len(parts),
        out_specs=VMEM,
        compiler_params=params(),
        name="assemble_cache",
    )(*parts)


def per_device(plan, queries, keys, values, spikes, gain):
    halves = range(plan.halves)

    def swap(array, axes, offset, size):
        return lax.ppermute(array, axes, [(i, i ^ offset) for i in range(size)])

    def in_level(array, offset):
        return swap(array, ("inner", "y"), offset, plan.plane)

    def to_later(array, distance):
        pairs = [(i, i + distance) for i in range(plan.n_outer - distance)]
        return lax.ppermute(array, "outer", pairs)

    gain = gain.reshape(1, plan.width)
    arrays = decode(plan, spikes, keys, values)
    parts = [arrays[k : k + plan.halves] for k in range(0, len(arrays), plan.halves)]

    def with_siblings(mine, theirs):
        return [(a, swap(b, "core", 1, CORES)) for a, b in zip(mine, theirs)]

    key, value = with_siblings(*parts[0:2]), with_siblings(*parts[2:4])
    spiked = spike_queries(plan, queries, [*parts[4], *parts[5]])
    query = with_siblings(spiked[: plan.halves], spiked[plan.halves :])

    own, first, others = [], [], []

    def owner_stage(half, after):
        with_gain = gain if half == 0 else None
        mine, of_first, *sends = chunk_states(
            plan, key[half], value[half], half, after, with_gain
        )
        own.append(mine)
        first.append(of_first)
        others.append([in_level(a, o) for o, a in enumerate(sends, 1)])

    of_group = [list(range(y, plan.plane, plan.n_y)) for y in range(plan.n_y)]
    abroad = [o for offsets in of_group[1:] for o in offsets]

    def part_of(half, offsets, carry, after):
        return attend(
            plan,
            query[half],
            key[half],
            value[half],
            [carry[o] for o in offsets],
            first[half],
            others[0][offsets[0] % plan.n_y - 1] if offsets[0] % plan.n_y else gain,
            half,
            offsets,
            after,
        )

    def carry_stage(half, after):
        sends = carries(plan, own[half], others[half], levels[half], half, abroad, after)
        return sends[0], {o: in_level(a, o) for o, a in zip(abroad, sends)}

    parts = []

    def send_stage(half, carry, after):
        for y in range(1, plan.n_y):
            part = part_of(half, of_group[y], carry, after)
            parts.append((swap(part, "y", y, plan.n_y), half, of_group[y]))
            after = [part]
        return after

    after = [query[0][0]]
    for half in halves:
        owner_stage(half, after)
        after = [own[-1], *[a for _, a in query]]
    levels = []
    for half in halves:
        level = level_states(plan, own[half], others[half][::-1], half, after)
        distances = [*range(1, plan.n_outer)]
        if half == 0:
            distances = [*distances[1:], *distances[:1]]
        levels.append([to_later(level, d) for d in distances])
        after = [level]
    carry = []
    for half in halves:
        done, of_half = carry_stage(half, after)
        carry.append(of_half)
        after = [done]
    for half in halves:
        after = send_stage(half, carry[half], after)
    sends = own_carries(plan, own, others, levels, of_group[0], after)
    own_carry = {o: in_level(a, o) if o else a for o, a in zip(of_group[0], sends)}
    caches = [
        swap(a, "inner", o, plan.n_inner) if o else a
        for o, a in enumerate(sends[len(of_group[0]) :])
    ]
    early = []
    for half in halves:
        part = part_of(half, of_group[0], own_carry, after)
        early.append((part, half, of_group[0]))
        after = [part]
    out = assemble(plan, early + parts[:-1])
    out = assemble(plan, parts[-1:], out)
    return out, assemble_cache(plan, caches)


def solution(mesh):
    tokens = P(("outer", "inner", "y", "core"), None)
    seq, head = ("outer", "inner"), ("y", "core")

    def whole(queries, keys, values, spikes, gain):
        plan = Plan(mesh, spikes.shape[0] // mesh.size, spikes.shape[1])
        sizes = (plan.n_outer, plan.n_inner, plan.n_y, CORES)
        split = Mesh(mesh.devices.reshape(sizes), ("outer", "inner", "y", "core"))
        return jax.shard_map(
            functools.partial(per_device, plan),
            mesh=split,
            in_specs=(tokens, tokens, tokens, tokens, P(head)),
            out_specs=(P(seq, head), P(seq, head, None, None)),
            check_vma=False,
        )(queries, keys, values, spikes, gain)

    return whole
```

```python
import functools

import jax
import jax.numpy as jnp
from jax import lax
from jax.experimental import pallas as pl
from jax.experimental.pallas import tpu as pltpu
from jax.sharding import Mesh
from jax.sharding import PartitionSpec as P

HD = 128
SCORE_SCALE = HD ** (-0.5)
CORES = 2
VMEM_BYTES = 24 * 1024 * 1024
DECODE_VMEM_BYTES = 50 * 1024 * 1024
PAD = 16
TOP = 32767.0

VMEM = pl.BlockSpec(memory_space=pltpu.VMEM)
HBM = pl.BlockSpec(memory_space=pltpu.HBM)
ANY = pl.BlockSpec(memory_space=pl.ANY)


def params(vmem=VMEM_BYTES):
    return pltpu.CompilerParams(vmem_limit_bytes=vmem)


def cost(flops, bytes_accessed):
    return pl.CostEstimate(flops=flops, bytes_accessed=bytes_accessed, transcendentals=0)


def at_place(kernel):
    def placed(*refs):
        place = [lax.axis_index(a) for a in ("core", "inner", "y", "outer")]
        kernel(place, *refs)

    return placed


class Plan:
    def __init__(self, mesh, rows, model):
        n_seq, n_head = mesh.shape["seq"], mesh.shape["head"]
        self.n_y = n_head // CORES
        self.width = model // n_head
        group = self.width // HD
        self.n_inner = 2 if n_seq % 2 == 0 and group % 2 == 0 else 1
        self.n_outer = n_seq // self.n_inner
        self.halves = 2 if group // self.n_inner % 2 == 0 else 1
        self.each = group // (self.n_inner * self.halves)
        self.plane = self.n_inner * self.n_y
        self.rows = rows
        self.block = rows * n_head
        self.piece = self.each * HD
        self.half_width = self.width // self.halves


def counts_of(spikes):
    one, two = jnp.ones_like(spikes), jnp.full_like(spikes, 2)
    zero = jnp.zeros_like(spikes)

    def ternary(rest, unit):
        return jnp.where(rest >= 2 * unit, two, jnp.where(rest >= unit, one, zero))

    value = ternary(spikes, 9)
    rest = spikes - 9 * value
    key = ternary(rest, 3)
    return value, key, rest - 3 * key


def sides(plan, core):
    width = plan.half_width
    for y in range(plan.n_y):
        for side in range(CORES):
            of = core if side == 0 else 1 - core
            for half in range(plan.halves):
                start = ((y * CORES + of) * plan.halves + half) * width
                at = pl.ds(pl.multiple_of(start, width), width)
                yield side, half, slice(y * width, (y + 1) * width), at


def decode(plan, spikes, keys, values, half):
    rows, _ = spikes.shape
    step = min(rows, 64)
    chunks = rows // step
    width = plan.half_width
    groups = plan.n_y * CORES

    def kernel(*refs):
        core = lax.axis_index("core")
        sources, outs, buffers, sems = refs[:3], refs[3:9], refs[9:12], refs[12]

        def fetch(chunk, index, group):
            at = pl.ds(chunk * step, step)
            columns = pl.ds((group * plan.halves + half) * width, width)
            return pltpu.make_async_copy(
                sources[index].at[at, columns],
                buffers[index].at[at, pl.ds(group * width, width)],
                sems.at[chunk, index, group],
            )

        every = [(index, group) for index in range(3) for group in range(groups)]
        for chunk in range(chunks):
            for index, group in every:
                fetch(chunk, index, group).start()

        @pl.loop(0, chunks)
        def _(chunk):
            for index, group in every:
                fetch(chunk, index, group).wait()
            at = pl.ds(pl.multiple_of(chunk * step, step), step)
            for y in range(plan.n_y):
                mine = slice(y * width, (y + 1) * width)
                for side in range(CORES):
                    of = core if side == 0 else 1 - core
                    columns = pl.ds(pl.multiple_of((y * CORES + of) * width, width), width)
                    codes = buffers[0][at, columns].astype(jnp.float32).astype(jnp.bfloat16)
                    value, key, query = counts_of(codes)
                    outs[side][at, mine] = buffers[1][at, columns] * key
                    outs[2 + side][at, mine] = buffers[2][at, columns] * value
                    outs[4 + side][at, mine] = query

    return pl.pallas_call(
        kernel,
        out_shape=[jax.ShapeDtypeStruct((rows, plan.n_y * width), jnp.bfloat16)] * 6,
        in_specs=[HBM] * 3,
        out_specs=[VMEM] * 6,
        scratch_shapes=[
            pltpu.VMEM((rows, groups * width), jnp.int32),
            pltpu.VMEM((rows, groups * width), jnp.bfloat16),
            pltpu.VMEM((rows, groups * width), jnp.bfloat16),
            pltpu.SemaphoreType.DMA((chunks, 3, groups)),
        ],
        compiler_params=params(DECODE_VMEM_BYTES),
        cost_estimate=cost(rows * groups * width * 4, rows * groups * width * 14),
        name=f"decode_{half}",
    )(spikes, keys, values)


def spike_queries(plan, queries, counts):
    n = len(counts)

    def kernel(place_ref, queries_ref, *refs):
        for side, half, mine, columns in sides(plan, place_ref[0]):
            at = side * plan.halves + half
            refs[n + at][:, mine] = queries_ref[:, columns] * refs[at][:, mine]

    return pl.pallas_call(
        at_place(kernel),
        out_shape=[jax.ShapeDtypeStruct(a.shape, jnp.bfloat16) for a in counts],
        in_specs=[VMEM] * (1 + n),
        out_specs=[VMEM] * n,
        compiler_params=params(),
        cost_estimate=cost(queries.size, queries.size * 6),
        name="spike_queries",
    )(queries, *counts)


def contract_rows(left, right):
    return lax.dot_general(
        left, right, (((0,), (0,)), ((), ())), preferred_element_type=jnp.float32
    )


def contract_columns(left, right):
    return lax.dot_general(
        left, right, (((1,), (1,)), ((), ())), preferred_element_type=jnp.float32
    )


def code(states, ref):
    line = lax.broadcasted_iota(jnp.int32, (PAD, HD), 0)
    exponents = jnp.zeros((PAD, HD), jnp.float32)
    for i, state in enumerate(states):
        top = jnp.max(jnp.abs(state), axis=0, keepdims=True)
        exponent = jnp.floor(jnp.log2(jnp.maximum(top, 1e-30))) + 1
        scaled = jnp.round(state * jnp.exp2(15 - exponent))
        scaled = jnp.clip(scaled, -TOP, TOP)
        ref[i * HD : (i + 1) * HD] = scaled.astype(jnp.int32).astype(jnp.int16)
        exponents = jnp.where(line == i, exponent, exponents)
    ref[len(states) * HD : len(states) * HD + PAD] = exponents.astype(jnp.int32).astype(jnp.int16)


def decoded(ref):
    count = ref.shape[0] // HD
    exponents = ref[count * HD : count * HD + PAD].astype(jnp.int32).astype(jnp.float32)
    return [
        ref[i * HD : (i + 1) * HD].astype(jnp.int32).astype(jnp.float32)
        * jnp.exp2(exponents[i : i + 1] - 15)
        for i in range(count)
    ]


def code_gain(gain_ref, ref):
    line = lax.broadcasted_iota(jnp.int32, (PAD // 2, HD), 0)
    gain = jnp.zeros((PAD // 2, HD), jnp.float32)
    for i in range(gain_ref.shape[1] // HD):
        gain = jnp.where(line == i, gain_ref[:, i * HD : (i + 1) * HD], gain)
    coarse = jnp.round(gain * 2.0**12)
    fine = jnp.round((gain - coarse * 2.0**-12) * 2.0**27)
    planes = jnp.concatenate([coarse, fine], axis=0)
    ref[ref.shape[0] - PAD :] = planes.astype(jnp.int32).astype(jnp.int16)


def decoded_gain(ref):
    planes = ref[ref.shape[0] - PAD :].astype(jnp.int32).astype(jnp.float32)
    return planes[: PAD // 2] * 2.0**-12 + planes[PAD // 2 :] * 2.0**-27


def plus(left, right):
    return [a + b for a, b in zip(left, right)]


def total_of(refs, each):
    total = [jnp.zeros((HD, HD), jnp.float32)] * each
    for ref in refs:
        coded = ref.dtype == jnp.int16
        total = plus(total, decoded(ref) if coded else [ref[i] for i in range(each)])
    return total


def coded_shape(heads, more=0):
    return jax.ShapeDtypeStruct((heads * HD + PAD + more, HD), jnp.int16)


def states_shape(*lead):
    return jax.ShapeDtypeStruct((*lead, HD, HD), jnp.float32)


def owned_columns(plan, place_ref, offset, i):
    x = place_ref[1] ^ (offset // plan.n_y)
    y = place_ref[2] ^ (offset % plan.n_y)
    start = ((y * plan.n_inner + x) * plan.each + i) * HD
    return pl.ds(pl.multiple_of(start, HD), HD)


def chunk_states(plan, key, value, half, after, gain=None):
    gains = [] if gain is None else [gain]

    def kernel(place_ref, k_ref, k_sib_ref, v_ref, v_sib_ref, *refs):
        own_ref, first_ref, *send_refs = refs[len(gains) + len(after) :]
        is_first = jnp.full((HD, HD), place_ref[0], jnp.int32) == 0
        for offset in (*range(1, plan.plane), 0):
            states = []
            for i in range(plan.each):
                at = owned_columns(plan, place_ref, offset, i)
                mine = contract_rows(v_ref[:, at], k_ref[:, at])
                sib = contract_rows(v_sib_ref[:, at], k_sib_ref[:, at])
                first_ref[offset, i] = jnp.where(is_first, mine, sib)
                states.append(mine + sib)
            if offset:
                code(states, send_refs[offset - 1])
                if gains and offset < plan.n_y:
                    code_gain(refs[0], send_refs[offset - 1])
            else:
                for i, state in enumerate(states):
                    own_ref[i] = state

    heads = plan.plane * plan.each
    return pl.pallas_call(
        at_place(kernel),
        out_shape=[states_shape(plan.each), states_shape(plan.plane, plan.each)]
        + [
            coded_shape(plan.each, PAD if gains and o < plan.n_y else 0)
            for o in range(1, plan.plane)
        ],
        in_specs=[VMEM] * (4 + len(gains)) + [ANY] * len(after),
        out_specs=[VMEM] * (1 + plan.plane),
        compiler_params=params(),
        cost_estimate=cost(
            4 * plan.rows * HD * HD * heads, 8 * plan.rows * HD * heads + 6 * heads * HD * HD
        ),
        name=f"chunk_states_{half}",
    )(*key, *value, *gains, *after)


def level_states(plan, own, others, half, after):
    def kernel(own_ref, *refs):
        code(total_of((own_ref, *refs[: len(others)]), plan.each), refs[-1])

    return pl.pallas_call(
        kernel,
        out_shape=coded_shape(plan.each),
        in_specs=[VMEM] * plan.plane + [ANY] * len(after),
        out_specs=VMEM,
        compiler_params=params(),
        cost_estimate=cost(0, plan.plane * plan.each * HD * HD * 2),
        name=f"level_states_{half}",
    )(own, *others, *after)


def carried(plan, place_ref, own, others, levels, offsets):
    x, y = place_ref[1], place_ref[2]
    here = x * plan.n_y + y
    earlier = total_of(levels, plan.each)
    states = [[own[i] for i in range(plan.each)]] + [decoded(ref) for ref in others]

    def add(totals, keep_of):
        for offset, terms in enumerate(states):
            keep = jnp.full((HD, HD), keep_of(here ^ offset), jnp.int32) == 1
            totals = plus(totals, [jnp.where(keep, s, 0.0) for s in terms])
        return totals

    before = [add(earlier, lambda chip: (chip < here ^ o).astype(jnp.int32)) for o in offsets]
    blocks = [
        add(earlier, lambda chip: (chip // plan.n_y <= x ^ o).astype(jnp.int32))
        for o in range(plan.n_inner)
    ]
    return before, blocks


def carries(plan, own, others, levels, half, offsets, after):
    n_others, n_levels = len(others), len(levels)

    def kernel(place_ref, own_ref, *refs):
        before, _ = carried(
            plan, place_ref, own_ref, refs[:n_others], refs[n_others : n_others + n_levels], offsets
        )
        for states, ref in zip(before, refs[n_others + n_levels + len(after) :]):
            code(states, ref)

    return pl.pallas_call(
        at_place(kernel),
        out_shape=[coded_shape(plan.each)] * len(offsets),
        in_specs=[VMEM] * (1 + n_others + n_levels) + [ANY] * len(after),
        out_specs=[VMEM] * len(offsets),
        compiler_params=params(),
        cost_estimate=cost(0, (plan.plane * 4 + n_levels) * plan.each * HD * HD * 2),
        name=f"carries_{half}",
    )(own, *others, *levels, *after)


def own_carries(plan, own, others, levels, offsets, after):
    n_others = len(others[0])
    operands = [(own[h], *others[h], *levels[h]) for h in range(plan.halves)]
    starts = [sum(map(len, operands[:h])) for h in range(plan.halves + 1)]

    def kernel(place_ref, *refs):
        outs = refs[starts[-1] + len(after) :]
        befores = [[] for _ in offsets]
        for half in range(plan.halves):
            own_ref, *of_half = refs[starts[half] : starts[half + 1]]
            before, blocks = carried(
                plan, place_ref, own_ref, of_half[:n_others], of_half[n_others:], offsets
            )
            for all_states, states in zip(befores, before):
                all_states.extend(states)
            for offset, (totals, ref) in enumerate(zip(blocks, outs[len(offsets) :])):
                block = place_ref[3] * plan.n_inner + (place_ref[1] ^ offset)
                seen = jnp.full((1, HD), (block + 1) * plan.block, jnp.int32).astype(jnp.float32)
                for i, total in enumerate(totals):
                    ref[half, i] = total.T * lax.rsqrt(seen)
        for states, ref in zip(befores, outs):
            code(states, ref)

    return pl.pallas_call(
        at_place(kernel),
        out_shape=[coded_shape(plan.halves * plan.each)] * len(offsets)
        + [states_shape(plan.halves, plan.each)] * plan.n_inner,
        in_specs=[VMEM] * starts[-1] + [ANY] * len(after),
        out_specs=[VMEM] * (len(offsets) + plan.n_inner),
        compiler_params=params(),
        cost_estimate=cost(0, plan.plane * plan.each * HD * HD * 20),
        name="own_carries",
    )(*[a for arrays in operands for a in arrays], *after)


def local_part(q_ref, k_ref, v_ref, at):
    rows = q_ref.shape[0]
    causal = lax.broadcasted_iota(jnp.int32, (rows, rows), 0) >= lax.broadcasted_iota(
        jnp.int32, (rows, rows), 1
    )
    scores = contract_columns(q_ref[:, at], k_ref[:, at]) * SCORE_SCALE
    weights = jnp.where(causal, scores, 0.0).astype(jnp.bfloat16)
    return jnp.dot(weights, v_ref[:, at], preferred_element_type=jnp.float32)


def finished(queries, local, carried, gain):
    carried = carried * SCORE_SCALE
    high = carried.astype(jnp.bfloat16)
    low = (carried - high.astype(jnp.float32)).astype(jnp.bfloat16)
    both = contract_columns(queries, jnp.concatenate([high, low], axis=0))
    raw = local + (both[:, :HD] + both[:, HD:])
    mean = jnp.mean(raw * raw, axis=-1, keepdims=True)
    return (raw * lax.rsqrt(mean + 1e-06) * gain).astype(jnp.bfloat16)


def attend(plan, query, key, value, carry, first, gain, half, offsets, after):
    rows = plan.rows
    operands = [*query, *key, *value]
    n = len(operands)

    def kernel(place_ref, *refs):
        core = place_ref[0]
        first_ref, gain_ref, *carry_refs = refs[n : n + 2 + len(offsets)]
        out_ref = refs[-1]
        is_second = jnp.full((HD, HD), core, jnp.int32) == 1
        coded_gain = gain_ref.dtype == jnp.int16
        line = lax.broadcasted_iota(jnp.int32, (PAD // 2, HD), 0)
        for piece, offset in enumerate(offsets):
            x = place_ref[1] ^ (offset // plan.n_y)
            carry_states = decoded(carry_refs[piece])
            skip = half * plan.each if len(carry_states) > plan.each else 0
            for i in range(plan.each):
                at = owned_columns(plan, place_ref, offset, i)
                head = (half * plan.n_inner + x) * plan.each + i
                if coded_gain:
                    gain = jnp.where(line == head, decoded_gain(gain_ref), 0.0)
                    gain = jnp.sum(gain, axis=0, keepdims=True)
                else:
                    gain = gain_ref[:, pl.ds(pl.multiple_of(head * HD, HD), HD)]
                out_at = slice(piece * plan.piece + i * HD, piece * plan.piece + (i + 1) * HD)
                carried = carry_states[skip + i]
                first = first_ref[offset, i]
                for side in range(CORES):
                    raw = local_part(refs[side], refs[2 + side], refs[4 + side], at)
                    behind = is_second if side == 0 else ~is_second
                    state = carried + jnp.where(behind, first, 0.0)
                    of = core if side == 0 else 1 - core
                    out_rows = pl.ds(pl.multiple_of(of * rows, rows), rows)
                    out_ref[out_rows, out_at] = finished(refs[side][:, at], raw, state, gain)

    heads = len(offsets) * plan.each
    return pl.pallas_call(
        at_place(kernel),
        out_shape=jax.ShapeDtypeStruct((CORES * rows, heads * HD), jnp.bfloat16),
        in_specs=[VMEM] * (n + 2 + len(offsets)) + [ANY] * len(after),
        out_specs=VMEM,
        compiler_params=params(),
        cost_estimate=cost(
            heads * (8 * rows * rows * HD + 8 * rows * HD * HD), 16 * rows * heads * HD
        ),
        name=f"attend_{half}_" + "_".join(map(str, offsets)),
    )(*operands, first, gain, *carry, *after)


def assemble(plan, parts, into=None):
    rows = CORES * plan.rows
    copies = [(n, piece, half, o) for n, (_, half, os) in enumerate(parts) for piece, o in enumerate(os)]

    def kernel(place_ref, *refs):
        out_ref, sems = refs[-2:]
        started = []
        for at, (n, piece, half, offset) in enumerate(copies):
            x = place_ref[1] ^ (offset // plan.n_y)
            y = place_ref[2] ^ (offset % plan.n_y)
            column = (half * plan.n_inner + x) * plan.piece
            to_rows = pl.ds(pl.multiple_of(y * rows, rows), rows)
            to_columns = pl.ds(pl.multiple_of(column, plan.piece), plan.piece)
            started.append(
                pltpu.make_async_copy(
                    refs[n].at[:, pl.ds(piece * plan.piece, plan.piece)],
                    out_ref.at[to_rows, to_columns],
                    sems.at[at],
                )
            )
            started[-1].start()
        for copy in started:
            copy.wait()

    arrays = [array for array, _, _ in parts]
    aliased = [] if into is None else [into]
    return pl.pallas_call(
        at_place(kernel),
        out_shape=jax.ShapeDtypeStruct((plan.n_y * rows, plan.width), jnp.bfloat16),
        in_specs=[VMEM] * len(arrays) + [HBM] * len(aliased),
        out_specs=HBM,
        scratch_shapes=[pltpu.SemaphoreType.DMA((len(copies),))],
        input_output_aliases={len(arrays): 0} if aliased else {},
        compiler_params=params(),
        name="assemble" if into is None else "finish",
    )(*arrays, *aliased)


def assemble_cache(plan, parts):
    group = plan.n_inner * plan.each

    def kernel(place_ref, *refs):
        for half in range(plan.halves):
            for offset, ref in enumerate(refs[:-1]):
                start = half * group + (place_ref[1] ^ offset) * plan.each
                refs[-1][0, pl.ds(start, plan.each)] = ref[half]

    return pl.pallas_call(
        at_place(kernel),
        out_shape=states_shape(1, plan.halves * group),
        in_specs=[VMEM] * len(parts),
        out_specs=VMEM,
        compiler_params=params(),
        name="assemble_cache",
    )(*parts)


def per_device(plan, queries, keys, values, spikes, gain):
    halves = range(plan.halves)

    def swap(array, axes, offset, size):
        return lax.ppermute(array, axes, [(i, i ^ offset) for i in range(size)])

    def in_level(array, offset):
        return swap(array, ("inner", "y"), offset, plan.plane)

    def to_later(array, distance):
        pairs = [(i, i + distance) for i in range(plan.n_outer - distance)]
        return lax.ppermute(array, "outer", pairs)

    gain = gain.reshape(1, plan.width)
    arrays = [decode(plan, spikes, keys, values, half) for half in halves]
    parts = [list(of_halves) for of_halves in zip(*arrays)]

    def with_siblings(mine, theirs):
        return [(a, swap(b, "core", 1, CORES)) for a, b in zip(mine, theirs)]

    key, value = with_siblings(*parts[0:2]), with_siblings(*parts[2:4])
    spiked = spike_queries(plan, queries, [*parts[4], *parts[5]])
    query = with_siblings(spiked[: plan.halves], spiked[plan.halves :])

    own, first, others = [], [], []

    def owner_stage(half, after):
        with_gain = gain if half == 0 else None
        mine, of_first, *sends = chunk_states(
            plan, key[half], value[half], half, after, with_gain
        )
        own.append(mine)
        first.append(of_first)
        others.append([in_level(a, o) for o, a in enumerate(sends, 1)])

    of_group = [list(range(y, plan.plane, plan.n_y)) for y in range(plan.n_y)]
    abroad = [o for offsets in of_group[1:] for o in offsets]

    def part_of(half, offsets, carry, after):
        return attend(
            plan,
            query[half],
            key[half],
            value[half],
            [carry[o] for o in offsets],
            first[half],
            others[0][offsets[0] % plan.n_y - 1] if offsets[0] % plan.n_y else gain,
            half,
            offsets,
            after,
        )

    def carry_stage(half, after):
        sends = carries(plan, own[half], others[half], levels[half], half, abroad, after)
        return sends[0], {o: in_level(a, o) for o, a in zip(abroad, sends)}

    parts = []

    def send_stage(half, carry, after):
        for y in range(1, plan.n_y):
            part = part_of(half, of_group[y], carry, after)
            parts.append((swap(part, "y", y, plan.n_y), half, of_group[y]))
            after = [part]
        return after

    after = [query[0][0]]
    for half in halves:
        owner_stage(half, after)
        after = [own[-1], *[a for _, a in query]]
    levels = []
    for half in halves:
        level = level_states(plan, own[half], others[half][::-1], half, after)
        distances = [*range(1, plan.n_outer)]
        if half == 0:
            distances = [*distances[1:], *distances[:1]]
        levels.append([to_later(level, d) for d in distances])
        after = [level]
    carry = []
    for half in halves:
        done, of_half = carry_stage(half, after)
        carry.append(of_half)
        after = [done]
    for half in halves:
        after = send_stage(half, carry[half], after)
    sends = own_carries(plan, own, others, levels, of_group[0], after)
    own_carry = {o: in_level(a, o) if o else a for o, a in zip(of_group[0], sends)}
    caches = [
        swap(a, "inner", o, plan.n_inner) if o else a
        for o, a in enumerate(sends[len(of_group[0]) :])
    ]
    early = []
    for half in halves:
        part = part_of(half, of_group[0], own_carry, after)
        early.append((part, half, of_group[0]))
        after = [part]
    out = assemble(plan, early + parts[:-1])
    out = assemble(plan, parts[-1:], out)
    return out, assemble_cache(plan, caches)


def solution(mesh):
    tokens = P(("outer", "inner", "y", "core"), None)
    seq, head = ("outer", "inner"), ("y", "core")

    def whole(queries, keys, values, spikes, gain):
        plan = Plan(mesh, spikes.shape[0] // mesh.size, spikes.shape[1])
        sizes = (plan.n_outer, plan.n_inner, plan.n_y, CORES)
        split = Mesh(mesh.devices.reshape(sizes), ("outer", "inner", "y", "core"))
        return jax.shard_map(
            functools.partial(per_device, plan),
            mesh=split,
            in_specs=(tokens, tokens, tokens, tokens, P(head)),
            out_specs=(P(seq, head), P(seq, head, None, None)),
            check_vma=False,
        )(queries, keys, values, spikes, gain)

    return whole
```

```python
import functools

import jax
import jax.numpy as jnp
from jax import lax
from jax.experimental import pallas as pl
from jax.experimental.pallas import tpu as pltpu
from jax.sharding import Mesh
from jax.sharding import PartitionSpec as P

HD = 128
SCORE_SCALE = HD ** (-0.5)
CORES = 2
VMEM_BYTES = 24 * 1024 * 1024
DECODE_VMEM_BYTES = 46 * 1024 * 1024
PAD = 16
TOP = 32767.0

VMEM = pl.BlockSpec(memory_space=pltpu.VMEM)
HBM = pl.BlockSpec(memory_space=pltpu.HBM)
ANY = pl.BlockSpec(memory_space=pl.ANY)


def params(vmem=VMEM_BYTES):
    return pltpu.CompilerParams(vmem_limit_bytes=vmem)


def cost(flops, bytes_accessed):
    return pl.CostEstimate(flops=flops, bytes_accessed=bytes_accessed, transcendentals=0)


def at_place(kernel):
    def placed(*refs):
        place = [lax.axis_index(a) for a in ("core", "inner", "y", "outer")]
        kernel(place, *refs)

    return placed


class Plan:
    def __init__(self, mesh, rows, model):
        n_seq, n_head = mesh.shape["seq"], mesh.shape["head"]
        self.n_y = n_head // CORES
        self.width = model // n_head
        group = self.width // HD
        self.n_inner = 2 if n_seq % 2 == 0 and group % 2 == 0 else 1
        self.n_outer = n_seq // self.n_inner
        self.halves = 2 if group // self.n_inner % 2 == 0 else 1
        self.each = group // (self.n_inner * self.halves)
        self.plane = self.n_inner * self.n_y
        self.rows = rows
        self.block = rows * n_head
        self.piece = self.each * HD
        self.half_width = self.width // self.halves


def counts_of(spikes):
    one, two = jnp.ones_like(spikes), jnp.full_like(spikes, 2)
    zero = jnp.zeros_like(spikes)

    def ternary(rest, unit):
        return jnp.where(rest >= 2 * unit, two, jnp.where(rest >= unit, one, zero))

    value = ternary(spikes, 9)
    rest = spikes - 9 * value
    key = ternary(rest, 3)
    return value, key, rest - 3 * key


def sides(plan, core):
    width = plan.half_width
    for y in range(plan.n_y):
        for side in range(CORES):
            of = core if side == 0 else 1 - core
            for half in range(plan.halves):
                start = ((y * CORES + of) * plan.halves + half) * width
                at = pl.ds(pl.multiple_of(start, width), width)
                yield side, half, slice(y * width, (y + 1) * width), at


def decode(plan, spikes, keys, values):
    rows, model = spikes.shape
    step = min(rows, 32)
    chunks = rows // step
    n_out = 3 * CORES * plan.halves

    def kernel(*refs):
        core = lax.axis_index("core")
        sources, *outs, b0, b1, b2, sems = refs[:3], *refs[3:]
        buffers = (b0, b1, b2)

        def fetch(chunk, index):
            at = pl.ds(chunk * step, step)
            return pltpu.make_async_copy(
                sources[index].at[at], buffers[index].at[at], sems.at[chunk, index]
            )

        for chunk in range(chunks):
            for index in range(3):
                fetch(chunk, index).start()

        @pl.loop(0, chunks)
        def _(chunk):
            for index in range(3):
                fetch(chunk, index).wait()
            at = pl.ds(pl.multiple_of(chunk * step, step), step)
            for side, half, mine, columns in sides(plan, core):
                spikes = buffers[0][at, columns].astype(jnp.float32).astype(jnp.bfloat16)
                value, key, query = counts_of(spikes)
                spiked = (buffers[1][at, columns] * key, buffers[2][at, columns] * value, query)
                for index, array in enumerate(spiked):
                    outs[(index * CORES + side) * plan.halves + half][at, mine] = array

    return pl.pallas_call(
        kernel,
        out_shape=[jax.ShapeDtypeStruct((rows, plan.n_y * plan.half_width), jnp.bfloat16)] * n_out,
        in_specs=[HBM] * 3,
        out_specs=[VMEM] * n_out,
        scratch_shapes=[
            pltpu.VMEM((rows, model), jnp.int32),
            pltpu.VMEM((rows, model), jnp.bfloat16),
            pltpu.VMEM((rows, model), jnp.bfloat16),
            pltpu.SemaphoreType.DMA((chunks, 3)),
        ],
        compiler_params=params(DECODE_VMEM_BYTES),
        cost_estimate=cost(rows * model * 4, rows * model * 14),
        name="decode",
    )(spikes, keys, values)


def spike_queries(plan, queries, counts, after):
    n = len(counts)

    def kernel(place_ref, queries_ref, *refs):
        for side, half, mine, columns in sides(plan, place_ref[0]):
            at = side * plan.halves + half
            refs[n + len(after) + at][:, mine] = queries_ref[:, columns] * refs[at][:, mine]

    return pl.pallas_call(
        at_place(kernel),
        out_shape=[jax.ShapeDtypeStruct(a.shape, jnp.bfloat16) for a in counts],
        in_specs=[VMEM] * (1 + n) + [ANY] * len(after),
        out_specs=[VMEM] * n,
        compiler_params=params(),
        cost_estimate=cost(queries.size, queries.size * 6),
        name="spike_queries",
    )(queries, *counts, *after)


def contract_rows(left, right):
    return lax.dot_general(
        left, right, (((0,), (0,)), ((), ())), preferred_element_type=jnp.float32
    )


def contract_columns(left, right):
    return lax.dot_general(
        left, right, (((1,), (1,)), ((), ())), preferred_element_type=jnp.float32
    )


def code(states, ref):
    line = lax.broadcasted_iota(jnp.int32, (PAD, HD), 0)
    exponents = jnp.zeros((PAD, HD), jnp.float32)
    for i, state in enumerate(states):
        top = jnp.max(jnp.abs(state), axis=0, keepdims=True)
        exponent = jnp.floor(jnp.log2(jnp.maximum(top, 1e-30))) + 1
        scaled = jnp.round(state * jnp.exp2(15 - exponent))
        scaled = jnp.clip(scaled, -TOP, TOP)
        ref[i * HD : (i + 1) * HD] = scaled.astype(jnp.int32).astype(jnp.int16)
        exponents = jnp.where(line == i, exponent, exponents)
    ref[len(states) * HD : len(states) * HD + PAD] = exponents.astype(jnp.int32).astype(jnp.int16)


def decoded(ref):
    count = ref.shape[0] // HD
    exponents = ref[count * HD : count * HD + PAD].astype(jnp.int32).astype(jnp.float32)
    return [
        ref[i * HD : (i + 1) * HD].astype(jnp.int32).astype(jnp.float32)
        * jnp.exp2(exponents[i : i + 1] - 15)
        for i in range(count)
    ]


def code_gain(gain_ref, ref):
    line = lax.broadcasted_iota(jnp.int32, (PAD // 2, HD), 0)
    gain = jnp.zeros((PAD // 2, HD), jnp.float32)
    for i in range(gain_ref.shape[1] // HD):
        gain = jnp.where(line == i, gain_ref[:, i * HD : (i + 1) * HD], gain)
    coarse = jnp.round(gain * 2.0**12)
    fine = jnp.round((gain - coarse * 2.0**-12) * 2.0**27)
    planes = jnp.concatenate([coarse, fine], axis=0)
    ref[ref.shape[0] - PAD :] = planes.astype(jnp.int32).astype(jnp.int16)


def decoded_gain(ref):
    planes = ref[ref.shape[0] - PAD :].astype(jnp.int32).astype(jnp.float32)
    return planes[: PAD // 2] * 2.0**-12 + planes[PAD // 2 :] * 2.0**-27


def plus(left, right):
    return [a + b for a, b in zip(left, right)]


def total_of(refs, each):
    total = [jnp.zeros((HD, HD), jnp.float32)] * each
    for ref in refs:
        coded = ref.dtype == jnp.int16
        total = plus(total, decoded(ref) if coded else [ref[i] for i in range(each)])
    return total


def coded_shape(heads, more=0):
    return jax.ShapeDtypeStruct((heads * HD + PAD + more, HD), jnp.int16)


def states_shape(*lead):
    return jax.ShapeDtypeStruct((*lead, HD, HD), jnp.float32)


def owned_columns(plan, place_ref, offset, i):
    x = place_ref[1] ^ (offset // plan.n_y)
    y = place_ref[2] ^ (offset % plan.n_y)
    start = ((y * plan.n_inner + x) * plan.each + i) * HD
    return pl.ds(pl.multiple_of(start, HD), HD)


def chunk_states(plan, key, value, half, after, gain=None):
    gains = [] if gain is None else [gain]

    def kernel(place_ref, k_ref, k_sib_ref, v_ref, v_sib_ref, *refs):
        own_ref, first_ref, *send_refs = refs[len(gains) + len(after) :]
        is_first = jnp.full((HD, HD), place_ref[0], jnp.int32) == 0
        for offset in (*range(1, plan.plane), 0):
            states = []
            for i in range(plan.each):
                at = owned_columns(plan, place_ref, offset, i)
                mine = contract_rows(v_ref[:, at], k_ref[:, at])
                sib = contract_rows(v_sib_ref[:, at], k_sib_ref[:, at])
                first_ref[offset, i] = jnp.where(is_first, mine, sib)
                states.append(mine + sib)
            if offset:
                code(states, send_refs[offset - 1])
                if gains and offset < plan.n_y:
                    code_gain(refs[0], send_refs[offset - 1])
            else:
                for i, state in enumerate(states):
                    own_ref[i] = state

    heads = plan.plane * plan.each
    return pl.pallas_call(
        at_place(kernel),
        out_shape=[states_shape(plan.each), states_shape(plan.plane, plan.each)]
        + [
            coded_shape(plan.each, PAD if gains and o < plan.n_y else 0)
            for o in range(1, plan.plane)
        ],
        in_specs=[VMEM] * (4 + len(gains)) + [ANY] * len(after),
        out_specs=[VMEM] * (1 + plan.plane),
        compiler_params=params(),
        cost_estimate=cost(
            4 * plan.rows * HD * HD * heads, 8 * plan.rows * HD * heads + 6 * heads * HD * HD
        ),
        name=f"chunk_states_{half}",
    )(*key, *value, *gains, *after)


def level_states(plan, own, others, half, after):
    def kernel(own_ref, *refs):
        code(total_of((own_ref, *refs[: len(others)]), plan.each), refs[-1])

    return pl.pallas_call(
        kernel,
        out_shape=coded_shape(plan.each),
        in_specs=[VMEM] * plan.plane + [ANY] * len(after),
        out_specs=VMEM,
        compiler_params=params(),
        cost_estimate=cost(0, plan.plane * plan.each * HD * HD * 2),
        name=f"level_states_{half}",
    )(own, *others, *after)


def carried(plan, place_ref, own, others, levels, offsets):
    x, y = place_ref[1], place_ref[2]
    here = x * plan.n_y + y
    earlier = total_of(levels, plan.each)
    states = [[own[i] for i in range(plan.each)]] + [decoded(ref) for ref in others]

    def add(totals, keep_of):
        for offset, terms in enumerate(states):
            keep = jnp.full((HD, HD), keep_of(here ^ offset), jnp.int32) == 1
            totals = plus(totals, [jnp.where(keep, s, 0.0) for s in terms])
        return totals

    before = [add(earlier, lambda chip: (chip < here ^ o).astype(jnp.int32)) for o in offsets]
    blocks = [
        add(earlier, lambda chip: (chip // plan.n_y <= x ^ o).astype(jnp.int32))
        for o in range(plan.n_inner)
    ]
    return before, blocks


def carries(plan, own, others, levels, half, offsets, after):
    n_others, n_levels = len(others), len(levels)

    def kernel(place_ref, own_ref, *refs):
        before, _ = carried(
            plan, place_ref, own_ref, refs[:n_others], refs[n_others : n_others + n_levels], offsets
        )
        for states, ref in zip(before, refs[n_others + n_levels + len(after) :]):
            code(states, ref)

    return pl.pallas_call(
        at_place(kernel),
        out_shape=[coded_shape(plan.each)] * len(offsets),
        in_specs=[VMEM] * (1 + n_others + n_levels) + [ANY] * len(after),
        out_specs=[VMEM] * len(offsets),
        compiler_params=params(),
        cost_estimate=cost(0, (plan.plane * 4 + n_levels) * plan.each * HD * HD * 2),
        name=f"carries_{half}",
    )(own, *others, *levels, *after)


def own_carries(plan, own, others, levels, offsets, after):
    n_others = len(others[0])
    operands = [(own[h], *others[h], *levels[h]) for h in range(plan.halves)]
    starts = [sum(map(len, operands[:h])) for h in range(plan.halves + 1)]

    def kernel(place_ref, *refs):
        outs = refs[starts[-1] + len(after) :]
        befores = [[] for _ in offsets]
        for half in range(plan.halves):
            own_ref, *of_half = refs[starts[half] : starts[half + 1]]
            before, blocks = carried(
                plan, place_ref, own_ref, of_half[:n_others], of_half[n_others:], offsets
            )
            for all_states, states in zip(befores, before):
                all_states.extend(states)
            for offset, (totals, ref) in enumerate(zip(blocks, outs[len(offsets) :])):
                block = place_ref[3] * plan.n_inner + (place_ref[1] ^ offset)
                seen = jnp.full((1, HD), (block + 1) * plan.block, jnp.int32).astype(jnp.float32)
                for i, total in enumerate(totals):
                    ref[half, i] = total.T * lax.rsqrt(seen)
        for states, ref in zip(befores, outs):
            code(states, ref)

    return pl.pallas_call(
        at_place(kernel),
        out_shape=[coded_shape(plan.halves * plan.each)] * len(offsets)
        + [states_shape(plan.halves, plan.each)] * plan.n_inner,
        in_specs=[VMEM] * starts[-1] + [ANY] * len(after),
        out_specs=[VMEM] * (len(offsets) + plan.n_inner),
        compiler_params=params(),
        cost_estimate=cost(0, plan.plane * plan.each * HD * HD * 20),
        name="own_carries",
    )(*[a for arrays in operands for a in arrays], *after)


def local_part(q_ref, k_ref, v_ref, at):
    rows = q_ref.shape[0]
    causal = lax.broadcasted_iota(jnp.int32, (rows, rows), 0) >= lax.broadcasted_iota(
        jnp.int32, (rows, rows), 1
    )
    scores = contract_columns(q_ref[:, at], k_ref[:, at]) * SCORE_SCALE
    weights = jnp.where(causal, scores, 0.0).astype(jnp.bfloat16)
    return jnp.dot(weights, v_ref[:, at], preferred_element_type=jnp.float32)


def finished(queries, local, carried, gain):
    carried = carried * SCORE_SCALE
    high = carried.astype(jnp.bfloat16)
    low = (carried - high.astype(jnp.float32)).astype(jnp.bfloat16)
    both = contract_columns(queries, jnp.concatenate([high, low], axis=0))
    raw = local + (both[:, :HD] + both[:, HD:])
    mean = jnp.mean(raw * raw, axis=-1, keepdims=True)
    return (raw * lax.rsqrt(mean + 1e-06) * gain).astype(jnp.bfloat16)


def attend(plan, query, key, value, carry, first, gain, half, offsets, after):
    rows = plan.rows
    operands = [*query, *key, *value]
    n = len(operands)

    def kernel(place_ref, *refs):
        core = place_ref[0]
        first_ref, gain_ref, *carry_refs = refs[n : n + 2 + len(offsets)]
        out_ref = refs[-1]
        is_second = jnp.full((HD, HD), core, jnp.int32) == 1
        coded_gain = gain_ref.dtype == jnp.int16
        line = lax.broadcasted_iota(jnp.int32, (PAD // 2, HD), 0)
        for piece, offset in enumerate(offsets):
            x = place_ref[1] ^ (offset // plan.n_y)
            carry_states = decoded(carry_refs[piece])
            skip = half * plan.each if len(carry_states) > plan.each else 0
            for i in range(plan.each):
                at = owned_columns(plan, place_ref, offset, i)
                head = (half * plan.n_inner + x) * plan.each + i
                if coded_gain:
                    gain = jnp.where(line == head, decoded_gain(gain_ref), 0.0)
                    gain = jnp.sum(gain, axis=0, keepdims=True)
                else:
                    gain = gain_ref[:, pl.ds(pl.multiple_of(head * HD, HD), HD)]
                out_at = slice(piece * plan.piece + i * HD, piece * plan.piece + (i + 1) * HD)
                carried = carry_states[skip + i]
                first = first_ref[offset, i]
                for side in range(CORES):
                    raw = local_part(refs[side], refs[2 + side], refs[4 + side], at)
                    behind = is_second if side == 0 else ~is_second
                    state = carried + jnp.where(behind, first, 0.0)
                    of = core if side == 0 else 1 - core
                    out_rows = pl.ds(pl.multiple_of(of * rows, rows), rows)
                    out_ref[out_rows, out_at] = finished(refs[side][:, at], raw, state, gain)

    heads = len(offsets) * plan.each
    return pl.pallas_call(
        at_place(kernel),
        out_shape=jax.ShapeDtypeStruct((CORES * rows, heads * HD), jnp.bfloat16),
        in_specs=[VMEM] * (n + 2 + len(offsets)) + [ANY] * len(after),
        out_specs=VMEM,
        compiler_params=params(),
        cost_estimate=cost(
            heads * (8 * rows * rows * HD + 8 * rows * HD * HD), 16 * rows * heads * HD
        ),
        name=f"attend_{half}_" + "_".join(map(str, offsets)),
    )(*operands, first, gain, *carry, *after)


def assemble(plan, parts, into=None):
    rows = CORES * plan.rows
    copies = [(n, piece, half, o) for n, (_, half, os) in enumerate(parts) for piece, o in enumerate(os)]

    def kernel(place_ref, *refs):
        out_ref, sems = refs[-2:]
        started = []
        for at, (n, piece, half, offset) in enumerate(copies):
            x = place_ref[1] ^ (offset // plan.n_y)
            y = place_ref[2] ^ (offset % plan.n_y)
            column = (half * plan.n_inner + x) * plan.piece
            to_rows = pl.ds(pl.multiple_of(y * rows, rows), rows)
            to_columns = pl.ds(pl.multiple_of(column, plan.piece), plan.piece)
            started.append(
                pltpu.make_async_copy(
                    refs[n].at[:, pl.ds(piece * plan.piece, plan.piece)],
                    out_ref.at[to_rows, to_columns],
                    sems.at[at],
                )
            )
            started[-1].start()
        for copy in started:
            copy.wait()

    arrays = [array for array, _, _ in parts]
    aliased = [] if into is None else [into]
    return pl.pallas_call(
        at_place(kernel),
        out_shape=jax.ShapeDtypeStruct((plan.n_y * rows, plan.width), jnp.bfloat16),
        in_specs=[VMEM] * len(arrays) + [HBM] * len(aliased),
        out_specs=HBM,
        scratch_shapes=[pltpu.SemaphoreType.DMA((len(copies),))],
        input_output_aliases={len(arrays): 0} if aliased else {},
        compiler_params=params(),
        name="assemble" if into is None else "finish",
    )(*arrays, *aliased)


def assemble_cache(plan, parts):
    group = plan.n_inner * plan.each

    def kernel(place_ref, *refs):
        for half in range(plan.halves):
            for offset, ref in enumerate(refs[:-1]):
                start = half * group + (place_ref[1] ^ offset) * plan.each
                refs[-1][0, pl.ds(start, plan.each)] = ref[half]

    return pl.pallas_call(
        at_place(kernel),
        out_shape=states_shape(1, plan.halves * group),
        in_specs=[VMEM] * len(parts),
        out_specs=VMEM,
        compiler_params=params(),
        name="assemble_cache",
    )(*parts)


def per_device(plan, queries, keys, values, spikes, gain):
    halves = range(plan.halves)

    def swap(array, axes, offset, size):
        return lax.ppermute(array, axes, [(i, i ^ offset) for i in range(size)])

    def in_level(array, offset):
        return swap(array, ("inner", "y"), offset, plan.plane)

    def to_later(array, distance):
        pairs = [(i, i + distance) for i in range(plan.n_outer - distance)]
        return lax.ppermute(array, "outer", pairs)

    gain = gain.reshape(1, plan.width)
    arrays = decode(plan, spikes, keys, values)
    parts = [arrays[k : k + plan.halves] for k in range(0, len(arrays), plan.halves)]

    def with_siblings(mine, theirs):
        return [(a, swap(b, "core", 1, CORES)) for a, b in zip(mine, theirs)]

    key, value = with_siblings(*parts[0:2]), with_siblings(*parts[2:4])
    counts = [*parts[4], *parts[5]]

    own, first, others = [], [], []

    def owner_stage(half, after):
        with_gain = gain if half == 0 else None
        mine, of_first, *sends = chunk_states(
            plan, key[half], value[half], half, after, with_gain
        )
        own.append(mine)
        first.append(of_first)
        others.append([in_level(a, o) for o, a in enumerate(sends, 1)])

    of_group = [list(range(y, plan.plane, plan.n_y)) for y in range(plan.n_y)]
    abroad = [o for offsets in of_group[1:] for o in offsets]

    def part_of(half, offsets, carry, after):
        return attend(
            plan,
            query[half],
            key[half],
            value[half],
            [carry[o] for o in offsets],
            first[half],
            others[0][offsets[0] % plan.n_y - 1] if offsets[0] % plan.n_y else gain,
            half,
            offsets,
            after,
        )

    def carry_stage(half, after):
        sends = carries(plan, own[half], others[half], levels[half], half, abroad, after)
        return sends[0], {o: in_level(a, o) for o, a in zip(abroad, sends)}

    parts = []

    def send_stage(half, carry, after):
        for y in range(1, plan.n_y):
            part = part_of(half, of_group[y], carry, after)
            parts.append((swap(part, "y", y, plan.n_y), half, of_group[y]))
            after = [part]
        return after

    after = []
    for half in halves:
        owner_stage(half, after)
        if half == 0:
            spiked = spike_queries(plan, queries, counts, [own[0]])
            query = with_siblings(spiked[: plan.halves], spiked[plan.halves :])
        after = [own[-1], *[b for _, b in query]]
    levels = []
    for half in halves:
        level = level_states(plan, own[half], others[half][::-1], half, after)
        distances = [*range(1, plan.n_outer)]
        if half == 0:
            distances = [*distances[1:], *distances[:1]]
        levels.append([to_later(level, d) for d in distances])
        after = [level]
    carry = []
    for half in halves:
        done, of_half = carry_stage(half, after)
        carry.append(of_half)
        after = [done]
    for half in halves:
        after = send_stage(half, carry[half], after)
    sends = own_carries(plan, own, others, levels, of_group[0], after)
    own_carry = {o: in_level(a, o) if o else a for o, a in zip(of_group[0], sends)}
    caches = [
        swap(a, "inner", o, plan.n_inner) if o else a
        for o, a in enumerate(sends[len(of_group[0]) :])
    ]
    early = []
    for half in halves:
        part = part_of(half, of_group[0], own_carry, after)
        early.append((part, half, of_group[0]))
        after = [part]
    out = assemble(plan, early + parts[:-1])
    out = assemble(plan, parts[-1:], out)
    return out, assemble_cache(plan, caches)


def solution(mesh):
    tokens = P(("outer", "inner", "y", "core"), None)
    seq, head = ("outer", "inner"), ("y", "core")

    def whole(queries, keys, values, spikes, gain):
        plan = Plan(mesh, spikes.shape[0] // mesh.size, spikes.shape[1])
        sizes = (plan.n_outer, plan.n_inner, plan.n_y, CORES)
        split = Mesh(mesh.devices.reshape(sizes), ("outer", "inner", "y", "core"))
        return jax.shard_map(
            functools.partial(per_device, plan),
            mesh=split,
            in_specs=(tokens, tokens, tokens, tokens, P(head)),
            out_specs=(P(seq, head), P(seq, head, None, None)),
            check_vma=False,
        )(queries, keys, values, spikes, gain)

    return whole
```

```python
import functools

import jax
import jax.numpy as jnp
from jax import lax
from jax.experimental import pallas as pl
from jax.experimental.pallas import tpu as pltpu
from jax.sharding import Mesh
from jax.sharding import PartitionSpec as P

HD = 128
SCORE_SCALE = HD ** (-0.5)
CORES = 2
VMEM_BYTES = 24 * 1024 * 1024
DECODE_VMEM_BYTES = 46 * 1024 * 1024
PAD = 16
TOP = 32767.0

VMEM = pl.BlockSpec(memory_space=pltpu.VMEM)
HBM = pl.BlockSpec(memory_space=pltpu.HBM)
ANY = pl.BlockSpec(memory_space=pl.ANY)


def params(vmem=VMEM_BYTES):
    return pltpu.CompilerParams(vmem_limit_bytes=vmem)


def cost(flops, bytes_accessed):
    return pl.CostEstimate(flops=flops, bytes_accessed=bytes_accessed, transcendentals=0)


def at_place(kernel):
    def placed(*refs):
        place = [lax.axis_index(a) for a in ("core", "inner", "y", "outer")]
        kernel(place, *refs)

    return placed


class Plan:
    def __init__(self, mesh, rows, model):
        n_seq, n_head = mesh.shape["seq"], mesh.shape["head"]
        self.n_y = n_head // CORES
        self.width = model // n_head
        group = self.width // HD
        self.n_inner = 2 if n_seq % 2 == 0 and group % 2 == 0 else 1
        self.n_outer = n_seq // self.n_inner
        self.halves = 2 if group // self.n_inner % 2 == 0 else 1
        self.each = group // (self.n_inner * self.halves)
        self.plane = self.n_inner * self.n_y
        self.rows = rows
        self.block = rows * n_head
        self.piece = self.each * HD
        self.half_width = self.width // self.halves


def counts_of(spikes):
    one, two = jnp.ones_like(spikes), jnp.full_like(spikes, 2)
    zero = jnp.zeros_like(spikes)

    def ternary(rest, unit):
        return jnp.where(rest >= 2 * unit, two, jnp.where(rest >= unit, one, zero))

    value = ternary(spikes, 9)
    rest = spikes - 9 * value
    key = ternary(rest, 3)
    return value, key, rest - 3 * key


def sides(plan, core):
    width = plan.half_width
    for y in range(plan.n_y):
        for side in range(CORES):
            of = core if side == 0 else 1 - core
            for half in range(plan.halves):
                start = ((y * CORES + of) * plan.halves + half) * width
                at = pl.ds(pl.multiple_of(start, width), width)
                yield side, half, slice(y * width, (y + 1) * width), at


def decode(plan, spikes, keys, values):
    rows, model = spikes.shape
    step = min(rows, 32)
    chunks = rows // step
    n_out = 3 * CORES * plan.halves

    def kernel(*refs):
        core = lax.axis_index("core")
        sources, *outs, b0, b1, b2, sems = refs[:3], *refs[3:]
        buffers = (b0, b1, b2)

        def fetch(chunk, index):
            at = pl.ds(chunk * step, step)
            return pltpu.make_async_copy(
                sources[index].at[at], buffers[index].at[at], sems.at[chunk, index]
            )

        for chunk in range(chunks):
            for index in range(3):
                fetch(chunk, index).start()

        @pl.loop(0, chunks)
        def _(chunk):
            for index in range(3):
                fetch(chunk, index).wait()
            at = pl.ds(pl.multiple_of(chunk * step, step), step)
            for side, half, mine, columns in sides(plan, core):
                spikes = buffers[0][at, columns].astype(jnp.float32).astype(jnp.bfloat16)
                value, key, query = counts_of(spikes)
                spiked = (buffers[1][at, columns] * key, buffers[2][at, columns] * value, query)
                for index, array in enumerate(spiked):
                    outs[(index * CORES + side) * plan.halves + half][at, mine] = array

    return pl.pallas_call(
        kernel,
        out_shape=[jax.ShapeDtypeStruct((rows, plan.n_y * plan.half_width), jnp.bfloat16)] * n_out,
        in_specs=[HBM] * 3,
        out_specs=[VMEM] * n_out,
        scratch_shapes=[
            pltpu.VMEM((rows, model), jnp.int32),
            pltpu.VMEM((rows, model), jnp.bfloat16),
            pltpu.VMEM((rows, model), jnp.bfloat16),
            pltpu.SemaphoreType.DMA((chunks, 3)),
        ],
        compiler_params=params(DECODE_VMEM_BYTES),
        cost_estimate=cost(rows * model * 4, rows * model * 14),
        name="decode",
    )(spikes, keys, values)


def spike_queries(plan, queries, counts):
    n = len(counts)

    def kernel(place_ref, queries_ref, *refs):
        for side, half, mine, columns in sides(plan, place_ref[0]):
            at = side * plan.halves + half
            refs[n + at][:, mine] = queries_ref[:, columns] * refs[at][:, mine]

    return pl.pallas_call(
        at_place(kernel),
        out_shape=[jax.ShapeDtypeStruct(a.shape, jnp.bfloat16) for a in counts],
        in_specs=[VMEM] * (1 + n),
        out_specs=[VMEM] * n,
        compiler_params=params(),
        cost_estimate=cost(queries.size, queries.size * 6),
        name="spike_queries",
    )(queries, *counts)


def contract_rows(left, right):
    return lax.dot_general(
        left, right, (((0,), (0,)), ((), ())), preferred_element_type=jnp.float32
    )


def contract_columns(left, right):
    return lax.dot_general(
        left, right, (((1,), (1,)), ((), ())), preferred_element_type=jnp.float32
    )


def code(states, ref):
    line = lax.broadcasted_iota(jnp.int32, (PAD, HD), 0)
    exponents = jnp.zeros((PAD, HD), jnp.float32)
    for i, state in enumerate(states):
        top = jnp.max(jnp.abs(state), axis=0, keepdims=True)
        exponent = jnp.floor(jnp.log2(jnp.maximum(top, 1e-30))) + 1
        scaled = jnp.round(state * jnp.exp2(15 - exponent))
        scaled = jnp.clip(scaled, -TOP, TOP)
        ref[i * HD : (i + 1) * HD] = scaled.astype(jnp.int32).astype(jnp.int16)
        exponents = jnp.where(line == i, exponent, exponents)
    ref[len(states) * HD : len(states) * HD + PAD] = exponents.astype(jnp.int32).astype(jnp.int16)


def decoded(ref):
    count = ref.shape[0] // HD
    exponents = ref[count * HD : count * HD + PAD].astype(jnp.int32).astype(jnp.float32)
    return [
        ref[i * HD : (i + 1) * HD].astype(jnp.int32).astype(jnp.float32)
        * jnp.exp2(exponents[i : i + 1] - 15)
        for i in range(count)
    ]


def code_gain(gain_ref, ref):
    line = lax.broadcasted_iota(jnp.int32, (PAD // 2, HD), 0)
    gain = jnp.zeros((PAD // 2, HD), jnp.float32)
    for i in range(gain_ref.shape[1] // HD):
        gain = jnp.where(line == i, gain_ref[:, i * HD : (i + 1) * HD], gain)
    coarse = jnp.round(gain * 2.0**12)
    fine = jnp.round((gain - coarse * 2.0**-12) * 2.0**27)
    planes = jnp.concatenate([coarse, fine], axis=0)
    ref[ref.shape[0] - PAD :] = planes.astype(jnp.int32).astype(jnp.int16)


def decoded_gain(ref):
    planes = ref[ref.shape[0] - PAD :].astype(jnp.int32).astype(jnp.float32)
    return planes[: PAD // 2] * 2.0**-12 + planes[PAD // 2 :] * 2.0**-27


def plus(left, right):
    return [a + b for a, b in zip(left, right)]


def total_of(refs, each):
    total = [jnp.zeros((HD, HD), jnp.float32)] * each
    for ref in refs:
        coded = ref.dtype == jnp.int16
        total = plus(total, decoded(ref) if coded else [ref[i] for i in range(each)])
    return total


def coded_shape(heads, more=0):
    return jax.ShapeDtypeStruct((heads * HD + PAD + more, HD), jnp.int16)


def states_shape(*lead):
    return jax.ShapeDtypeStruct((*lead, HD, HD), jnp.float32)


def owned_columns(plan, place_ref, offset, i):
    x = place_ref[1] ^ (offset // plan.n_y)
    y = place_ref[2] ^ (offset % plan.n_y)
    start = ((y * plan.n_inner + x) * plan.each + i) * HD
    return pl.ds(pl.multiple_of(start, HD), HD)


def chunk_states(plan, key, value, half, after, gain=None):
    gains = [] if gain is None else [gain]

    def kernel(place_ref, k_ref, k_sib_ref, v_ref, v_sib_ref, *refs):
        own_ref, first_ref, *send_refs = refs[len(gains) + len(after) :]
        is_first = jnp.full((HD, HD), place_ref[0], jnp.int32) == 0
        for offset in (*range(1, plan.plane), 0):
            states = []
            for i in range(plan.each):
                at = owned_columns(plan, place_ref, offset, i)
                mine = contract_rows(v_ref[:, at], k_ref[:, at])
                sib = contract_rows(v_sib_ref[:, at], k_sib_ref[:, at])
                first_ref[offset, i] = jnp.where(is_first, mine, sib)
                states.append(mine + sib)
            if offset:
                code(states, send_refs[offset - 1])
                if gains and offset < plan.n_y:
                    code_gain(refs[0], send_refs[offset - 1])
            else:
                for i, state in enumerate(states):
                    own_ref[i] = state

    heads = plan.plane * plan.each
    return pl.pallas_call(
        at_place(kernel),
        out_shape=[states_shape(plan.each), states_shape(plan.plane, plan.each)]
        + [
            coded_shape(plan.each, PAD if gains and o < plan.n_y else 0)
            for o in range(1, plan.plane)
        ],
        in_specs=[VMEM] * (4 + len(gains)) + [ANY] * len(after),
        out_specs=[VMEM] * (1 + plan.plane),
        compiler_params=params(),
        cost_estimate=cost(
            4 * plan.rows * HD * HD * heads, 8 * plan.rows * HD * heads + 6 * heads * HD * HD
        ),
        name=f"chunk_states_{half}",
    )(*key, *value, *gains, *after)


def level_states(plan, own, others, half, after):
    def kernel(own_ref, *refs):
        code(total_of((own_ref, *refs[: len(others)]), plan.each), refs[-1])

    return pl.pallas_call(
        kernel,
        out_shape=coded_shape(plan.each),
        in_specs=[VMEM] * plan.plane + [ANY] * len(after),
        out_specs=VMEM,
        compiler_params=params(),
        cost_estimate=cost(0, plan.plane * plan.each * HD * HD * 2),
        name=f"level_states_{half}",
    )(own, *others, *after)


def carried(plan, place_ref, own, others, levels, offsets):
    x, y = place_ref[1], place_ref[2]
    here = x * plan.n_y + y
    earlier = total_of(levels, plan.each)
    states = [[own[i] for i in range(plan.each)]] + [decoded(ref) for ref in others]

    def add(totals, keep_of):
        for offset, terms in enumerate(states):
            keep = jnp.full((HD, HD), keep_of(here ^ offset), jnp.int32) == 1
            totals = plus(totals, [jnp.where(keep, s, 0.0) for s in terms])
        return totals

    before = [add(earlier, lambda chip: (chip < here ^ o).astype(jnp.int32)) for o in offsets]
    blocks = [
        add(earlier, lambda chip: (chip // plan.n_y <= x ^ o).astype(jnp.int32))
        for o in range(plan.n_inner)
    ]
    return before, blocks


def carries(plan, own, others, levels, half, offsets, after):
    n_others, n_levels = len(others), len(levels)

    def kernel(place_ref, own_ref, *refs):
        before, _ = carried(
            plan, place_ref, own_ref, refs[:n_others], refs[n_others : n_others + n_levels], offsets
        )
        for states, ref in zip(before, refs[n_others + n_levels + len(after) :]):
            code(states, ref)

    return pl.pallas_call(
        at_place(kernel),
        out_shape=[coded_shape(plan.each)] * len(offsets),
        in_specs=[VMEM] * (1 + n_others + n_levels) + [ANY] * len(after),
        out_specs=[VMEM] * len(offsets),
        compiler_params=params(),
        cost_estimate=cost(0, (plan.plane * 4 + n_levels) * plan.each * HD * HD * 2),
        name=f"carries_{half}",
    )(own, *others, *levels, *after)


def own_carries(plan, own, others, levels, offsets, after):
    n_others = len(others[0])
    operands = [(own[h], *others[h], *levels[h]) for h in range(plan.halves)]
    starts = [sum(map(len, operands[:h])) for h in range(plan.halves + 1)]

    def kernel(place_ref, *refs):
        outs = refs[starts[-1] + len(after) :]
        befores = [[] for _ in offsets]
        for half in range(plan.halves):
            own_ref, *of_half = refs[starts[half] : starts[half + 1]]
            before, blocks = carried(
                plan, place_ref, own_ref, of_half[:n_others], of_half[n_others:], offsets
            )
            for all_states, states in zip(befores, before):
                all_states.extend(states)
            for offset, (totals, ref) in enumerate(zip(blocks, outs[len(offsets) :])):
                block = place_ref[3] * plan.n_inner + (place_ref[1] ^ offset)
                seen = jnp.full((1, HD), (block + 1) * plan.block, jnp.int32).astype(jnp.float32)
                for i, total in enumerate(totals):
                    ref[half, i] = total.T * lax.rsqrt(seen)
        for states, ref in zip(befores, outs):
            code(states, ref)

    return pl.pallas_call(
        at_place(kernel),
        out_shape=[coded_shape(plan.halves * plan.each)] * len(offsets)
        + [states_shape(plan.halves, plan.each)] * plan.n_inner,
        in_specs=[VMEM] * starts[-1] + [ANY] * len(after),
        out_specs=[VMEM] * (len(offsets) + plan.n_inner),
        compiler_params=params(),
        cost_estimate=cost(0, plan.plane * plan.each * HD * HD * 20),
        name="own_carries",
    )(*[a for arrays in operands for a in arrays], *after)


def local_part(q_ref, k_ref, v_ref, at):
    rows = q_ref.shape[0]
    causal = lax.broadcasted_iota(jnp.int32, (rows, rows), 0) >= lax.broadcasted_iota(
        jnp.int32, (rows, rows), 1
    )
    scores = contract_columns(q_ref[:, at], k_ref[:, at]) * SCORE_SCALE
    weights = jnp.where(causal, scores, 0.0).astype(jnp.bfloat16)
    return jnp.dot(weights, v_ref[:, at], preferred_element_type=jnp.float32)


def finished(queries, local, carried, gain):
    carried = carried * SCORE_SCALE
    high = carried.astype(jnp.bfloat16)
    low = (carried - high.astype(jnp.float32)).astype(jnp.bfloat16)
    both = contract_columns(queries, jnp.concatenate([high, low], axis=0))
    raw = local + (both[:, :HD] + both[:, HD:])
    mean = jnp.mean(raw * raw, axis=-1, keepdims=True)
    return (raw * lax.rsqrt(mean + 1e-06) * gain).astype(jnp.bfloat16)


def attend(plan, query, key, value, carry, first, gain, half, offsets, after):
    rows = plan.rows
    operands = [*query, *key, *value]
    n = len(operands)

    def kernel(place_ref, *refs):
        core = place_ref[0]
        first_ref, gain_ref, *carry_refs = refs[n : n + 2 + len(offsets)]
        out_ref = refs[-1]
        is_second = jnp.full((HD, HD), core, jnp.int32) == 1
        coded_gain = gain_ref.dtype == jnp.int16
        line = lax.broadcasted_iota(jnp.int32, (PAD // 2, HD), 0)
        for piece, offset in enumerate(offsets):
            x = place_ref[1] ^ (offset // plan.n_y)
            carry_states = decoded(carry_refs[piece])
            skip = half * plan.each if len(carry_states) > plan.each else 0
            for i in range(plan.each):
                at = owned_columns(plan, place_ref, offset, i)
                head = (half * plan.n_inner + x) * plan.each + i
                if coded_gain:
                    gain = jnp.where(line == head, decoded_gain(gain_ref), 0.0)
                    gain = jnp.sum(gain, axis=0, keepdims=True)
                else:
                    gain = gain_ref[:, pl.ds(pl.multiple_of(head * HD, HD), HD)]
                out_at = slice(piece * plan.piece + i * HD, piece * plan.piece + (i + 1) * HD)
                carried = carry_states[skip + i]
                first = first_ref[offset, i]
                for side in range(CORES):
                    raw = local_part(refs[side], refs[2 + side], refs[4 + side], at)
                    behind = is_second if side == 0 else ~is_second
                    state = carried + jnp.where(behind, first, 0.0)
                    of = core if side == 0 else 1 - core
                    out_rows = pl.ds(pl.multiple_of(of * rows, rows), rows)
                    out_ref[out_rows, out_at] = finished(refs[side][:, at], raw, state, gain)

    heads = len(offsets) * plan.each
    return pl.pallas_call(
        at_place(kernel),
        out_shape=jax.ShapeDtypeStruct((CORES * rows, heads * HD), jnp.bfloat16),
        in_specs=[VMEM] * (n + 2 + len(offsets)) + [ANY] * len(after),
        out_specs=VMEM,
        compiler_params=params(),
        cost_estimate=cost(
            heads * (8 * rows * rows * HD + 8 * rows * HD * HD), 16 * rows * heads * HD
        ),
        name=f"attend_{half}_" + "_".join(map(str, offsets)),
    )(*operands, first, gain, *carry, *after)


def assemble(plan, parts, into=None):
    rows = CORES * plan.rows
    copies = [(n, piece, half, o) for n, (_, half, os) in enumerate(parts) for piece, o in enumerate(os)]

    def kernel(place_ref, *refs):
        out_ref, sems = refs[-2:]
        started = []
        for at, (n, piece, half, offset) in enumerate(copies):
            x = place_ref[1] ^ (offset // plan.n_y)
            y = place_ref[2] ^ (offset % plan.n_y)
            column = (half * plan.n_inner + x) * plan.piece
            to_rows = pl.ds(pl.multiple_of(y * rows, rows), rows)
            to_columns = pl.ds(pl.multiple_of(column, plan.piece), plan.piece)
            started.append(
                pltpu.make_async_copy(
                    refs[n].at[:, pl.ds(piece * plan.piece, plan.piece)],
                    out_ref.at[to_rows, to_columns],
                    sems.at[at],
                )
            )
            started[-1].start()
        for copy in started:
            copy.wait()

    arrays = [array for array, _, _ in parts]
    aliased = [] if into is None else [into]
    return pl.pallas_call(
        at_place(kernel),
        out_shape=jax.ShapeDtypeStruct((plan.n_y * rows, plan.width), jnp.bfloat16),
        in_specs=[VMEM] * len(arrays) + [HBM] * len(aliased),
        out_specs=HBM,
        scratch_shapes=[pltpu.SemaphoreType.DMA((len(copies),))],
        input_output_aliases={len(arrays): 0} if aliased else {},
        compiler_params=params(),
        name="assemble" if into is None else "finish",
    )(*arrays, *aliased)


def assemble_cache(plan, parts):
    group = plan.n_inner * plan.each

    def kernel(place_ref, *refs):
        for half in range(plan.halves):
            for offset, ref in enumerate(refs[:-1]):
                start = half * group + (place_ref[1] ^ offset) * plan.each
                refs[-1][0, pl.ds(start, plan.each)] = ref[half]

    return pl.pallas_call(
        at_place(kernel),
        out_shape=states_shape(1, plan.halves * group),
        in_specs=[VMEM] * len(parts),
        out_specs=VMEM,
        compiler_params=params(),
        name="assemble_cache",
    )(*parts)


def per_device(plan, queries, keys, values, spikes, gain):
    halves = range(plan.halves)

    def swap(array, axes, offset, size):
        return lax.ppermute(array, axes, [(i, i ^ offset) for i in range(size)])

    def in_level(array, offset):
        return swap(array, ("inner", "y"), offset, plan.plane)

    def to_later(array, distance):
        pairs = [(i, i + distance) for i in range(plan.n_outer - distance)]
        return lax.ppermute(array, "outer", pairs)

    gain = gain.reshape(1, plan.width)
    arrays = decode(plan, spikes, keys, values)
    parts = [arrays[k : k + plan.halves] for k in range(0, len(arrays), plan.halves)]

    def with_siblings(mine, theirs):
        return [(a, swap(b, "core", 1, CORES)) for a, b in zip(mine, theirs)]

    key, value = with_siblings(*parts[0:2]), with_siblings(*parts[2:4])
    spiked = spike_queries(plan, queries, [*parts[4], *parts[5]])
    query = with_siblings(spiked[: plan.halves], spiked[plan.halves :])

    own, first, others = [], [], []

    def owner_stage(half, after):
        with_gain = gain if half == 0 else None
        mine, of_first, *sends = chunk_states(
            plan, key[half], value[half], half, after, with_gain
        )
        own.append(mine)
        first.append(of_first)
        others.append([in_level(a, o) for o, a in enumerate(sends, 1)])

    of_group = [list(range(y, plan.plane, plan.n_y)) for y in range(plan.n_y)]
    abroad = [o for offsets in of_group[1:] for o in offsets]

    def part_of(half, offsets, carry, after):
        return attend(
            plan,
            query[half],
            key[half],
            value[half],
            [carry[o] for o in offsets],
            first[half],
            others[0][offsets[0] % plan.n_y - 1] if offsets[0] % plan.n_y else gain,
            half,
            offsets,
            after,
        )

    def carry_stage(half, after):
        sends = carries(plan, own[half], others[half], levels[half], half, abroad, after)
        return sends[0], {o: in_level(a, o) for o, a in zip(abroad, sends)}

    parts = []

    def send_stage(half, carry, after):
        for y in range(1, plan.n_y):
            part = part_of(half, of_group[y], carry, after)
            parts.append((swap(part, "y", y, plan.n_y), half, of_group[y]))
            after = [part]
        return after

    after = [query[0][0]]
    for half in halves:
        owner_stage(half, after)
        after = [own[-1], *[a for _, a in query]]
    levels = []
    for half in halves:
        level = level_states(plan, own[half], others[half][::-1], half, after)
        distances = [*range(1, plan.n_outer)]
        distances = [*distances[1:], *distances[:1]]
        levels.append([to_later(level, d) for d in distances])
        after = [level]
    carry = []
    for half in halves:
        done, of_half = carry_stage(half, after)
        carry.append(of_half)
        after = [done]
    for half in halves:
        after = send_stage(half, carry[half], after)
    sends = own_carries(plan, own, others, levels, of_group[0], after)
    own_carry = {o: in_level(a, o) if o else a for o, a in zip(of_group[0], sends)}
    caches = [
        swap(a, "inner", o, plan.n_inner) if o else a
        for o, a in enumerate(sends[len(of_group[0]) :])
    ]
    early = []
    for half in halves:
        part = part_of(half, of_group[0], own_carry, after)
        early.append((part, half, of_group[0]))
        after = [part]
    out = assemble(plan, early + parts[:-1])
    out = assemble(plan, parts[-1:], out)
    return out, assemble_cache(plan, caches)


def solution(mesh):
    tokens = P(("outer", "inner", "y", "core"), None)
    seq, head = ("outer", "inner"), ("y", "core")

    def whole(queries, keys, values, spikes, gain):
        plan = Plan(mesh, spikes.shape[0] // mesh.size, spikes.shape[1])
        sizes = (plan.n_outer, plan.n_inner, plan.n_y, CORES)
        split = Mesh(mesh.devices.reshape(sizes), ("outer", "inner", "y", "core"))
        return jax.shard_map(
            functools.partial(per_device, plan),
            mesh=split,
            in_specs=(tokens, tokens, tokens, tokens, P(head)),
            out_specs=(P(seq, head), P(seq, head, None, None)),
            check_vma=False,
        )(queries, keys, values, spikes, gain)

    return whole
```

```python
import functools

import jax
import jax.numpy as jnp
from jax import lax
from jax.experimental import pallas as pl
from jax.experimental.pallas import tpu as pltpu
from jax.sharding import Mesh
from jax.sharding import PartitionSpec as P

HD = 128
SCORE_SCALE = HD ** (-0.5)
CORES = 2
VMEM_BYTES = 24 * 1024 * 1024
DECODE_VMEM_BYTES = 46 * 1024 * 1024
PAD = 16
TOP = 32767.0

VMEM = pl.BlockSpec(memory_space=pltpu.VMEM)
HBM = pl.BlockSpec(memory_space=pltpu.HBM)
ANY = pl.BlockSpec(memory_space=pl.ANY)


def params(vmem=VMEM_BYTES):
    return pltpu.CompilerParams(vmem_limit_bytes=vmem)


def cost(flops, bytes_accessed):
    return pl.CostEstimate(flops=flops, bytes_accessed=bytes_accessed, transcendentals=0)


def at_place(kernel):
    def placed(*refs):
        place = [lax.axis_index(a) for a in ("core", "inner", "y", "outer")]
        kernel(place, *refs)

    return placed


class Plan:
    def __init__(self, mesh, rows, model):
        n_seq, n_head = mesh.shape["seq"], mesh.shape["head"]
        self.n_y = n_head // CORES
        self.width = model // n_head
        group = self.width // HD
        self.n_inner = 2 if n_seq % 2 == 0 and group % 2 == 0 else 1
        self.n_outer = n_seq // self.n_inner
        self.halves = 2 if group // self.n_inner % 2 == 0 else 1
        self.each = group // (self.n_inner * self.halves)
        self.plane = self.n_inner * self.n_y
        self.rows = rows
        self.block = rows * n_head
        self.piece = self.each * HD
        self.half_width = self.width // self.halves


def counts_of(spikes):
    one, two = jnp.ones_like(spikes), jnp.full_like(spikes, 2)
    zero = jnp.zeros_like(spikes)

    def ternary(rest, unit):
        return jnp.where(rest >= 2 * unit, two, jnp.where(rest >= unit, one, zero))

    value = ternary(spikes, 9)
    rest = spikes - 9 * value
    key = ternary(rest, 3)
    return value, key, rest - 3 * key


def sides(plan, core):
    width = plan.half_width
    for y in range(plan.n_y):
        for side in range(CORES):
            of = core if side == 0 else 1 - core
            for half in range(plan.halves):
                start = ((y * CORES + of) * plan.halves + half) * width
                at = pl.ds(pl.multiple_of(start, width), width)
                yield side, half, slice(y * width, (y + 1) * width), at


def decode(plan, spikes, keys, values):
    rows, model = spikes.shape
    step = min(rows, 16)
    chunks = rows // step
    n_out = 3 * CORES * plan.halves

    def kernel(*refs):
        core = lax.axis_index("core")
        sources, *outs, b0, b1, b2, sems = refs[:3], *refs[3:]
        buffers = (b0, b1, b2)

        def fetch(chunk, index):
            at = pl.ds(chunk * step, step)
            return pltpu.make_async_copy(
                sources[index].at[at], buffers[index].at[at], sems.at[chunk, index]
            )

        for chunk in range(chunks):
            for index in range(3):
                fetch(chunk, index).start()

        @pl.loop(0, chunks)
        def _(chunk):
            for index in range(3):
                fetch(chunk, index).wait()
            at = pl.ds(pl.multiple_of(chunk * step, step), step)
            for side, half, mine, columns in sides(plan, core):
                spikes = buffers[0][at, columns].astype(jnp.float32).astype(jnp.bfloat16)
                value, key, query = counts_of(spikes)
                spiked = (buffers[1][at, columns] * key, buffers[2][at, columns] * value, query)
                for index, array in enumerate(spiked):
                    outs[(index * CORES + side) * plan.halves + half][at, mine] = array

    return pl.pallas_call(
        kernel,
        out_shape=[jax.ShapeDtypeStruct((rows, plan.n_y * plan.half_width), jnp.bfloat16)] * n_out,
        in_specs=[HBM] * 3,
        out_specs=[VMEM] * n_out,
        scratch_shapes=[
            pltpu.VMEM((rows, model), jnp.int32),
            pltpu.VMEM((rows, model), jnp.bfloat16),
            pltpu.VMEM((rows, model), jnp.bfloat16),
            pltpu.SemaphoreType.DMA((chunks, 3)),
        ],
        compiler_params=params(DECODE_VMEM_BYTES),
        cost_estimate=cost(rows * model * 4, rows * model * 14),
        name="decode",
    )(spikes, keys, values)


def spike_queries(plan, queries, counts):
    n = len(counts)

    def kernel(place_ref, queries_ref, *refs):
        for side, half, mine, columns in sides(plan, place_ref[0]):
            at = side * plan.halves + half
            refs[n + at][:, mine] = queries_ref[:, columns] * refs[at][:, mine]

    return pl.pallas_call(
        at_place(kernel),
        out_shape=[jax.ShapeDtypeStruct(a.shape, jnp.bfloat16) for a in counts],
        in_specs=[VMEM] * (1 + n),
        out_specs=[VMEM] * n,
        compiler_params=params(),
        cost_estimate=cost(queries.size, queries.size * 6),
        name="spike_queries",
    )(queries, *counts)


def contract_rows(left, right):
    return lax.dot_general(
        left, right, (((0,), (0,)), ((), ())), preferred_element_type=jnp.float32
    )


def contract_columns(left, right):
    return lax.dot_general(
        left, right, (((1,), (1,)), ((), ())), preferred_element_type=jnp.float32
    )


def code(states, ref):
    line = lax.broadcasted_iota(jnp.int32, (PAD, HD), 0)
    exponents = jnp.zeros((PAD, HD), jnp.float32)
    for i, state in enumerate(states):
        top = jnp.max(jnp.abs(state), axis=0, keepdims=True)
        exponent = jnp.floor(jnp.log2(jnp.maximum(top, 1e-30))) + 1
        scaled = jnp.round(state * jnp.exp2(15 - exponent))
        scaled = jnp.clip(scaled, -TOP, TOP)
        ref[i * HD : (i + 1) * HD] = scaled.astype(jnp.int32).astype(jnp.int16)
        exponents = jnp.where(line == i, exponent, exponents)
    ref[len(states) * HD : len(states) * HD + PAD] = exponents.astype(jnp.int32).astype(jnp.int16)


def decoded(ref):
    count = ref.shape[0] // HD
    exponents = ref[count * HD : count * HD + PAD].astype(jnp.int32).astype(jnp.float32)
    return [
        ref[i * HD : (i + 1) * HD].astype(jnp.int32).astype(jnp.float32)
        * jnp.exp2(exponents[i : i + 1] - 15)
        for i in range(count)
    ]


def code_gain(gain_ref, ref):
    line = lax.broadcasted_iota(jnp.int32, (PAD // 2, HD), 0)
    gain = jnp.zeros((PAD // 2, HD), jnp.float32)
    for i in range(gain_ref.shape[1] // HD):
        gain = jnp.where(line == i, gain_ref[:, i * HD : (i + 1) * HD], gain)
    coarse = jnp.round(gain * 2.0**12)
    fine = jnp.round((gain - coarse * 2.0**-12) * 2.0**27)
    planes = jnp.concatenate([coarse, fine], axis=0)
    ref[ref.shape[0] - PAD :] = planes.astype(jnp.int32).astype(jnp.int16)


def decoded_gain(ref):
    planes = ref[ref.shape[0] - PAD :].astype(jnp.int32).astype(jnp.float32)
    return planes[: PAD // 2] * 2.0**-12 + planes[PAD // 2 :] * 2.0**-27


def plus(left, right):
    return [a + b for a, b in zip(left, right)]


def total_of(refs, each):
    total = [jnp.zeros((HD, HD), jnp.float32)] * each
    for ref in refs:
        coded = ref.dtype == jnp.int16
        total = plus(total, decoded(ref) if coded else [ref[i] for i in range(each)])
    return total


def coded_shape(heads, more=0):
    return jax.ShapeDtypeStruct((heads * HD + PAD + more, HD), jnp.int16)


def states_shape(*lead):
    return jax.ShapeDtypeStruct((*lead, HD, HD), jnp.float32)


def owned_columns(plan, place_ref, offset, i):
    x = place_ref[1] ^ (offset // plan.n_y)
    y = place_ref[2] ^ (offset % plan.n_y)
    start = ((y * plan.n_inner + x) * plan.each + i) * HD
    return pl.ds(pl.multiple_of(start, HD), HD)


def chunk_states(plan, key, value, half, after, gain=None):
    gains = [] if gain is None else [gain]

    def kernel(place_ref, k_ref, k_sib_ref, v_ref, v_sib_ref, *refs):
        own_ref, first_ref, *send_refs = refs[len(gains) + len(after) :]
        is_first = jnp.full((HD, HD), place_ref[0], jnp.int32) == 0
        for offset in (*range(1, plan.plane), 0):
            states = []
            for i in range(plan.each):
                at = owned_columns(plan, place_ref, offset, i)
                mine = contract_rows(v_ref[:, at], k_ref[:, at])
                sib = contract_rows(v_sib_ref[:, at], k_sib_ref[:, at])
                first_ref[offset, i] = jnp.where(is_first, mine, sib)
                states.append(mine + sib)
            if offset:
                code(states, send_refs[offset - 1])
                if gains and offset < plan.n_y:
                    code_gain(refs[0], send_refs[offset - 1])
            else:
                for i, state in enumerate(states):
                    own_ref[i] = state

    heads = plan.plane * plan.each
    return pl.pallas_call(
        at_place(kernel),
        out_shape=[states_shape(plan.each), states_shape(plan.plane, plan.each)]
        + [
            coded_shape(plan.each, PAD if gains and o < plan.n_y else 0)
            for o in range(1, plan.plane)
        ],
        in_specs=[VMEM] * (4 + len(gains)) + [ANY] * len(after),
        out_specs=[VMEM] * (1 + plan.plane),
        compiler_params=params(),
        cost_estimate=cost(
            4 * plan.rows * HD * HD * heads, 8 * plan.rows * HD * heads + 6 * heads * HD * HD
        ),
        name=f"chunk_states_{half}",
    )(*key, *value, *gains, *after)


def level_states(plan, own, others, half, after):
    def kernel(own_ref, *refs):
        code(total_of((own_ref, *refs[: len(others)]), plan.each), refs[-1])

    return pl.pallas_call(
        kernel,
        out_shape=coded_shape(plan.each),
        in_specs=[VMEM] * plan.plane + [ANY] * len(after),
        out_specs=VMEM,
        compiler_params=params(),
        cost_estimate=cost(0, plan.plane * plan.each * HD * HD * 2),
        name=f"level_states_{half}",
    )(own, *others, *after)


def carried(plan, place_ref, own, others, levels, offsets):
    x, y = place_ref[1], place_ref[2]
    here = x * plan.n_y + y
    earlier = total_of(levels, plan.each)
    states = [[own[i] for i in range(plan.each)]] + [decoded(ref) for ref in others]

    def add(totals, keep_of):
        for offset, terms in enumerate(states):
            keep = jnp.full((HD, HD), keep_of(here ^ offset), jnp.int32) == 1
            totals = plus(totals, [jnp.where(keep, s, 0.0) for s in terms])
        return totals

    before = [add(earlier, lambda chip: (chip < here ^ o).astype(jnp.int32)) for o in offsets]
    blocks = [
        add(earlier, lambda chip: (chip // plan.n_y <= x ^ o).astype(jnp.int32))
        for o in range(plan.n_inner)
    ]
    return before, blocks


def carries(plan, own, others, levels, half, offsets, after):
    n_others, n_levels = len(others), len(levels)

    def kernel(place_ref, own_ref, *refs):
        before, _ = carried(
            plan, place_ref, own_ref, refs[:n_others], refs[n_others : n_others + n_levels], offsets
        )
        for states, ref in zip(before, refs[n_others + n_levels + len(after) :]):
            code(states, ref)

    return pl.pallas_call(
        at_place(kernel),
        out_shape=[coded_shape(plan.each)] * len(offsets),
        in_specs=[VMEM] * (1 + n_others + n_levels) + [ANY] * len(after),
        out_specs=[VMEM] * len(offsets),
        compiler_params=params(),
        cost_estimate=cost(0, (plan.plane * 4 + n_levels) * plan.each * HD * HD * 2),
        name=f"carries_{half}",
    )(own, *others, *levels, *after)


def own_carries(plan, own, others, levels, offsets, after):
    n_others = len(others[0])
    operands = [(own[h], *others[h], *levels[h]) for h in range(plan.halves)]
    starts = [sum(map(len, operands[:h])) for h in range(plan.halves + 1)]

    def kernel(place_ref, *refs):
        outs = refs[starts[-1] + len(after) :]
        befores = [[] for _ in offsets]
        for half in range(plan.halves):
            own_ref, *of_half = refs[starts[half] : starts[half + 1]]
            before, blocks = carried(
                plan, place_ref, own_ref, of_half[:n_others], of_half[n_others:], offsets
            )
            for all_states, states in zip(befores, before):
                all_states.extend(states)
            for offset, (totals, ref) in enumerate(zip(blocks, outs[len(offsets) :])):
                block = place_ref[3] * plan.n_inner + (place_ref[1] ^ offset)
                seen = jnp.full((1, HD), (block + 1) * plan.block, jnp.int32).astype(jnp.float32)
                for i, total in enumerate(totals):
                    ref[half, i] = total.T * lax.rsqrt(seen)
        for states, ref in zip(befores, outs):
            code(states, ref)

    return pl.pallas_call(
        at_place(kernel),
        out_shape=[coded_shape(plan.halves * plan.each)] * len(offsets)
        + [states_shape(plan.halves, plan.each)] * plan.n_inner,
        in_specs=[VMEM] * starts[-1] + [ANY] * len(after),
        out_specs=[VMEM] * (len(offsets) + plan.n_inner),
        compiler_params=params(),
        cost_estimate=cost(0, plan.plane * plan.each * HD * HD * 20),
        name="own_carries",
    )(*[a for arrays in operands for a in arrays], *after)


def local_part(q_ref, k_ref, v_ref, at):
    rows = q_ref.shape[0]
    causal = lax.broadcasted_iota(jnp.int32, (rows, rows), 0) >= lax.broadcasted_iota(
        jnp.int32, (rows, rows), 1
    )
    scores = contract_columns(q_ref[:, at], k_ref[:, at]) * SCORE_SCALE
    weights = jnp.where(causal, scores, 0.0).astype(jnp.bfloat16)
    return jnp.dot(weights, v_ref[:, at], preferred_element_type=jnp.float32)


def finished(queries, local, carried, gain):
    carried = carried * SCORE_SCALE
    high = carried.astype(jnp.bfloat16)
    low = (carried - high.astype(jnp.float32)).astype(jnp.bfloat16)
    both = contract_columns(queries, jnp.concatenate([high, low], axis=0))
    raw = local + (both[:, :HD] + both[:, HD:])
    mean = jnp.mean(raw * raw, axis=-1, keepdims=True)
    return (raw * lax.rsqrt(mean + 1e-06) * gain).astype(jnp.bfloat16)


def attend(plan, query, key, value, carry, first, gain, half, offsets, after):
    rows = plan.rows
    operands = [*query, *key, *value]
    n = len(operands)

    def kernel(place_ref, *refs):
        core = place_ref[0]
        first_ref, gain_ref, *carry_refs = refs[n : n + 2 + len(offsets)]
        out_ref = refs[-1]
        is_second = jnp.full((HD, HD), core, jnp.int32) == 1
        coded_gain = gain_ref.dtype == jnp.int16
        line = lax.broadcasted_iota(jnp.int32, (PAD // 2, HD), 0)
        for piece, offset in enumerate(offsets):
            x = place_ref[1] ^ (offset // plan.n_y)
            carry_states = decoded(carry_refs[piece])
            skip = half * plan.each if len(carry_states) > plan.each else 0
            for i in range(plan.each):
                at = owned_columns(plan, place_ref, offset, i)
                head = (half * plan.n_inner + x) * plan.each + i
                if coded_gain:
                    gain = jnp.where(line == head, decoded_gain(gain_ref), 0.0)
                    gain = jnp.sum(gain, axis=0, keepdims=True)
                else:
                    gain = gain_ref[:, pl.ds(pl.multiple_of(head * HD, HD), HD)]
                out_at = slice(piece * plan.piece + i * HD, piece * plan.piece + (i + 1) * HD)
                carried = carry_states[skip + i]
                first = first_ref[offset, i]
                for side in range(CORES):
                    raw = local_part(refs[side], refs[2 + side], refs[4 + side], at)
                    behind = is_second if side == 0 else ~is_second
                    state = carried + jnp.where(behind, first, 0.0)
                    of = core if side == 0 else 1 - core
                    out_rows = pl.ds(pl.multiple_of(of * rows, rows), rows)
                    out_ref[out_rows, out_at] = finished(refs[side][:, at], raw, state, gain)

    heads = len(offsets) * plan.each
    return pl.pallas_call(
        at_place(kernel),
        out_shape=jax.ShapeDtypeStruct((CORES * rows, heads * HD), jnp.bfloat16),
        in_specs=[VMEM] * (n + 2 + len(offsets)) + [ANY] * len(after),
        out_specs=VMEM,
        compiler_params=params(),
        cost_estimate=cost(
            heads * (8 * rows * rows * HD + 8 * rows * HD * HD), 16 * rows * heads * HD
        ),
        name=f"attend_{half}_" + "_".join(map(str, offsets)),
    )(*operands, first, gain, *carry, *after)


def assemble(plan, parts, into=None):
    rows = CORES * plan.rows
    copies = [(n, piece, half, o) for n, (_, half, os) in enumerate(parts) for piece, o in enumerate(os)]

    def kernel(place_ref, *refs):
        out_ref, sems = refs[-2:]
        started = []
        for at, (n, piece, half, offset) in enumerate(copies):
            x = place_ref[1] ^ (offset // plan.n_y)
            y = place_ref[2] ^ (offset % plan.n_y)
            column = (half * plan.n_inner + x) * plan.piece
            to_rows = pl.ds(pl.multiple_of(y * rows, rows), rows)
            to_columns = pl.ds(pl.multiple_of(column, plan.piece), plan.piece)
            started.append(
                pltpu.make_async_copy(
                    refs[n].at[:, pl.ds(piece * plan.piece, plan.piece)],
                    out_ref.at[to_rows, to_columns],
                    sems.at[at],
                )
            )
            started[-1].start()
        for copy in started:
            copy.wait()

    arrays = [array for array, _, _ in parts]
    aliased = [] if into is None else [into]
    return pl.pallas_call(
        at_place(kernel),
        out_shape=jax.ShapeDtypeStruct((plan.n_y * rows, plan.width), jnp.bfloat16),
        in_specs=[VMEM] * len(arrays) + [HBM] * len(aliased),
        out_specs=HBM,
        scratch_shapes=[pltpu.SemaphoreType.DMA((len(copies),))],
        input_output_aliases={len(arrays): 0} if aliased else {},
        compiler_params=params(),
        name="assemble" if into is None else "finish",
    )(*arrays, *aliased)


def assemble_cache(plan, parts):
    group = plan.n_inner * plan.each

    def kernel(place_ref, *refs):
        for half in range(plan.halves):
            for offset, ref in enumerate(refs[:-1]):
                start = half * group + (place_ref[1] ^ offset) * plan.each
                refs[-1][0, pl.ds(start, plan.each)] = ref[half]

    return pl.pallas_call(
        at_place(kernel),
        out_shape=states_shape(1, plan.halves * group),
        in_specs=[VMEM] * len(parts),
        out_specs=VMEM,
        compiler_params=params(),
        name="assemble_cache",
    )(*parts)


def per_device(plan, queries, keys, values, spikes, gain):
    halves = range(plan.halves)

    def swap(array, axes, offset, size):
        return lax.ppermute(array, axes, [(i, i ^ offset) for i in range(size)])

    def in_level(array, offset):
        return swap(array, ("inner", "y"), offset, plan.plane)

    def to_later(array, distance):
        pairs = [(i, i + distance) for i in range(plan.n_outer - distance)]
        return lax.ppermute(array, "outer", pairs)

    gain = gain.reshape(1, plan.width)
    arrays = decode(plan, spikes, keys, values)
    parts = [arrays[k : k + plan.halves] for k in range(0, len(arrays), plan.halves)]

    def with_siblings(mine, theirs):
        return [(a, swap(b, "core", 1, CORES)) for a, b in zip(mine, theirs)]

    key, value = with_siblings(*parts[0:2]), with_siblings(*parts[2:4])
    spiked = spike_queries(plan, queries, [*parts[4], *parts[5]])
    query = with_siblings(spiked[: plan.halves], spiked[plan.halves :])

    own, first, others = [], [], []

    def owner_stage(half, after):
        with_gain = gain if half == 0 else None
        mine, of_first, *sends = chunk_states(
            plan, key[half], value[half], half, after, with_gain
        )
        own.append(mine)
        first.append(of_first)
        others.append([in_level(a, o) for o, a in enumerate(sends, 1)])

    of_group = [list(range(y, plan.plane, plan.n_y)) for y in range(plan.n_y)]
    abroad = [o for offsets in of_group[1:] for o in offsets]

    def part_of(half, offsets, carry, after):
        return attend(
            plan,
            query[half],
            key[half],
            value[half],
            [carry[o] for o in offsets],
            first[half],
            others[0][offsets[0] % plan.n_y - 1] if offsets[0] % plan.n_y else gain,
            half,
            offsets,
            after,
        )

    def carry_stage(half, after):
        sends = carries(plan, own[half], others[half], levels[half], half, abroad, after)
        return sends[0], {o: in_level(a, o) for o, a in zip(abroad, sends)}

    parts = []

    def send_stage(half, carry, after):
        for y in range(1, plan.n_y):
            part = part_of(half, of_group[y], carry, after)
            parts.append((swap(part, "y", y, plan.n_y), half, of_group[y]))
            after = [part]
        return after

    after = [query[0][0]]
    for half in halves:
        owner_stage(half, after)
        after = [own[-1], *[a for _, a in query]]
    levels = []
    for half in halves:
        level = level_states(plan, own[half], others[half][::-1], half, after)
        distances = [*range(1, plan.n_outer)]
        distances = [*distances[1:], *distances[:1]]
        levels.append([to_later(level, d) for d in distances])
        after = [level]
    carry = []
    for half in halves:
        done, of_half = carry_stage(half, after)
        carry.append(of_half)
        after = [done]
    for half in halves:
        after = send_stage(half, carry[half], after)
    sends = own_carries(plan, own, others, levels, of_group[0], after)
    own_carry = {o: in_level(a, o) if o else a for o, a in zip(of_group[0], sends)}
    caches = [
        swap(a, "inner", o, plan.n_inner) if o else a
        for o, a in enumerate(sends[len(of_group[0]) :])
    ]
    early = []
    for half in halves:
        part = part_of(half, of_group[0], own_carry, after)
        early.append((part, half, of_group[0]))
        after = [part]
    out = assemble(plan, early + parts[:-1])
    out = assemble(plan, parts[-1:], out)
    return out, assemble_cache(plan, caches)


def solution(mesh):
    tokens = P(("outer", "inner", "y", "core"), None)
    seq, head = ("outer", "inner"), ("y", "core")

    def whole(queries, keys, values, spikes, gain):
        plan = Plan(mesh, spikes.shape[0] // mesh.size, spikes.shape[1])
        sizes = (plan.n_outer, plan.n_inner, plan.n_y, CORES)
        split = Mesh(mesh.devices.reshape(sizes), ("outer", "inner", "y", "core"))
        return jax.shard_map(
            functools.partial(per_device, plan),
            mesh=split,
            in_specs=(tokens, tokens, tokens, tokens, P(head)),
            out_specs=(P(seq, head), P(seq, head, None, None)),
            check_vma=False,
        )(queries, keys, values, spikes, gain)

    return whole
```
